32 devices in a mesh: parts: 2 (over y), blk: 4 (over z), rows: 4 (over x, core).
Axes of the slice: x: 2, y: 2, z: 4, core: 2. Of those that a mesh axis runs over, the one named last changes fastest.
Arguments:
- tiles: float32 [16, 1024, 1024], P(('parts', 'blk'), 'rows'), parts along dimension 0, may hold values from -6 to 6
- pairs: int32 [8, 2, 2], P(('parts', 'blk')), parts along dimension 0, may hold values from 0 to 3, as said below
- counts: int32 [8], P(('parts', 'blk')), parts along dimension 0, may hold values from 1 to 2, as said below
Outputs:
- surfaces: float32 [16, 1024, 1024], P(('parts', 'blk'), 'rows'), parts along dimension 0
The draws below stay inside these ranges and needn't reach their ends.
There are 2 independent parts, one for each index of `parts`. The reference program is written for one: setup_inputs(seed, part) draws one part's arguments, and reference() takes and returns one part's arrays. A program takes and returns all parts, laid end to end along the dimension named above; each array names one. Nothing has to cross between parts.
Inputs may be any that keep to these rules, and one draw needn't show every extreme that they name: pairs[b, k] = (a, c) with a < 2; c below 2 names a tile of group b, otherwise a tile of the group half the groups away; slot 0 of every group names a tile of that other group. Slots k < counts[b] of group b are live; some group has all 2 slots live.
All inputs are finite; a program needn't handle non-finite values.
Results may differ from the reference program's by a relative error of at most 0.011.
Values may be sent and summed in bfloat16 or wider, within the bound.
No kernel may reach another device: no remote copies, remote signals or barrier semaphores. Data moves between devices by JAX's collectives and lax.ppermute only.
A program may use at most 64 MiB of HBM per device.

```python
import math
import jax
import jax.numpy as jnp
from jax import lax

H = 1024
W = 1024
TILES_DEV = 2
PAIR_CAP = 2
TILES = 8
N_BLK = 4


def draw_pairs(key, part):
    first_key = jax.random.fold_in(key, 11)
    second_key = jax.random.fold_in(key, 12)
    first = jax.random.randint(first_key, (N_BLK, PAIR_CAP), 0, TILES_DEV)
    second = jax.random.randint(second_key, (N_BLK, PAIR_CAP), 0, 2 * TILES_DEV)
    slot = jnp.arange(PAIR_CAP, dtype=jnp.int32)[None, :]
    second = jnp.where(slot == 0, TILES_DEV + second % TILES_DEV, second)
    return jnp.stack([first, second], axis=2).astype(jnp.int32)


def draw_counts(key, part):
    count_key = jax.random.fold_in(key, 21)
    pick_key = jax.random.fold_in(key, 22)
    drawn = jax.random.randint(count_key, (N_BLK,), 1, PAIR_CAP + 1)
    chosen = jax.random.randint(pick_key, (), 0, N_BLK)
    group = jnp.arange(N_BLK, dtype=jnp.int32)
    return jnp.where(group == chosen, PAIR_CAP, drawn).astype(jnp.int32)


def steps_of(key, shape, cuts, least, largest):
    level = 1.0
    for axis_at, shards_of in cuts:
        draws = jax.random.uniform(jax.random.fold_in(jax.random.fold_in(key, 6), axis_at), (shards_of,), jnp.float32, least / len(cuts), largest / len(cuts))
        level = level * jnp.repeat(jnp.exp(draws), shape[axis_at] // shards_of).reshape((-1,) + (1,) * (len(shape) - 1 - axis_at))
    return level


def bell_draw(rng, dims, scale, reach, cuts=(), kind=jnp.bfloat16):
    level = steps_of(rng, dims, cuts, -0.22, 0.18) if cuts else 1.0
    values = jax.random.normal(rng, dims, jnp.float32) * scale * level
    return jnp.minimum(jnp.maximum(values, -reach), reach).astype(kind)


def setup_inputs(seed: int = 0, part: int = 0) -> dict:
    splits = jax.random.split(jax.random.key(seed), 4)
    part_keys = jax.random.split(jax.random.fold_in(splits[3], part), 4)
    tiles = bell_draw(part_keys[0], (TILES, H, W), 1.0, 6.0, ((0, 4), (1, 4)), jnp.float32)
    pairs = draw_pairs(jax.random.fold_in(jax.random.fold_in(splits[3], part), 71), part)
    counts = draw_counts(jax.random.fold_in(jax.random.fold_in(splits[3], part), 71), part)
    return {"tiles": tiles, "pairs": pairs, "counts": counts}


FLOOR = 0.05

def dft_tables(length):
    index = jnp.arange(length, dtype=jnp.int32)
    phase = index[:, None] * index[None, :] % length
    angle = 2.0 * math.pi / length * phase.astype(jnp.float32)
    factor = 1.0 / math.sqrt(length)
    return ((jnp.cos(angle) * factor).astype(jnp.bfloat16), (jnp.sin(angle) * factor).astype(jnp.bfloat16))

def hann(length, first, number):
    index = (first + jnp.arange(number, dtype=jnp.int32)).astype(jnp.float32)
    return 0.5 - 0.5 * jnp.cos(2.0 * math.pi / length * index)

def reference(tiles, pairs, counts):
    cos_h, sin_h = dft_tables(H)
    cos_w, sin_w = dft_tables(W)
    window = hann(H, 0, H)[:, None] * hann(W, 0, W)[None, :]

    def forward(tile):
        shaded = (tile * window).astype(jnp.bfloat16)
        y_real = jnp.dot(shaded, cos_w, preferred_element_type=jnp.float32).astype(jnp.bfloat16)
        y_imag = (-jnp.dot(shaded, sin_w, preferred_element_type=jnp.float32)).astype(jnp.bfloat16)
        f_real = jnp.dot(cos_h, y_real, preferred_element_type=jnp.float32) + jnp.dot(sin_h, y_imag, preferred_element_type=jnp.float32)
        f_imag = jnp.dot(cos_h, y_imag, preferred_element_type=jnp.float32) - jnp.dot(sin_h, y_real, preferred_element_type=jnp.float32)
        return jnp.stack([f_real, f_imag]).astype(jnp.bfloat16)
    spectra = lax.map(forward, tiles)

    def one_pair(slot):
        group = slot // PAIR_CAP
        within = slot % PAIR_CAP
        first = pairs[group, within, 0]
        second = pairs[group, within, 1]
        other = (group + N_BLK - N_BLK // 2) % N_BLK
        source = jnp.where(second < TILES_DEV, group, other)
        left = spectra[group * TILES_DEV + first].astype(jnp.float32)
        right = spectra[source * TILES_DEV + second % TILES_DEV].astype(jnp.float32)
        cross_real = left[0] * right[0] + left[1] * right[1]
        cross_imag = left[1] * right[0] - left[0] * right[1]
        factor = 1.0 / (jnp.sqrt(cross_real * cross_real + cross_imag * cross_imag) + FLOOR)
        q_real = (cross_real * factor).astype(jnp.bfloat16)
        q_imag = (cross_imag * factor).astype(jnp.bfloat16)
        z_real = (jnp.dot(cos_h, q_real, preferred_element_type=jnp.float32) - jnp.dot(sin_h, q_imag, preferred_element_type=jnp.float32)).astype(jnp.bfloat16)
        z_imag = (jnp.dot(sin_h, q_real, preferred_element_type=jnp.float32) + jnp.dot(cos_h, q_imag, preferred_element_type=jnp.float32)).astype(jnp.bfloat16)
        surface = jnp.dot(z_real, cos_w, preferred_element_type=jnp.float32) - jnp.dot(z_imag, sin_w, preferred_element_type=jnp.float32)
        live = (within < counts[group]).astype(jnp.float32)
        return surface * live
    return lax.map(one_pair, jnp.arange(N_BLK * PAIR_CAP, dtype=jnp.int32))
```

```python
import math

import jax
import jax.numpy as jnp
import numpy as np
from jax import lax
from jax.experimental import pallas as pl
from jax.experimental.pallas import tpu as pltpu

FLOOR = 0.05
VMEM_LIMIT = 56 * 1024 * 1024


def hann(length, first, number):
    index = (first + jnp.arange(number, dtype=jnp.int32)).astype(jnp.float32)
    return 0.5 - 0.5 * jnp.cos(2.0 * math.pi / length * index)


def width_table(width, owners):
    half = width // 2
    phase = np.arange(half)[:, None] * np.arange(width)[None, :] % width
    angle = 2.0 * math.pi / width * phase
    factor = 1.0 / math.sqrt(width)
    cosine = np.cos(angle) * factor
    sine = -np.sin(angle) * factor
    sine[0] = np.where(np.arange(width) % 2 == 0, factor, -factor)
    shape = (owners, half // owners, width)
    table = np.stack([cosine.reshape(shape), sine.reshape(shape)], axis=1)
    return table.reshape(width, width).astype(jnp.bfloat16)


def height_table(height):
    fine = 32
    coarse = height // fine
    column = np.arange(height)[None, :]
    rough = 2.0 * math.pi / height * (np.arange(coarse)[:, None] * fine * column % height)
    small = 2.0 * math.pi / height * (np.arange(fine)[:, None] * column % height)
    factor = 1.0 / math.sqrt(height)
    rc = jnp.asarray(np.cos(rough) * factor, jnp.float32)[:, None, :]
    rs = jnp.asarray(np.sin(rough) * factor, jnp.float32)[:, None, :]
    sc = jnp.asarray(np.cos(small), jnp.float32)[None, :, :]
    ss = jnp.asarray(np.sin(small), jnp.float32)[None, :, :]
    cosine = (rc * sc - rs * ss).reshape(height, height)
    sine = (rs * sc + rc * ss).reshape(height, height)
    return jnp.concatenate([cosine, sine], axis=1).astype(jnp.bfloat16)


def params():
    return pltpu.CompilerParams(vmem_limit_bytes=VMEM_LIMIT)


def row_transform(tiles, down, across, table, scalars, peers):
    count, rows, width = tiles.shape
    span = table.shape[0] // 2
    block = span // peers

    def body(s_ref, tile_ref, down_ref, across_ref, table_ref, *refs):
        outs, work = refs[:-1], refs[-1]
        window = down_ref[...] * across_ref[...]
        shaded = (tile_ref[0] * window).astype(jnp.bfloat16)
        y = lax.dot_general(
            table_ref[...], shaded, (((1,), (1,)), ((), ())), preferred_element_type=jnp.float32
        )
        work[...] = y.astype(jnp.bfloat16)
        me = s_ref[1]
        for k in range(peers):
            start = pl.multiple_of((me ^ k) * block, block)
            outs[k][0] = work[pl.ds(start, block), :]

    return pl.pallas_call(
        body,
        grid_spec=pltpu.PrefetchScalarGridSpec(
            num_scalar_prefetch=1,
            grid=(count,),
            in_specs=[
                pl.BlockSpec((1, rows, width), lambda t, s: (t, 0, 0)),
                pl.BlockSpec((rows, 1), lambda t, s: (0, 0)),
                pl.BlockSpec((1, width), lambda t, s: (0, 0)),
                pl.BlockSpec((span, width), lambda t, s: (s[0], 0)),
            ],
            out_specs=[pl.BlockSpec((1, block, rows), lambda t, s: (t, 0, 0))] * peers,
            scratch_shapes=[pltpu.VMEM((span, rows), jnp.bfloat16)],
        ),
        out_shape=[jax.ShapeDtypeStruct((count, block, rows), jnp.bfloat16)] * peers,
        compiler_params=params(),
        name="row_transform",
    )(scalars, tiles, down, across, table)


def gather_rows(s_ref, pieces, table_ref):
    me = s_ref[1]
    total = None
    for k, piece in enumerate(pieces):
        count, block, rows = piece.shape
        start = pl.multiple_of((me ^ k) * rows, rows)
        term = jnp.dot(
            piece[...].reshape(count * block, rows),
            table_ref[pl.ds(start, rows), :],
            preferred_element_type=jnp.float32,
        )
        total = term if total is None else total + term
    return total


def store_spectra(s_ref, total, spectra, edge, first):
    block = spectra.shape[2]
    height = spectra.shape[3]
    row = lax.broadcasted_iota(jnp.int32, (block, height), 0)
    packed = (row == 0) & (s_ref[2] == 1)
    for t in range(total.shape[0] // (2 * block)):
        real = total[2 * t * block : (2 * t + 1) * block]
        imag = total[(2 * t + 1) * block : (2 * t + 2) * block]
        cr, sr = real[:, :height], real[:, height:]
        ci, si = imag[:, :height], imag[:, height:]
        spectra[first + t, 0] = jnp.where(packed, cr, cr + si).astype(jnp.bfloat16)
        spectra[first + t, 1] = jnp.where(packed, -sr, ci - sr).astype(jnp.bfloat16)
        edge[first + t, 0] = ci[:16].astype(jnp.bfloat16)
        edge[first + t, 1] = (-si[:16]).astype(jnp.bfloat16)


def normalised(left_real, left_imag, right_real, right_imag):
    lr = left_real.astype(jnp.float32)
    li = left_imag.astype(jnp.float32)
    rr = right_real.astype(jnp.float32)
    ri = right_imag.astype(jnp.float32)
    cross_real = lr * rr + li * ri
    cross_imag = li * rr - lr * ri
    factor = 1.0 / (jnp.sqrt(cross_real * cross_real + cross_imag * cross_imag) + FLOOR)
    return (
        (cross_real * factor).astype(jnp.bfloat16),
        (cross_imag * factor).astype(jnp.bfloat16),
    )


def correlate(s_ref, base, spectra, edge, table_ref, phases, outs):
    block = spectra.shape[2]
    height = spectra.shape[3]
    slots = outs[0].shape[0]
    rows = outs[0].shape[2]
    lead = lax.broadcasted_iota(jnp.int32, (16, height), 0)
    packed = (lead == 0) & (s_ref[2] == 1)
    for p in range(slots):
        a = s_ref[base + 2 * p]
        c = s_ref[base + 2 * p + 1]
        q_real, q_imag = normalised(spectra[a, 0], spectra[a, 1], spectra[c, 0], spectra[c, 1])
        e_real, e_imag = normalised(edge[a, 0], edge[a, 1], edge[c, 0], edge[c, 1])
        phases[2 * p] = q_real
        phases[2 * p + 1] = q_imag
        top_real = q_real[:16].astype(jnp.float32)
        top_imag = q_imag[:16].astype(jnp.float32)
        mixed_real = jnp.where(packed, top_real - e_imag.astype(jnp.float32), top_real)
        mixed_imag = jnp.where(packed, top_imag + e_real.astype(jnp.float32), top_imag)
        phases[2 * p, :16] = mixed_real.astype(jnp.bfloat16)
        phases[2 * p + 1, :16] = mixed_imag.astype(jnp.bfloat16)
    row = lax.broadcasted_iota(jnp.int32, (block, rows), 0)
    twice = jnp.where((row == 0) & (s_ref[2] == 1), 1.0, 2.0)
    flat = phases[...].reshape(2 * slots * block, height)
    me = s_ref[1]
    for k in range(len(outs)):
        start = pl.multiple_of((me ^ k) * rows, rows)
        c_part = jnp.dot(
            flat, table_ref[:, pl.ds(start, rows)], preferred_element_type=jnp.float32
        )
        start = pl.multiple_of(height + (me ^ k) * rows, rows)
        s_part = jnp.dot(
            flat, table_ref[:, pl.ds(start, rows)], preferred_element_type=jnp.float32
        )
        for p in range(slots):
            re = slice(2 * p * block, (2 * p + 1) * block)
            im = slice((2 * p + 1) * block, (2 * p + 2) * block)
            outs[k][p, :block] = ((c_part[re] - s_part[im]) * twice).astype(jnp.bfloat16)
            outs[k][p, block:] = ((s_part[re] + c_part[im]) * twice).astype(jnp.bfloat16)


def own_spectra(scalars, pieces, table):
    peers = len(pieces)
    count, double, rows = pieces[0].shape
    height = table.shape[0]

    def body(s_ref, *refs):
        inputs, table_ref = refs[:peers], refs[peers]
        spectra, edge = refs[peers + 1 :]
        store_spectra(s_ref, gather_rows(s_ref, inputs, table_ref), spectra, edge, 0)

    return pl.pallas_call(
        body,
        in_specs=[pl.BlockSpec(memory_space=pltpu.SMEM)]
        + [pl.BlockSpec(memory_space=pltpu.VMEM)] * (peers + 1),
        out_specs=[pl.BlockSpec(memory_space=pltpu.VMEM)] * 2,
        out_shape=[
            jax.ShapeDtypeStruct((count, 2, double // 2, height), jnp.bfloat16),
            jax.ShapeDtypeStruct((count, 2, 16, height), jnp.bfloat16),
        ],
        compiler_params=params(),
        name="own_spectra",
    )(scalars, *pieces, table)


def partner_slots(scalars, pieces, table, spectra, edge, slots):
    peers = len(pieces)
    count, double, rows = pieces[0].shape
    height = table.shape[0]
    block = double // 2

    def body(s_ref, *refs):
        inputs, table_ref, own_ref, own_edge = refs[:peers], *refs[peers : peers + 3]
        outs = refs[peers + 3 : 2 * peers + 3]
        every, edges, phases = refs[2 * peers + 3 :]
        every[:count] = own_ref[...]
        edges[:count] = own_edge[...]
        store_spectra(s_ref, gather_rows(s_ref, inputs, table_ref), every, edges, count)
        correlate(s_ref, 3 + 2 * slots, every, edges, table_ref, phases, outs)

    return pl.pallas_call(
        body,
        in_specs=[pl.BlockSpec(memory_space=pltpu.SMEM)]
        + [pl.BlockSpec(memory_space=pltpu.VMEM)] * (peers + 3),
        out_specs=[pl.BlockSpec(memory_space=pltpu.VMEM)] * (peers + 2),
        out_shape=[jax.ShapeDtypeStruct((slots, double, rows), jnp.bfloat16)] * peers
        + [
            jax.ShapeDtypeStruct((2 * count, 2, block, height), jnp.bfloat16),
            jax.ShapeDtypeStruct((2 * count, 2, 16, height), jnp.bfloat16),
        ],
        scratch_shapes=[pltpu.VMEM((2 * slots, block, height), jnp.bfloat16)],
        compiler_params=params(),
        name="partner_slots",
    )(scalars, *pieces, table, spectra, edge)


def own_slots(scalars, table, spectra, edge, peers, slots):
    block, height = spectra.shape[2:]
    rows = height // peers

    def body(s_ref, table_ref, every, edges, *refs):
        correlate(s_ref, 3, every, edges, table_ref, refs[-1], refs[:-1])

    return pl.pallas_call(
        body,
        in_specs=[pl.BlockSpec(memory_space=pltpu.SMEM)]
        + [pl.BlockSpec(memory_space=pltpu.VMEM)] * 3,
        out_specs=[pl.BlockSpec(memory_space=pltpu.VMEM)] * peers,
        out_shape=[jax.ShapeDtypeStruct((slots, 2 * block, rows), jnp.bfloat16)] * peers,
        scratch_shapes=[pltpu.VMEM((2 * slots, block, height), jnp.bfloat16)],
        compiler_params=params(),
        name="own_slots",
    )(scalars, table, spectra, edge)


def surfaces_of(scalars, own, other, table):
    peers = len(own)
    slots, double, rows = own[0].shape
    width = table.shape[0]
    span = peers * double

    def body(s_ref, *refs):
        own_refs, other_refs = refs[:peers], refs[peers : 2 * peers]
        table_ref, out_ref, work = refs[2 * peers :]
        half = s_ref[0]
        me = s_ref[1]
        for k in range(peers):
            place = (me ^ k) * double
            here = pl.multiple_of(half * span + place, double)
            there = pl.multiple_of((1 - half) * span + place, double)
            work[pl.ds(here, double), :] = own_refs[k][0]
            work[pl.ds(there, double), :] = other_refs[k][0]
        surface = lax.dot_general(
            work[...], table_ref[...], (((0,), (0,)), ((), ())), preferred_element_type=jnp.float32
        )
        live = pl.program_id(0) < s_ref[2]
        out_ref[0] = jnp.where(live, surface, 0.0)

    piece = pl.BlockSpec((1, double, rows), lambda p, s: (p, 0, 0))
    return pl.pallas_call(
        body,
        grid_spec=pltpu.PrefetchScalarGridSpec(
            num_scalar_prefetch=1,
            grid=(slots,),
            in_specs=[piece] * (2 * peers) + [pl.BlockSpec((width, width), lambda p, s: (0, 0))],
            out_specs=pl.BlockSpec((1, rows, width), lambda p, s: (p, 0, 0)),
            scratch_shapes=[pltpu.VMEM((width, rows), jnp.bfloat16)],
        ),
        out_shape=jax.ShapeDtypeStruct((slots, rows, width), jnp.float32),
        compiler_params=params(),
        name="surfaces",
    )(scalars, *own, *other, table)


def local(tiles, pairs, counts):
    groups = lax.axis_size("blk")
    peers = lax.axis_size("rows")
    group = lax.axis_index("blk")
    me = lax.axis_index("rows")
    count, rows, width = tiles.shape
    slots = pairs.shape[1]
    height = rows * peers
    turn = groups // 2
    half = group // turn
    axes = ("blk", "rows")

    def across(value, k):
        moves = [
            (b * peers + r, (b + turn) % groups * peers + (r ^ k))
            for b in range(groups)
            for r in range(peers)
        ]
        return lax.ppermute(value, axes, moves)

    def along(value, k):
        return lax.ppermute(value, "rows", [(r, r ^ k) for r in range(peers)])

    table_w = jnp.asarray(width_table(width, 2 * peers))
    down = hann(height, me * rows, rows)[:, None]
    sideways = hann(width, 0, width)[None, :]

    first = jnp.stack([1 - half, me])
    sent = row_transform(tiles, down, sideways, table_w, first, peers)
    arrived = [across(sent[k], k) for k in range(peers)]
    kept = row_transform(tiles, down, sideways, table_w, jnp.stack([half, me]), peers)
    mine = [kept[0]] + [along(kept[k], k) for k in range(1, peers)]

    table_h = height_table(height)
    theirs = across(pairs, 0)
    packed = ((half == 0) & (me == 0)).astype(jnp.int32)
    their_pairs = jnp.stack([theirs[0, :, 0] + count, (theirs[0, :, 1] + count) % (2 * count)], 1)
    scalars = jnp.concatenate(
        [jnp.stack([half, me, packed]), pairs.reshape(-1), their_pairs.reshape(-1)]
    )
    spectra, edge = own_spectra(scalars, mine, table_h)
    *back, spectra, edge = partner_slots(scalars, arrived, table_h, spectra, edge, slots)
    other = [across(back[k], k) for k in range(peers)]
    out = own_slots(scalars, table_h, spectra, edge, peers, slots)
    own = [out[0]] + [along(out[k], k) for k in range(1, peers)]
    return surfaces_of(jnp.stack([half, me, counts[0]]), own, other, table_w)


def solution(mesh):
    from jax.sharding import PartitionSpec as P

    return jax.shard_map(
        local,
        mesh=mesh,
        in_specs=(
            P(("parts", "blk"), "rows", None),
            P(("parts", "blk"), None, None),
            P(("parts", "blk")),
        ),
        out_specs=P(("parts", "blk"), "rows", None),
        check_vma=False,
    )
```

```python
import math

import jax
import jax.numpy as jnp
import numpy as np
from jax import lax
from jax.experimental import pallas as pl
from jax.experimental.pallas import tpu as pltpu

FLOOR = 0.05
VMEM_LIMIT = 56 * 1024 * 1024


def hann(length):
    return np.asarray(0.5 - 0.5 * np.cos(2.0 * math.pi / length * np.arange(length)), np.float32)


def scalar(value):
    return jnp.reshape(value, (1,)).astype(jnp.int32)


def width_table(width, owners):
    half = width // 2
    phase = np.arange(half)[:, None] * np.arange(width)[None, :] % width
    angle = 2.0 * math.pi / width * phase
    factor = 1.0 / math.sqrt(width)
    cosine = np.cos(angle) * factor
    sine = -np.sin(angle) * factor
    sine[0] = np.where(np.arange(width) % 2 == 0, factor, -factor)
    shape = (owners, half // owners, width)
    table = np.stack([cosine.reshape(shape), sine.reshape(shape)], axis=1)
    return table.reshape(width, width).astype(jnp.bfloat16)


def height_table(height):
    fine = 32
    coarse = height // fine
    column = np.arange(height)[None, :]
    rough = 2.0 * math.pi / height * (np.arange(coarse)[:, None] * fine * column % height)
    small = 2.0 * math.pi / height * (np.arange(fine)[:, None] * column % height)
    factor = 1.0 / math.sqrt(height)
    rc = jnp.asarray(np.cos(rough) * factor, jnp.float32)[:, None, :]
    rs = jnp.asarray(np.sin(rough) * factor, jnp.float32)[:, None, :]
    sc = jnp.asarray(np.cos(small), jnp.float32)[None, :, :]
    ss = jnp.asarray(np.sin(small), jnp.float32)[None, :, :]
    cosine = (rc * sc - rs * ss).reshape(height, height)
    sine = (rs * sc + rc * ss).reshape(height, height)
    return jnp.concatenate([cosine, sine], axis=1).astype(jnp.bfloat16)


def cost(flops, moved):
    return pl.CostEstimate(flops=flops, transcendentals=0, bytes_accessed=moved)


def params():
    return pltpu.CompilerParams(vmem_limit_bytes=VMEM_LIMIT)


def row_transform(tiles, down, across, table, half, me, peers, apart):
    count, rows, width = tiles.shape
    span = table.shape[0] // 2
    block = span // peers

    def body(half_ref, me_ref, tile_ref, down_ref, across_ref, table_ref, *refs):
        outs, work = refs[:-1], refs[-1]
        window = down_ref[...].T[:, :1] * across_ref[...]
        shaded = (tile_ref[0] * window).astype(jnp.bfloat16)
        y = lax.dot_general(
            table_ref[...], shaded, (((1,), (1,)), ((), ())), preferred_element_type=jnp.float32
        )
        if not apart:
            outs[0][:, 0] = y.astype(jnp.bfloat16).reshape(peers, block, rows)
            return
        work[...] = y.astype(jnp.bfloat16)
        me = me_ref[0]
        for k in range(peers):
            start = pl.multiple_of((me ^ k) * block, block)
            outs[k][0] = work[pl.ds(start, block), :]

    if apart:
        out_specs = [pl.BlockSpec((1, block, rows), lambda t, half, me: (t, 0, 0))] * peers
        out_shape = [jax.ShapeDtypeStruct((count, block, rows), jnp.bfloat16)] * peers
    else:
        out_specs = [pl.BlockSpec((peers, 1, block, rows), lambda t, half, me: (0, t, 0, 0))]
        out_shape = [jax.ShapeDtypeStruct((peers, count, block, rows), jnp.bfloat16)]
    return pl.pallas_call(
        body,
        grid_spec=pltpu.PrefetchScalarGridSpec(
            num_scalar_prefetch=2,
            grid=(count,),
            in_specs=[
                pl.BlockSpec((1, rows, width), lambda t, half, me: (t, 0, 0)),
                pl.BlockSpec((8, rows), lambda t, half, me: (0, me[0])),
                pl.BlockSpec((1, width), lambda t, half, me: (0, 0)),
                pl.BlockSpec((span, width), lambda t, half, me: (half[0], 0)),
            ],
            out_specs=out_specs,
            scratch_shapes=[pltpu.VMEM((span, rows), jnp.bfloat16)],
        ),
        out_shape=out_shape,
        compiler_params=params(),
        cost_estimate=cost(2 * count * rows * width * span, 4 * tiles.size + 2 * span * width),
        name="row_transform",
    )(scalar(half), scalar(me), tiles, down, across, table)


def gather_rows(pieces, table_ref, me):
    total = None
    for k, piece in enumerate(pieces):
        count, block, rows = piece.shape
        start = pl.multiple_of((me ^ k) * rows, rows)
        term = jnp.dot(
            piece[...].reshape(count * block, rows),
            table_ref[pl.ds(start, rows), :],
            preferred_element_type=jnp.float32,
        )
        total = term if total is None else total + term
    return total


def store_spectra(s_ref, total, spectra, edge, first):
    block = spectra.shape[2]
    height = spectra.shape[3]
    row = lax.broadcasted_iota(jnp.int32, (block, height), 0)
    packed = (row == 0) & (s_ref[2] == 1)
    for t in range(total.shape[0] // (2 * block)):
        real = total[2 * t * block : (2 * t + 1) * block]
        imag = total[(2 * t + 1) * block : (2 * t + 2) * block]
        cr, sr = real[:, :height], real[:, height:]
        ci, si = imag[:, :height], imag[:, height:]
        spectra[first + t, 0] = jnp.where(packed, cr, cr + si).astype(jnp.bfloat16)
        spectra[first + t, 1] = jnp.where(packed, -sr, ci - sr).astype(jnp.bfloat16)
        edge[first + t, 0] = ci[:16].astype(jnp.bfloat16)
        edge[first + t, 1] = (-si[:16]).astype(jnp.bfloat16)


def normalised(left_real, left_imag, right_real, right_imag):
    lr = left_real.astype(jnp.float32)
    li = left_imag.astype(jnp.float32)
    rr = right_real.astype(jnp.float32)
    ri = right_imag.astype(jnp.float32)
    cross_real = lr * rr + li * ri
    cross_imag = li * rr - lr * ri
    factor = 1.0 / (jnp.sqrt(cross_real * cross_real + cross_imag * cross_imag) + FLOOR)
    return (
        (cross_real * factor).astype(jnp.bfloat16),
        (cross_imag * factor).astype(jnp.bfloat16),
    )


def correlate(s_ref, me, base, spectra, edge, table_ref, phases, outs):
    block = spectra.shape[2]
    height = spectra.shape[3]
    slots, _, rows = outs[0].shape
    lead = lax.broadcasted_iota(jnp.int32, (16, height), 0)
    packed = (lead == 0) & (s_ref[2] == 1)
    for p in range(slots):
        a = s_ref[base + 2 * p]
        c = s_ref[base + 2 * p + 1]
        q_real, q_imag = normalised(spectra[a, 0], spectra[a, 1], spectra[c, 0], spectra[c, 1])
        e_real, e_imag = normalised(edge[a, 0], edge[a, 1], edge[c, 0], edge[c, 1])
        phases[2 * p] = q_real
        phases[2 * p + 1] = q_imag
        top_real = q_real[:16].astype(jnp.float32)
        top_imag = q_imag[:16].astype(jnp.float32)
        mixed_real = jnp.where(packed, top_real - e_imag.astype(jnp.float32), top_real)
        mixed_imag = jnp.where(packed, top_imag + e_real.astype(jnp.float32), top_imag)
        phases[2 * p, :16] = mixed_real.astype(jnp.bfloat16)
        phases[2 * p + 1, :16] = mixed_imag.astype(jnp.bfloat16)
    row = lax.broadcasted_iota(jnp.int32, (block, rows), 0)
    twice = jnp.where((row == 0) & (s_ref[2] == 1), 1.0, 2.0)
    flat = phases[...].reshape(2 * slots * block, height)
    for k in range(len(outs)):
        start = pl.multiple_of((me ^ k) * rows, rows)
        c_part = jnp.dot(
            flat, table_ref[:, pl.ds(start, rows)], preferred_element_type=jnp.float32
        )
        start = pl.multiple_of(height + (me ^ k) * rows, rows)
        s_part = jnp.dot(
            flat, table_ref[:, pl.ds(start, rows)], preferred_element_type=jnp.float32
        )
        for p in range(slots):
            re = slice(2 * p * block, (2 * p + 1) * block)
            im = slice((2 * p + 1) * block, (2 * p + 2) * block)
            outs[k][p, :block] = ((c_part[re] - s_part[im]) * twice).astype(jnp.bfloat16)
            outs[k][p, block:] = ((s_part[re] + c_part[im]) * twice).astype(jnp.bfloat16)


def own_spectra(scalars, pieces, table):
    peers, count, double, rows = pieces.shape
    height = table.shape[0]

    def body(s_ref, pieces_ref, table_ref, spectra, edge):
        inputs = [pieces_ref.at[k] for k in range(peers)]
        store_spectra(s_ref, gather_rows(inputs, table_ref, 0), spectra, edge, 0)

    return pl.pallas_call(
        body,
        in_specs=[pl.BlockSpec(memory_space=pltpu.SMEM)]
        + [pl.BlockSpec(memory_space=pltpu.VMEM)] * 2,
        out_specs=[pl.BlockSpec(memory_space=pltpu.VMEM)] * 2,
        out_shape=[
            jax.ShapeDtypeStruct((count, 2, double // 2, height), jnp.bfloat16),
            jax.ShapeDtypeStruct((count, 2, 16, height), jnp.bfloat16),
        ],
        compiler_params=params(),
        cost_estimate=cost(4 * count * double * height * height, 8 * height * height),
        name="own_spectra",
    )(scalars, pieces, table)


def partner_slots(scalars, pieces, table, spectra, edge, slots):
    peers = len(pieces)
    count, double, rows = pieces[0].shape
    height = table.shape[0]
    block = double // 2

    def body(s_ref, *refs):
        inputs, table_ref, own_ref, own_edge = refs[:peers], *refs[peers : peers + 3]
        outs = [refs[peers + 3 + k // 2].at[k % 2] for k in range(peers)]
        every, edges, phases = refs[-3:]
        every[:count] = own_ref[...]
        edges[:count] = own_edge[...]
        store_spectra(s_ref, gather_rows(inputs, table_ref, s_ref[1]), every, edges, count)
        correlate(s_ref, s_ref[1], 3 + 2 * slots, every, edges, table_ref, phases, outs)

    return pl.pallas_call(
        body,
        in_specs=[pl.BlockSpec(memory_space=pltpu.SMEM)]
        + [pl.BlockSpec(memory_space=pltpu.VMEM)] * (peers + 3),
        out_specs=[pl.BlockSpec(memory_space=pltpu.VMEM)] * (peers // 2 + 2),
        out_shape=[jax.ShapeDtypeStruct((2, slots, double, rows), jnp.bfloat16)] * (peers // 2)
        + [
            jax.ShapeDtypeStruct((2 * count, 2, block, height), jnp.bfloat16),
            jax.ShapeDtypeStruct((2 * count, 2, 16, height), jnp.bfloat16),
        ],
        scratch_shapes=[pltpu.VMEM((2 * slots, block, height), jnp.bfloat16)],
        compiler_params=params(),
        cost_estimate=cost(4 * (count + slots) * double * height * height, 8 * height * height),
        name="partner_slots",
    )(scalars, *pieces, table, spectra, edge)


def own_slots(scalars, table, spectra, edge, peers, slots):
    block, height = spectra.shape[2:]
    rows = height // peers

    def body(s_ref, table_ref, every, edges, *refs):
        out_ref, phases = refs
        outs = [out_ref.at[k] for k in range(peers)]
        correlate(s_ref, 0, 3, every, edges, table_ref, phases, outs)

    return pl.pallas_call(
        body,
        in_specs=[pl.BlockSpec(memory_space=pltpu.SMEM)]
        + [pl.BlockSpec(memory_space=pltpu.VMEM)] * 3,
        out_specs=pl.BlockSpec(memory_space=pltpu.VMEM),
        out_shape=jax.ShapeDtypeStruct((peers, slots, 2 * block, rows), jnp.bfloat16),
        scratch_shapes=[pltpu.VMEM((2 * slots, block, height), jnp.bfloat16)],
        compiler_params=params(),
        cost_estimate=cost(8 * slots * block * height * height, 8 * height * height),
        name="own_slots",
    )(scalars, table, spectra, edge)


def own_surfaces(half, own, table):
    peers, slots, double, rows = own.shape
    width = table.shape[0]
    span = peers * double

    def body(half_ref, own_ref, table_ref, out_ref):
        out_ref[0] = lax.dot_general(
            own_ref[:, 0].reshape(span, rows),
            table_ref[...],
            (((0,), (0,)), ((), ())),
            preferred_element_type=jnp.float32,
        )

    return pl.pallas_call(
        body,
        grid_spec=pltpu.PrefetchScalarGridSpec(
            num_scalar_prefetch=1,
            grid=(slots,),
            in_specs=[
                pl.BlockSpec((peers, 1, double, rows), lambda p, half: (0, p, 0, 0)),
                pl.BlockSpec((span, width), lambda p, half: (half[0], 0)),
            ],
            out_specs=pl.BlockSpec((1, rows, width), lambda p, half: (p, 0, 0)),
        ),
        out_shape=jax.ShapeDtypeStruct((slots, rows, width), jnp.float32),
        compiler_params=params(),
        cost_estimate=cost(2 * slots * rows * width * span, 4 * slots * rows * width),
        name="own_surfaces",
    )(scalar(half), own, table)


def surfaces_of(half, me, counts, part, came, swapped, table):
    peers = 2 * len(came)
    slots, double, rows = swapped[0].shape
    width = table.shape[0]
    span = peers * double

    def body(half_ref, me_ref, counts_ref, part_ref, *refs):
        other_refs = refs[:peers]
        table_ref, out_ref, work = refs[peers:]
        for k in range(peers):
            place = pl.multiple_of((me_ref[0] ^ k) * double, double)
            piece = other_refs[k][0] if k % 2 else other_refs[k][0, 0]
            work[pl.ds(place, double), :] = piece
        rest = lax.dot_general(
            work[...], table_ref[...], (((0,), (0,)), ((), ())), preferred_element_type=jnp.float32
        )
        live = pl.program_id(0) < counts_ref[0]
        out_ref[0] = jnp.where(live, part_ref[0] + rest, 0.0)

    pair = pl.BlockSpec((1, 1, double, rows), lambda p, half, me, counts: (0, p, 0, 0))
    piece = pl.BlockSpec((1, double, rows), lambda p, half, me, counts: (p, 0, 0))
    other = [swapped[k // 2] if k % 2 else came[k // 2] for k in range(peers)]
    plane = pl.BlockSpec((1, rows, width), lambda p, half, me, counts: (p, 0, 0))
    return pl.pallas_call(
        body,
        grid_spec=pltpu.PrefetchScalarGridSpec(
            num_scalar_prefetch=3,
            grid=(slots,),
            in_specs=[
                plane,
                *[pair, piece] * (peers // 2),
                pl.BlockSpec((span, width), lambda p, half, me, counts: (1 - half[0], 0)),
            ],
            out_specs=plane,
            scratch_shapes=[pltpu.VMEM((span, rows), jnp.bfloat16)],
        ),
        out_shape=jax.ShapeDtypeStruct((slots, rows, width), jnp.float32),
        compiler_params=params(),
        cost_estimate=cost(2 * slots * rows * width * span, 8 * slots * rows * width),
        name="surfaces",
    )(scalar(half), scalar(me), counts, part, *other, table)


def local(tiles, pairs, counts):
    groups = lax.axis_size("blk")
    peers = lax.axis_size("rows")
    group = lax.axis_index("blk")
    me = lax.axis_index("rows")
    count, rows, width = tiles.shape
    slots = pairs.shape[1]
    height = rows * peers
    turn = groups // 2
    half = group // turn
    axes = ("blk", "rows")

    def across(value, k):
        moves = [
            (b * peers + r, (b + turn) % groups * peers + (r ^ k))
            for b in range(groups)
            for r in range(peers)
        ]
        return lax.ppermute(value, axes, moves)

    def along(blocks):
        return lax.all_to_all(blocks, "rows", split_axis=0, concat_axis=0)

    def swap(value):
        return lax.ppermute(value, "rows", [(r, r ^ 1) for r in range(peers)])

    table_w = jnp.asarray(width_table(width, 2 * peers))
    down = jnp.asarray(np.tile(hann(height), (8, 1)))
    sideways = jnp.asarray(hann(width)[None, :])

    sent = row_transform(tiles, down, sideways, table_w, 1 - half, me, peers, True)
    arrived = [across(sent[k], k) for k in range(peers)]
    *sent, held, pairs = lax.optimization_barrier((*sent, half, pairs))
    (kept,) = row_transform(tiles, down, sideways, table_w, held, me, peers, False)
    mine = along(kept)

    table_h = height_table(height)
    theirs = across(pairs, 0)
    packed = ((half == 0) & (me == 0)).astype(jnp.int32)
    their_pairs = jnp.stack([theirs[0, :, 0] + count, (theirs[0, :, 1] + count) % (2 * count)], 1)
    scalars = jnp.concatenate(
        [jnp.stack([half, me, packed]), pairs.reshape(-1), their_pairs.reshape(-1)]
    )
    spectra, edge = own_spectra(scalars, mine, table_h)
    *back, spectra, edge = partner_slots(scalars, arrived, table_h, spectra, edge, slots)
    came = [across(back[j], 2 * j) for j in range(peers // 2)]
    swapped = [swap(value[1]) for value in came]
    own = along(own_slots(scalars, table_h, spectra, edge, peers, slots))
    return surfaces_of(half, me, counts, own_surfaces(half, own, table_w), came, swapped, table_w)


def solution(mesh):
    from jax.sharding import PartitionSpec as P

    return jax.shard_map(
        local,
        mesh=mesh,
        in_specs=(
            P(("parts", "blk"), "rows", None),
            P(("parts", "blk"), None, None),
            P(("parts", "blk")),
        ),
        out_specs=P(("parts", "blk"), "rows", None),
        check_vma=False,
    )
```

```python
import math

import jax
import jax.numpy as jnp
import numpy as np
from jax import lax
from jax.experimental import pallas as pl
from jax.experimental.pallas import tpu as pltpu

FLOOR = 0.05
VMEM_LIMIT = 56 * 1024 * 1024


def hann(length):
    return np.asarray(0.5 - 0.5 * np.cos(2.0 * math.pi / length * np.arange(length)), np.float32)


def scalar(value):
    return jnp.reshape(value, (1,)).astype(jnp.int32)


def width_table(width, owners):
    half = width // 2
    phase = np.arange(half)[:, None] * np.arange(width)[None, :] % width
    angle = 2.0 * math.pi / width * phase
    factor = 1.0 / math.sqrt(width)
    cosine = np.cos(angle) * factor
    sine = -np.sin(angle) * factor
    sine[0] = np.where(np.arange(width) % 2 == 0, factor, -factor)
    shape = (owners, half // owners, width)
    table = np.stack([cosine.reshape(shape), sine.reshape(shape)], axis=1)
    return table.reshape(width, width).astype(jnp.bfloat16)


def height_table(height):
    fine = 32
    coarse = height // fine
    column = np.arange(height)[None, :]
    rough = 2.0 * math.pi / height * (np.arange(coarse)[:, None] * fine * column % height)
    small = 2.0 * math.pi / height * (np.arange(fine)[:, None] * column % height)
    factor = 1.0 / math.sqrt(height)
    rc = jnp.asarray(np.cos(rough) * factor, jnp.float32)[:, None, :]
    rs = jnp.asarray(np.sin(rough) * factor, jnp.float32)[:, None, :]
    sc = jnp.asarray(np.cos(small), jnp.float32)[None, :, :]
    ss = jnp.asarray(np.sin(small), jnp.float32)[None, :, :]
    cosine = (rc * sc - rs * ss).reshape(height, height)
    sine = (rs * sc + rc * ss).reshape(height, height)
    return jnp.concatenate([cosine, sine], axis=1).astype(jnp.bfloat16)


def cost(flops, moved):
    return pl.CostEstimate(flops=flops, transcendentals=0, bytes_accessed=moved)


def params():
    return pltpu.CompilerParams(vmem_limit_bytes=VMEM_LIMIT)


def row_transform(tiles, down, across, table, half, me, peers, apart):
    count, rows, width = tiles.shape
    span = table.shape[0] // 2
    block = span // peers

    def body(half_ref, me_ref, tile_ref, down_ref, across_ref, table_ref, *refs):
        outs, work = refs[:-1], refs[-1]
        window = down_ref[...].T[:, :1] * across_ref[...]
        shaded = (tile_ref[0] * window).astype(jnp.bfloat16)
        y = lax.dot_general(
            table_ref[...], shaded, (((1,), (1,)), ((), ())), preferred_element_type=jnp.float32
        )
        if not apart:
            outs[0][:, 0] = y.astype(jnp.bfloat16).reshape(peers, block, rows)
            return
        work[...] = y.astype(jnp.bfloat16)
        me = me_ref[0]
        for k in range(peers):
            start = pl.multiple_of((me ^ k) * block, block)
            outs[k][0] = work[pl.ds(start, block), :]

    if apart:
        out_specs = [pl.BlockSpec((1, block, rows), lambda t, half, me: (t, 0, 0))] * peers
        out_shape = [jax.ShapeDtypeStruct((count, block, rows), jnp.bfloat16)] * peers
    else:
        out_specs = [pl.BlockSpec((peers, 1, block, rows), lambda t, half, me: (0, t, 0, 0))]
        out_shape = [jax.ShapeDtypeStruct((peers, count, block, rows), jnp.bfloat16)]
    return pl.pallas_call(
        body,
        grid_spec=pltpu.PrefetchScalarGridSpec(
            num_scalar_prefetch=2,
            grid=(count,),
            in_specs=[
                pl.BlockSpec((1, rows, width), lambda t, half, me: (t, 0, 0)),
                pl.BlockSpec((8, rows), lambda t, half, me: (0, me[0])),
                pl.BlockSpec((1, width), lambda t, half, me: (0, 0)),
                pl.BlockSpec((span, width), lambda t, half, me: (half[0], 0)),
            ],
            out_specs=out_specs,
            scratch_shapes=[pltpu.VMEM((span, rows), jnp.bfloat16)],
        ),
        out_shape=out_shape,
        compiler_params=params(),
        cost_estimate=cost(2 * count * rows * width * span, 4 * tiles.size + 2 * span * width),
        name="row_transform",
    )(scalar(half), scalar(me), tiles, down, across, table)


def gather_rows(pieces, table_ref, me):
    total = None
    for k, piece in enumerate(pieces):
        count, block, rows = piece.shape
        start = pl.multiple_of((me ^ k) * rows, rows)
        term = jnp.dot(
            piece[...].reshape(count * block, rows),
            table_ref[pl.ds(start, rows), :],
            preferred_element_type=jnp.float32,
        )
        total = term if total is None else total + term
    return total


def store_spectra(s_ref, total, spectra, edge, first):
    block = spectra.shape[2]
    height = spectra.shape[3]
    row = lax.broadcasted_iota(jnp.int32, (block, height), 0)
    packed = (row == 0) & (s_ref[2] == 1)
    for t in range(total.shape[0] // (2 * block)):
        real = total[2 * t * block : (2 * t + 1) * block]
        imag = total[(2 * t + 1) * block : (2 * t + 2) * block]
        cr, sr = real[:, :height], real[:, height:]
        ci, si = imag[:, :height], imag[:, height:]
        spectra[first + t, 0] = jnp.where(packed, cr, cr + si).astype(jnp.bfloat16)
        spectra[first + t, 1] = jnp.where(packed, -sr, ci - sr).astype(jnp.bfloat16)
        edge[first + t, 0] = ci[:16].astype(jnp.bfloat16)
        edge[first + t, 1] = (-si[:16]).astype(jnp.bfloat16)


def normalised(left_real, left_imag, right_real, right_imag):
    lr = left_real.astype(jnp.float32)
    li = left_imag.astype(jnp.float32)
    rr = right_real.astype(jnp.float32)
    ri = right_imag.astype(jnp.float32)
    cross_real = lr * rr + li * ri
    cross_imag = li * rr - lr * ri
    factor = 1.0 / (jnp.sqrt(cross_real * cross_real + cross_imag * cross_imag) + FLOOR)
    return (
        (cross_real * factor).astype(jnp.bfloat16),
        (cross_imag * factor).astype(jnp.bfloat16),
    )


def correlate(s_ref, me, base, spectra, edge, table_ref, phases, outs):
    block = spectra.shape[2]
    height = spectra.shape[3]
    slots, _, rows = outs[0].shape
    lead = lax.broadcasted_iota(jnp.int32, (16, height), 0)
    packed = (lead == 0) & (s_ref[2] == 1)
    for p in range(slots):
        a = s_ref[base + 2 * p]
        c = s_ref[base + 2 * p + 1]
        q_real, q_imag = normalised(spectra[a, 0], spectra[a, 1], spectra[c, 0], spectra[c, 1])
        e_real, e_imag = normalised(edge[a, 0], edge[a, 1], edge[c, 0], edge[c, 1])
        phases[2 * p] = q_real
        phases[2 * p + 1] = q_imag
        top_real = q_real[:16].astype(jnp.float32)
        top_imag = q_imag[:16].astype(jnp.float32)
        mixed_real = jnp.where(packed, top_real - e_imag.astype(jnp.float32), top_real)
        mixed_imag = jnp.where(packed, top_imag + e_real.astype(jnp.float32), top_imag)
        phases[2 * p, :16] = mixed_real.astype(jnp.bfloat16)
        phases[2 * p + 1, :16] = mixed_imag.astype(jnp.bfloat16)
    row = lax.broadcasted_iota(jnp.int32, (block, rows), 0)
    twice = jnp.where((row == 0) & (s_ref[2] == 1), 1.0, 2.0)
    flat = phases[...].reshape(2 * slots * block, height)
    for k in range(len(outs)):
        start = pl.multiple_of((me ^ k) * rows, rows)
        c_part = jnp.dot(
            flat, table_ref[:, pl.ds(start, rows)], preferred_element_type=jnp.float32
        )
        start = pl.multiple_of(height + (me ^ k) * rows, rows)
        s_part = jnp.dot(
            flat, table_ref[:, pl.ds(start, rows)], preferred_element_type=jnp.float32
        )
        for p in range(slots):
            re = slice(2 * p * block, (2 * p + 1) * block)
            im = slice((2 * p + 1) * block, (2 * p + 2) * block)
            outs[k][p, :block] = ((c_part[re] - s_part[im]) * twice).astype(jnp.bfloat16)
            outs[k][p, block:] = ((s_part[re] + c_part[im]) * twice).astype(jnp.bfloat16)


def own_spectra(scalars, pieces, table):
    peers, count, double, rows = pieces.shape
    height = table.shape[0]

    def body(s_ref, pieces_ref, table_ref, spectra, edge):
        inputs = [pieces_ref.at[k] for k in range(peers)]
        store_spectra(s_ref, gather_rows(inputs, table_ref, 0), spectra, edge, 0)

    return pl.pallas_call(
        body,
        in_specs=[pl.BlockSpec(memory_space=pltpu.SMEM)]
        + [pl.BlockSpec(memory_space=pltpu.VMEM)] * 2,
        out_specs=[pl.BlockSpec(memory_space=pltpu.VMEM)] * 2,
        out_shape=[
            jax.ShapeDtypeStruct((count, 2, double // 2, height), jnp.bfloat16),
            jax.ShapeDtypeStruct((count, 2, 16, height), jnp.bfloat16),
        ],
        compiler_params=params(),
        cost_estimate=cost(4 * count * double * height * height, 8 * height * height),
        name="own_spectra",
    )(scalars, pieces, table)


def partner_slots(scalars, pieces, table, spectra, edge, slots):
    peers = len(pieces)
    count, double, rows = pieces[0].shape
    height = table.shape[0]
    block = double // 2

    def body(s_ref, *refs):
        inputs, table_ref, own_ref, own_edge = refs[:peers], *refs[peers : peers + 3]
        outs = [refs[peers + 3 + k // 2].at[k % 2] for k in range(peers)]
        every, edges, phases = refs[-3:]
        every[:count] = own_ref[...]
        edges[:count] = own_edge[...]
        store_spectra(s_ref, gather_rows(inputs, table_ref, s_ref[1]), every, edges, count)
        correlate(s_ref, s_ref[1], 3 + 2 * slots, every, edges, table_ref, phases, outs)

    return pl.pallas_call(
        body,
        in_specs=[pl.BlockSpec(memory_space=pltpu.SMEM)]
        + [pl.BlockSpec(memory_space=pltpu.VMEM)] * (peers + 3),
        out_specs=[pl.BlockSpec(memory_space=pltpu.VMEM)] * (peers // 2 + 2),
        out_shape=[jax.ShapeDtypeStruct((2, slots, double, rows), jnp.bfloat16)] * (peers // 2)
        + [
            jax.ShapeDtypeStruct((2 * count, 2, block, height), jnp.bfloat16),
            jax.ShapeDtypeStruct((2 * count, 2, 16, height), jnp.bfloat16),
        ],
        scratch_shapes=[pltpu.VMEM((2 * slots, block, height), jnp.bfloat16)],
        compiler_params=params(),
        cost_estimate=cost(4 * (count + slots) * double * height * height, 8 * height * height),
        name="partner_slots",
    )(scalars, *pieces, table, spectra, edge)


def own_slots(scalars, table, spectra, edge, peers, slots):
    block, height = spectra.shape[2:]
    rows = height // peers

    def body(s_ref, table_ref, every, edges, *refs):
        out_ref, phases = refs
        outs = [out_ref.at[k] for k in range(peers)]
        correlate(s_ref, 0, 3, every, edges, table_ref, phases, outs)

    return pl.pallas_call(
        body,
        in_specs=[pl.BlockSpec(memory_space=pltpu.SMEM)]
        + [pl.BlockSpec(memory_space=pltpu.VMEM)] * 3,
        out_specs=pl.BlockSpec(memory_space=pltpu.VMEM),
        out_shape=jax.ShapeDtypeStruct((peers, slots, 2 * block, rows), jnp.bfloat16),
        scratch_shapes=[pltpu.VMEM((2 * slots, block, height), jnp.bfloat16)],
        compiler_params=params(),
        cost_estimate=cost(8 * slots * block * height * height, 8 * height * height),
        name="own_slots",
    )(scalars, table, spectra, edge)


def own_surfaces(half, own, table):
    peers, slots, double, rows = own.shape
    width = table.shape[0]
    span = peers * double

    def body(half_ref, own_ref, table_ref, out_ref):
        out_ref[0] = lax.dot_general(
            own_ref[:, 0].reshape(span, rows),
            table_ref[...],
            (((0,), (0,)), ((), ())),
            preferred_element_type=jnp.float32,
        )

    return pl.pallas_call(
        body,
        grid_spec=pltpu.PrefetchScalarGridSpec(
            num_scalar_prefetch=1,
            grid=(slots,),
            in_specs=[
                pl.BlockSpec((peers, 1, double, rows), lambda p, half: (0, p, 0, 0)),
                pl.BlockSpec((span, width), lambda p, half: (half[0], 0)),
            ],
            out_specs=pl.BlockSpec((1, rows, width), lambda p, half: (p, 0, 0)),
        ),
        out_shape=jax.ShapeDtypeStruct((slots, rows, width), jnp.float32),
        compiler_params=params(),
        cost_estimate=cost(2 * slots * rows * width * span, 4 * slots * rows * width),
        name="own_surfaces",
    )(scalar(half), own, table)


def surfaces_of(half, me, counts, part, came, swapped, table):
    peers = 2 * len(came)
    slots, double, rows = swapped[0].shape
    width = table.shape[0]
    span = peers * double

    def body(half_ref, me_ref, counts_ref, part_ref, *refs):
        other_refs = refs[:peers]
        table_ref, out_ref, work = refs[peers:]
        for k in range(peers):
            place = pl.multiple_of((me_ref[0] ^ k) * double, double)
            piece = other_refs[k][0] if k % 2 else other_refs[k][0, 0]
            work[pl.ds(place, double), :] = piece
        rest = lax.dot_general(
            work[...], table_ref[...], (((0,), (0,)), ((), ())), preferred_element_type=jnp.float32
        )
        live = pl.program_id(0) < counts_ref[0]
        out_ref[0] = jnp.where(live, part_ref[0] + rest, 0.0)

    pair = pl.BlockSpec((1, 1, double, rows), lambda p, half, me, counts: (0, p, 0, 0))
    piece = pl.BlockSpec((1, double, rows), lambda p, half, me, counts: (p, 0, 0))
    other = [swapped[k // 2] if k % 2 else came[k // 2] for k in range(peers)]
    plane = pl.BlockSpec((1, rows, width), lambda p, half, me, counts: (p, 0, 0))
    return pl.pallas_call(
        body,
        grid_spec=pltpu.PrefetchScalarGridSpec(
            num_scalar_prefetch=3,
            grid=(slots,),
            in_specs=[
                plane,
                *[pair, piece] * (peers // 2),
                pl.BlockSpec((span, width), lambda p, half, me, counts: (1 - half[0], 0)),
            ],
            out_specs=plane,
            scratch_shapes=[pltpu.VMEM((span, rows), jnp.bfloat16)],
        ),
        out_shape=jax.ShapeDtypeStruct((slots, rows, width), jnp.float32),
        compiler_params=params(),
        cost_estimate=cost(2 * slots * rows * width * span, 8 * slots * rows * width),
        name="surfaces",
    )(scalar(half), scalar(me), counts, part, *other, table)


def local(tiles, pairs, counts):
    groups = lax.axis_size("blk")
    peers = lax.axis_size("rows")
    group = lax.axis_index("blk")
    me = lax.axis_index("rows")
    count, rows, width = tiles.shape
    slots = pairs.shape[1]
    height = rows * peers
    turn = groups // 2
    half = group // turn
    axes = ("blk", "rows")

    def across(value, k):
        moves = [
            (b * peers + r, (b + turn) % groups * peers + (r ^ k))
            for b in range(groups)
            for r in range(peers)
        ]
        return lax.ppermute(value, axes, moves)

    def along(blocks):
        return lax.all_to_all(blocks, "rows", split_axis=0, concat_axis=0)

    def swap(value):
        return lax.ppermute(value, "rows", [(r, r ^ 1) for r in range(peers)])

    table_w = jnp.asarray(width_table(width, 2 * peers))
    down = jnp.asarray(np.tile(hann(height), (8, 1)))
    sideways = jnp.asarray(hann(width)[None, :])

    sent = row_transform(tiles, down, sideways, table_w, 1 - half, me, peers, True)
    arrived = [across(sent[k], k) for k in range(peers)]
    *sent, held, pairs = lax.optimization_barrier((*sent, half, pairs))
    (kept,) = row_transform(tiles, down, sideways, table_w, held, me, peers, False)
    mine = along(kept)

    table_h = height_table(height)
    theirs = across(pairs, 0)
    packed = ((half == 0) & (me == 0)).astype(jnp.int32)
    their_pairs = jnp.stack([theirs[0, :, 0] + count, (theirs[0, :, 1] + count) % (2 * count)], 1)
    place = jnp.stack([half, me, packed])
    spectra, edge = own_spectra(place, mine, table_h)
    scalars = jnp.concatenate([place, pairs.reshape(-1), their_pairs.reshape(-1)])
    *back, spectra, edge = partner_slots(scalars, arrived, table_h, spectra, edge, slots)
    came = [across(back[j], 2 * j) for j in range(peers // 2)]
    own = along(own_slots(scalars, table_h, spectra, edge, peers, slots))
    part = own_surfaces(half, own, table_w)
    came[-1], part = lax.optimization_barrier((came[-1], part))
    swapped = [swap(value[1]) for value in came]
    return surfaces_of(half, me, counts, part, came, swapped, table_w)


def solution(mesh):
    from jax.sharding import PartitionSpec as P

    return jax.shard_map(
        local,
        mesh=mesh,
        in_specs=(
            P(("parts", "blk"), "rows", None),
            P(("parts", "blk"), None, None),
            P(("parts", "blk")),
        ),
        out_specs=P(("parts", "blk"), "rows", None),
        check_vma=False,
    )
```

```python
import math

import jax
import jax.numpy as jnp
import numpy as np
from jax import lax
from jax.experimental import pallas as pl
from jax.experimental.pallas import tpu as pltpu

FLOOR = 0.05
VMEM_LIMIT = 24 * 1024 * 1024


def hann(length):
    return np.asarray(0.5 - 0.5 * np.cos(2.0 * math.pi / length * np.arange(length)), np.float32)


def scalar(value):
    return jnp.reshape(value, (1,)).astype(jnp.int32)


def width_table(width, owners):
    half = width // 2
    phase = np.arange(half)[:, None] * np.arange(width)[None, :] % width
    angle = 2.0 * math.pi / width * phase
    factor = 1.0 / math.sqrt(width)
    cosine = np.cos(angle) * factor
    sine = -np.sin(angle) * factor
    sine[0] = np.where(np.arange(width) % 2 == 0, factor, -factor)
    shape = (owners, half // owners, width)
    table = np.stack([cosine.reshape(shape), sine.reshape(shape)], axis=1)
    return table.reshape(width, width).astype(jnp.bfloat16)


def height_table(height):
    fine = 32
    coarse = height // fine
    column = np.arange(height)[None, :]
    rough = 2.0 * math.pi / height * (np.arange(coarse)[:, None] * fine * column % height)
    small = 2.0 * math.pi / height * (np.arange(fine)[:, None] * column % height)
    factor = 1.0 / math.sqrt(height)
    rc = jnp.asarray(np.cos(rough) * factor, jnp.float32)[:, None, :]
    rs = jnp.asarray(np.sin(rough) * factor, jnp.float32)[:, None, :]
    sc = jnp.asarray(np.cos(small), jnp.float32)[None, :, :]
    ss = jnp.asarray(np.sin(small), jnp.float32)[None, :, :]
    cosine = (rc * sc - rs * ss).reshape(height, height)
    sine = (rs * sc + rc * ss).reshape(height, height)
    return jnp.concatenate([cosine, sine], axis=1).astype(jnp.bfloat16)


def cost(flops, moved):
    return pl.CostEstimate(flops=flops, transcendentals=0, bytes_accessed=moved)


def params():
    return pltpu.CompilerParams(vmem_limit_bytes=VMEM_LIMIT)


def row_transform(tiles, down, across, table, half, me, peers, apart):
    count, rows, width = tiles.shape
    span = table.shape[0] // 2
    block = span // peers

    def body(half_ref, me_ref, tile_ref, down_ref, across_ref, table_ref, *refs):
        outs, work = refs[:-1], refs[-1]
        window = down_ref[...].T[:, :1] * across_ref[...]
        shaded = (tile_ref[0] * window).astype(jnp.bfloat16)
        y = lax.dot_general(
            table_ref[...], shaded, (((1,), (1,)), ((), ())), preferred_element_type=jnp.float32
        )
        if not apart:
            outs[0][:, 0] = y.astype(jnp.bfloat16).reshape(peers, block, rows)
            return
        work[...] = y.astype(jnp.bfloat16)
        me = me_ref[0]
        for k in range(peers):
            start = pl.multiple_of((me ^ k) * block, block)
            outs[k][0] = work[pl.ds(start, block), :]

    if apart:
        out_specs = [pl.BlockSpec((1, block, rows), lambda t, half, me: (t, 0, 0))] * peers
        out_shape = [jax.ShapeDtypeStruct((count, block, rows), jnp.bfloat16)] * peers
    else:
        out_specs = [pl.BlockSpec((peers, 1, block, rows), lambda t, half, me: (0, t, 0, 0))]
        out_shape = [jax.ShapeDtypeStruct((peers, count, block, rows), jnp.bfloat16)]
    return pl.pallas_call(
        body,
        grid_spec=pltpu.PrefetchScalarGridSpec(
            num_scalar_prefetch=2,
            grid=(count,),
            in_specs=[
                pl.BlockSpec((1, rows, width), lambda t, half, me: (t, 0, 0)),
                pl.BlockSpec((8, rows), lambda t, half, me: (0, me[0])),
                pl.BlockSpec((1, width), lambda t, half, me: (0, 0)),
                pl.BlockSpec((span, width), lambda t, half, me: (half[0], 0)),
            ],
            out_specs=out_specs,
            scratch_shapes=[pltpu.VMEM((span, rows), jnp.bfloat16)],
        ),
        out_shape=out_shape,
        compiler_params=params(),
        cost_estimate=cost(2 * count * rows * width * span, 4 * tiles.size + 2 * span * width),
        name="row_transform",
    )(scalar(half), scalar(me), tiles, down, across, table)


def gather_rows(pieces, table_ref, me):
    total = None
    for k, piece in enumerate(pieces):
        count, block, rows = piece.shape
        start = pl.multiple_of((me ^ k) * rows, rows)
        term = jnp.dot(
            piece[...].reshape(count * block, rows),
            table_ref[pl.ds(start, rows), :],
            preferred_element_type=jnp.float32,
        )
        total = term if total is None else total + term
    return total


def store_spectra(s_ref, total, spectra, edge, first):
    block = spectra.shape[2]
    height = spectra.shape[3]
    row = lax.broadcasted_iota(jnp.int32, (block, height), 0)
    packed = (row == 0) & (s_ref[2] == 1)
    for t in range(total.shape[0] // (2 * block)):
        real = total[2 * t * block : (2 * t + 1) * block]
        imag = total[(2 * t + 1) * block : (2 * t + 2) * block]
        cr, sr = real[:, :height], real[:, height:]
        ci, si = imag[:, :height], imag[:, height:]
        spectra[first + t, 0] = jnp.where(packed, cr, cr + si).astype(jnp.bfloat16)
        spectra[first + t, 1] = jnp.where(packed, -sr, ci - sr).astype(jnp.bfloat16)
        edge[first + t, 0] = ci[:16].astype(jnp.bfloat16)
        edge[first + t, 1] = (-si[:16]).astype(jnp.bfloat16)


def normalised(left_real, left_imag, right_real, right_imag):
    lr = left_real.astype(jnp.float32)
    li = left_imag.astype(jnp.float32)
    rr = right_real.astype(jnp.float32)
    ri = right_imag.astype(jnp.float32)
    cross_real = lr * rr + li * ri
    cross_imag = li * rr - lr * ri
    factor = 1.0 / (jnp.sqrt(cross_real * cross_real + cross_imag * cross_imag) + FLOOR)
    return (
        (cross_real * factor).astype(jnp.bfloat16),
        (cross_imag * factor).astype(jnp.bfloat16),
    )


def correlate(s_ref, me, base, spectra, edge, table_ref, phases, outs):
    block = spectra.shape[2]
    height = spectra.shape[3]
    slots, _, rows = outs[0].shape
    lead = lax.broadcasted_iota(jnp.int32, (16, height), 0)
    packed = (lead == 0) & (s_ref[2] == 1)
    for p in range(slots):
        a = s_ref[base + 2 * p]
        c = s_ref[base + 2 * p + 1]
        q_real, q_imag = normalised(spectra[a, 0], spectra[a, 1], spectra[c, 0], spectra[c, 1])
        e_real, e_imag = normalised(edge[a, 0], edge[a, 1], edge[c, 0], edge[c, 1])
        phases[2 * p] = q_real
        phases[2 * p + 1] = q_imag
        top_real = q_real[:16].astype(jnp.float32)
        top_imag = q_imag[:16].astype(jnp.float32)
        mixed_real = jnp.where(packed, top_real - e_imag.astype(jnp.float32), top_real)
        mixed_imag = jnp.where(packed, top_imag + e_real.astype(jnp.float32), top_imag)
        phases[2 * p, :16] = mixed_real.astype(jnp.bfloat16)
        phases[2 * p + 1, :16] = mixed_imag.astype(jnp.bfloat16)
    row = lax.broadcasted_iota(jnp.int32, (block, rows), 0)
    twice = jnp.where((row == 0) & (s_ref[2] == 1), 1.0, 2.0)
    flat = phases[...].reshape(2 * slots * block, height)
    for k in range(len(outs)):
        start = pl.multiple_of((me ^ k) * rows, rows)
        c_part = jnp.dot(
            flat, table_ref[:, pl.ds(start, rows)], preferred_element_type=jnp.float32
        )
        start = pl.multiple_of(height + (me ^ k) * rows, rows)
        s_part = jnp.dot(
            flat, table_ref[:, pl.ds(start, rows)], preferred_element_type=jnp.float32
        )
        for p in range(slots):
            re = slice(2 * p * block, (2 * p + 1) * block)
            im = slice((2 * p + 1) * block, (2 * p + 2) * block)
            outs[k][p, :block] = ((c_part[re] - s_part[im]) * twice).astype(jnp.bfloat16)
            outs[k][p, block:] = ((s_part[re] + c_part[im]) * twice).astype(jnp.bfloat16)


def own_spectra(scalars, pieces, table):
    peers, count, double, rows = pieces.shape
    height = table.shape[0]

    def body(s_ref, pieces_ref, table_ref, spectra, edge):
        inputs = [pieces_ref.at[k] for k in range(peers)]
        store_spectra(s_ref, gather_rows(inputs, table_ref, 0), spectra, edge, 0)

    return pl.pallas_call(
        body,
        in_specs=[pl.BlockSpec(memory_space=pltpu.SMEM)]
        + [pl.BlockSpec(memory_space=pltpu.VMEM)] * 2,
        out_specs=[pl.BlockSpec(memory_space=pltpu.VMEM)] * 2,
        out_shape=[
            jax.ShapeDtypeStruct((count, 2, double // 2, height), jnp.bfloat16),
            jax.ShapeDtypeStruct((count, 2, 16, height), jnp.bfloat16),
        ],
        compiler_params=params(),
        cost_estimate=cost(4 * count * double * height * height, 8 * height * height),
        name="own_spectra",
    )(scalars, pieces, table)


def partner_slots(scalars, pieces, table, spectra, edge, slots):
    peers = len(pieces)
    count, double, rows = pieces[0].shape
    height = table.shape[0]
    block = double // 2

    def body(s_ref, *refs):
        inputs, table_ref, own_ref, own_edge = refs[:peers], *refs[peers : peers + 3]
        outs = [refs[peers + 3 + k // 2].at[k % 2] for k in range(peers)]
        every, edges, phases = refs[-3:]
        every[:count] = own_ref[...]
        edges[:count] = own_edge[...]
        store_spectra(s_ref, gather_rows(inputs, table_ref, s_ref[1]), every, edges, count)
        correlate(s_ref, s_ref[1], 3 + 2 * slots, every, edges, table_ref, phases, outs)

    return pl.pallas_call(
        body,
        in_specs=[pl.BlockSpec(memory_space=pltpu.SMEM)]
        + [pl.BlockSpec(memory_space=pltpu.VMEM)] * (peers + 3),
        out_specs=[pl.BlockSpec(memory_space=pltpu.VMEM)] * (peers // 2 + 2),
        out_shape=[jax.ShapeDtypeStruct((2, slots, double, rows), jnp.bfloat16)] * (peers // 2)
        + [
            jax.ShapeDtypeStruct((2 * count, 2, block, height), jnp.bfloat16),
            jax.ShapeDtypeStruct((2 * count, 2, 16, height), jnp.bfloat16),
        ],
        scratch_shapes=[pltpu.VMEM((2 * slots, block, height), jnp.bfloat16)],
        compiler_params=params(),
        cost_estimate=cost(4 * (count + slots) * double * height * height, 8 * height * height),
        name="partner_slots",
    )(scalars, *pieces, table, spectra, edge)


def own_slots(scalars, table, spectra, edge, peers, slots):
    block, height = spectra.shape[2:]
    rows = height // peers

    def body(s_ref, table_ref, every, edges, *refs):
        out_ref, phases = refs
        outs = [out_ref.at[k] for k in range(peers)]
        correlate(s_ref, 0, 3, every, edges, table_ref, phases, outs)

    return pl.pallas_call(
        body,
        in_specs=[pl.BlockSpec(memory_space=pltpu.SMEM)]
        + [pl.BlockSpec(memory_space=pltpu.VMEM)] * 3,
        out_specs=pl.BlockSpec(memory_space=pltpu.VMEM),
        out_shape=jax.ShapeDtypeStruct((peers, slots, 2 * block, rows), jnp.bfloat16),
        scratch_shapes=[pltpu.VMEM((2 * slots, block, height), jnp.bfloat16)],
        compiler_params=params(),
        cost_estimate=cost(8 * slots * block * height * height, 8 * height * height),
        name="own_slots",
    )(scalars, table, spectra, edge)


def own_surfaces(half, own, table):
    peers, slots, double, rows = own.shape
    width = table.shape[0]
    span = peers * double

    def body(half_ref, own_ref, table_ref, out_ref):
        out_ref[0] = lax.dot_general(
            own_ref[:, 0].reshape(span, rows),
            table_ref[...],
            (((0,), (0,)), ((), ())),
            preferred_element_type=jnp.float32,
        )

    return pl.pallas_call(
        body,
        grid_spec=pltpu.PrefetchScalarGridSpec(
            num_scalar_prefetch=1,
            grid=(slots,),
            in_specs=[
                pl.BlockSpec((peers, 1, double, rows), lambda p, half: (0, p, 0, 0)),
                pl.BlockSpec((span, width), lambda p, half: (half[0], 0)),
            ],
            out_specs=pl.BlockSpec((1, rows, width), lambda p, half: (p, 0, 0)),
        ),
        out_shape=jax.ShapeDtypeStruct((slots, rows, width), jnp.float32),
        compiler_params=params(),
        cost_estimate=cost(2 * slots * rows * width * span, 4 * slots * rows * width),
        name="own_surfaces",
    )(scalar(half), own, table)


def surfaces_of(half, me, counts, part, came, swapped, table):
    peers = 2 * len(came)
    slots, double, rows = swapped[0].shape
    width = table.shape[0]
    span = peers * double

    def body(half_ref, me_ref, counts_ref, part_ref, *refs):
        other_refs = refs[:peers]
        table_ref, out_ref, work = refs[peers:]
        for k in range(peers):
            place = pl.multiple_of((me_ref[0] ^ k) * double, double)
            piece = other_refs[k][0] if k % 2 else other_refs[k][0, 0]
            work[pl.ds(place, double), :] = piece
        rest = lax.dot_general(
            work[...], table_ref[...], (((0,), (0,)), ((), ())), preferred_element_type=jnp.float32
        )
        live = pl.program_id(0) < counts_ref[0]
        out_ref[0] = jnp.where(live, part_ref[0] + rest, 0.0)

    pair = pl.BlockSpec((1, 1, double, rows), lambda p, half, me, counts: (0, p, 0, 0))
    piece = pl.BlockSpec((1, double, rows), lambda p, half, me, counts: (p, 0, 0))
    other = [swapped[k // 2] if k % 2 else came[k // 2] for k in range(peers)]
    plane = pl.BlockSpec((1, rows, width), lambda p, half, me, counts: (p, 0, 0))
    return pl.pallas_call(
        body,
        grid_spec=pltpu.PrefetchScalarGridSpec(
            num_scalar_prefetch=3,
            grid=(slots,),
            in_specs=[
                plane,
                *[pair, piece] * (peers // 2),
                pl.BlockSpec((span, width), lambda p, half, me, counts: (1 - half[0], 0)),
            ],
            out_specs=plane,
            scratch_shapes=[pltpu.VMEM((span, rows), jnp.bfloat16)],
        ),
        out_shape=jax.ShapeDtypeStruct((slots, rows, width), jnp.float32),
        compiler_params=params(),
        cost_estimate=cost(2 * slots * rows * width * span, 8 * slots * rows * width),
        name="surfaces",
    )(scalar(half), scalar(me), counts, part, *other, table)


def local(tiles, pairs, counts):
    groups = lax.axis_size("blk")
    peers = lax.axis_size("rows")
    group = lax.axis_index("blk")
    me = lax.axis_index("rows")
    count, rows, width = tiles.shape
    slots = pairs.shape[1]
    height = rows * peers
    turn = groups // 2
    half = group // turn
    axes = ("blk", "rows")

    def across(value, k):
        moves = [
            (b * peers + r, (b + turn) % groups * peers + (r ^ k))
            for b in range(groups)
            for r in range(peers)
        ]
        return lax.ppermute(value, axes, moves)

    def along(blocks):
        return lax.all_to_all(blocks, "rows", split_axis=0, concat_axis=0)

    def swap(value):
        return lax.ppermute(value, "rows", [(r, r ^ 1) for r in range(peers)])

    table_w = jnp.asarray(width_table(width, 2 * peers))
    down = jnp.asarray(np.tile(hann(height), (8, 1)))
    sideways = jnp.asarray(hann(width)[None, :])

    sent = row_transform(tiles, down, sideways, table_w, 1 - half, me, peers, True)
    arrived = [across(sent[k], k) for k in range(peers)]
    *sent, held, pairs = lax.optimization_barrier((*sent, half, pairs))
    (kept,) = row_transform(tiles, down, sideways, table_w, held, me, peers, False)
    mine = along(kept)

    table_h = height_table(height)
    theirs = across(pairs, 0)
    packed = ((half == 0) & (me == 0)).astype(jnp.int32)
    their_pairs = jnp.stack([theirs[0, :, 0] + count, (theirs[0, :, 1] + count) % (2 * count)], 1)
    place = jnp.stack([half, me, packed])
    spectra, edge = own_spectra(place, mine, table_h)
    scalars = jnp.concatenate([place, pairs.reshape(-1), their_pairs.reshape(-1)])
    *back, spectra, edge = partner_slots(scalars, arrived, table_h, spectra, edge, slots)
    came = [across(back[j], 2 * j) for j in range(peers // 2)]
    own = along(own_slots(scalars, table_h, spectra, edge, peers, slots))
    part = own_surfaces(half, own, table_w)
    came[-1], part = lax.optimization_barrier((came[-1], part))
    swapped = [swap(value[1]) for value in came]
    return surfaces_of(half, me, counts, part, came, swapped, table_w)


def solution(mesh):
    from jax.sharding import PartitionSpec as P

    return jax.shard_map(
        local,
        mesh=mesh,
        in_specs=(
            P(("parts", "blk"), "rows", None),
            P(("parts", "blk"), None, None),
            P(("parts", "blk")),
        ),
        out_specs=P(("parts", "blk"), "rows", None),
        check_vma=False,
    )
```

```python
import math

import jax
import jax.numpy as jnp
import numpy as np
from jax import lax
from jax.experimental import pallas as pl
from jax.experimental.pallas import tpu as pltpu

FLOOR = 0.05
VMEM_LIMIT = 24 * 1024 * 1024


def hann(length):
    return np.asarray(0.5 - 0.5 * np.cos(2.0 * math.pi / length * np.arange(length)), np.float32)


def scalar(value):
    return jnp.reshape(value, (1,)).astype(jnp.int32)


def width_table(width, owners):
    half = width // 2
    phase = np.arange(half)[:, None] * np.arange(width)[None, :] % width
    angle = 2.0 * math.pi / width * phase
    factor = 1.0 / math.sqrt(width)
    cosine = np.cos(angle) * factor
    sine = -np.sin(angle) * factor
    sine[0] = np.where(np.arange(width) % 2 == 0, factor, -factor)
    shape = (owners, half // owners, width)
    table = np.stack([cosine.reshape(shape), sine.reshape(shape)], axis=1)
    return table.reshape(width, width).astype(jnp.bfloat16)


def height_table(height):
    fine = 32
    coarse = height // fine
    column = np.arange(height)[None, :]
    rough = 2.0 * math.pi / height * (np.arange(coarse)[:, None] * fine * column % height)
    small = 2.0 * math.pi / height * (np.arange(fine)[:, None] * column % height)
    factor = 1.0 / math.sqrt(height)
    rc = jnp.asarray(np.cos(rough) * factor, jnp.float32)[:, None, :]
    rs = jnp.asarray(np.sin(rough) * factor, jnp.float32)[:, None, :]
    sc = jnp.asarray(np.cos(small), jnp.float32)[None, :, :]
    ss = jnp.asarray(np.sin(small), jnp.float32)[None, :, :]
    cosine = (rc * sc - rs * ss).reshape(height, height)
    sine = (rs * sc + rc * ss).reshape(height, height)
    return jnp.concatenate([cosine, sine], axis=1).astype(jnp.bfloat16)


def cost(flops, moved):
    return pl.CostEstimate(flops=flops, transcendentals=0, bytes_accessed=moved)


def params():
    return pltpu.CompilerParams(vmem_limit_bytes=VMEM_LIMIT)


def shade(tile, down_ref, across_ref):
    return (tile * (down_ref[...].T[:, :1] * across_ref[...])).astype(jnp.bfloat16)


def times_table(table, shaded):
    y = lax.dot_general(
        table, shaded, (((1,), (1,)), ((), ())), preferred_element_type=jnp.float32
    )
    return y.astype(jnp.bfloat16)


def sent_columns(tiles, down, across, table, half, me, peers):
    count, rows, width = tiles.shape
    span = table.shape[0] // 2
    block = span // peers

    def body(half_ref, me_ref, tile_hbm, down_ref, across_ref, table_hbm, *refs):
        outs = refs[:peers]
        tile_ref, table_ref, work, done = refs[peers:]
        t = pl.program_id(0)
        start = pl.multiple_of((1 - half_ref[0]) * span, span)
        fetch = pltpu.make_async_copy(
            table_hbm.at[pl.ds(start, span)], table_ref, done.at[count]
        )
        loads = [
            pltpu.make_async_copy(tile_hbm.at[i], tile_ref.at[i], done.at[i]) for i in range(count)
        ]

        @pl.when(t == 0)
        def _():
            loads[0].start()
            fetch.start()
            for load in loads[1:]:
                load.start()
            fetch.wait()

        for i in range(count):

            @pl.when(t == i)
            def _():
                loads[i].wait()
                work[...] = times_table(table_ref[...], shade(tile_ref[i], down_ref, across_ref))

        for k in range(peers):
            place = pl.multiple_of((me_ref[0] ^ k) * block, block)
            outs[k][0] = work[pl.ds(place, block), :]

    return pl.pallas_call(
        body,
        grid_spec=pltpu.PrefetchScalarGridSpec(
            num_scalar_prefetch=2,
            grid=(count,),
            in_specs=[
                pl.BlockSpec(memory_space=pltpu.HBM),
                pl.BlockSpec((8, rows), lambda t, half, me: (0, me[0])),
                pl.BlockSpec((1, width), lambda t, half, me: (0, 0)),
                pl.BlockSpec(memory_space=pltpu.HBM),
            ],
            out_specs=[pl.BlockSpec((1, block, rows), lambda t, half, me: (t, 0, 0))] * peers,
            scratch_shapes=[
                pltpu.VMEM((count, rows, width), tiles.dtype),
                pltpu.VMEM((span, width), table.dtype),
                pltpu.VMEM((span, rows), jnp.bfloat16),
                pltpu.SemaphoreType.DMA((count + 1,)),
            ],
        ),
        out_shape=[jax.ShapeDtypeStruct((count, block, rows), jnp.bfloat16)] * peers,
        compiler_params=params(),
        cost_estimate=cost(2 * count * rows * width * span, 4 * tiles.size + 2 * span * width),
        name="sent_columns",
    )(scalar(half), scalar(me), tiles, down, across, table)


def kept_columns(tiles, down, across, table, half, me, peers):
    count, rows, width = tiles.shape
    span = table.shape[0] // 2
    block = span // peers

    def body(half_ref, me_ref, tile_ref, down_ref, across_ref, table_ref, out_ref):
        y = times_table(table_ref[...], shade(tile_ref[0], down_ref, across_ref))
        out_ref[:, 0] = y.reshape(peers, block, rows)

    return pl.pallas_call(
        body,
        grid_spec=pltpu.PrefetchScalarGridSpec(
            num_scalar_prefetch=2,
            grid=(count,),
            in_specs=[
                pl.BlockSpec((1, rows, width), lambda t, half, me: (t, 0, 0)),
                pl.BlockSpec((8, rows), lambda t, half, me: (0, me[0])),
                pl.BlockSpec((1, width), lambda t, half, me: (0, 0)),
                pl.BlockSpec((span, width), lambda t, half, me: (half[0], 0)),
            ],
            out_specs=pl.BlockSpec((peers, 1, block, rows), lambda t, half, me: (0, t, 0, 0)),
        ),
        out_shape=jax.ShapeDtypeStruct((peers, count, block, rows), jnp.bfloat16),
        compiler_params=params(),
        cost_estimate=cost(2 * count * rows * width * span, 4 * tiles.size + 2 * span * width),
        name="kept_columns",
    )(scalar(half), scalar(me), tiles, down, across, table)


def gather_rows(pieces, table_ref, me):
    total = None
    for k, piece in enumerate(pieces):
        count, block, rows = piece.shape
        start = pl.multiple_of((me ^ k) * rows, rows)
        term = jnp.dot(
            piece[...].reshape(count * block, rows),
            table_ref[pl.ds(start, rows), :],
            preferred_element_type=jnp.float32,
        )
        total = term if total is None else total + term
    return total


def store_spectra(s_ref, total, spectra, edge, first):
    block = spectra.shape[2]
    height = spectra.shape[3]
    row = lax.broadcasted_iota(jnp.int32, (block, height), 0)
    packed = (row == 0) & (s_ref[2] == 1)
    for t in range(total.shape[0] // (2 * block)):
        real = total[2 * t * block : (2 * t + 1) * block]
        imag = total[(2 * t + 1) * block : (2 * t + 2) * block]
        cr, sr = real[:, :height], real[:, height:]
        ci, si = imag[:, :height], imag[:, height:]
        spectra[first + t, 0] = jnp.where(packed, cr, cr + si).astype(jnp.bfloat16)
        spectra[first + t, 1] = jnp.where(packed, -sr, ci - sr).astype(jnp.bfloat16)
        edge[first + t, 0] = ci[:16].astype(jnp.bfloat16)
        edge[first + t, 1] = (-si[:16]).astype(jnp.bfloat16)


def normalised(left_real, left_imag, right_real, right_imag):
    lr = left_real.astype(jnp.float32)
    li = left_imag.astype(jnp.float32)
    rr = right_real.astype(jnp.float32)
    ri = right_imag.astype(jnp.float32)
    cross_real = lr * rr + li * ri
    cross_imag = li * rr - lr * ri
    factor = 1.0 / (jnp.sqrt(cross_real * cross_real + cross_imag * cross_imag) + FLOOR)
    return (
        (cross_real * factor).astype(jnp.bfloat16),
        (cross_imag * factor).astype(jnp.bfloat16),
    )


def correlate(s_ref, me, base, spectra, edge, table_ref, phases, outs):
    block = spectra.shape[2]
    height = spectra.shape[3]
    slots, _, rows = outs[0].shape
    lead = lax.broadcasted_iota(jnp.int32, (16, height), 0)
    packed = (lead == 0) & (s_ref[2] == 1)
    for p in range(slots):
        a = s_ref[base + 2 * p]
        c = s_ref[base + 2 * p + 1]
        q_real, q_imag = normalised(spectra[a, 0], spectra[a, 1], spectra[c, 0], spectra[c, 1])
        e_real, e_imag = normalised(edge[a, 0], edge[a, 1], edge[c, 0], edge[c, 1])
        phases[2 * p] = q_real
        phases[2 * p + 1] = q_imag
        top_real = q_real[:16].astype(jnp.float32)
        top_imag = q_imag[:16].astype(jnp.float32)
        mixed_real = jnp.where(packed, top_real - e_imag.astype(jnp.float32), top_real)
        mixed_imag = jnp.where(packed, top_imag + e_real.astype(jnp.float32), top_imag)
        phases[2 * p, :16] = mixed_real.astype(jnp.bfloat16)
        phases[2 * p + 1, :16] = mixed_imag.astype(jnp.bfloat16)
    row = lax.broadcasted_iota(jnp.int32, (block, rows), 0)
    twice = jnp.where((row == 0) & (s_ref[2] == 1), 1.0, 2.0)
    flat = phases[...].reshape(2 * slots * block, height)
    for k in range(len(outs)):
        start = pl.multiple_of((me ^ k) * rows, rows)
        c_part = jnp.dot(
            flat, table_ref[:, pl.ds(start, rows)], preferred_element_type=jnp.float32
        )
        start = pl.multiple_of(height + (me ^ k) * rows, rows)
        s_part = jnp.dot(
            flat, table_ref[:, pl.ds(start, rows)], preferred_element_type=jnp.float32
        )
        for p in range(slots):
            re = slice(2 * p * block, (2 * p + 1) * block)
            im = slice((2 * p + 1) * block, (2 * p + 2) * block)
            outs[k][p, :block] = ((c_part[re] - s_part[im]) * twice).astype(jnp.bfloat16)
            outs[k][p, block:] = ((s_part[re] + c_part[im]) * twice).astype(jnp.bfloat16)


def own_spectra(scalars, pieces, table):
    peers, count, double, rows = pieces.shape
    height = table.shape[0]

    def body(s_ref, pieces_ref, table_ref, spectra, edge):
        inputs = [pieces_ref.at[k] for k in range(peers)]
        store_spectra(s_ref, gather_rows(inputs, table_ref, 0), spectra, edge, 0)

    return pl.pallas_call(
        body,
        in_specs=[pl.BlockSpec(memory_space=pltpu.SMEM)]
        + [pl.BlockSpec(memory_space=pltpu.VMEM)] * 2,
        out_specs=[pl.BlockSpec(memory_space=pltpu.VMEM)] * 2,
        out_shape=[
            jax.ShapeDtypeStruct((count, 2, double // 2, height), jnp.bfloat16),
            jax.ShapeDtypeStruct((count, 2, 16, height), jnp.bfloat16),
        ],
        compiler_params=params(),
        cost_estimate=cost(4 * count * double * height * height, 8 * height * height),
        name="own_spectra",
    )(scalars, pieces, table)


def partner_slots(scalars, pieces, table, spectra, edge, slots):
    peers = len(pieces)
    count, double, rows = pieces[0].shape
    height = table.shape[0]
    block = double // 2

    def body(s_ref, *refs):
        inputs, table_ref, own_ref, own_edge = refs[:peers], *refs[peers : peers + 3]
        outs = [refs[peers + 3 + k // 2].at[k % 2] for k in range(peers)]
        every, edges, phases, landed, done = refs[-5:]
        loads = [
            pltpu.make_async_copy(inputs[k], landed.at[k], done.at[k]) for k in range(peers)
        ]
        for load in loads:
            load.start()
        every[:count] = own_ref[...]
        edges[:count] = own_edge[...]
        for load in loads:
            load.wait()
        inputs = [landed.at[k] for k in range(peers)]
        store_spectra(s_ref, gather_rows(inputs, table_ref, s_ref[1]), every, edges, count)
        correlate(s_ref, s_ref[1], 3 + 2 * slots, every, edges, table_ref, phases, outs)

    return pl.pallas_call(
        body,
        in_specs=[pl.BlockSpec(memory_space=pltpu.SMEM)]
        + [pl.BlockSpec(memory_space=pltpu.HBM)] * peers
        + [pl.BlockSpec(memory_space=pltpu.VMEM)] * 3,
        out_specs=[pl.BlockSpec(memory_space=pltpu.VMEM)] * (peers // 2 + 2),
        out_shape=[jax.ShapeDtypeStruct((2, slots, double, rows), jnp.bfloat16)] * (peers // 2)
        + [
            jax.ShapeDtypeStruct((2 * count, 2, block, height), jnp.bfloat16),
            jax.ShapeDtypeStruct((2 * count, 2, 16, height), jnp.bfloat16),
        ],
        scratch_shapes=[
            pltpu.VMEM((2 * slots, block, height), jnp.bfloat16),
            pltpu.VMEM((peers, count, double, rows), jnp.bfloat16),
            pltpu.SemaphoreType.DMA((peers,)),
        ],
        compiler_params=params(),
        cost_estimate=cost(4 * (count + slots) * double * height * height, 8 * height * height),
        name="partner_slots",
    )(scalars, *pieces, table, spectra, edge)


def own_slots(scalars, table, spectra, edge, peers, slots):
    block, height = spectra.shape[2:]
    rows = height // peers

    def body(s_ref, table_ref, every, edges, *refs):
        out_ref, phases = refs
        outs = [out_ref.at[k] for k in range(peers)]
        correlate(s_ref, 0, 3, every, edges, table_ref, phases, outs)

    return pl.pallas_call(
        body,
        in_specs=[pl.BlockSpec(memory_space=pltpu.SMEM)]
        + [pl.BlockSpec(memory_space=pltpu.VMEM)] * 3,
        out_specs=pl.BlockSpec(memory_space=pltpu.VMEM),
        out_shape=jax.ShapeDtypeStruct((peers, slots, 2 * block, rows), jnp.bfloat16),
        scratch_shapes=[pltpu.VMEM((2 * slots, block, height), jnp.bfloat16)],
        compiler_params=params(),
        cost_estimate=cost(8 * slots * block * height * height, 8 * height * height),
        name="own_slots",
    )(scalars, table, spectra, edge)


def own_surfaces(half, own, table):
    peers, slots, double, rows = own.shape
    width = table.shape[0]
    span = peers * double

    def body(half_ref, own_ref, table_ref, out_ref):
        out_ref[0] = lax.dot_general(
            own_ref[:, 0].reshape(span, rows),
            table_ref[...],
            (((0,), (0,)), ((), ())),
            preferred_element_type=jnp.float32,
        )

    return pl.pallas_call(
        body,
        grid_spec=pltpu.PrefetchScalarGridSpec(
            num_scalar_prefetch=1,
            grid=(slots,),
            in_specs=[
                pl.BlockSpec((peers, 1, double, rows), lambda p, half: (0, p, 0, 0)),
                pl.BlockSpec((span, width), lambda p, half: (half[0], 0)),
            ],
            out_specs=pl.BlockSpec((1, rows, width), lambda p, half: (p, 0, 0)),
        ),
        out_shape=jax.ShapeDtypeStruct((slots, rows, width), jnp.float32),
        compiler_params=params(),
        cost_estimate=cost(2 * slots * rows * width * span, 4 * slots * rows * width),
        name="own_surfaces",
    )(scalar(half), own, table)


def surfaces_of(half, me, counts, part, came, swapped, table):
    peers = 2 * len(came)
    slots, double, rows = swapped[0].shape
    width = table.shape[0]
    span = peers * double

    def body(half_ref, me_ref, counts_ref, part_ref, *refs):
        other_refs = refs[:peers]
        table_ref, out_ref, work = refs[peers:]
        for k in range(peers):
            place = pl.multiple_of((me_ref[0] ^ k) * double, double)
            piece = other_refs[k][0] if k % 2 else other_refs[k][0, 0]
            work[pl.ds(place, double), :] = piece
        rest = lax.dot_general(
            work[...], table_ref[...], (((0,), (0,)), ((), ())), preferred_element_type=jnp.float32
        )
        live = pl.program_id(0) < counts_ref[0]
        out_ref[0] = jnp.where(live, part_ref[0] + rest, 0.0)

    pair = pl.BlockSpec((1, 1, double, rows), lambda p, half, me, counts: (0, p, 0, 0))
    piece = pl.BlockSpec((1, double, rows), lambda p, half, me, counts: (p, 0, 0))
    other = [swapped[k // 2] if k % 2 else came[k // 2] for k in range(peers)]
    plane = pl.BlockSpec((1, rows, width), lambda p, half, me, counts: (p, 0, 0))
    return pl.pallas_call(
        body,
        grid_spec=pltpu.PrefetchScalarGridSpec(
            num_scalar_prefetch=3,
            grid=(slots,),
            in_specs=[
                plane,
                *[pair, piece] * (peers // 2),
                pl.BlockSpec((span, width), lambda p, half, me, counts: (1 - half[0], 0)),
            ],
            out_specs=plane,
            scratch_shapes=[pltpu.VMEM((span, rows), jnp.bfloat16)],
        ),
        out_shape=jax.ShapeDtypeStruct((slots, rows, width), jnp.float32),
        compiler_params=params(),
        cost_estimate=cost(2 * slots * rows * width * span, 8 * slots * rows * width),
        name="surfaces",
    )(scalar(half), scalar(me), counts, part, *other, table)


def local(tiles, pairs, counts):
    groups = lax.axis_size("blk")
    peers = lax.axis_size("rows")
    group = lax.axis_index("blk")
    me = lax.axis_index("rows")
    count, rows, width = tiles.shape
    slots = pairs.shape[1]
    height = rows * peers
    turn = groups // 2
    half = group // turn
    axes = ("blk", "rows")

    def across(value, k):
        moves = [
            (b * peers + r, (b + turn) % groups * peers + (r ^ k))
            for b in range(groups)
            for r in range(peers)
        ]
        return lax.ppermute(value, axes, moves)

    def along(blocks):
        return lax.all_to_all(blocks, "rows", split_axis=0, concat_axis=0)

    def swap(value):
        return lax.ppermute(value, "rows", [(r, r ^ 1) for r in range(peers)])

    table_w = jnp.asarray(width_table(width, 2 * peers))
    down = jnp.asarray(np.tile(hann(height), (8, 1)))
    sideways = jnp.asarray(hann(width)[None, :])

    sent = sent_columns(tiles, down, sideways, table_w, half, me, peers)
    arrived = [across(sent[k], k) for k in range(peers)]
    *sent, held = lax.optimization_barrier((*sent, half))
    kept = kept_columns(tiles, down, sideways, table_w, held, me, peers)
    kept, pairs = lax.optimization_barrier((kept, pairs))
    mine = along(kept)

    table_h = height_table(height)
    theirs = across(pairs, 0)
    packed = ((half == 0) & (me == 0)).astype(jnp.int32)
    their_pairs = theirs[0]
    place = jnp.stack([half, me, packed])
    spectra, edge = own_spectra(place, mine, table_h)
    their_pairs, spectra = lax.optimization_barrier((their_pairs, spectra))
    scalars = jnp.concatenate([place, pairs.reshape(-1), ((their_pairs + count) % (2 * count)).reshape(-1)])
    *back, spectra, edge = partner_slots(scalars, arrived, table_h, spectra, edge, slots)
    came = [across(back[j], 2 * j) for j in range(peers // 2)]
    own = along(own_slots(scalars, table_h, spectra, edge, peers, slots))
    part = own_surfaces(half, own, table_w)
    came[-1], part = lax.optimization_barrier((came[-1], part))
    swapped = [swap(value[1]) for value in came]
    return surfaces_of(half, me, counts, part, came, swapped, table_w)


def solution(mesh):
    from jax.sharding import PartitionSpec as P

    return jax.shard_map(
        local,
        mesh=mesh,
        in_specs=(
            P(("parts", "blk"), "rows", None),
            P(("parts", "blk"), None, None),
            P(("parts", "blk")),
        ),
        out_specs=P(("parts", "blk"), "rows", None),
        check_vma=False,
    )
```

```python
import math

import jax
import jax.numpy as jnp
import numpy as np
from jax import lax
from jax.experimental import pallas as pl
from jax.experimental.pallas import tpu as pltpu

FLOOR = 0.05
VMEM_LIMIT = 24 * 1024 * 1024
FIRST_LIMIT = 60 * 1024 * 1024


def hann(length):
    return np.asarray(0.5 - 0.5 * np.cos(2.0 * math.pi / length * np.arange(length)), np.float32)


def scalar(value):
    return jnp.reshape(value, (1,)).astype(jnp.int32)


def width_table(width, owners):
    half = width // 2
    phase = np.arange(half)[:, None] * np.arange(width)[None, :] % width
    angle = 2.0 * math.pi / width * phase
    factor = 1.0 / math.sqrt(width)
    cosine = np.cos(angle) * factor
    sine = -np.sin(angle) * factor
    sine[0] = np.where(np.arange(width) % 2 == 0, factor, -factor)
    shape = (owners, half // owners, width)
    table = np.stack([cosine.reshape(shape), sine.reshape(shape)], axis=1)
    return table.reshape(width, width).astype(jnp.bfloat16)


def height_table(height):
    fine = 32
    coarse = height // fine
    column = np.arange(height)[None, :]
    rough = 2.0 * math.pi / height * (np.arange(coarse)[:, None] * fine * column % height)
    small = 2.0 * math.pi / height * (np.arange(fine)[:, None] * column % height)
    factor = 1.0 / math.sqrt(height)
    tables = [np.cos(rough) * factor, np.sin(rough) * factor, np.cos(small), np.sin(small)]

    def body(rc_ref, rs_ref, sc_ref, ss_ref, out_ref):
        sc, ss = sc_ref[...], ss_ref[...]
        for a in range(coarse):
            rc, rs = rc_ref[a : a + 1, :], rs_ref[a : a + 1, :]
            here = slice(a * fine, (a + 1) * fine)
            out_ref[here, :height] = (rc * sc - rs * ss).astype(jnp.bfloat16)
            out_ref[here, height:] = (rs * sc + rc * ss).astype(jnp.bfloat16)

    return pl.pallas_call(
        body,
        in_specs=[pl.BlockSpec(memory_space=pltpu.VMEM)] * 4,
        out_specs=pl.BlockSpec(memory_space=pltpu.VMEM),
        out_shape=jax.ShapeDtypeStruct((height, 2 * height), jnp.bfloat16),
        compiler_params=params(),
        cost_estimate=cost(1 << 33, 4 * height * height),
        name="height_table",
    )(*[jnp.asarray(table, jnp.float32) for table in tables])


def cost(flops, moved):
    return pl.CostEstimate(flops=flops, transcendentals=0, bytes_accessed=moved)


def params(limit=VMEM_LIMIT):
    return pltpu.CompilerParams(vmem_limit_bytes=limit)


def shade(tile, down_ref, across_ref):
    return (tile * (down_ref[...].T[:, :1] * across_ref[...])).astype(jnp.bfloat16)


def times_table(table, shaded):
    y = lax.dot_general(
        table, shaded, (((1,), (1,)), ((), ())), preferred_element_type=jnp.float32
    )
    return y.astype(jnp.bfloat16)


def sent_columns(tiles, down, across, table, half, me, peers):
    count, rows, width = tiles.shape
    span = table.shape[0] // 2
    block = span // peers

    def body(half_ref, me_ref, tile_hbm, down_ref, across_ref, table_hbm, *refs):
        outs = refs[:peers]
        tile_ref, table_ref, work, done = refs[peers:]
        t = pl.program_id(0)
        start = pl.multiple_of((1 - half_ref[0]) * span, span)
        fetch = pltpu.make_async_copy(
            table_hbm.at[pl.ds(start, span)], table_ref, done.at[count]
        )
        loads = [
            pltpu.make_async_copy(tile_hbm.at[i], tile_ref.at[i], done.at[i]) for i in range(count)
        ]

        @pl.when(t == 0)
        def _():
            loads[0].start()
            fetch.start()
            for load in loads[1:]:
                load.start()
            fetch.wait()

        for i in range(count):

            @pl.when(t == i)
            def _():
                loads[i].wait()
                work[...] = times_table(table_ref[...], shade(tile_ref[i], down_ref, across_ref))

        for k in range(peers):
            place = pl.multiple_of((me_ref[0] ^ k) * block, block)
            outs[k][0] = work[pl.ds(place, block), :]

    return pl.pallas_call(
        body,
        grid_spec=pltpu.PrefetchScalarGridSpec(
            num_scalar_prefetch=2,
            grid=(count,),
            in_specs=[
                pl.BlockSpec(memory_space=pltpu.HBM),
                pl.BlockSpec((8, rows), lambda t, half, me: (0, me[0])),
                pl.BlockSpec((1, width), lambda t, half, me: (0, 0)),
                pl.BlockSpec(memory_space=pltpu.HBM),
            ],
            out_specs=[pl.BlockSpec((1, block, rows), lambda t, half, me: (t, 0, 0))] * peers,
            scratch_shapes=[
                pltpu.VMEM((count, rows, width), tiles.dtype),
                pltpu.VMEM((span, width), table.dtype),
                pltpu.VMEM((span, rows), jnp.bfloat16),
                pltpu.SemaphoreType.DMA((count + 1,)),
            ],
        ),
        out_shape=[jax.ShapeDtypeStruct((count, block, rows), jnp.bfloat16)] * peers,
        compiler_params=params(FIRST_LIMIT),
        cost_estimate=cost(2 * count * rows * width * span, 4 * tiles.size + 2 * span * width),
        name="sent_columns",
    )(scalar(half), scalar(me), tiles, down, across, table)


def kept_columns(tiles, down, across, table, half, me, peers):
    count, rows, width = tiles.shape
    span = table.shape[0] // 2
    block = span // peers

    def body(half_ref, me_ref, tile_ref, down_ref, across_ref, table_ref, out_ref):
        y = times_table(table_ref[...], shade(tile_ref[0], down_ref, across_ref))
        out_ref[:, 0] = y.reshape(peers, block, rows)

    return pl.pallas_call(
        body,
        grid_spec=pltpu.PrefetchScalarGridSpec(
            num_scalar_prefetch=2,
            grid=(count,),
            in_specs=[
                pl.BlockSpec((1, rows, width), lambda t, half, me: (t, 0, 0)),
                pl.BlockSpec((8, rows), lambda t, half, me: (0, me[0])),
                pl.BlockSpec((1, width), lambda t, half, me: (0, 0)),
                pl.BlockSpec((span, width), lambda t, half, me: (half[0], 0)),
            ],
            out_specs=pl.BlockSpec((peers, 1, block, rows), lambda t, half, me: (0, t, 0, 0)),
        ),
        out_shape=jax.ShapeDtypeStruct((peers, count, block, rows), jnp.bfloat16),
        compiler_params=params(),
        cost_estimate=cost(2 * count * rows * width * span, 4 * tiles.size + 2 * span * width),
        name="kept_columns",
    )(scalar(half), scalar(me), tiles, down, across, table)


def gather_rows(pieces, table_ref, me):
    total = None
    for k, piece in enumerate(pieces):
        count, block, rows = piece.shape
        start = pl.multiple_of((me ^ k) * rows, rows)
        term = jnp.dot(
            piece[...].reshape(count * block, rows),
            table_ref[pl.ds(start, rows), :],
            preferred_element_type=jnp.float32,
        )
        total = term if total is None else total + term
    return total


def holds_packed(place):
    half_ref, me_ref = place
    return (half_ref[0] == 0) & (me_ref[0] == 0)


def store_spectra(s_ref, total, spectra, edge, first):
    block = spectra.shape[2]
    height = spectra.shape[3]
    row = lax.broadcasted_iota(jnp.int32, (block, height), 0)
    packed = (row == 0) & holds_packed(s_ref)
    for t in range(total.shape[0] // (2 * block)):
        real = total[2 * t * block : (2 * t + 1) * block]
        imag = total[(2 * t + 1) * block : (2 * t + 2) * block]
        cr, sr = real[:, :height], real[:, height:]
        ci, si = imag[:, :height], imag[:, height:]
        spectra[first + t, 0] = jnp.where(packed, cr, cr + si).astype(jnp.bfloat16)
        spectra[first + t, 1] = jnp.where(packed, -sr, ci - sr).astype(jnp.bfloat16)
        edge[first + t, 0] = ci[:16].astype(jnp.bfloat16)
        edge[first + t, 1] = (-si[:16]).astype(jnp.bfloat16)


def normalised(left_real, left_imag, right_real, right_imag):
    lr = left_real.astype(jnp.float32)
    li = left_imag.astype(jnp.float32)
    rr = right_real.astype(jnp.float32)
    ri = right_imag.astype(jnp.float32)
    cross_real = lr * rr + li * ri
    cross_imag = li * rr - lr * ri
    factor = 1.0 / (jnp.sqrt(cross_real * cross_real + cross_imag * cross_imag) + FLOOR)
    return (
        (cross_real * factor).astype(jnp.bfloat16),
        (cross_imag * factor).astype(jnp.bfloat16),
    )


def correlate(s_ref, me, picks, spectra, edge, table_ref, phases, outs):
    block = spectra.shape[2]
    height = spectra.shape[3]
    slots, _, rows = outs[0].shape
    lead = lax.broadcasted_iota(jnp.int32, (16, height), 0)
    packed = (lead == 0) & holds_packed(s_ref)
    for p in range(slots):
        a, c = picks[p]
        q_real, q_imag = normalised(spectra[a, 0], spectra[a, 1], spectra[c, 0], spectra[c, 1])
        e_real, e_imag = normalised(edge[a, 0], edge[a, 1], edge[c, 0], edge[c, 1])
        phases[2 * p] = q_real
        phases[2 * p + 1] = q_imag
        top_real = q_real[:16].astype(jnp.float32)
        top_imag = q_imag[:16].astype(jnp.float32)
        mixed_real = jnp.where(packed, top_real - e_imag.astype(jnp.float32), top_real)
        mixed_imag = jnp.where(packed, top_imag + e_real.astype(jnp.float32), top_imag)
        phases[2 * p, :16] = mixed_real.astype(jnp.bfloat16)
        phases[2 * p + 1, :16] = mixed_imag.astype(jnp.bfloat16)
    row = lax.broadcasted_iota(jnp.int32, (block, rows), 0)
    twice = jnp.where((row == 0) & holds_packed(s_ref), 1.0, 2.0)
    flat = phases[...].reshape(2 * slots * block, height)
    for k in range(len(outs)):
        start = pl.multiple_of((me ^ k) * rows, rows)
        c_part = jnp.dot(
            flat, table_ref[:, pl.ds(start, rows)], preferred_element_type=jnp.float32
        )
        start = pl.multiple_of(height + (me ^ k) * rows, rows)
        s_part = jnp.dot(
            flat, table_ref[:, pl.ds(start, rows)], preferred_element_type=jnp.float32
        )
        for p in range(slots):
            re = slice(2 * p * block, (2 * p + 1) * block)
            im = slice((2 * p + 1) * block, (2 * p + 2) * block)
            outs[k][p, :block] = ((c_part[re] - s_part[im]) * twice).astype(jnp.bfloat16)
            outs[k][p, block:] = ((s_part[re] + c_part[im]) * twice).astype(jnp.bfloat16)


def own_spectra(place, pieces, table):
    peers, count, double, rows = pieces.shape
    height = table.shape[0]

    def body(half_ref, me_ref, pieces_ref, table_ref, spectra, edge):
        inputs = [pieces_ref.at[k] for k in range(peers)]
        store_spectra((half_ref, me_ref), gather_rows(inputs, table_ref, 0), spectra, edge, 0)

    return pl.pallas_call(
        body,
        in_specs=[pl.BlockSpec(memory_space=pltpu.SMEM)] * 2
        + [pl.BlockSpec(memory_space=pltpu.VMEM)] * 2,
        out_specs=[pl.BlockSpec(memory_space=pltpu.VMEM)] * 2,
        out_shape=[
            jax.ShapeDtypeStruct((count, 2, double // 2, height), jnp.bfloat16),
            jax.ShapeDtypeStruct((count, 2, 16, height), jnp.bfloat16),
        ],
        compiler_params=params(),
        cost_estimate=cost(4 * count * double * height * height, 8 * height * height),
        name="own_spectra",
    )(*place, pieces, table)


def partner_slots(place, theirs, pieces, table, spectra, edge):
    peers = len(pieces)
    count, double, rows = pieces[0].shape
    height = table.shape[0]
    block = double // 2
    slots = theirs.shape[1]

    def body(half_ref, me_ref, theirs_ref, *refs):
        s_ref = (half_ref, me_ref)
        me = me_ref[0]
        picks = [
            [(theirs_ref[0, p, i] + count) % (2 * count) for i in range(2)] for p in range(slots)
        ]
        inputs, table_ref, own_ref, own_edge = refs[:peers], *refs[peers : peers + 3]
        outs = [refs[peers + 3 + k // 2].at[k % 2] for k in range(peers)]
        every, edges, phases = refs[-3:]
        every[:count] = own_ref[...]
        edges[:count] = own_edge[...]
        store_spectra(s_ref, gather_rows(inputs, table_ref, me), every, edges, count)
        correlate(s_ref, me, picks, every, edges, table_ref, phases, outs)

    return pl.pallas_call(
        body,
        in_specs=[pl.BlockSpec(memory_space=pltpu.SMEM)] * 3
        + [pl.BlockSpec(memory_space=pltpu.VMEM)] * (peers + 3),
        out_specs=[pl.BlockSpec(memory_space=pltpu.VMEM)] * (peers // 2 + 2),
        out_shape=[jax.ShapeDtypeStruct((2, slots, double, rows), jnp.bfloat16)] * (peers // 2)
        + [
            jax.ShapeDtypeStruct((2 * count, 2, block, height), jnp.bfloat16),
            jax.ShapeDtypeStruct((2 * count, 2, 16, height), jnp.bfloat16),
        ],
        scratch_shapes=[pltpu.VMEM((2 * slots, block, height), jnp.bfloat16)],
        compiler_params=params(),
        cost_estimate=cost(4 * (count + slots) * double * height * height, 8 * height * height),
        name="partner_slots",
    )(*place, theirs, *pieces, table, spectra, edge)


def own_slots(place, pairs, table, spectra, edge, peers):
    block, height = spectra.shape[2:]
    rows = height // peers
    slots = pairs.shape[1]

    def body(half_ref, me_ref, pairs_ref, table_ref, every, edges, *refs):
        picks = [[pairs_ref[0, p, i] for i in range(2)] for p in range(slots)]
        out_ref, phases = refs
        outs = [out_ref.at[k] for k in range(peers)]
        correlate((half_ref, me_ref), 0, picks, every, edges, table_ref, phases, outs)

    return pl.pallas_call(
        body,
        in_specs=[pl.BlockSpec(memory_space=pltpu.SMEM)] * 3
        + [pl.BlockSpec(memory_space=pltpu.VMEM)] * 3,
        out_specs=pl.BlockSpec(memory_space=pltpu.VMEM),
        out_shape=jax.ShapeDtypeStruct((peers, slots, 2 * block, rows), jnp.bfloat16),
        scratch_shapes=[pltpu.VMEM((2 * slots, block, height), jnp.bfloat16)],
        compiler_params=params(),
        cost_estimate=cost(8 * slots * block * height * height, 8 * height * height),
        name="own_slots",
    )(*place, pairs, table, spectra, edge)


def own_surfaces(half, own, table):
    peers, slots, double, rows = own.shape
    width = table.shape[0]
    span = peers * double

    def body(half_ref, own_ref, table_ref, out_ref):
        out_ref[0] = lax.dot_general(
            own_ref[:, 0].reshape(span, rows),
            table_ref[...],
            (((0,), (0,)), ((), ())),
            preferred_element_type=jnp.float32,
        )

    return pl.pallas_call(
        body,
        grid_spec=pltpu.PrefetchScalarGridSpec(
            num_scalar_prefetch=1,
            grid=(slots,),
            in_specs=[
                pl.BlockSpec((peers, 1, double, rows), lambda p, half: (0, p, 0, 0)),
                pl.BlockSpec((span, width), lambda p, half: (half[0], 0)),
            ],
            out_specs=pl.BlockSpec((1, rows, width), lambda p, half: (p, 0, 0)),
        ),
        out_shape=jax.ShapeDtypeStruct((slots, rows, width), jnp.float32),
        compiler_params=params(),
        cost_estimate=cost(2 * slots * rows * width * span, 4 * slots * rows * width),
        name="own_surfaces",
    )(scalar(half), own, table)


def surfaces_of(half, me, counts, part, came, swapped, table):
    peers = 2 * len(came)
    slots, double, rows = swapped[0].shape
    width = table.shape[0]
    span = peers * double

    def body(half_ref, me_ref, counts_ref, part_ref, *refs):
        other_refs = refs[:peers]
        table_ref, out_ref, work = refs[peers:]
        for k in range(peers):
            place = pl.multiple_of((me_ref[0] ^ k) * double, double)
            piece = other_refs[k][0] if k % 2 else other_refs[k][0, 0]
            work[pl.ds(place, double), :] = piece
        rest = lax.dot_general(
            work[...], table_ref[...], (((0,), (0,)), ((), ())), preferred_element_type=jnp.float32
        )
        live = pl.program_id(0) < counts_ref[0]
        out_ref[0] = jnp.where(live, part_ref[0] + rest, 0.0)

    pair = pl.BlockSpec((1, 1, double, rows), lambda p, half, me, counts: (0, p, 0, 0))
    piece = pl.BlockSpec((1, double, rows), lambda p, half, me, counts: (p, 0, 0))
    other = [swapped[k // 2] if k % 2 else came[k // 2] for k in range(peers)]
    plane = pl.BlockSpec((1, rows, width), lambda p, half, me, counts: (p, 0, 0))
    return pl.pallas_call(
        body,
        grid_spec=pltpu.PrefetchScalarGridSpec(
            num_scalar_prefetch=3,
            grid=(slots,),
            in_specs=[
                plane,
                *[pair, piece] * (peers // 2),
                pl.BlockSpec((span, width), lambda p, half, me, counts: (1 - half[0], 0)),
            ],
            out_specs=plane,
            scratch_shapes=[pltpu.VMEM((span, rows), jnp.bfloat16)],
        ),
        out_shape=jax.ShapeDtypeStruct((slots, rows, width), jnp.float32),
        compiler_params=params(),
        cost_estimate=cost(2 * slots * rows * width * span, 8 * slots * rows * width),
        name="surfaces",
    )(scalar(half), scalar(me), counts, part, *other, table)


def local(tiles, pairs, counts):
    groups = lax.axis_size("blk")
    peers = lax.axis_size("rows")
    group = lax.axis_index("blk")
    me = lax.axis_index("rows")
    count, rows, width = tiles.shape
    height = rows * peers
    turn = groups // 2
    half = group // turn
    axes = ("blk", "rows")

    def across(value, k):
        moves = [
            (b * peers + r, (b + turn) % groups * peers + (r ^ k))
            for b in range(groups)
            for r in range(peers)
        ]
        return lax.ppermute(value, axes, moves)

    def along(blocks):
        return lax.all_to_all(blocks, "rows", split_axis=0, concat_axis=0)

    def swap(value):
        return lax.ppermute(value, "rows", [(r, r ^ 1) for r in range(peers)])

    table_w = jnp.asarray(width_table(width, 2 * peers))
    down = jnp.asarray(np.tile(hann(height), (8, 1)))
    sideways = jnp.asarray(hann(width)[None, :])

    sent = sent_columns(tiles, down, sideways, table_w, half, me, peers)
    arrived = [across(sent[k], k) for k in range(peers)]
    *sent, held = lax.optimization_barrier((*sent, half))
    kept = kept_columns(tiles, down, sideways, table_w, held, me, peers)
    kept, pairs = lax.optimization_barrier((kept, pairs))
    mine = along(kept)

    table_h = height_table(height)
    theirs = across(pairs, 0)
    place = (scalar(half), scalar(me))
    spectra, edge = own_spectra(place, mine, table_h)
    *back, spectra, edge = partner_slots(place, theirs, arrived, table_h, spectra, edge)
    came = [across(back[j], 2 * j) for j in range(peers // 2)]
    own = along(own_slots(place, pairs, table_h, spectra, edge, peers))
    part = own_surfaces(half, own, table_w)
    came[-1], part = lax.optimization_barrier((came[-1], part))
    swapped = [swap(value[1]) for value in came]
    return surfaces_of(half, me, counts, part, came, swapped, table_w)


def solution(mesh):
    from jax.sharding import PartitionSpec as P

    return jax.shard_map(
        local,
        mesh=mesh,
        in_specs=(
            P(("parts", "blk"), "rows", None),
            P(("parts", "blk"), None, None),
            P(("parts", "blk")),
        ),
        out_specs=P(("parts", "blk"), "rows", None),
        check_vma=False,
    )
```

```python
import math

import jax
import jax.numpy as jnp
import numpy as np
from jax import lax
from jax.experimental import pallas as pl
from jax.experimental.pallas import tpu as pltpu

FLOOR = 0.05
VMEM_LIMIT = 24 * 1024 * 1024
FIRST_LIMIT = 60 * 1024 * 1024


def hann(length):
    return np.asarray(0.5 - 0.5 * np.cos(2.0 * math.pi / length * np.arange(length)), np.float32)


def scalar(value):
    return jnp.reshape(value, (1,)).astype(jnp.int32)


def width_table(width, owners):
    half = width // 2
    phase = np.arange(half)[:, None] * np.arange(width)[None, :] % width
    angle = 2.0 * math.pi / width * phase
    factor = 1.0 / math.sqrt(width)
    cosine = np.cos(angle) * factor
    sine = -np.sin(angle) * factor
    sine[0] = np.where(np.arange(width) % 2 == 0, factor, -factor)
    shape = (owners, half // owners, width)
    table = np.stack([cosine.reshape(shape), sine.reshape(shape)], axis=1)
    return table.reshape(width, width).astype(jnp.bfloat16)


def height_table(height):
    fine = 32
    coarse = height // fine
    column = np.arange(height)[None, :]
    rough = 2.0 * math.pi / height * (np.arange(coarse)[:, None] * fine * column % height)
    small = 2.0 * math.pi / height * (np.arange(fine)[:, None] * column % height)
    factor = 1.0 / math.sqrt(height)
    tables = [np.cos(rough) * factor, np.sin(rough) * factor, np.cos(small), np.sin(small)]

    def body(rc_ref, rs_ref, sc_ref, ss_ref, out_ref):
        sc, ss = sc_ref[...], ss_ref[...]
        for a in range(coarse):
            rc, rs = rc_ref[a : a + 1, :], rs_ref[a : a + 1, :]
            here = slice(a * fine, (a + 1) * fine)
            out_ref[here, :height] = (rc * sc - rs * ss).astype(jnp.bfloat16)
            out_ref[here, height:] = (rs * sc + rc * ss).astype(jnp.bfloat16)

    return pl.pallas_call(
        body,
        in_specs=[pl.BlockSpec(memory_space=pltpu.VMEM)] * 4,
        out_specs=pl.BlockSpec(memory_space=pltpu.VMEM),
        out_shape=jax.ShapeDtypeStruct((height, 2 * height), jnp.bfloat16),
        compiler_params=params(),
        cost_estimate=cost(1 << 33, 4 * height * height),
        name="height_table",
    )(*[jnp.asarray(table, jnp.float32) for table in tables])


def cost(flops, moved):
    return pl.CostEstimate(flops=flops, transcendentals=0, bytes_accessed=moved)


def params(limit=VMEM_LIMIT):
    return pltpu.CompilerParams(vmem_limit_bytes=limit)


def shade(tile, down_ref, across_ref):
    return (tile * (down_ref[...].T[:, :1] * across_ref[...])).astype(jnp.bfloat16)


def times_table(table, shaded):
    y = lax.dot_general(
        table, shaded, (((1,), (1,)), ((), ())), preferred_element_type=jnp.float32
    )
    return y.astype(jnp.bfloat16)


def sent_columns(tiles, down, across, table, half, me, peers):
    count, rows, width = tiles.shape
    span = table.shape[0] // 2
    block = span // peers

    def body(half_ref, me_ref, tile_hbm, down_ref, across_ref, table_hbm, *refs):
        outs = refs[:peers]
        tile_ref, table_ref, work, done = refs[peers:]
        t = pl.program_id(0)
        start = pl.multiple_of((1 - half_ref[0]) * span, span)
        fetch = pltpu.make_async_copy(
            table_hbm.at[pl.ds(start, span)], table_ref, done.at[count]
        )
        loads = [
            pltpu.make_async_copy(tile_hbm.at[i], tile_ref.at[i], done.at[i]) for i in range(count)
        ]

        @pl.when(t == 0)
        def _():
            loads[0].start()
            fetch.start()
            fetch.wait()

        for i in range(count):

            @pl.when(t == i)
            def _():
                loads[i].wait()
                if i + 1 < count:
                    loads[i + 1].start()
                work[...] = times_table(table_ref[...], shade(tile_ref[i], down_ref, across_ref))

        for k in range(peers):
            place = pl.multiple_of((me_ref[0] ^ k) * block, block)
            outs[k][0] = work[pl.ds(place, block), :]

    return pl.pallas_call(
        body,
        grid_spec=pltpu.PrefetchScalarGridSpec(
            num_scalar_prefetch=2,
            grid=(count,),
            in_specs=[
                pl.BlockSpec(memory_space=pltpu.HBM),
                pl.BlockSpec((8, rows), lambda t, half, me: (0, me[0])),
                pl.BlockSpec((1, width), lambda t, half, me: (0, 0)),
                pl.BlockSpec(memory_space=pltpu.HBM),
            ],
            out_specs=[pl.BlockSpec((1, block, rows), lambda t, half, me: (t, 0, 0))] * peers,
            scratch_shapes=[
                pltpu.VMEM((count, rows, width), tiles.dtype),
                pltpu.VMEM((span, width), table.dtype),
                pltpu.VMEM((span, rows), jnp.bfloat16),
                pltpu.SemaphoreType.DMA((count + 1,)),
            ],
        ),
        out_shape=[jax.ShapeDtypeStruct((count, block, rows), jnp.bfloat16)] * peers,
        compiler_params=params(FIRST_LIMIT),
        cost_estimate=cost(2 * count * rows * width * span, 4 * tiles.size + 2 * span * width),
        name="sent_columns",
    )(scalar(half), scalar(me), tiles, down, across, table)


def kept_columns(tiles, down, across, table, half, me, peers):
    count, rows, width = tiles.shape
    span = table.shape[0] // 2
    block = span // peers

    def body(half_ref, me_ref, tile_ref, down_ref, across_ref, table_ref, out_ref):
        y = times_table(table_ref[...], shade(tile_ref[0], down_ref, across_ref))
        out_ref[:, 0] = y.reshape(peers, block, rows)

    return pl.pallas_call(
        body,
        grid_spec=pltpu.PrefetchScalarGridSpec(
            num_scalar_prefetch=2,
            grid=(count,),
            in_specs=[
                pl.BlockSpec((1, rows, width), lambda t, half, me: (t, 0, 0)),
                pl.BlockSpec((8, rows), lambda t, half, me: (0, me[0])),
                pl.BlockSpec((1, width), lambda t, half, me: (0, 0)),
                pl.BlockSpec((span, width), lambda t, half, me: (half[0], 0)),
            ],
            out_specs=pl.BlockSpec((peers, 1, block, rows), lambda t, half, me: (0, t, 0, 0)),
        ),
        out_shape=jax.ShapeDtypeStruct((peers, count, block, rows), jnp.bfloat16),
        compiler_params=params(),
        cost_estimate=cost(2 * count * rows * width * span, 4 * tiles.size + 2 * span * width),
        name="kept_columns",
    )(scalar(half), scalar(me), tiles, down, across, table)


def gather_rows(pieces, table_ref, me):
    total = None
    for k, piece in enumerate(pieces):
        count, block, rows = piece.shape
        start = pl.multiple_of((me ^ k) * rows, rows)
        term = jnp.dot(
            piece[...].reshape(count * block, rows),
            table_ref[pl.ds(start, rows), :],
            preferred_element_type=jnp.float32,
        )
        total = term if total is None else total + term
    return total


def holds_packed(place):
    half_ref, me_ref = place
    return (half_ref[0] == 0) & (me_ref[0] == 0)


def store_spectra(s_ref, total, spectra, edge, first):
    block = spectra.shape[2]
    height = spectra.shape[3]
    row = lax.broadcasted_iota(jnp.int32, (block, height), 0)
    packed = (row == 0) & holds_packed(s_ref)
    for t in range(total.shape[0] // (2 * block)):
        real = total[2 * t * block : (2 * t + 1) * block]
        imag = total[(2 * t + 1) * block : (2 * t + 2) * block]
        cr, sr = real[:, :height], real[:, height:]
        ci, si = imag[:, :height], imag[:, height:]
        spectra[first + t, 0] = jnp.where(packed, cr, cr + si).astype(jnp.bfloat16)
        spectra[first + t, 1] = jnp.where(packed, -sr, ci - sr).astype(jnp.bfloat16)
        edge[first + t, 0] = ci[:16].astype(jnp.bfloat16)
        edge[first + t, 1] = (-si[:16]).astype(jnp.bfloat16)


def normalised(left_real, left_imag, right_real, right_imag):
    lr = left_real.astype(jnp.float32)
    li = left_imag.astype(jnp.float32)
    rr = right_real.astype(jnp.float32)
    ri = right_imag.astype(jnp.float32)
    cross_real = lr * rr + li * ri
    cross_imag = li * rr - lr * ri
    factor = 1.0 / (jnp.sqrt(cross_real * cross_real + cross_imag * cross_imag) + FLOOR)
    return (
        (cross_real * factor).astype(jnp.bfloat16),
        (cross_imag * factor).astype(jnp.bfloat16),
    )


def correlate(s_ref, me, picks, spectra, edge, table_ref, phases, outs):
    block = spectra.shape[2]
    height = spectra.shape[3]
    slots, _, rows = outs[0].shape
    lead = lax.broadcasted_iota(jnp.int32, (16, height), 0)
    packed = (lead == 0) & holds_packed(s_ref)
    for p in range(slots):
        a, c = picks[p]
        q_real, q_imag = normalised(spectra[a, 0], spectra[a, 1], spectra[c, 0], spectra[c, 1])
        e_real, e_imag = normalised(edge[a, 0], edge[a, 1], edge[c, 0], edge[c, 1])
        phases[2 * p] = q_real
        phases[2 * p + 1] = q_imag
        top_real = q_real[:16].astype(jnp.float32)
        top_imag = q_imag[:16].astype(jnp.float32)
        mixed_real = jnp.where(packed, top_real - e_imag.astype(jnp.float32), top_real)
        mixed_imag = jnp.where(packed, top_imag + e_real.astype(jnp.float32), top_imag)
        phases[2 * p, :16] = mixed_real.astype(jnp.bfloat16)
        phases[2 * p + 1, :16] = mixed_imag.astype(jnp.bfloat16)
    row = lax.broadcasted_iota(jnp.int32, (block, rows), 0)
    twice = jnp.where((row == 0) & holds_packed(s_ref), 1.0, 2.0)
    flat = phases[...].reshape(2 * slots * block, height)
    for k in range(len(outs)):
        start = pl.multiple_of((me ^ k) * rows, rows)
        c_part = jnp.dot(
            flat, table_ref[:, pl.ds(start, rows)], preferred_element_type=jnp.float32
        )
        start = pl.multiple_of(height + (me ^ k) * rows, rows)
        s_part = jnp.dot(
            flat, table_ref[:, pl.ds(start, rows)], preferred_element_type=jnp.float32
        )
        for p in range(slots):
            re = slice(2 * p * block, (2 * p + 1) * block)
            im = slice((2 * p + 1) * block, (2 * p + 2) * block)
            outs[k][p, :block] = ((c_part[re] - s_part[im]) * twice).astype(jnp.bfloat16)
            outs[k][p, block:] = ((s_part[re] + c_part[im]) * twice).astype(jnp.bfloat16)


def own_spectra(place, pieces, table):
    peers, count, double, rows = pieces.shape
    height = table.shape[0]

    def body(half_ref, me_ref, pieces_ref, table_ref, spectra, edge):
        inputs = [pieces_ref.at[k] for k in range(peers)]
        store_spectra((half_ref, me_ref), gather_rows(inputs, table_ref, 0), spectra, edge, 0)

    return pl.pallas_call(
        body,
        in_specs=[pl.BlockSpec(memory_space=pltpu.SMEM)] * 2
        + [pl.BlockSpec(memory_space=pltpu.VMEM)] * 2,
        out_specs=[pl.BlockSpec(memory_space=pltpu.VMEM)] * 2,
        out_shape=[
            jax.ShapeDtypeStruct((count, 2, double // 2, height), jnp.bfloat16),
            jax.ShapeDtypeStruct((count, 2, 16, height), jnp.bfloat16),
        ],
        compiler_params=params(),
        cost_estimate=cost(4 * count * double * height * height, 8 * height * height),
        name="own_spectra",
    )(*place, pieces, table)


def partner_slots(place, theirs, pieces, table, spectra, edge):
    peers = len(pieces)
    count, double, rows = pieces[0].shape
    height = table.shape[0]
    block = double // 2
    slots = theirs.shape[1]

    def body(half_ref, me_ref, theirs_ref, *refs):
        s_ref = (half_ref, me_ref)
        me = me_ref[0]
        picks = [
            [(theirs_ref[0, p, i] + count) % (2 * count) for i in range(2)] for p in range(slots)
        ]
        inputs, table_ref, own_ref, own_edge = refs[:peers], *refs[peers : peers + 3]
        outs = [refs[peers + 3 + k // 2].at[k % 2] for k in range(peers)]
        every, edges, phases = refs[-3:]
        every[:count] = own_ref[...]
        edges[:count] = own_edge[...]
        store_spectra(s_ref, gather_rows(inputs, table_ref, me), every, edges, count)
        correlate(s_ref, me, picks, every, edges, table_ref, phases, outs)

    return pl.pallas_call(
        body,
        in_specs=[pl.BlockSpec(memory_space=pltpu.SMEM)] * 3
        + [pl.BlockSpec(memory_space=pltpu.VMEM)] * (peers + 3),
        out_specs=[pl.BlockSpec(memory_space=pltpu.VMEM)] * (peers // 2 + 2),
        out_shape=[jax.ShapeDtypeStruct((2, slots, double, rows), jnp.bfloat16)] * (peers // 2)
        + [
            jax.ShapeDtypeStruct((2 * count, 2, block, height), jnp.bfloat16),
            jax.ShapeDtypeStruct((2 * count, 2, 16, height), jnp.bfloat16),
        ],
        scratch_shapes=[pltpu.VMEM((2 * slots, block, height), jnp.bfloat16)],
        compiler_params=params(),
        cost_estimate=cost(4 * (count + slots) * double * height * height, 8 * height * height),
        name="partner_slots",
    )(*place, theirs, *pieces, table, spectra, edge)


def own_slots(place, pairs, table, spectra, edge, peers):
    block, height = spectra.shape[2:]
    rows = height // peers
    slots = pairs.shape[1]

    def body(half_ref, me_ref, pairs_ref, table_ref, every, edges, *refs):
        picks = [[pairs_ref[0, p, i] for i in range(2)] for p in range(slots)]
        out_ref, phases = refs
        outs = [out_ref.at[k] for k in range(peers)]
        correlate((half_ref, me_ref), 0, picks, every, edges, table_ref, phases, outs)

    return pl.pallas_call(
        body,
        in_specs=[pl.BlockSpec(memory_space=pltpu.SMEM)] * 3
        + [pl.BlockSpec(memory_space=pltpu.VMEM)] * 3,
        out_specs=pl.BlockSpec(memory_space=pltpu.VMEM),
        out_shape=jax.ShapeDtypeStruct((peers, slots, 2 * block, rows), jnp.bfloat16),
        scratch_shapes=[pltpu.VMEM((2 * slots, block, height), jnp.bfloat16)],
        compiler_params=params(),
        cost_estimate=cost(8 * slots * block * height * height, 8 * height * height),
        name="own_slots",
    )(*place, pairs, table, spectra, edge)


def own_surfaces(half, own, table):
    peers, slots, double, rows = own.shape
    width = table.shape[0]
    span = peers * double

    def body(half_ref, own_ref, table_ref, out_ref):
        out_ref[0] = lax.dot_general(
            own_ref[:, 0].reshape(span, rows),
            table_ref[...],
            (((0,), (0,)), ((), ())),
            preferred_element_type=jnp.float32,
        )

    return pl.pallas_call(
        body,
        grid_spec=pltpu.PrefetchScalarGridSpec(
            num_scalar_prefetch=1,
            grid=(slots,),
            in_specs=[
                pl.BlockSpec((peers, 1, double, rows), lambda p, half: (0, p, 0, 0)),
                pl.BlockSpec((span, width), lambda p, half: (half[0], 0)),
            ],
            out_specs=pl.BlockSpec((1, rows, width), lambda p, half: (p, 0, 0)),
        ),
        out_shape=jax.ShapeDtypeStruct((slots, rows, width), jnp.float32),
        compiler_params=params(),
        cost_estimate=cost(2 * slots * rows * width * span, 4 * slots * rows * width),
        name="own_surfaces",
    )(scalar(half), own, table)


def surfaces_of(half, me, counts, part, came, swapped, table):
    peers = 2 * len(came)
    slots, double, rows = swapped[0].shape
    width = table.shape[0]
    span = peers * double

    def body(half_ref, me_ref, counts_ref, part_ref, *refs):
        other_refs = refs[:peers]
        table_ref, out_ref, work = refs[peers:]
        for k in range(peers):
            place = pl.multiple_of((me_ref[0] ^ k) * double, double)
            piece = other_refs[k][0] if k % 2 else other_refs[k][0, 0]
            work[pl.ds(place, double), :] = piece
        rest = lax.dot_general(
            work[...], table_ref[...], (((0,), (0,)), ((), ())), preferred_element_type=jnp.float32
        )
        live = pl.program_id(0) < counts_ref[0]
        out_ref[0] = jnp.where(live, part_ref[0] + rest, 0.0)

    pair = pl.BlockSpec((1, 1, double, rows), lambda p, half, me, counts: (0, p, 0, 0))
    piece = pl.BlockSpec((1, double, rows), lambda p, half, me, counts: (p, 0, 0))
    other = [swapped[k // 2] if k % 2 else came[k // 2] for k in range(peers)]
    plane = pl.BlockSpec((1, rows, width), lambda p, half, me, counts: (p, 0, 0))
    return pl.pallas_call(
        body,
        grid_spec=pltpu.PrefetchScalarGridSpec(
            num_scalar_prefetch=3,
            grid=(slots,),
            in_specs=[
                plane,
                *[pair, piece] * (peers // 2),
                pl.BlockSpec((span, width), lambda p, half, me, counts: (1 - half[0], 0)),
            ],
            out_specs=plane,
            scratch_shapes=[pltpu.VMEM((span, rows), jnp.bfloat16)],
        ),
        out_shape=jax.ShapeDtypeStruct((slots, rows, width), jnp.float32),
        compiler_params=params(),
        cost_estimate=cost(2 * slots * rows * width * span, 8 * slots * rows * width),
        name="surfaces",
    )(scalar(half), scalar(me), counts, part, *other, table)


def local(tiles, pairs, counts):
    groups = lax.axis_size("blk")
    peers = lax.axis_size("rows")
    group = lax.axis_index("blk")
    me = lax.axis_index("rows")
    count, rows, width = tiles.shape
    height = rows * peers
    turn = groups // 2
    half = group // turn
    axes = ("blk", "rows")

    def across(value, k):
        moves = [
            (b * peers + r, (b + turn) % groups * peers + (r ^ k))
            for b in range(groups)
            for r in range(peers)
        ]
        return lax.ppermute(value, axes, moves)

    def along(blocks):
        return lax.all_to_all(blocks, "rows", split_axis=0, concat_axis=0)

    def swap(value):
        return lax.ppermute(value, "rows", [(r, r ^ 1) for r in range(peers)])

    table_w = jnp.asarray(width_table(width, 2 * peers))
    down = jnp.asarray(np.tile(hann(height), (8, 1)))
    sideways = jnp.asarray(hann(width)[None, :])

    sent = sent_columns(tiles, down, sideways, table_w, half, me, peers)
    arrived = [across(sent[k], k) for k in range(2)]
    *sent, held = lax.optimization_barrier((*sent, half))
    kept = kept_columns(tiles, down, sideways, table_w, held, me, peers)
    *sent, kept, pairs = lax.optimization_barrier((*sent, kept, pairs))
    arrived += [across(sent[k], k) for k in range(2, peers)]
    mine = along(kept)

    table_h = height_table(height)
    theirs = across(pairs, 0)
    place = (scalar(half), scalar(me))
    spectra, edge = own_spectra(place, mine, table_h)
    *back, spectra, edge = partner_slots(place, theirs, arrived, table_h, spectra, edge)
    came = [across(back[j], 2 * j) for j in range(peers // 2)]
    own = along(own_slots(place, pairs, table_h, spectra, edge, peers))
    part = own_surfaces(half, own, table_w)
    came[-1], part = lax.optimization_barrier((came[-1], part))
    swapped = [swap(value[1]) for value in came]
    return surfaces_of(half, me, counts, part, came, swapped, table_w)


def solution(mesh):
    from jax.sharding import PartitionSpec as P

    return jax.shard_map(
        local,
        mesh=mesh,
        in_specs=(
            P(("parts", "blk"), "rows", None),
            P(("parts", "blk"), None, None),
            P(("parts", "blk")),
        ),
        out_specs=P(("parts", "blk"), "rows", None),
        check_vma=False,
    )
```

```python
import math

import jax
import jax.numpy as jnp
import numpy as np
from jax import lax
from jax.experimental import pallas as pl
from jax.experimental.pallas import tpu as pltpu

FLOOR = 0.05
VMEM_LIMIT = 24 * 1024 * 1024
FIRST_LIMIT = 60 * 1024 * 1024


def hann(length):
    return np.asarray(0.5 - 0.5 * np.cos(2.0 * math.pi / length * np.arange(length)), np.float32)


def scalar(value):
    return jnp.reshape(value, (1,)).astype(jnp.int32)


def width_table(width, owners):
    half = width // 2
    phase = np.arange(half)[:, None] * np.arange(width)[None, :] % width
    angle = 2.0 * math.pi / width * phase
    factor = 1.0 / math.sqrt(width)
    cosine = np.cos(angle) * factor
    sine = -np.sin(angle) * factor
    sine[0] = np.where(np.arange(width) % 2 == 0, factor, -factor)
    shape = (owners, half // owners, width)
    table = np.stack([cosine.reshape(shape), sine.reshape(shape)], axis=1)
    return table.reshape(width, width).astype(jnp.bfloat16)


def height_table(height):
    fine = 32
    coarse = height // fine
    column = np.arange(height)[None, :]
    rough = 2.0 * math.pi / height * (np.arange(coarse)[:, None] * fine * column % height)
    small = 2.0 * math.pi / height * (np.arange(fine)[:, None] * column % height)
    factor = 1.0 / math.sqrt(height)
    tables = [np.cos(rough) * factor, np.sin(rough) * factor, np.cos(small), np.sin(small)]

    def body(rc_ref, rs_ref, sc_ref, ss_ref, out_ref):
        sc, ss = sc_ref[...], ss_ref[...]
        for a in range(coarse):
            rc, rs = rc_ref[a : a + 1, :], rs_ref[a : a + 1, :]
            here = slice(a * fine, (a + 1) * fine)
            out_ref[here, :height] = (rc * sc - rs * ss).astype(jnp.bfloat16)
            out_ref[here, height:] = (rs * sc + rc * ss).astype(jnp.bfloat16)

    return pl.pallas_call(
        body,
        in_specs=[pl.BlockSpec(memory_space=pltpu.VMEM)] * 4,
        out_specs=pl.BlockSpec(memory_space=pltpu.VMEM),
        out_shape=jax.ShapeDtypeStruct((height, 2 * height), jnp.bfloat16),
        compiler_params=params(),
        cost_estimate=cost(1 << 33, 4 * height * height),
        name="height_table",
    )(*[jnp.asarray(table, jnp.float32) for table in tables])


def cost(flops, moved):
    return pl.CostEstimate(flops=flops, transcendentals=0, bytes_accessed=moved)


def params(limit=VMEM_LIMIT):
    return pltpu.CompilerParams(vmem_limit_bytes=limit)


def shade(tile, down_ref, across_ref):
    return (tile * (down_ref[...].T[:, :1] * across_ref[...])).astype(jnp.bfloat16)


def times_table(table, shaded):
    y = lax.dot_general(
        table, shaded, (((1,), (1,)), ((), ())), preferred_element_type=jnp.float32
    )
    return y.astype(jnp.bfloat16)


def near_columns(tiles, down, across, table, half, me, peers):
    count, rows, width = tiles.shape
    span = table.shape[0] // 2
    block = span // peers

    def body(half_ref, me_ref, tile_hbm, down_ref, across_ref, table_hbm, *refs):
        outs = refs[:2]
        tile_ref, table_ref, work, done = refs[2:]
        t = pl.program_id(0)
        me = me_ref[0]
        start = pl.multiple_of((1 - half_ref[0]) * span + me // 2 * 2 * block, 2 * block)
        fetch = pltpu.make_async_copy(
            table_hbm.at[pl.ds(start, 2 * block)], table_ref, done.at[count]
        )
        loads = [
            pltpu.make_async_copy(tile_hbm.at[i], tile_ref.at[i], done.at[i]) for i in range(count)
        ]

        @pl.when(t == 0)
        def _():
            fetch.start()
            for load in loads:
                load.start()
            fetch.wait()

        for i in range(count):

            @pl.when(t == i)
            def _():
                loads[i].wait()
                work[...] = times_table(table_ref[...], shade(tile_ref[i], down_ref, across_ref))

        for k in range(2):
            place = pl.multiple_of((me % 2 ^ k) * block, block)
            outs[k][0] = work[pl.ds(place, block), :]

    return pl.pallas_call(
        body,
        grid_spec=pltpu.PrefetchScalarGridSpec(
            num_scalar_prefetch=2,
            grid=(count,),
            in_specs=[
                pl.BlockSpec(memory_space=pltpu.HBM),
                pl.BlockSpec((8, rows), lambda t, half, me: (0, me[0])),
                pl.BlockSpec((1, width), lambda t, half, me: (0, 0)),
                pl.BlockSpec(memory_space=pltpu.HBM),
            ],
            out_specs=[pl.BlockSpec((1, block, rows), lambda t, half, me: (t, 0, 0))] * 2,
            scratch_shapes=[
                pltpu.VMEM((count, rows, width), tiles.dtype),
                pltpu.VMEM((2 * block, width), table.dtype),
                pltpu.VMEM((2 * block, rows), jnp.bfloat16),
                pltpu.SemaphoreType.DMA((count + 1,)),
            ],
        ),
        out_shape=[jax.ShapeDtypeStruct((count, block, rows), jnp.bfloat16)] * 2,
        compiler_params=params(FIRST_LIMIT),
        cost_estimate=cost(4 * count * rows * width * block, 4 * tiles.size + 4 * block * width),
        name="near_columns",
    )(scalar(half), scalar(me), tiles, down, across, table)


def rest_columns(tiles, down, across, table, half, me, peers):
    count, rows, width = tiles.shape
    span = table.shape[0] // 2
    block = span // peers

    def body(half_ref, me_ref, tile_ref, down_ref, across_ref, table_ref, *refs):
        out_ref, far, work = refs[0], refs[1:-1], refs[-1]
        half, me = half_ref[0], me_ref[0]
        shaded = shade(tile_ref[0], down_ref, across_ref)
        for j in range(1, peers // 2):
            start = pl.multiple_of((1 - half) * span + (me // 2 ^ j) * 2 * block, 2 * block)
            work[...] = times_table(table_ref[pl.ds(start, 2 * block), :], shaded)
            for k in range(2):
                place = pl.multiple_of((me % 2 ^ k) * block, block)
                far[2 * j - 2 + k][0] = work[pl.ds(place, block), :]
        start = pl.multiple_of(half * span, span)
        y = times_table(table_ref[pl.ds(start, span), :], shaded)
        out_ref[:, 0] = y.reshape(peers, block, rows)

    piece = pl.BlockSpec((1, block, rows), lambda t, half, me: (t, 0, 0))
    return pl.pallas_call(
        body,
        grid_spec=pltpu.PrefetchScalarGridSpec(
            num_scalar_prefetch=2,
            grid=(count,),
            in_specs=[
                pl.BlockSpec((1, rows, width), lambda t, half, me: (t, 0, 0)),
                pl.BlockSpec((8, rows), lambda t, half, me: (0, me[0])),
                pl.BlockSpec((1, width), lambda t, half, me: (0, 0)),
                pl.BlockSpec((width, width), lambda t, half, me: (0, 0)),
            ],
            out_specs=[
                pl.BlockSpec((peers, 1, block, rows), lambda t, half, me: (0, t, 0, 0)),
                *[piece] * (peers - 2),
            ],
            scratch_shapes=[pltpu.VMEM((2 * block, rows), jnp.bfloat16)],
        ),
        out_shape=[
            jax.ShapeDtypeStruct((peers, count, block, rows), jnp.bfloat16),
            *[jax.ShapeDtypeStruct((count, block, rows), jnp.bfloat16)] * (peers - 2),
        ],
        compiler_params=params(),
        cost_estimate=cost(3 * count * rows * width * span, 4 * tiles.size + 2 * width * width),
        name="rest_columns",
    )(scalar(half), scalar(me), tiles, down, across, table)


def gather_rows(pieces, table_ref, me):
    total = None
    for k, piece in enumerate(pieces):
        count, block, rows = piece.shape
        start = pl.multiple_of((me ^ k) * rows, rows)
        term = jnp.dot(
            piece[...].reshape(count * block, rows),
            table_ref[pl.ds(start, rows), :],
            preferred_element_type=jnp.float32,
        )
        total = term if total is None else total + term
    return total


def holds_packed(place):
    half_ref, me_ref = place
    return (half_ref[0] == 0) & (me_ref[0] == 0)


def store_spectra(s_ref, total, spectra, edge, first):
    block = spectra.shape[2]
    height = spectra.shape[3]
    row = lax.broadcasted_iota(jnp.int32, (block, height), 0)
    packed = (row == 0) & holds_packed(s_ref)
    for t in range(total.shape[0] // (2 * block)):
        real = total[2 * t * block : (2 * t + 1) * block]
        imag = total[(2 * t + 1) * block : (2 * t + 2) * block]
        cr, sr = real[:, :height], real[:, height:]
        ci, si = imag[:, :height], imag[:, height:]
        spectra[first + t, 0] = jnp.where(packed, cr, cr + si).astype(jnp.bfloat16)
        spectra[first + t, 1] = jnp.where(packed, -sr, ci - sr).astype(jnp.bfloat16)
        edge[first + t, 0] = ci[:16].astype(jnp.bfloat16)
        edge[first + t, 1] = (-si[:16]).astype(jnp.bfloat16)


def normalised(left_real, left_imag, right_real, right_imag):
    lr = left_real.astype(jnp.float32)
    li = left_imag.astype(jnp.float32)
    rr = right_real.astype(jnp.float32)
    ri = right_imag.astype(jnp.float32)
    cross_real = lr * rr + li * ri
    cross_imag = li * rr - lr * ri
    factor = 1.0 / (jnp.sqrt(cross_real * cross_real + cross_imag * cross_imag) + FLOOR)
    return (
        (cross_real * factor).astype(jnp.bfloat16),
        (cross_imag * factor).astype(jnp.bfloat16),
    )


def correlate(s_ref, picks, spectra, edge, phases):
    slots = len(picks)
    height = spectra.shape[3]
    lead = lax.broadcasted_iota(jnp.int32, (16, height), 0)
    packed = (lead == 0) & holds_packed(s_ref)
    for p in range(slots):
        a, c = picks[p]
        q_real, q_imag = normalised(spectra[a, 0], spectra[a, 1], spectra[c, 0], spectra[c, 1])
        e_real, e_imag = normalised(edge[a, 0], edge[a, 1], edge[c, 0], edge[c, 1])
        phases[2 * p] = q_real
        phases[2 * p + 1] = q_imag
        top_real = q_real[:16].astype(jnp.float32)
        top_imag = q_imag[:16].astype(jnp.float32)
        mixed_real = jnp.where(packed, top_real - e_imag.astype(jnp.float32), top_real)
        mixed_imag = jnp.where(packed, top_imag + e_real.astype(jnp.float32), top_imag)
        phases[2 * p, :16] = mixed_real.astype(jnp.bfloat16)
        phases[2 * p + 1, :16] = mixed_imag.astype(jnp.bfloat16)

def invert_columns(s_ref, me, phases, table_ref, outs):
    _, block, height = phases.shape
    slots = phases.shape[0] // 2
    rows = next(iter(outs.values())).shape[2]
    row = lax.broadcasted_iota(jnp.int32, (block, rows), 0)
    twice = jnp.where((row == 0) & holds_packed(s_ref), 1.0, 2.0)
    flat = phases[...].reshape(2 * slots * block, height)
    for k, out in outs.items():
        start = pl.multiple_of((me ^ k) * rows, rows)
        c_part = jnp.dot(
            flat, table_ref[:, pl.ds(start, rows)], preferred_element_type=jnp.float32
        )
        start = pl.multiple_of(height + (me ^ k) * rows, rows)
        s_part = jnp.dot(
            flat, table_ref[:, pl.ds(start, rows)], preferred_element_type=jnp.float32
        )
        for p in range(slots):
            re = slice(2 * p * block, (2 * p + 1) * block)
            im = slice((2 * p + 1) * block, (2 * p + 2) * block)
            out[p, :block] = ((c_part[re] - s_part[im]) * twice).astype(jnp.bfloat16)
            out[p, block:] = ((s_part[re] + c_part[im]) * twice).astype(jnp.bfloat16)


def own_spectra(place, pieces, table):
    peers, count, double, rows = pieces.shape
    height = table.shape[0]

    def body(half_ref, me_ref, pieces_ref, table_ref, spectra, edge):
        inputs = [pieces_ref.at[k] for k in range(peers)]
        store_spectra((half_ref, me_ref), gather_rows(inputs, table_ref, 0), spectra, edge, 0)

    return pl.pallas_call(
        body,
        in_specs=[pl.BlockSpec(memory_space=pltpu.SMEM)] * 2
        + [pl.BlockSpec(memory_space=pltpu.VMEM)] * 2,
        out_specs=[pl.BlockSpec(memory_space=pltpu.VMEM)] * 2,
        out_shape=[
            jax.ShapeDtypeStruct((count, 2, double // 2, height), jnp.bfloat16),
            jax.ShapeDtypeStruct((count, 2, 16, height), jnp.bfloat16),
        ],
        compiler_params=params(),
        cost_estimate=cost(4 * count * double * height * height, 8 * height * height),
        name="own_spectra",
    )(*place, pieces, table)


def partner_slots(place, theirs, pieces, table, spectra, edge):
    peers = len(pieces)
    count, double, rows = pieces[0].shape
    height = table.shape[0]
    block = double // 2
    slots = theirs.shape[1]

    def body(half_ref, me_ref, theirs_ref, *refs):
        s_ref = (half_ref, me_ref)
        me = me_ref[0]
        picks = [
            [(theirs_ref[0, p, i] + count) % (2 * count) for i in range(2)] for p in range(slots)
        ]
        inputs, table_ref, own_ref, own_edge = refs[:peers], *refs[peers : peers + 3]
        near, every, edges, phases = refs[peers + 3 :]
        every[:count] = own_ref[...]
        edges[:count] = own_edge[...]
        store_spectra(s_ref, gather_rows(inputs, table_ref, me), every, edges, count)
        correlate(s_ref, picks, every, edges, phases)
        invert_columns(s_ref, me, phases, table_ref, {k: near.at[k] for k in range(2)})

    return pl.pallas_call(
        body,
        in_specs=[pl.BlockSpec(memory_space=pltpu.SMEM)] * 3
        + [pl.BlockSpec(memory_space=pltpu.VMEM)] * (peers + 3),
        out_specs=[pl.BlockSpec(memory_space=pltpu.VMEM)] * 4,
        out_shape=[
            jax.ShapeDtypeStruct((2, slots, double, rows), jnp.bfloat16),
            jax.ShapeDtypeStruct((2 * count, 2, block, height), jnp.bfloat16),
            jax.ShapeDtypeStruct((2 * count, 2, 16, height), jnp.bfloat16),
            jax.ShapeDtypeStruct((2 * slots, block, height), jnp.bfloat16),
        ],
        compiler_params=params(),
        cost_estimate=cost(4 * (count + slots) * double * height * height, 8 * height * height),
        name="partner_slots",
    )(*place, theirs, *pieces, table, spectra, edge)


def own_slots(place, pairs, table, spectra, edge, phases, peers):
    block, height = spectra.shape[2:]
    rows = height // peers
    slots = pairs.shape[1]

    def body(half_ref, me_ref, pairs_ref, table_ref, every, edges, theirs, out_ref, *refs):
        s_ref = (half_ref, me_ref)
        far, work = refs[:-1], refs[-1]
        picks = [[pairs_ref[0, p, i] for i in range(2)] for p in range(slots)]
        if far:
            outs = {k: far[k - 2] for k in range(2, peers)}
            invert_columns(s_ref, me_ref[0], theirs, table_ref, outs)
        correlate(s_ref, picks, every, edges, work)
        invert_columns(s_ref, 0, work, table_ref, {k: out_ref.at[k] for k in range(peers)})

    return pl.pallas_call(
        body,
        in_specs=[pl.BlockSpec(memory_space=pltpu.SMEM)] * 3
        + [pl.BlockSpec(memory_space=pltpu.VMEM)] * 4,
        out_specs=[pl.BlockSpec(memory_space=pltpu.VMEM)] * (peers - 1),
        out_shape=[
            jax.ShapeDtypeStruct((peers, slots, 2 * block, rows), jnp.bfloat16),
            *[jax.ShapeDtypeStruct((slots, 2 * block, rows), jnp.bfloat16)] * (peers - 2),
        ],
        scratch_shapes=[pltpu.VMEM((2 * slots, block, height), jnp.bfloat16)],
        compiler_params=params(),
        cost_estimate=cost(8 * slots * block * height * height, 8 * height * height),
        name="own_slots",
    )(*place, pairs, table, spectra, edge, phases)


def own_surfaces(half, own, table):
    peers, slots, double, rows = own.shape
    width = table.shape[0]
    span = peers * double

    def body(half_ref, own_ref, table_ref, out_ref):
        out_ref[0] = lax.dot_general(
            own_ref[:, 0].reshape(span, rows),
            table_ref[...],
            (((0,), (0,)), ((), ())),
            preferred_element_type=jnp.float32,
        )

    return pl.pallas_call(
        body,
        grid_spec=pltpu.PrefetchScalarGridSpec(
            num_scalar_prefetch=1,
            grid=(slots,),
            in_specs=[
                pl.BlockSpec((peers, 1, double, rows), lambda p, half: (0, p, 0, 0)),
                pl.BlockSpec((span, width), lambda p, half: (half[0], 0)),
            ],
            out_specs=pl.BlockSpec((1, rows, width), lambda p, half: (p, 0, 0)),
        ),
        out_shape=jax.ShapeDtypeStruct((slots, rows, width), jnp.float32),
        compiler_params=params(),
        cost_estimate=cost(2 * slots * rows * width * span, 4 * slots * rows * width),
        name="own_surfaces",
    )(scalar(half), own, table)


def surfaces_of(half, me, counts, part, near, other, table):
    peers = 1 + len(other)
    slots, double, rows = other[0].shape
    width = table.shape[0]
    span = peers * double

    def body(half_ref, me_ref, counts_ref, part_ref, *refs):
        other_refs = refs[:peers]
        table_ref, out_ref, work = refs[peers:]
        for k in range(peers):
            place = pl.multiple_of((me_ref[0] ^ k) * double, double)
            piece = other_refs[k][0] if k else other_refs[k][0, 0]
            work[pl.ds(place, double), :] = piece
        rest = lax.dot_general(
            work[...], table_ref[...], (((0,), (0,)), ((), ())), preferred_element_type=jnp.float32
        )
        live = pl.program_id(0) < counts_ref[0]
        out_ref[0] = jnp.where(live, part_ref[0] + rest, 0.0)

    pair = pl.BlockSpec((1, 1, double, rows), lambda p, half, me, counts: (0, p, 0, 0))
    piece = pl.BlockSpec((1, double, rows), lambda p, half, me, counts: (p, 0, 0))
    plane = pl.BlockSpec((1, rows, width), lambda p, half, me, counts: (p, 0, 0))
    return pl.pallas_call(
        body,
        grid_spec=pltpu.PrefetchScalarGridSpec(
            num_scalar_prefetch=3,
            grid=(slots,),
            in_specs=[
                plane,
                pair,
                *[piece] * (peers - 1),
                pl.BlockSpec((span, width), lambda p, half, me, counts: (1 - half[0], 0)),
            ],
            out_specs=plane,
            scratch_shapes=[pltpu.VMEM((span, rows), jnp.bfloat16)],
        ),
        out_shape=jax.ShapeDtypeStruct((slots, rows, width), jnp.float32),
        compiler_params=params(),
        cost_estimate=cost(2 * slots * rows * width * span, 8 * slots * rows * width),
        name="surfaces",
    )(scalar(half), scalar(me), counts, part, near, *other, table)


def local(tiles, pairs, counts):
    groups = lax.axis_size("blk")
    peers = lax.axis_size("rows")
    group = lax.axis_index("blk")
    me = lax.axis_index("rows")
    count, rows, width = tiles.shape
    height = rows * peers
    turn = groups // 2
    half = group // turn
    axes = ("blk", "rows")

    def across(value, k):
        moves = [
            (b * peers + r, (b + turn) % groups * peers + (r ^ k))
            for b in range(groups)
            for r in range(peers)
        ]
        return lax.ppermute(value, axes, moves)

    def along(blocks):
        return lax.all_to_all(blocks, "rows", split_axis=0, concat_axis=0)

    def swap(value):
        return lax.ppermute(value, "rows", [(r, r ^ 1) for r in range(peers)])

    table_w = jnp.asarray(width_table(width, 2 * peers))
    down = jnp.asarray(np.tile(hann(height), (8, 1)))
    sideways = jnp.asarray(hann(width)[None, :])

    sent = near_columns(tiles, down, sideways, table_w, half, me, peers)
    arrived = [across(sent[k], k) for k in range(2)]
    *sent, held = lax.optimization_barrier((*sent, half))
    kept, *sent = rest_columns(tiles, down, sideways, table_w, held, me, peers)
    *sent, kept, pairs = lax.optimization_barrier((*sent, kept, pairs))
    arrived += [across(sent[k - 2], k) for k in range(2, peers)]
    mine = along(kept)

    table_h = height_table(height)
    theirs = across(pairs, 0)
    place = (scalar(half), scalar(me))
    spectra, edge = own_spectra(place, mine, table_h)
    near, spectra, edge, phases = partner_slots(place, theirs, arrived, table_h, spectra, edge)
    near = across(near, 0)
    own, *far = own_slots(place, pairs, table_h, spectra, edge, phases, peers)
    far = [across(far[k - 2], k) for k in range(2, peers)]
    part = own_surfaces(half, along(own), table_w)
    *far, part = lax.optimization_barrier((*far, part))
    return surfaces_of(half, me, counts, part, near, [swap(near[1]), *far], table_w)


def solution(mesh):
    from jax.sharding import PartitionSpec as P

    return jax.shard_map(
        local,
        mesh=mesh,
        in_specs=(
            P(("parts", "blk"), "rows", None),
            P(("parts", "blk"), None, None),
            P(("parts", "blk")),
        ),
        out_specs=P(("parts", "blk"), "rows", None),
        check_vma=False,
    )
```

```python
import math

import jax
import jax.numpy as jnp
import numpy as np
from jax import lax
from jax.experimental import pallas as pl
from jax.experimental.pallas import tpu as pltpu

FLOOR = 0.05
VMEM_LIMIT = 24 * 1024 * 1024
FIRST_LIMIT = 60 * 1024 * 1024


def hann(length):
    return np.asarray(0.5 - 0.5 * np.cos(2.0 * math.pi / length * np.arange(length)), np.float32)


def scalar(value):
    return jnp.reshape(value, (1,)).astype(jnp.int32)


def width_table(width, owners):
    half = width // 2
    phase = np.arange(half)[:, None] * np.arange(width)[None, :] % width
    angle = 2.0 * math.pi / width * phase
    factor = 1.0 / math.sqrt(width)
    cosine = np.cos(angle) * factor
    sine = -np.sin(angle) * factor
    sine[0] = np.where(np.arange(width) % 2 == 0, factor, -factor)
    shape = (owners, half // owners, width)
    table = np.stack([cosine.reshape(shape), sine.reshape(shape)], axis=1)
    return table.reshape(width, width).astype(jnp.bfloat16)


def height_table(height):
    fine = 32
    coarse = height // fine
    column = np.arange(height)[None, :]
    rough = 2.0 * math.pi / height * (np.arange(coarse)[:, None] * fine * column % height)
    small = 2.0 * math.pi / height * (np.arange(fine)[:, None] * column % height)
    factor = 1.0 / math.sqrt(height)
    short = [np.cos(small), np.sin(small), np.cos(rough) * factor, np.sin(rough) * factor]

    def body(short_ref, out_ref):
        sc, ss = short_ref[:fine], short_ref[fine : 2 * fine]
        for a in range(2 * fine, 2 * fine + coarse):
            rc, rs = short_ref[a : a + 1, :], short_ref[a + coarse : a + coarse + 1, :]
            here = slice((a - 2 * fine) * fine, (a - 2 * fine + 1) * fine)
            out_ref[here, :height] = (rc * sc - rs * ss).astype(jnp.bfloat16)
            out_ref[here, height:] = (rs * sc + rc * ss).astype(jnp.bfloat16)

    return pl.pallas_call(
        body,
        in_specs=[pl.BlockSpec(memory_space=pltpu.VMEM)],
        out_specs=pl.BlockSpec(memory_space=pltpu.VMEM),
        out_shape=jax.ShapeDtypeStruct((height, 2 * height), jnp.bfloat16),
        compiler_params=params(),
        cost_estimate=cost(1 << 33, 4 * height * height),
        name="height_table",
    )(jnp.asarray(np.concatenate(short), jnp.float32))


def cost(flops, moved):
    return pl.CostEstimate(flops=flops, transcendentals=0, bytes_accessed=moved)


def params(limit=VMEM_LIMIT):
    return pltpu.CompilerParams(vmem_limit_bytes=limit)


def shade(tile, down_ref, across_ref):
    return (tile * (down_ref[...].T[:, :1] * across_ref[...])).astype(jnp.bfloat16)


def times_table(table, shaded):
    y = lax.dot_general(
        table, shaded, (((1,), (1,)), ((), ())), preferred_element_type=jnp.float32
    )
    return y.astype(jnp.bfloat16)


def near_columns(tiles, down, across, table, half, me, peers):
    count, rows, width = tiles.shape
    span = table.shape[0] // 2
    block = span // peers

    def body(half_ref, me_ref, tile_hbm, down_ref, across_ref, table_hbm, *refs):
        outs = refs[:2]
        tile_ref, table_ref, work, done = refs[2:]
        t = pl.program_id(0)
        me = me_ref[0]
        start = pl.multiple_of((1 - half_ref[0]) * span + me // 2 * 2 * block, 2 * block)
        fetch = pltpu.make_async_copy(
            table_hbm.at[pl.ds(start, 2 * block)], table_ref, done.at[count]
        )
        loads = [
            pltpu.make_async_copy(tile_hbm.at[i], tile_ref.at[i], done.at[i]) for i in range(count)
        ]

        @pl.when(t == 0)
        def _():
            fetch.start()
            for load in loads:
                load.start()
            fetch.wait()

        for i in range(count):

            @pl.when(t == i)
            def _():
                loads[i].wait()
                work[...] = times_table(table_ref[...], shade(tile_ref[i], down_ref, across_ref))

        for k in range(2):
            place = pl.multiple_of((me % 2 ^ k) * block, block)
            outs[k][0] = work[pl.ds(place, block), :]

    return pl.pallas_call(
        body,
        grid_spec=pltpu.PrefetchScalarGridSpec(
            num_scalar_prefetch=2,
            grid=(count,),
            in_specs=[
                pl.BlockSpec(memory_space=pltpu.HBM),
                pl.BlockSpec((8, rows), lambda t, half, me: (0, me[0])),
                pl.BlockSpec((1, width), lambda t, half, me: (0, 0)),
                pl.BlockSpec(memory_space=pltpu.HBM),
            ],
            out_specs=[pl.BlockSpec((1, block, rows), lambda t, half, me: (t, 0, 0))] * 2,
            scratch_shapes=[
                pltpu.VMEM((count, rows, width), tiles.dtype),
                pltpu.VMEM((2 * block, width), table.dtype),
                pltpu.VMEM((2 * block, rows), jnp.bfloat16),
                pltpu.SemaphoreType.DMA((count + 1,)),
            ],
        ),
        out_shape=[jax.ShapeDtypeStruct((count, block, rows), jnp.bfloat16)] * 2,
        compiler_params=params(FIRST_LIMIT),
        cost_estimate=cost(4 * count * rows * width * block, 4 * tiles.size + 4 * block * width),
        name="near_columns",
    )(scalar(half), scalar(me), tiles, down, across, table)


def rest_columns(tiles, down, across, table, half, me, peers):
    count, rows, width = tiles.shape
    span = table.shape[0] // 2
    block = span // peers

    def body(half_ref, me_ref, tile_ref, down_ref, across_ref, table_ref, *refs):
        out_ref, far, work = refs[0], refs[1:-1], refs[-1]
        half, me = half_ref[0], me_ref[0]
        shaded = shade(tile_ref[0], down_ref, across_ref)
        for j in range(1, peers // 2):
            start = pl.multiple_of((1 - half) * span + (me // 2 ^ j) * 2 * block, 2 * block)
            work[...] = times_table(table_ref[pl.ds(start, 2 * block), :], shaded)
            for k in range(2):
                place = pl.multiple_of((me % 2 ^ k) * block, block)
                far[2 * j - 2 + k][0] = work[pl.ds(place, block), :]
        start = pl.multiple_of(half * span, span)
        y = times_table(table_ref[pl.ds(start, span), :], shaded)
        out_ref[:, 0] = y.reshape(peers, block, rows)

    piece = pl.BlockSpec((1, block, rows), lambda t, half, me: (t, 0, 0))
    return pl.pallas_call(
        body,
        grid_spec=pltpu.PrefetchScalarGridSpec(
            num_scalar_prefetch=2,
            grid=(count,),
            in_specs=[
                pl.BlockSpec((1, rows, width), lambda t, half, me: (t, 0, 0)),
                pl.BlockSpec((8, rows), lambda t, half, me: (0, me[0])),
                pl.BlockSpec((1, width), lambda t, half, me: (0, 0)),
                pl.BlockSpec((width, width), lambda t, half, me: (0, 0)),
            ],
            out_specs=[
                pl.BlockSpec((peers, 1, block, rows), lambda t, half, me: (0, t, 0, 0)),
                *[piece] * (peers - 2),
            ],
            scratch_shapes=[pltpu.VMEM((2 * block, rows), jnp.bfloat16)],
        ),
        out_shape=[
            jax.ShapeDtypeStruct((peers, count, block, rows), jnp.bfloat16),
            *[jax.ShapeDtypeStruct((count, block, rows), jnp.bfloat16)] * (peers - 2),
        ],
        compiler_params=params(),
        cost_estimate=cost(3 * count * rows * width * span, 4 * tiles.size + 2 * width * width),
        name="rest_columns",
    )(scalar(half), scalar(me), tiles, down, across, table)


def gather_rows(pieces, table_ref, me):
    total = None
    for k, piece in enumerate(pieces):
        count, block, rows = piece.shape
        start = pl.multiple_of((me ^ k) * rows, rows)
        term = jnp.dot(
            piece[...].reshape(count * block, rows),
            table_ref[pl.ds(start, rows), :],
            preferred_element_type=jnp.float32,
        )
        total = term if total is None else total + term
    return total


def holds_packed(place):
    half_ref, me_ref = place
    return (half_ref[0] == 0) & (me_ref[0] == 0)


def store_spectra(s_ref, total, spectra, edge, first):
    block = spectra.shape[2]
    height = spectra.shape[3]
    row = lax.broadcasted_iota(jnp.int32, (block, height), 0)
    packed = (row == 0) & holds_packed(s_ref)
    for t in range(total.shape[0] // (2 * block)):
        real = total[2 * t * block : (2 * t + 1) * block]
        imag = total[(2 * t + 1) * block : (2 * t + 2) * block]
        cr, sr = real[:, :height], real[:, height:]
        ci, si = imag[:, :height], imag[:, height:]
        spectra[first + t, 0] = jnp.where(packed, cr, cr + si).astype(jnp.bfloat16)
        spectra[first + t, 1] = jnp.where(packed, -sr, ci - sr).astype(jnp.bfloat16)
        edge[first + t, 0] = ci[:16].astype(jnp.bfloat16)
        edge[first + t, 1] = (-si[:16]).astype(jnp.bfloat16)


def normalised(left_real, left_imag, right_real, right_imag):
    lr = left_real.astype(jnp.float32)
    li = left_imag.astype(jnp.float32)
    rr = right_real.astype(jnp.float32)
    ri = right_imag.astype(jnp.float32)
    cross_real = lr * rr + li * ri
    cross_imag = li * rr - lr * ri
    factor = 1.0 / (jnp.sqrt(cross_real * cross_real + cross_imag * cross_imag) + FLOOR)
    return (
        (cross_real * factor).astype(jnp.bfloat16),
        (cross_imag * factor).astype(jnp.bfloat16),
    )


def correlate(s_ref, picks, spectra, edge, phases):
    slots = len(picks)
    height = spectra.shape[3]
    lead = lax.broadcasted_iota(jnp.int32, (16, height), 0)
    packed = (lead == 0) & holds_packed(s_ref)
    for p in range(slots):
        a, c = picks[p]
        q_real, q_imag = normalised(spectra[a, 0], spectra[a, 1], spectra[c, 0], spectra[c, 1])
        e_real, e_imag = normalised(edge[a, 0], edge[a, 1], edge[c, 0], edge[c, 1])
        phases[2 * p] = q_real
        phases[2 * p + 1] = q_imag
        top_real = q_real[:16].astype(jnp.float32)
        top_imag = q_imag[:16].astype(jnp.float32)
        mixed_real = jnp.where(packed, top_real - e_imag.astype(jnp.float32), top_real)
        mixed_imag = jnp.where(packed, top_imag + e_real.astype(jnp.float32), top_imag)
        phases[2 * p, :16] = mixed_real.astype(jnp.bfloat16)
        phases[2 * p + 1, :16] = mixed_imag.astype(jnp.bfloat16)

def invert_columns(s_ref, me, phases, table_ref, outs):
    _, block, height = phases.shape
    slots = phases.shape[0] // 2
    rows = next(iter(outs.values())).shape[2]
    row = lax.broadcasted_iota(jnp.int32, (block, rows), 0)
    twice = jnp.where((row == 0) & holds_packed(s_ref), 1.0, 2.0)
    flat = phases[...].reshape(2 * slots * block, height)
    for k, out in outs.items():
        start = pl.multiple_of((me ^ k) * rows, rows)
        c_part = jnp.dot(
            flat, table_ref[:, pl.ds(start, rows)], preferred_element_type=jnp.float32
        )
        start = pl.multiple_of(height + (me ^ k) * rows, rows)
        s_part = jnp.dot(
            flat, table_ref[:, pl.ds(start, rows)], preferred_element_type=jnp.float32
        )
        for p in range(slots):
            re = slice(2 * p * block, (2 * p + 1) * block)
            im = slice((2 * p + 1) * block, (2 * p + 2) * block)
            out[p, :block] = ((c_part[re] - s_part[im]) * twice).astype(jnp.bfloat16)
            out[p, block:] = ((s_part[re] + c_part[im]) * twice).astype(jnp.bfloat16)


def own_spectra(place, pieces, table):
    peers, count, double, rows = pieces.shape
    height = table.shape[0]

    def body(half_ref, me_ref, pieces_ref, table_ref, spectra, edge):
        inputs = [pieces_ref.at[k] for k in range(peers)]
        store_spectra((half_ref, me_ref), gather_rows(inputs, table_ref, 0), spectra, edge, 0)

    return pl.pallas_call(
        body,
        in_specs=[pl.BlockSpec(memory_space=pltpu.SMEM)] * 2
        + [pl.BlockSpec(memory_space=pltpu.VMEM)] * 2,
        out_specs=[pl.BlockSpec(memory_space=pltpu.VMEM)] * 2,
        out_shape=[
            jax.ShapeDtypeStruct((count, 2, double // 2, height), jnp.bfloat16),
            jax.ShapeDtypeStruct((count, 2, 16, height), jnp.bfloat16),
        ],
        compiler_params=params(),
        cost_estimate=cost(4 * count * double * height * height, 8 * height * height),
        name="own_spectra",
    )(*place, pieces, table)


def partner_slots(place, theirs, pieces, table, spectra, edge):
    peers = len(pieces)
    count, double, rows = pieces[0].shape
    height = table.shape[0]
    block = double // 2
    slots = theirs.shape[1]

    def body(half_ref, me_ref, theirs_ref, *refs):
        s_ref = (half_ref, me_ref)
        me = me_ref[0]
        picks = [
            [(theirs_ref[0, p, i] + count) % (2 * count) for i in range(2)] for p in range(slots)
        ]
        inputs, table_ref, own_ref, own_edge = refs[:peers], *refs[peers : peers + 3]
        near, every, edges, phases = refs[peers + 3 :]
        every[:count] = own_ref[...]
        edges[:count] = own_edge[...]
        store_spectra(s_ref, gather_rows(inputs, table_ref, me), every, edges, count)
        correlate(s_ref, picks, every, edges, phases)
        invert_columns(s_ref, me, phases, table_ref, {k: near.at[k] for k in range(2)})

    return pl.pallas_call(
        body,
        in_specs=[pl.BlockSpec(memory_space=pltpu.SMEM)] * 3
        + [pl.BlockSpec(memory_space=pltpu.VMEM)] * (peers + 3),
        out_specs=[pl.BlockSpec(memory_space=pltpu.VMEM)] * 4,
        out_shape=[
            jax.ShapeDtypeStruct((2, slots, double, rows), jnp.bfloat16),
            jax.ShapeDtypeStruct((2 * count, 2, block, height), jnp.bfloat16),
            jax.ShapeDtypeStruct((2 * count, 2, 16, height), jnp.bfloat16),
            jax.ShapeDtypeStruct((2 * slots, block, height), jnp.bfloat16),
        ],
        compiler_params=params(),
        cost_estimate=cost(4 * (count + slots) * double * height * height, 8 * height * height),
        name="partner_slots",
    )(*place, theirs, *pieces, table, spectra, edge)


def own_slots(place, pairs, table, spectra, edge, phases, peers):
    block, height = spectra.shape[2:]
    rows = height // peers
    slots = pairs.shape[1]

    def body(half_ref, me_ref, pairs_ref, table_ref, every, edges, theirs, out_ref, *refs):
        s_ref = (half_ref, me_ref)
        far, work = refs[:-1], refs[-1]
        picks = [[pairs_ref[0, p, i] for i in range(2)] for p in range(slots)]
        if far:
            outs = {k: far[k - 2] for k in range(2, peers)}
            invert_columns(s_ref, me_ref[0], theirs, table_ref, outs)
        correlate(s_ref, picks, every, edges, work)
        invert_columns(s_ref, 0, work, table_ref, {k: out_ref.at[k] for k in range(peers)})

    return pl.pallas_call(
        body,
        in_specs=[pl.BlockSpec(memory_space=pltpu.SMEM)] * 3
        + [pl.BlockSpec(memory_space=pltpu.VMEM)] * 4,
        out_specs=[pl.BlockSpec(memory_space=pltpu.VMEM)] * (peers - 1),
        out_shape=[
            jax.ShapeDtypeStruct((peers, slots, 2 * block, rows), jnp.bfloat16),
            *[jax.ShapeDtypeStruct((slots, 2 * block, rows), jnp.bfloat16)] * (peers - 2),
        ],
        scratch_shapes=[pltpu.VMEM((2 * slots, block, height), jnp.bfloat16)],
        compiler_params=params(),
        cost_estimate=cost(8 * slots * block * height * height, 8 * height * height),
        name="own_slots",
    )(*place, pairs, table, spectra, edge, phases)


def own_surfaces(half, own, table):
    peers, slots, double, rows = own.shape
    width = table.shape[0]
    span = peers * double

    def body(half_ref, own_ref, table_ref, out_ref):
        out_ref[0] = lax.dot_general(
            own_ref[:, 0].reshape(span, rows),
            table_ref[...],
            (((0,), (0,)), ((), ())),
            preferred_element_type=jnp.float32,
        )

    return pl.pallas_call(
        body,
        grid_spec=pltpu.PrefetchScalarGridSpec(
            num_scalar_prefetch=1,
            grid=(slots,),
            in_specs=[
                pl.BlockSpec((peers, 1, double, rows), lambda p, half: (0, p, 0, 0)),
                pl.BlockSpec((span, width), lambda p, half: (half[0], 0)),
            ],
            out_specs=pl.BlockSpec((1, rows, width), lambda p, half: (p, 0, 0)),
        ),
        out_shape=jax.ShapeDtypeStruct((slots, rows, width), jnp.float32),
        compiler_params=params(),
        cost_estimate=cost(2 * slots * rows * width * span, 4 * slots * rows * width),
        name="own_surfaces",
    )(scalar(half), own, table)


def surfaces_of(half, me, counts, part, near, other, table):
    peers = 1 + len(other)
    slots, double, rows = other[0].shape
    width = table.shape[0]
    span = peers * double

    def body(half_ref, me_ref, counts_ref, part_ref, *refs):
        other_refs = refs[:peers]
        table_ref, out_ref, work = refs[peers:]
        for k in range(peers):
            place = pl.multiple_of((me_ref[0] ^ k) * double, double)
            piece = other_refs[k][0] if k else other_refs[k][0, 0]
            work[pl.ds(place, double), :] = piece
        rest = lax.dot_general(
            work[...], table_ref[...], (((0,), (0,)), ((), ())), preferred_element_type=jnp.float32
        )
        live = pl.program_id(0) < counts_ref[0]
        out_ref[0] = jnp.where(live, part_ref[0] + rest, 0.0)

    pair = pl.BlockSpec((1, 1, double, rows), lambda p, half, me, counts: (0, p, 0, 0))
    piece = pl.BlockSpec((1, double, rows), lambda p, half, me, counts: (p, 0, 0))
    plane = pl.BlockSpec((1, rows, width), lambda p, half, me, counts: (p, 0, 0))
    return pl.pallas_call(
        body,
        grid_spec=pltpu.PrefetchScalarGridSpec(
            num_scalar_prefetch=3,
            grid=(slots,),
            in_specs=[
                plane,
                pair,
                *[piece] * (peers - 1),
                pl.BlockSpec((span, width), lambda p, half, me, counts: (1 - half[0], 0)),
            ],
            out_specs=plane,
            scratch_shapes=[pltpu.VMEM((span, rows), jnp.bfloat16)],
        ),
        out_shape=jax.ShapeDtypeStruct((slots, rows, width), jnp.float32),
        compiler_params=params(),
        cost_estimate=cost(2 * slots * rows * width * span, 8 * slots * rows * width),
        name="surfaces",
    )(scalar(half), scalar(me), counts, part, near, *other, table)


def local(tiles, pairs, counts):
    groups = lax.axis_size("blk")
    peers = lax.axis_size("rows")
    group = lax.axis_index("blk")
    me = lax.axis_index("rows")
    count, rows, width = tiles.shape
    height = rows * peers
    turn = groups // 2
    half = group // turn
    axes = ("blk", "rows")

    def across(value, k):
        moves = [
            (b * peers + r, (b + turn) % groups * peers + (r ^ k))
            for b in range(groups)
            for r in range(peers)
        ]
        return lax.ppermute(value, axes, moves)

    def along(blocks):
        return lax.all_to_all(blocks, "rows", split_axis=0, concat_axis=0)

    def swap(value):
        return lax.ppermute(value, "rows", [(r, r ^ 1) for r in range(peers)])

    table_w = jnp.asarray(width_table(width, 2 * peers))
    down = jnp.asarray(np.tile(hann(height), (8, 1)))
    sideways = jnp.asarray(hann(width)[None, :])

    sent = near_columns(tiles, down, sideways, table_w, half, me, peers)
    arrived = [across(sent[k], k) for k in range(2)]
    *sent, held = lax.optimization_barrier((*sent, half))
    kept, *sent = rest_columns(tiles, down, sideways, table_w, held, me, peers)
    *sent, kept, pairs = lax.optimization_barrier((*sent, kept, pairs))
    arrived += [across(sent[k - 2], k) for k in range(2, peers)]
    mine = along(kept)

    table_h = height_table(height)
    theirs = across(pairs, 0)
    place = (scalar(half), scalar(me))
    spectra, edge = own_spectra(place, mine, table_h)
    near, spectra, edge, phases = partner_slots(place, theirs, arrived, table_h, spectra, edge)
    near = across(near, 0)
    own, *far = own_slots(place, pairs, table_h, spectra, edge, phases, peers)
    far = [across(far[k - 2], k) for k in range(2, peers)]
    part = own_surfaces(half, along(own), table_w)
    *far, part = lax.optimization_barrier((*far, part))
    return surfaces_of(half, me, counts, part, near, [swap(near[1]), *far], table_w)


def solution(mesh):
    from jax.sharding import PartitionSpec as P

    return jax.shard_map(
        local,
        mesh=mesh,
        in_specs=(
            P(("parts", "blk"), "rows", None),
            P(("parts", "blk"), None, None),
            P(("parts", "blk")),
        ),
        out_specs=P(("parts", "blk"), "rows", None),
        check_vma=False,
    )
```

```python
import math

import jax
import jax.numpy as jnp
import numpy as np
from jax import lax
from jax.experimental import pallas as pl
from jax.experimental.pallas import tpu as pltpu

FLOOR = 0.05
VMEM_LIMIT = 24 * 1024 * 1024
FIRST_LIMIT = 60 * 1024 * 1024


def hann(length):
    return np.asarray(0.5 - 0.5 * np.cos(2.0 * math.pi / length * np.arange(length)), np.float32)


def scalar(value):
    return jnp.reshape(value, (1,)).astype(jnp.int32)


def width_table(width, owners):
    half = width // 2
    phase = np.arange(half)[:, None] * np.arange(width)[None, :] % width
    angle = 2.0 * math.pi / width * phase
    factor = 1.0 / math.sqrt(width)
    cosine = np.cos(angle) * factor
    sine = -np.sin(angle) * factor
    sine[0] = np.where(np.arange(width) % 2 == 0, factor, -factor)
    shape = (owners, half // owners, width)
    table = np.stack([cosine.reshape(shape), sine.reshape(shape)], axis=1)
    return table.reshape(width, width).astype(jnp.bfloat16)


def height_table(height, after):
    fine = 32
    coarse = height // fine
    column = np.arange(height)[None, :]
    rough = 2.0 * math.pi / height * (np.arange(coarse)[:, None] * fine * column % height)
    small = 2.0 * math.pi / height * (np.arange(fine)[:, None] * column % height)
    factor = 1.0 / math.sqrt(height)
    short = [np.cos(small), np.sin(small), np.cos(rough) * factor, np.sin(rough) * factor]

    def body(short_ref, *refs):
        out_ref = refs[-1]
        sc, ss = short_ref[:fine], short_ref[fine : 2 * fine]
        for a in range(2 * fine, 2 * fine + coarse):
            rc, rs = short_ref[a : a + 1, :], short_ref[a + coarse : a + coarse + 1, :]
            here = slice((a - 2 * fine) * fine, (a - 2 * fine + 1) * fine)
            out_ref[here, :height] = (rc * sc - rs * ss).astype(jnp.bfloat16)
            out_ref[here, height:] = (rs * sc + rc * ss).astype(jnp.bfloat16)

    return pl.pallas_call(
        body,
        in_specs=[pl.BlockSpec(memory_space=pltpu.VMEM)]
        + [pl.BlockSpec(memory_space=pl.ANY)] * len(after),
        out_specs=pl.BlockSpec(memory_space=pltpu.VMEM),
        out_shape=jax.ShapeDtypeStruct((height, 2 * height), jnp.bfloat16),
        compiler_params=params(),
        cost_estimate=cost(1 << 33, 4 * height * height),
        name="height_table",
    )(jnp.asarray(np.concatenate(short), jnp.float32), *after)


def cost(flops, moved):
    return pl.CostEstimate(flops=flops, transcendentals=0, bytes_accessed=moved)


def params(limit=VMEM_LIMIT):
    return pltpu.CompilerParams(vmem_limit_bytes=limit)


def shade(tile, down_ref, across_ref):
    return (tile * (down_ref[...].T[:, :1] * across_ref[...])).astype(jnp.bfloat16)


def times_table(table, shaded):
    y = lax.dot_general(
        table, shaded, (((1,), (1,)), ((), ())), preferred_element_type=jnp.float32
    )
    return y.astype(jnp.bfloat16)


def near_columns(tiles, down, across, table, half, me, peers):
    count, rows, width = tiles.shape
    span = table.shape[0] // 2
    block = span // peers

    def body(half_ref, me_ref, tile_hbm, down_ref, across_ref, table_hbm, *refs):
        outs = refs[:2]
        tile_ref, table_ref, work, done = refs[2:]
        t = pl.program_id(0)
        me = me_ref[0]
        start = pl.multiple_of((1 - half_ref[0]) * span + me // 2 * 2 * block, 2 * block)
        fetch = pltpu.make_async_copy(
            table_hbm.at[pl.ds(start, 2 * block)], table_ref, done.at[count]
        )
        loads = [
            pltpu.make_async_copy(tile_hbm.at[i], tile_ref.at[i], done.at[i]) for i in range(count)
        ]

        @pl.when(t == 0)
        def _():
            fetch.start()
            for load in loads:
                load.start()
            fetch.wait()

        for i in range(count):

            @pl.when(t == i)
            def _():
                loads[i].wait()
                work[...] = times_table(table_ref[...], shade(tile_ref[i], down_ref, across_ref))

        for k in range(2):
            place = pl.multiple_of((me % 2 ^ k) * block, block)
            outs[k][0] = work[pl.ds(place, block), :]

    return pl.pallas_call(
        body,
        grid_spec=pltpu.PrefetchScalarGridSpec(
            num_scalar_prefetch=2,
            grid=(count,),
            in_specs=[
                pl.BlockSpec(memory_space=pltpu.HBM),
                pl.BlockSpec((8, rows), lambda t, half, me: (0, me[0])),
                pl.BlockSpec((1, width), lambda t, half, me: (0, 0)),
                pl.BlockSpec(memory_space=pltpu.HBM),
            ],
            out_specs=[pl.BlockSpec((1, block, rows), lambda t, half, me: (t, 0, 0))] * 2,
            scratch_shapes=[
                pltpu.VMEM((count, rows, width), tiles.dtype),
                pltpu.VMEM((2 * block, width), table.dtype),
                pltpu.VMEM((2 * block, rows), jnp.bfloat16),
                pltpu.SemaphoreType.DMA((count + 1,)),
            ],
        ),
        out_shape=[jax.ShapeDtypeStruct((count, block, rows), jnp.bfloat16)] * 2,
        compiler_params=params(FIRST_LIMIT),
        cost_estimate=cost(4 * count * rows * width * block, 4 * tiles.size + 4 * block * width),
        name="near_columns",
    )(scalar(half), scalar(me), tiles, down, across, table)


def rest_columns(tiles, down, across, table, half, me, first, peers):
    count, rows, width = tiles.shape
    span = table.shape[0] // 2
    block = span // peers
    distant = peers - 2

    def body(half_ref, me_ref, first_ref, tile_ref, down_ref, across_ref, table_ref, *refs):
        out_ref, far, work = refs[0], refs[1:-1], refs[-1]
        half, me = half_ref[0], me_ref[0]
        t = pl.program_id(0)
        shaded = shade(tile_ref[0], down_ref, across_ref)
        for j in range(1, peers // 2):
            start = pl.multiple_of((1 - half) * span + (me // 2 ^ j) * 2 * block, 2 * block)
            work[...] = times_table(table_ref[pl.ds(start, 2 * block), :], shaded)
            for k in range(2):
                place = pl.multiple_of((me % 2 ^ k) * block, block)
                for i in range(count):

                    @pl.when(t == i)
                    def _():
                        far[i * distant + 2 * j - 2 + k][...] = work[pl.ds(place, block), :]

        start = pl.multiple_of(half * span, span)
        y = times_table(table_ref[pl.ds(start, span), :], shaded)
        out_ref[:, 0] = y.reshape(peers, block, rows)

    return pl.pallas_call(
        body,
        grid_spec=pltpu.PrefetchScalarGridSpec(
            num_scalar_prefetch=3,
            grid=(count,),
            in_specs=[
                pl.BlockSpec((1, rows, width), lambda t, half, me, a: ((a[0] + t) % count, 0, 0)),
                pl.BlockSpec((8, rows), lambda t, half, me, a: (0, me[0])),
                pl.BlockSpec((1, width), lambda t, half, me, a: (0, 0)),
                pl.BlockSpec((width, width), lambda t, half, me, a: (0, 0)),
            ],
            out_specs=[
                pl.BlockSpec(
                    (peers, 1, block, rows), lambda t, half, me, a: (0, (a[0] + t) % count, 0, 0)
                ),
                *[pl.BlockSpec((block, rows), lambda t, half, me, a: (0, 0))] * (count * distant),
            ],
            scratch_shapes=[pltpu.VMEM((2 * block, rows), jnp.bfloat16)],
        ),
        out_shape=[
            jax.ShapeDtypeStruct((peers, count, block, rows), jnp.bfloat16),
            *[jax.ShapeDtypeStruct((block, rows), jnp.bfloat16)] * (count * distant),
        ],
        compiler_params=params(),
        cost_estimate=cost(3 * count * rows * width * span, 4 * tiles.size + 2 * width * width),
        name="rest_columns",
    )(scalar(half), scalar(me), scalar(first), tiles, down, across, table)


def gather_rows(pieces, table_ref, me):
    total = None
    for k, piece in enumerate(pieces):
        rows = piece.shape[1]
        start = pl.multiple_of((me ^ k) * rows, rows)
        term = jnp.dot(
            piece, table_ref[pl.ds(start, rows), :], preferred_element_type=jnp.float32
        )
        total = term if total is None else total + term
    return total


def holds_packed(place):
    half_ref, me_ref = place
    return (half_ref[0] == 0) & (me_ref[0] == 0)


def store_spectra(s_ref, total, spectra, edge, first):
    block = spectra.shape[2]
    height = spectra.shape[3]
    row = lax.broadcasted_iota(jnp.int32, (block, height), 0)
    packed = (row == 0) & holds_packed(s_ref)
    for t in range(total.shape[0] // (2 * block)):
        real = total[2 * t * block : (2 * t + 1) * block]
        imag = total[(2 * t + 1) * block : (2 * t + 2) * block]
        cr, sr = real[:, :height], real[:, height:]
        ci, si = imag[:, :height], imag[:, height:]
        spectra[first + t, 0] = jnp.where(packed, cr, cr + si).astype(jnp.bfloat16)
        spectra[first + t, 1] = jnp.where(packed, -sr, ci - sr).astype(jnp.bfloat16)
        edge[first + t, 0] = ci[:16].astype(jnp.bfloat16)
        edge[first + t, 1] = (-si[:16]).astype(jnp.bfloat16)


def normalised(left_real, left_imag, right_real, right_imag):
    lr = left_real.astype(jnp.float32)
    li = left_imag.astype(jnp.float32)
    rr = right_real.astype(jnp.float32)
    ri = right_imag.astype(jnp.float32)
    cross_real = lr * rr + li * ri
    cross_imag = li * rr - lr * ri
    factor = 1.0 / (jnp.sqrt(cross_real * cross_real + cross_imag * cross_imag) + FLOOR)
    return (
        (cross_real * factor).astype(jnp.bfloat16),
        (cross_imag * factor).astype(jnp.bfloat16),
    )


def correlate(s_ref, picks, phases):
    height = phases.shape[2]
    lead = lax.broadcasted_iota(jnp.int32, (16, height), 0)
    packed = (lead == 0) & holds_packed(s_ref)
    for p, ((left, left_edge, a), (right, right_edge, c)) in enumerate(picks):
        q_real, q_imag = normalised(left[a, 0], left[a, 1], right[c, 0], right[c, 1])
        e_real, e_imag = normalised(
            left_edge[a, 0], left_edge[a, 1], right_edge[c, 0], right_edge[c, 1]
        )
        phases[2 * p] = q_real
        phases[2 * p + 1] = q_imag
        top_real = q_real[:16].astype(jnp.float32)
        top_imag = q_imag[:16].astype(jnp.float32)
        mixed_real = jnp.where(packed, top_real - e_imag.astype(jnp.float32), top_real)
        mixed_imag = jnp.where(packed, top_imag + e_real.astype(jnp.float32), top_imag)
        phases[2 * p, :16] = mixed_real.astype(jnp.bfloat16)
        phases[2 * p + 1, :16] = mixed_imag.astype(jnp.bfloat16)

def invert_columns(s_ref, me, phases, table_ref, outs):
    _, block, height = phases.shape
    slots = phases.shape[0] // 2
    rows = next(iter(outs.values())).shape[2]
    row = lax.broadcasted_iota(jnp.int32, (block, rows), 0)
    twice = jnp.where((row == 0) & holds_packed(s_ref), 1.0, 2.0)
    flat = phases[...].reshape(2 * slots * block, height)
    for k, out in outs.items():
        start = pl.multiple_of((me ^ k) * rows, rows)
        c_part = jnp.dot(
            flat, table_ref[:, pl.ds(start, rows)], preferred_element_type=jnp.float32
        )
        start = pl.multiple_of(height + (me ^ k) * rows, rows)
        s_part = jnp.dot(
            flat, table_ref[:, pl.ds(start, rows)], preferred_element_type=jnp.float32
        )
        for p in range(slots):
            re = slice(2 * p * block, (2 * p + 1) * block)
            im = slice((2 * p + 1) * block, (2 * p + 2) * block)
            out[p, :block] = ((c_part[re] - s_part[im]) * twice).astype(jnp.bfloat16)
            out[p, block:] = ((s_part[re] + c_part[im]) * twice).astype(jnp.bfloat16)


def own_spectra(place, pieces, table):
    peers, count, double, rows = pieces.shape
    height = table.shape[0]

    def body(half_ref, me_ref, pieces_ref, table_ref, spectra, edge):
        inputs = [pieces_ref[k].reshape(count * double, rows) for k in range(peers)]
        store_spectra((half_ref, me_ref), gather_rows(inputs, table_ref, 0), spectra, edge, 0)

    return pl.pallas_call(
        body,
        in_specs=[pl.BlockSpec(memory_space=pltpu.SMEM)] * 2
        + [pl.BlockSpec(memory_space=pltpu.VMEM)] * 2,
        out_specs=[pl.BlockSpec(memory_space=pltpu.VMEM)] * 2,
        out_shape=[
            jax.ShapeDtypeStruct((count, 2, double // 2, height), jnp.bfloat16),
            jax.ShapeDtypeStruct((count, 2, 16, height), jnp.bfloat16),
        ],
        compiler_params=params(),
        cost_estimate=cost(4 * count * double * height * height, 8 * height * height),
        name="own_spectra",
    )(*place, pieces, table)


def first_slot(place, theirs, near, far, table, spectra, edge):
    peers = len(near) + len(far)
    count, double, rows = near[0].shape
    height = table.shape[0]
    block = double // 2

    def body(half_ref, me_ref, theirs_ref, *refs):
        s_ref = (half_ref, me_ref)
        me = me_ref[0]
        left = theirs_ref[0, 0, 0]
        pieces = [ref[left] for ref in refs[:2]] + [ref[...] for ref in refs[2:peers]]
        table_ref, own, own_edge, out, lead, lead_edge, phases = refs[peers:]
        store_spectra(s_ref, gather_rows(pieces, table_ref, me), lead, lead_edge, 0)
        right = theirs_ref[0, 0, 1] - count
        correlate(s_ref, [((lead, lead_edge, 0), (own, own_edge, right))], phases)
        invert_columns(s_ref, me, phases, table_ref, {k: out.at[k] for k in range(2)})

    return pl.pallas_call(
        body,
        in_specs=[pl.BlockSpec(memory_space=pltpu.SMEM)] * 3
        + [pl.BlockSpec(memory_space=pltpu.VMEM)] * (peers + 3),
        out_specs=[pl.BlockSpec(memory_space=pltpu.VMEM)] * 4,
        out_shape=[
            jax.ShapeDtypeStruct((2, 1, double, rows), jnp.bfloat16),
            jax.ShapeDtypeStruct((1, 2, block, height), jnp.bfloat16),
            jax.ShapeDtypeStruct((1, 2, 16, height), jnp.bfloat16),
            jax.ShapeDtypeStruct((2, block, height), jnp.bfloat16),
        ],
        compiler_params=params(),
        cost_estimate=cost(8 * double * height * height, 8 * height * height),
        name="first_slot",
    )(*place, theirs, *near, *far, table, spectra, edge)


def other_slots(place, theirs, near, far, table, spectra, edge, lead, lead_edge, phases):
    peers = 2 + len(far[0])
    count, double, rows = near[0].shape
    height = table.shape[0]
    block = double // 2
    slots = theirs.shape[1]
    rest = count - 1

    def body(half_ref, me_ref, theirs_ref, *refs):
        s_ref = (half_ref, me_ref)
        me = me_ref[0]
        first = theirs_ref[0, 0, 0]
        near_refs = refs[:2]
        far_refs = refs[2 : 2 + rest * (peers - 2)]
        tail = refs[2 + rest * (peers - 2) :]
        table_ref, own, own_edge, lead_ref, lead_edge_ref, done_ref = tail[:6]
        out, every, edges, phases_ref = tail[6:]
        every[:count] = own[...]
        edges[:count] = own_edge[...]
        every[count : count + 1] = lead_ref[...]
        edges[count : count + 1] = lead_edge_ref[...]
        for i in range(1, count):
            pieces = [ref[(first + i) % count] for ref in near_refs]
            pieces += [ref[...] for ref in far_refs[(i - 1) * (peers - 2) : i * (peers - 2)]]
            store_spectra(s_ref, gather_rows(pieces, table_ref, me), every, edges, count + i)
        picks = []
        for p in range(1, slots):
            a, c = theirs_ref[0, p, 0], theirs_ref[0, p, 1]
            left = count + (a + count - first) % count
            right = jnp.where(c < count, count + (c + count - first) % count, c - count)
            picks.append(((every, edges, left), (every, edges, right)))
        phases_ref[:2] = done_ref[...]
        fresh = phases_ref.at[pl.ds(2, 2 * slots - 2)]
        correlate(s_ref, picks, fresh)
        invert_columns(s_ref, me, fresh, table_ref, {k: out.at[k] for k in range(2)})

    flat = [piece for pieces in far for piece in pieces]
    return pl.pallas_call(
        body,
        in_specs=[pl.BlockSpec(memory_space=pltpu.SMEM)] * 3
        + [pl.BlockSpec(memory_space=pltpu.VMEM)] * (8 + len(flat)),
        out_specs=[pl.BlockSpec(memory_space=pltpu.VMEM)] * 4,
        out_shape=[
            jax.ShapeDtypeStruct((2, slots - 1, double, rows), jnp.bfloat16),
            jax.ShapeDtypeStruct((2 * count, 2, block, height), jnp.bfloat16),
            jax.ShapeDtypeStruct((2 * count, 2, 16, height), jnp.bfloat16),
            jax.ShapeDtypeStruct((2 * slots, block, height), jnp.bfloat16),
        ],
        compiler_params=params(),
        cost_estimate=cost(8 * double * height * height, 8 * height * height),
        name="other_slots",
    )(*place, theirs, *near, *flat, table, spectra, edge, lead, lead_edge, phases)


def own_slots(place, pairs, theirs, table, spectra, edge, phases, peers):
    block, height = spectra.shape[2:]
    count = spectra.shape[0] // 2
    rows = height // peers
    slots = pairs.shape[1]

    def body(half_ref, me_ref, pairs_ref, theirs_ref, table_ref, every, edges, done, out_ref, *refs):
        s_ref = (half_ref, me_ref)
        far, work = refs[:-1], refs[-1]
        first = theirs_ref[0, 0, 0]
        picks = []
        for p in range(slots):
            a, c = pairs_ref[0, p, 0], pairs_ref[0, p, 1]
            right = jnp.where(c < count, c, count + (c - first) % count)
            picks.append(((every, edges, a), (every, edges, right)))
        if far:
            outs = {k: far[k - 2] for k in range(2, peers)}
            invert_columns(s_ref, me_ref[0], done, table_ref, outs)
        correlate(s_ref, picks, work)
        invert_columns(s_ref, 0, work, table_ref, {k: out_ref.at[k] for k in range(peers)})

    return pl.pallas_call(
        body,
        in_specs=[pl.BlockSpec(memory_space=pltpu.SMEM)] * 4
        + [pl.BlockSpec(memory_space=pltpu.VMEM)] * 4,
        out_specs=[pl.BlockSpec(memory_space=pltpu.VMEM)] * (peers - 1),
        out_shape=[
            jax.ShapeDtypeStruct((peers, slots, 2 * block, rows), jnp.bfloat16),
            *[jax.ShapeDtypeStruct((slots, 2 * block, rows), jnp.bfloat16)] * (peers - 2),
        ],
        scratch_shapes=[pltpu.VMEM((2 * slots, block, height), jnp.bfloat16)],
        compiler_params=params(),
        cost_estimate=cost(8 * slots * block * height * height, 8 * height * height),
        name="own_slots",
    )(*place, pairs, theirs, table, spectra, edge, phases)


def own_surfaces(half, own, table):
    peers, slots, double, rows = own.shape
    width = table.shape[0]
    span = peers * double

    def body(half_ref, own_ref, table_ref, out_ref):
        out_ref[0] = lax.dot_general(
            own_ref[:, 0].reshape(span, rows),
            table_ref[...],
            (((0,), (0,)), ((), ())),
            preferred_element_type=jnp.float32,
        )

    return pl.pallas_call(
        body,
        grid_spec=pltpu.PrefetchScalarGridSpec(
            num_scalar_prefetch=1,
            grid=(slots,),
            in_specs=[
                pl.BlockSpec((peers, 1, double, rows), lambda p, half: (0, p, 0, 0)),
                pl.BlockSpec((span, width), lambda p, half: (half[0], 0)),
            ],
            out_specs=pl.BlockSpec((1, rows, width), lambda p, half: (p, 0, 0)),
        ),
        out_shape=jax.ShapeDtypeStruct((slots, rows, width), jnp.float32),
        compiler_params=params(),
        cost_estimate=cost(2 * slots * rows * width * span, 4 * slots * rows * width),
        name="own_surfaces",
    )(scalar(half), own, table)


def surfaces_of(half, me, counts, part, lead, rest, far, table):
    peers = 2 + len(far)
    slots, rows, width = part.shape
    double = lead[1].shape[1]
    span = peers * double

    def body(half_ref, me_ref, counts_ref, part_ref, *refs):
        leads, rests, fars = refs[:2], refs[2:4], refs[4:-3]
        table_ref, out_ref, work = refs[-3:]
        slot = pl.program_id(0)

        def put(k, piece):
            place = pl.multiple_of((me_ref[0] ^ k) * double, double)
            work[pl.ds(place, double), :] = piece

        @pl.when(slot == 0)
        def _():
            put(0, leads[0][0, 0])
            put(1, leads[1][0])

        @pl.when(slot > 0)
        def _():
            put(0, rests[0][0, 0])
            put(1, rests[1][0])

        for k, ref in enumerate(fars):
            put(k + 2, ref[0])
        total = lax.dot_general(
            work[...], table_ref[...], (((0,), (0,)), ((), ())), preferred_element_type=jnp.float32
        )
        live = slot < counts_ref[0]
        out_ref[0] = jnp.where(live, part_ref[0] + total, 0.0)

    plane = pl.BlockSpec((1, rows, width), lambda p, half, me, counts: (p, 0, 0))
    piece = pl.BlockSpec((1, double, rows), lambda p, half, me, counts: (p, 0, 0))

    def late(p):
        return jnp.maximum(p - 1, 0)

    return pl.pallas_call(
        body,
        grid_spec=pltpu.PrefetchScalarGridSpec(
            num_scalar_prefetch=3,
            grid=(slots,),
            in_specs=[
                plane,
                pl.BlockSpec((1, 1, double, rows), lambda p, half, me, counts: (0, 0, 0, 0)),
                pl.BlockSpec((1, double, rows), lambda p, half, me, counts: (0, 0, 0)),
                pl.BlockSpec((1, 1, double, rows), lambda p, half, me, counts: (0, late(p), 0, 0)),
                pl.BlockSpec((1, double, rows), lambda p, half, me, counts: (late(p), 0, 0)),
                *[piece] * (peers - 2),
                pl.BlockSpec((span, width), lambda p, half, me, counts: (1 - half[0], 0)),
            ],
            out_specs=plane,
            scratch_shapes=[pltpu.VMEM((span, rows), jnp.bfloat16)],
        ),
        out_shape=jax.ShapeDtypeStruct((slots, rows, width), jnp.float32),
        compiler_params=params(),
        cost_estimate=cost(2 * slots * rows * width * span, 8 * slots * rows * width),
        name="surfaces",
    )(scalar(half), scalar(me), counts, part, *lead, *rest, *far, table)


def local(tiles, pairs, counts):
    groups = lax.axis_size("blk")
    peers = lax.axis_size("rows")
    group = lax.axis_index("blk")
    me = lax.axis_index("rows")
    count, rows, width = tiles.shape
    height = rows * peers
    turn = groups // 2
    half = group // turn
    axes = ("blk", "rows")

    def across(value, k):
        moves = [
            (b * peers + r, (b + turn) % groups * peers + (r ^ k))
            for b in range(groups)
            for r in range(peers)
        ]
        return lax.ppermute(value, axes, moves)

    def along(blocks):
        return lax.all_to_all(blocks, "rows", split_axis=0, concat_axis=0)

    def swap(value):
        return lax.ppermute(value, "rows", [(r, r ^ 1) for r in range(peers)])

    table_w = jnp.asarray(width_table(width, 2 * peers))
    down = jnp.asarray(np.tile(hann(height), (8, 1)))
    sideways = jnp.asarray(hann(width)[None, :])

    sent = near_columns(tiles, down, sideways, table_w, half, me, peers)
    near = [across(sent[k], k) for k in range(2)]
    *sent, held = lax.optimization_barrier((*sent, half))
    kept, *sent = rest_columns(
        tiles, down, sideways, table_w, held, me, pairs[0, 0, 0], peers
    )
    *sent, kept, told = lax.optimization_barrier((*sent, kept, pairs))
    distant = peers - 2
    far = [[across(sent[k - 2], k) for k in range(2, peers)]]
    theirs = across(told, 0)
    for i in range(1, count):
        far.append([across(sent[i * distant + k - 2], k) for k in range(2, peers)])
    mine = along(kept)

    table_h = height_table(height, near)
    place = (scalar(half), scalar(me))
    spectra, edge = own_spectra(place, mine, table_h)
    lead, lead_spectra, lead_edge, phases = first_slot(
        place, theirs, near, far[0], table_h, spectra, edge
    )
    lead = across(lead, 0)
    rest, spectra, edge, phases = other_slots(
        place, theirs, near, far[1:], table_h, spectra, edge, lead_spectra, lead_edge, phases
    )
    rest = across(rest, 0)
    lead, spectra, edge = lax.optimization_barrier((lead, spectra, edge))
    own, *back = own_slots(place, pairs, theirs, table_h, spectra, edge, phases, peers)
    back = [across(back[k - 2], k) for k in range(2, peers)]
    part = own_surfaces(half, along(own), table_w)
    *back, part = lax.optimization_barrier((*back, part))
    return surfaces_of(
        half, me, counts, part, (lead, swap(lead[1])), (rest, swap(rest[1])), back, table_w
    )


def solution(mesh):
    from jax.sharding import PartitionSpec as P

    return jax.shard_map(
        local,
        mesh=mesh,
        in_specs=(
            P(("parts", "blk"), "rows", None),
            P(("parts", "blk"), None, None),
            P(("parts", "blk")),
        ),
        out_specs=P(("parts", "blk"), "rows", None),
        check_vma=False,
    )
```

```python
import math

import jax
import jax.numpy as jnp
import numpy as np
from jax import lax
from jax.experimental import pallas as pl
from jax.experimental.pallas import tpu as pltpu

FLOOR = 0.05
VMEM_LIMIT = 24 * 1024 * 1024
FIRST_LIMIT = 60 * 1024 * 1024


def hann(length):
    return np.asarray(0.5 - 0.5 * np.cos(2.0 * math.pi / length * np.arange(length)), np.float32)


def scalar(value):
    return jnp.reshape(value, (1,)).astype(jnp.int32)


def width_table(width, owners):
    half = width // 2
    phase = np.arange(half)[:, None] * np.arange(width)[None, :] % width
    angle = 2.0 * math.pi / width * phase
    factor = 1.0 / math.sqrt(width)
    cosine = np.cos(angle) * factor
    sine = -np.sin(angle) * factor
    sine[0] = np.where(np.arange(width) % 2 == 0, factor, -factor)
    shape = (owners, half // owners, width)
    table = np.stack([cosine.reshape(shape), sine.reshape(shape)], axis=1)
    return table.reshape(width, width).astype(jnp.bfloat16)


def height_table(height, after):
    fine = 32
    coarse = height // fine
    column = np.arange(height)[None, :]
    rough = 2.0 * math.pi / height * (np.arange(coarse)[:, None] * fine * column % height)
    small = 2.0 * math.pi / height * (np.arange(fine)[:, None] * column % height)
    factor = 1.0 / math.sqrt(height)
    short = [np.cos(small), np.sin(small), np.cos(rough) * factor, np.sin(rough) * factor]

    def body(short_ref, *refs):
        out_ref = refs[-1]
        sc, ss = short_ref[:fine], short_ref[fine : 2 * fine]
        for a in range(2 * fine, 2 * fine + coarse):
            rc, rs = short_ref[a : a + 1, :], short_ref[a + coarse : a + coarse + 1, :]
            here = slice((a - 2 * fine) * fine, (a - 2 * fine + 1) * fine)
            out_ref[here, :height] = (rc * sc - rs * ss).astype(jnp.bfloat16)
            out_ref[here, height:] = (rs * sc + rc * ss).astype(jnp.bfloat16)

    return pl.pallas_call(
        body,
        in_specs=[pl.BlockSpec(memory_space=pltpu.VMEM)]
        + [pl.BlockSpec(memory_space=pl.ANY)] * len(after),
        out_specs=pl.BlockSpec(memory_space=pltpu.VMEM),
        out_shape=jax.ShapeDtypeStruct((height, 2 * height), jnp.bfloat16),
        compiler_params=params(),
        cost_estimate=cost(1 << 33, 4 * height * height),
        name="height_table",
    )(jnp.asarray(np.concatenate(short), jnp.float32), *after)


def cost(flops, moved):
    return pl.CostEstimate(flops=flops, transcendentals=0, bytes_accessed=moved)


def params(limit=VMEM_LIMIT):
    return pltpu.CompilerParams(vmem_limit_bytes=limit)


def shade(tile, down_ref, across_ref):
    return (tile * (down_ref[...].T[:, :1] * across_ref[...])).astype(jnp.bfloat16)


def times_table(table, shaded):
    y = lax.dot_general(
        table, shaded, (((1,), (1,)), ((), ())), preferred_element_type=jnp.float32
    )
    return y.astype(jnp.bfloat16)


def near_columns(tiles, down, across, table, half, me, peers):
    count, rows, width = tiles.shape
    span = table.shape[0] // 2
    block = span // peers

    def body(half_ref, me_ref, tile_hbm, down_ref, across_ref, table_hbm, *refs):
        outs = refs[:2]
        tile_ref, table_ref, work, done = refs[2:]
        t = pl.program_id(0)
        me = me_ref[0]
        start = pl.multiple_of((1 - half_ref[0]) * span + me // 2 * 2 * block, 2 * block)
        fetch = pltpu.make_async_copy(
            table_hbm.at[pl.ds(start, 2 * block)], table_ref, done.at[count]
        )
        loads = [
            pltpu.make_async_copy(tile_hbm.at[i], tile_ref.at[i], done.at[i]) for i in range(count)
        ]

        @pl.when(t == 0)
        def _():
            fetch.start()
            for load in loads:
                load.start()
            fetch.wait()

        for i in range(count):

            @pl.when(t == i)
            def _():
                loads[i].wait()
                work[...] = times_table(table_ref[...], shade(tile_ref[i], down_ref, across_ref))

        for k in range(2):
            place = pl.multiple_of((me % 2 ^ k) * block, block)
            outs[k][0] = work[pl.ds(place, block), :]

    return pl.pallas_call(
        body,
        grid_spec=pltpu.PrefetchScalarGridSpec(
            num_scalar_prefetch=2,
            grid=(count,),
            in_specs=[
                pl.BlockSpec(memory_space=pltpu.HBM),
                pl.BlockSpec((8, rows), lambda t, half, me: (0, me[0])),
                pl.BlockSpec((1, width), lambda t, half, me: (0, 0)),
                pl.BlockSpec(memory_space=pltpu.HBM),
            ],
            out_specs=[pl.BlockSpec((1, block, rows), lambda t, half, me: (t, 0, 0))] * 2,
            scratch_shapes=[
                pltpu.VMEM((count, rows, width), tiles.dtype),
                pltpu.VMEM((2 * block, width), table.dtype),
                pltpu.VMEM((2 * block, rows), jnp.bfloat16),
                pltpu.SemaphoreType.DMA((count + 1,)),
            ],
        ),
        out_shape=[jax.ShapeDtypeStruct((count, block, rows), jnp.bfloat16)] * 2,
        compiler_params=params(FIRST_LIMIT),
        cost_estimate=cost(4 * count * rows * width * block, 4 * tiles.size + 4 * block * width),
        name="near_columns",
    )(scalar(half), scalar(me), tiles, down, across, table)


def rest_columns(tiles, down, across, table, half, me, pairs, peers):
    count, rows, width = tiles.shape
    span = table.shape[0] // 2
    block = span // peers
    distant = peers - 2

    def body(half_ref, me_ref, pairs_ref, tile_ref, down_ref, across_ref, table_ref, *refs):
        out_ref, far, (work, stage, done) = refs[0], refs[1:-3], refs[-3:]
        copies = [
            pltpu.make_async_copy(stage.at[i], far[i], done.at[i]) for i in range(count * distant)
        ]
        half, me = half_ref[0], me_ref[0]
        t = pl.program_id(0)
        shaded = shade(tile_ref[0], down_ref, across_ref)
        for j in range(1, peers // 2):
            start = pl.multiple_of((1 - half) * span + (me // 2 ^ j) * 2 * block, 2 * block)
            work[...] = times_table(table_ref[pl.ds(start, 2 * block), :], shaded)
            for k in range(2):
                place = pl.multiple_of((me % 2 ^ k) * block, block)
                for i in range(count):

                    @pl.when(t == i)
                    def _():
                        to = i * distant + 2 * j - 2 + k
                        stage[to] = work[pl.ds(place, block), :]
                        copies[to].start()

        start = pl.multiple_of(half * span, span)
        y = times_table(table_ref[pl.ds(start, span), :], shaded)
        out_ref[:, 0] = y.reshape(peers, block, rows)

        @pl.when(t == count - 1)
        def _():
            for copy in copies:
                copy.wait()

    return pl.pallas_call(
        body,
        grid_spec=pltpu.PrefetchScalarGridSpec(
            num_scalar_prefetch=3,
            grid=(count,),
            in_specs=[
                pl.BlockSpec((1, rows, width), lambda t, half, me, a: ((a[0, 0, 0] + t) % count, 0, 0)),
                pl.BlockSpec((8, rows), lambda t, half, me, a: (0, me[0])),
                pl.BlockSpec((1, width), lambda t, half, me, a: (0, 0)),
                pl.BlockSpec((width, width), lambda t, half, me, a: (0, 0)),
            ],
            out_specs=[
                pl.BlockSpec(
                    (peers, 1, block, rows), lambda t, half, me, a: (0, (a[0, 0, 0] + t) % count, 0, 0)
                ),
                *[pl.BlockSpec(memory_space=pltpu.HBM)] * (count * distant),
            ],
            scratch_shapes=[
                pltpu.VMEM((2 * block, rows), jnp.bfloat16),
                pltpu.VMEM((count * distant, block, rows), jnp.bfloat16),
                pltpu.SemaphoreType.DMA((count * distant,)),
            ],
        ),
        out_shape=[
            jax.ShapeDtypeStruct((peers, count, block, rows), jnp.bfloat16),
            *[jax.ShapeDtypeStruct((block, rows), jnp.bfloat16)] * (count * distant),
        ],
        compiler_params=params(),
        cost_estimate=cost(3 * count * rows * width * span, 4 * tiles.size + 2 * width * width),
        name="rest_columns",
    )(scalar(half), scalar(me), pairs, tiles, down, across, table)


def gather_rows(pieces, table_ref, me):
    total = None
    for k, piece in enumerate(pieces):
        rows = piece.shape[1]
        start = pl.multiple_of((me ^ k) * rows, rows)
        term = jnp.dot(
            piece, table_ref[pl.ds(start, rows), :], preferred_element_type=jnp.float32
        )
        total = term if total is None else total + term
    return total


def holds_packed(place):
    half_ref, me_ref = place
    return (half_ref[0] == 0) & (me_ref[0] == 0)


def store_spectra(s_ref, total, spectra, edge, first):
    block = spectra.shape[2]
    height = spectra.shape[3]
    row = lax.broadcasted_iota(jnp.int32, (block, height), 0)
    packed = (row == 0) & holds_packed(s_ref)
    for t in range(total.shape[0] // (2 * block)):
        real = total[2 * t * block : (2 * t + 1) * block]
        imag = total[(2 * t + 1) * block : (2 * t + 2) * block]
        cr, sr = real[:, :height], real[:, height:]
        ci, si = imag[:, :height], imag[:, height:]
        spectra[first + t, 0] = jnp.where(packed, cr, cr + si).astype(jnp.bfloat16)
        spectra[first + t, 1] = jnp.where(packed, -sr, ci - sr).astype(jnp.bfloat16)
        edge[first + t, 0] = ci[:16].astype(jnp.bfloat16)
        edge[first + t, 1] = (-si[:16]).astype(jnp.bfloat16)


def normalised(left_real, left_imag, right_real, right_imag):
    lr = left_real.astype(jnp.float32)
    li = left_imag.astype(jnp.float32)
    rr = right_real.astype(jnp.float32)
    ri = right_imag.astype(jnp.float32)
    cross_real = lr * rr + li * ri
    cross_imag = li * rr - lr * ri
    factor = 1.0 / (jnp.sqrt(cross_real * cross_real + cross_imag * cross_imag) + FLOOR)
    return (
        (cross_real * factor).astype(jnp.bfloat16),
        (cross_imag * factor).astype(jnp.bfloat16),
    )


def correlate(s_ref, picks, phases):
    height = phases.shape[2]
    lead = lax.broadcasted_iota(jnp.int32, (16, height), 0)
    packed = (lead == 0) & holds_packed(s_ref)
    for p, ((left, left_edge, a), (right, right_edge, c)) in enumerate(picks):
        q_real, q_imag = normalised(left[a, 0], left[a, 1], right[c, 0], right[c, 1])
        e_real, e_imag = normalised(
            left_edge[a, 0], left_edge[a, 1], right_edge[c, 0], right_edge[c, 1]
        )
        phases[2 * p] = q_real
        phases[2 * p + 1] = q_imag
        top_real = q_real[:16].astype(jnp.float32)
        top_imag = q_imag[:16].astype(jnp.float32)
        mixed_real = jnp.where(packed, top_real - e_imag.astype(jnp.float32), top_real)
        mixed_imag = jnp.where(packed, top_imag + e_real.astype(jnp.float32), top_imag)
        phases[2 * p, :16] = mixed_real.astype(jnp.bfloat16)
        phases[2 * p + 1, :16] = mixed_imag.astype(jnp.bfloat16)

def invert_columns(s_ref, me, phases, table_ref, outs):
    _, block, height = phases.shape
    slots = phases.shape[0] // 2
    rows = next(iter(outs.values())).shape[2]
    row = lax.broadcasted_iota(jnp.int32, (block, rows), 0)
    twice = jnp.where((row == 0) & holds_packed(s_ref), 1.0, 2.0)
    flat = phases[...].reshape(2 * slots * block, height)
    for k, out in outs.items():
        start = pl.multiple_of((me ^ k) * rows, rows)
        c_part = jnp.dot(
            flat, table_ref[:, pl.ds(start, rows)], preferred_element_type=jnp.float32
        )
        start = pl.multiple_of(height + (me ^ k) * rows, rows)
        s_part = jnp.dot(
            flat, table_ref[:, pl.ds(start, rows)], preferred_element_type=jnp.float32
        )
        for p in range(slots):
            re = slice(2 * p * block, (2 * p + 1) * block)
            im = slice((2 * p + 1) * block, (2 * p + 2) * block)
            out[p, :block] = ((c_part[re] - s_part[im]) * twice).astype(jnp.bfloat16)
            out[p, block:] = ((s_part[re] + c_part[im]) * twice).astype(jnp.bfloat16)


def own_spectra(place, pieces, table):
    peers, count, double, rows = pieces.shape
    height = table.shape[0]

    def body(half_ref, me_ref, pieces_ref, table_ref, spectra, edge):
        inputs = [pieces_ref[k].reshape(count * double, rows) for k in range(peers)]
        store_spectra((half_ref, me_ref), gather_rows(inputs, table_ref, 0), spectra, edge, 0)

    return pl.pallas_call(
        body,
        in_specs=[pl.BlockSpec(memory_space=pltpu.SMEM)] * 2
        + [pl.BlockSpec(memory_space=pltpu.VMEM)] * 2,
        out_specs=[pl.BlockSpec(memory_space=pltpu.VMEM)] * 2,
        out_shape=[
            jax.ShapeDtypeStruct((count, 2, double // 2, height), jnp.bfloat16),
            jax.ShapeDtypeStruct((count, 2, 16, height), jnp.bfloat16),
        ],
        compiler_params=params(),
        cost_estimate=cost(4 * count * double * height * height, 8 * height * height),
        name="own_spectra",
    )(*place, pieces, table)


def first_slot(place, theirs, near, far, table, spectra, edge):
    peers = len(near) + len(far)
    count, double, rows = near[0].shape
    height = table.shape[0]
    block = double // 2

    def body(half_ref, me_ref, theirs_ref, *refs):
        s_ref = (half_ref, me_ref)
        me = me_ref[0]
        left = theirs_ref[0, 0, 0]
        pieces = [ref[left] for ref in refs[:2]] + [ref[...] for ref in refs[2:peers]]
        table_ref, own, own_edge, out, lead, lead_edge, phases = refs[peers:]
        store_spectra(s_ref, gather_rows(pieces, table_ref, me), lead, lead_edge, 0)
        right = theirs_ref[0, 0, 1] - count
        correlate(s_ref, [((lead, lead_edge, 0), (own, own_edge, right))], phases)
        invert_columns(s_ref, me, phases, table_ref, {k: out.at[k] for k in range(2)})

    return pl.pallas_call(
        body,
        in_specs=[pl.BlockSpec(memory_space=pltpu.SMEM)] * 3
        + [pl.BlockSpec(memory_space=pltpu.VMEM)] * (peers + 3),
        out_specs=[pl.BlockSpec(memory_space=pltpu.VMEM)] * 4,
        out_shape=[
            jax.ShapeDtypeStruct((2, 1, double, rows), jnp.bfloat16),
            jax.ShapeDtypeStruct((1, 2, block, height), jnp.bfloat16),
            jax.ShapeDtypeStruct((1, 2, 16, height), jnp.bfloat16),
            jax.ShapeDtypeStruct((2, block, height), jnp.bfloat16),
        ],
        compiler_params=params(),
        cost_estimate=cost(8 * double * height * height, 8 * height * height),
        name="first_slot",
    )(*place, theirs, *near, *far, table, spectra, edge)


def other_slots(place, theirs, near, far, table, spectra, edge, lead, lead_edge, phases):
    peers = 2 + len(far[0])
    count, double, rows = near[0].shape
    height = table.shape[0]
    block = double // 2
    slots = theirs.shape[1]
    rest = count - 1

    def body(half_ref, me_ref, theirs_ref, *refs):
        s_ref = (half_ref, me_ref)
        me = me_ref[0]
        first = theirs_ref[0, 0, 0]
        near_refs = refs[:2]
        far_refs = refs[2 : 2 + rest * (peers - 2)]
        tail = refs[2 + rest * (peers - 2) :]
        table_ref, own, own_edge, lead_ref, lead_edge_ref, done_ref = tail[:6]
        out, every, edges = tail[6:9]
        distant, phases_ref = tail[9:-1], tail[-1]
        every[:count] = own[...]
        edges[:count] = own_edge[...]
        every[count : count + 1] = lead_ref[...]
        edges[count : count + 1] = lead_edge_ref[...]
        for i in range(1, count):
            pieces = [ref[(first + i) % count] for ref in near_refs]
            pieces += [ref[...] for ref in far_refs[(i - 1) * (peers - 2) : i * (peers - 2)]]
            store_spectra(s_ref, gather_rows(pieces, table_ref, me), every, edges, count + i)
        picks = []
        for p in range(1, slots):
            a, c = theirs_ref[0, p, 0], theirs_ref[0, p, 1]
            left = count + (a + count - first) % count
            right = jnp.where(c < count, count + (c + count - first) % count, c - count)
            picks.append(((every, edges, left), (every, edges, right)))
        phases_ref[:2] = done_ref[...]
        fresh = phases_ref.at[pl.ds(2, 2 * slots - 2)]
        correlate(s_ref, picks, fresh)
        invert_columns(s_ref, me, fresh, table_ref, {k: out.at[k] for k in range(2)})
        if distant:
            outs = {k: distant[k - 2] for k in range(2, peers)}
            invert_columns(s_ref, me, phases_ref, table_ref, outs)

    flat = [piece for pieces in far for piece in pieces]
    return pl.pallas_call(
        body,
        in_specs=[pl.BlockSpec(memory_space=pltpu.SMEM)] * 3
        + [pl.BlockSpec(memory_space=pltpu.VMEM)] * (8 + len(flat)),
        out_specs=[pl.BlockSpec(memory_space=pltpu.VMEM)] * (1 + peers),
        out_shape=[
            jax.ShapeDtypeStruct((2, slots - 1, double, rows), jnp.bfloat16),
            jax.ShapeDtypeStruct((2 * count, 2, block, height), jnp.bfloat16),
            jax.ShapeDtypeStruct((2 * count, 2, 16, height), jnp.bfloat16),
            *[jax.ShapeDtypeStruct((slots, double, rows), jnp.bfloat16)] * (peers - 2),
        ],
        scratch_shapes=[pltpu.VMEM((2 * slots, block, height), jnp.bfloat16)],
        compiler_params=params(),
        cost_estimate=cost(8 * double * height * height, 8 * height * height),
        name="other_slots",
    )(*place, theirs, *near, *flat, table, spectra, edge, lead, lead_edge, phases)


def own_slots(place, pairs, theirs, table, spectra, edge, peers):
    block, height = spectra.shape[2:]
    count = spectra.shape[0] // 2
    rows = height // peers
    slots = pairs.shape[1]

    def body(half_ref, me_ref, pairs_ref, theirs_ref, table_ref, every, edges, out_ref, work):
        s_ref = (half_ref, me_ref)
        first = theirs_ref[0, 0, 0]
        picks = []
        for p in range(slots):
            a, c = pairs_ref[0, p, 0], pairs_ref[0, p, 1]
            right = jnp.where(c < count, c, count + (c - first) % count)
            picks.append(((every, edges, a), (every, edges, right)))
        correlate(s_ref, picks, work)
        invert_columns(s_ref, 0, work, table_ref, {k: out_ref.at[k] for k in range(peers)})

    return pl.pallas_call(
        body,
        in_specs=[pl.BlockSpec(memory_space=pltpu.SMEM)] * 4
        + [pl.BlockSpec(memory_space=pltpu.VMEM)] * 3,
        out_specs=pl.BlockSpec(memory_space=pltpu.VMEM),
        out_shape=jax.ShapeDtypeStruct((peers, slots, 2 * block, rows), jnp.bfloat16),
        scratch_shapes=[pltpu.VMEM((2 * slots, block, height), jnp.bfloat16)],
        compiler_params=params(),
        cost_estimate=cost(8 * slots * block * height * height, 8 * height * height),
        name="own_slots",
    )(*place, pairs, theirs, table, spectra, edge)


def own_surfaces(half, own, table):
    peers, slots, double, rows = own.shape
    width = table.shape[0]
    span = peers * double

    def body(half_ref, own_ref, table_ref, out_ref):
        out_ref[0] = lax.dot_general(
            own_ref[:, 0].reshape(span, rows),
            table_ref[...],
            (((0,), (0,)), ((), ())),
            preferred_element_type=jnp.float32,
        )

    return pl.pallas_call(
        body,
        grid_spec=pltpu.PrefetchScalarGridSpec(
            num_scalar_prefetch=1,
            grid=(slots,),
            in_specs=[
                pl.BlockSpec((peers, 1, double, rows), lambda p, half: (0, p, 0, 0)),
                pl.BlockSpec((span, width), lambda p, half: (half[0], 0)),
            ],
            out_specs=pl.BlockSpec((1, rows, width), lambda p, half: (p, 0, 0)),
        ),
        out_shape=jax.ShapeDtypeStruct((slots, rows, width), jnp.float32),
        compiler_params=params(),
        cost_estimate=cost(2 * slots * rows * width * span, 4 * slots * rows * width),
        name="own_surfaces",
    )(scalar(half), own, table)


def surfaces_of(half, me, counts, part, lead, rest, far, table):
    peers = 2 + len(far)
    slots, rows, width = part.shape
    double = lead[1].shape[1]
    span = peers * double

    def body(half_ref, me_ref, counts_ref, part_ref, *refs):
        leads, rests, fars = refs[:2], refs[2:4], refs[4:-3]
        table_ref, out_ref, work = refs[-3:]
        slot = pl.program_id(0)

        def put(k, piece):
            place = pl.multiple_of((me_ref[0] ^ k) * double, double)
            work[pl.ds(place, double), :] = piece

        @pl.when(slot == 0)
        def _():
            put(0, leads[0][0, 0])
            put(1, leads[1][0])

        @pl.when(slot > 0)
        def _():
            put(0, rests[0][0, 0])
            put(1, rests[1][0])

        for k, ref in enumerate(fars):
            put(k + 2, ref[0])
        total = lax.dot_general(
            work[...], table_ref[...], (((0,), (0,)), ((), ())), preferred_element_type=jnp.float32
        )
        live = slot < counts_ref[0]
        out_ref[0] = jnp.where(live, part_ref[0] + total, 0.0)

    plane = pl.BlockSpec((1, rows, width), lambda p, half, me, counts: (p, 0, 0))
    piece = pl.BlockSpec((1, double, rows), lambda p, half, me, counts: (p, 0, 0))

    def late(p):
        return jnp.maximum(p - 1, 0)

    return pl.pallas_call(
        body,
        grid_spec=pltpu.PrefetchScalarGridSpec(
            num_scalar_prefetch=3,
            grid=(slots,),
            in_specs=[
                plane,
                pl.BlockSpec((1, 1, double, rows), lambda p, half, me, counts: (0, 0, 0, 0)),
                pl.BlockSpec((1, double, rows), lambda p, half, me, counts: (0, 0, 0)),
                pl.BlockSpec((1, 1, double, rows), lambda p, half, me, counts: (0, late(p), 0, 0)),
                pl.BlockSpec((1, double, rows), lambda p, half, me, counts: (late(p), 0, 0)),
                *[piece] * (peers - 2),
                pl.BlockSpec((span, width), lambda p, half, me, counts: (1 - half[0], 0)),
            ],
            out_specs=plane,
            scratch_shapes=[pltpu.VMEM((span, rows), jnp.bfloat16)],
        ),
        out_shape=jax.ShapeDtypeStruct((slots, rows, width), jnp.float32),
        compiler_params=params(),
        cost_estimate=cost(2 * slots * rows * width * span, 8 * slots * rows * width),
        name="surfaces",
    )(scalar(half), scalar(me), counts, part, *lead, *rest, *far, table)


def local(tiles, pairs, counts):
    groups = lax.axis_size("blk")
    peers = lax.axis_size("rows")
    group = lax.axis_index("blk")
    me = lax.axis_index("rows")
    count, rows, width = tiles.shape
    height = rows * peers
    turn = groups // 2
    half = group // turn
    axes = ("blk", "rows")

    def across(value, k):
        moves = [
            (b * peers + r, (b + turn) % groups * peers + (r ^ k))
            for b in range(groups)
            for r in range(peers)
        ]
        return lax.ppermute(value, axes, moves)

    def along(blocks):
        return lax.all_to_all(blocks, "rows", split_axis=0, concat_axis=0)

    def swap(value):
        return lax.ppermute(value, "rows", [(r, r ^ 1) for r in range(peers)])

    table_w = jnp.asarray(width_table(width, 2 * peers))
    down = jnp.asarray(np.tile(hann(height), (8, 1)))
    sideways = jnp.asarray(hann(width)[None, :])

    sent = near_columns(tiles, down, sideways, table_w, half, me, peers)
    near = [across(sent[k], k) for k in range(2)]
    *sent, held = lax.optimization_barrier((*sent, half))
    kept, *sent = rest_columns(
        tiles, down, sideways, table_w, held, me, pairs, peers
    )
    *sent, kept, told = lax.optimization_barrier((*sent, kept, pairs))
    distant = peers - 2
    far = [[across(sent[k - 2], k) for k in range(2, peers)]]
    theirs = across(told, 0)
    for i in range(1, count):
        far.append([across(sent[i * distant + k - 2], k) for k in range(2, peers)])
    mine = along(kept)

    table_h = height_table(height, near)
    place = (scalar(half), scalar(me))
    spectra, edge = own_spectra(place, mine, table_h)
    lead, lead_spectra, lead_edge, phases = first_slot(
        place, theirs, near, far[0], table_h, spectra, edge
    )
    lead = across(lead, 0)
    rest, spectra, edge, *back = other_slots(
        place, theirs, near, far[1:], table_h, spectra, edge, lead_spectra, lead_edge, phases
    )
    rest = across(rest, 0)
    back = [across(back[k - 2], k) for k in range(2, peers)]
    lead, spectra, edge = lax.optimization_barrier((lead, spectra, edge))
    own = own_slots(place, pairs, theirs, table_h, spectra, edge, peers)
    part = own_surfaces(half, along(own), table_w)
    *back, part = lax.optimization_barrier((*back, part))
    return surfaces_of(
        half, me, counts, part, (lead, swap(lead[1])), (rest, swap(rest[1])), back, table_w
    )


def solution(mesh):
    from jax.sharding import PartitionSpec as P

    return jax.shard_map(
        local,
        mesh=mesh,
        in_specs=(
            P(("parts", "blk"), "rows", None),
            P(("parts", "blk"), None, None),
            P(("parts", "blk")),
        ),
        out_specs=P(("parts", "blk"), "rows", None),
        check_vma=False,
    )
```

```python
import math

import jax
import jax.numpy as jnp
import numpy as np
from jax import lax
from jax.experimental import pallas as pl
from jax.experimental.pallas import tpu as pltpu

FLOOR = 0.05
VMEM_LIMIT = 24 * 1024 * 1024
FIRST_LIMIT = 60 * 1024 * 1024


def hann(length):
    return np.asarray(0.5 - 0.5 * np.cos(2.0 * math.pi / length * np.arange(length)), np.float32)


def scalar(value):
    return jnp.reshape(value, (1,)).astype(jnp.int32)


def width_table(width, owners):
    half = width // 2
    phase = np.arange(half)[:, None] * np.arange(width)[None, :] % width
    angle = 2.0 * math.pi / width * phase
    factor = 1.0 / math.sqrt(width)
    cosine = np.cos(angle) * factor
    sine = -np.sin(angle) * factor
    sine[0] = np.where(np.arange(width) % 2 == 0, factor, -factor)
    shape = (owners, half // owners, width)
    table = np.stack([cosine.reshape(shape), sine.reshape(shape)], axis=1)
    return table.reshape(width, width).astype(jnp.bfloat16)


FINE = 32


def short_tables(height):
    column = np.arange(height)[None, :]
    rough = 2.0 * math.pi / height * (np.arange(height // FINE)[:, None] * FINE * column % height)
    small = 2.0 * math.pi / height * (np.arange(FINE)[:, None] * column % height)
    short = [np.cos(small), np.sin(small), np.cos(rough), np.sin(rough)]
    return jnp.asarray(np.concatenate(short), jnp.float32)


def scaled_tables(height, after):
    factor = 1.0 / math.sqrt(height)

    def body(short_ref, *refs):
        refs[-1][: 2 * FINE] = short_ref[: 2 * FINE]
        refs[-1][2 * FINE :] = short_ref[2 * FINE :] * factor

    short = short_tables(height)
    return pl.pallas_call(
        body,
        in_specs=[pl.BlockSpec(memory_space=pltpu.VMEM)]
        + [pl.BlockSpec(memory_space=pl.ANY)] * len(after),
        out_specs=pl.BlockSpec(memory_space=pltpu.VMEM),
        out_shape=jax.ShapeDtypeStruct(short.shape, short.dtype),
        compiler_params=params(),
        cost_estimate=cost(1 << 33, 8 * short.size),
        name="scaled_tables",
    )(short, *after)


def make_table(short_ref, out_ref, first, rows):
    height = short_ref.shape[1]
    coarse = height // FINE
    sc, ss = short_ref[:FINE], short_ref[FINE : 2 * FINE]
    for j in range(first // FINE, (first + rows) // FINE):
        a = 2 * FINE + j
        rc, rs = short_ref[a : a + 1, :], short_ref[a + coarse : a + coarse + 1, :]
        here = slice(j * FINE, (j + 1) * FINE)
        out_ref[here, :height] = (rc * sc - rs * ss).astype(jnp.bfloat16)
        out_ref[here, height:] = (rs * sc + rc * ss).astype(jnp.bfloat16)


def cost(flops, moved):
    return pl.CostEstimate(flops=flops, transcendentals=0, bytes_accessed=moved)


def params(limit=VMEM_LIMIT):
    return pltpu.CompilerParams(vmem_limit_bytes=limit)


def shade(tile, down_ref, across_ref):
    return (tile * (down_ref[...].T[:, :1] * across_ref[...])).astype(jnp.bfloat16)


def times_table(table, shaded):
    y = lax.dot_general(
        table, shaded, (((1,), (1,)), ((), ())), preferred_element_type=jnp.float32
    )
    return y.astype(jnp.bfloat16)


def near_columns(tiles, down, across, table, half, me, peers):
    count, rows, width = tiles.shape
    span = table.shape[0] // 2
    block = span // peers

    def body(half_ref, me_ref, tile_hbm, down_ref, across_ref, table_hbm, *refs):
        outs = refs[:2]
        tile_ref, table_ref, work, done = refs[2:]
        t = pl.program_id(0)
        me = me_ref[0]
        start = pl.multiple_of((1 - half_ref[0]) * span + me // 2 * 2 * block, 2 * block)
        fetch = pltpu.make_async_copy(
            table_hbm.at[pl.ds(start, 2 * block)], table_ref, done.at[count]
        )
        loads = [
            pltpu.make_async_copy(tile_hbm.at[i], tile_ref.at[i], done.at[i]) for i in range(count)
        ]

        @pl.when(t == 0)
        def _():
            fetch.start()
            for load in loads:
                load.start()
            fetch.wait()

        for i in range(count):

            @pl.when(t == i)
            def _():
                loads[i].wait()
                work[...] = times_table(table_ref[...], shade(tile_ref[i], down_ref, across_ref))

        for k in range(2):
            place = pl.multiple_of((me % 2 ^ k) * block, block)
            outs[k][0] = work[pl.ds(place, block), :]

    return pl.pallas_call(
        body,
        grid_spec=pltpu.PrefetchScalarGridSpec(
            num_scalar_prefetch=2,
            grid=(count,),
            in_specs=[
                pl.BlockSpec(memory_space=pltpu.HBM),
                pl.BlockSpec((8, rows), lambda t, half, me: (0, me[0])),
                pl.BlockSpec((1, width), lambda t, half, me: (0, 0)),
                pl.BlockSpec(memory_space=pltpu.HBM),
            ],
            out_specs=[pl.BlockSpec((1, block, rows), lambda t, half, me: (t, 0, 0))] * 2,
            scratch_shapes=[
                pltpu.VMEM((count, rows, width), tiles.dtype),
                pltpu.VMEM((2 * block, width), table.dtype),
                pltpu.VMEM((2 * block, rows), jnp.bfloat16),
                pltpu.SemaphoreType.DMA((count + 1,)),
            ],
        ),
        out_shape=[jax.ShapeDtypeStruct((count, block, rows), jnp.bfloat16)] * 2,
        compiler_params=params(FIRST_LIMIT),
        cost_estimate=cost(4 * count * rows * width * block, 4 * tiles.size + 4 * block * width),
        name="near_columns",
    )(scalar(half), scalar(me), tiles, down, across, table)


def rest_columns(tiles, down, across, table, half, me, pairs, peers):
    count, rows, width = tiles.shape
    span = table.shape[0] // 2
    block = span // peers
    distant = peers - 2

    def body(half_ref, me_ref, pairs_ref, tile_ref, down_ref, across_ref, table_ref, *refs):
        out_ref, far, work = refs[0], refs[1:-1], refs[-1]
        half, me = half_ref[0], me_ref[0]
        t = pl.program_id(0)
        shaded = shade(tile_ref[0], down_ref, across_ref)
        for j in range(1, peers // 2):
            start = pl.multiple_of((1 - half) * span + (me // 2 ^ j) * 2 * block, 2 * block)
            work[...] = times_table(table_ref[pl.ds(start, 2 * block), :], shaded)
            for k in range(2):
                place = pl.multiple_of((me % 2 ^ k) * block, block)
                for i in range(count):

                    @pl.when(t == i)
                    def _():
                        far[i * distant + 2 * j - 2 + k][...] = work[pl.ds(place, block), :]

        start = pl.multiple_of(half * span, span)
        y = times_table(table_ref[pl.ds(start, span), :], shaded)
        out_ref[:, 0] = y.reshape(peers, block, rows)

    return pl.pallas_call(
        body,
        grid_spec=pltpu.PrefetchScalarGridSpec(
            num_scalar_prefetch=3,
            grid=(count,),
            in_specs=[
                pl.BlockSpec((1, rows, width), lambda t, half, me, a: ((a[0, 0, 0] + t) % count, 0, 0)),
                pl.BlockSpec((8, rows), lambda t, half, me, a: (0, me[0])),
                pl.BlockSpec((1, width), lambda t, half, me, a: (0, 0)),
                pl.BlockSpec((width, width), lambda t, half, me, a: (0, 0)),
            ],
            out_specs=[
                pl.BlockSpec(
                    (peers, 1, block, rows), lambda t, half, me, a: (0, (a[0, 0, 0] + t) % count, 0, 0)
                ),
                *[pl.BlockSpec((block, rows), lambda t, half, me, a: (0, 0))] * (count * distant),
            ],
            scratch_shapes=[pltpu.VMEM((2 * block, rows), jnp.bfloat16)],
        ),
        out_shape=[
            jax.ShapeDtypeStruct((peers, count, block, rows), jnp.bfloat16),
            *[jax.ShapeDtypeStruct((block, rows), jnp.bfloat16)] * (count * distant),
        ],
        compiler_params=params(),
        cost_estimate=cost(3 * count * rows * width * span, 4 * tiles.size + 2 * width * width),
        name="rest_columns",
    )(scalar(half), scalar(me), pairs, tiles, down, across, table)


def gather_rows(pieces, table_ref, me):
    total = None
    for k, piece in enumerate(pieces):
        rows = piece.shape[1]
        start = pl.multiple_of((me ^ k) * rows, rows)
        term = jnp.dot(
            piece, table_ref[pl.ds(start, rows), :], preferred_element_type=jnp.float32
        )
        total = term if total is None else total + term
    return total


def holds_packed(place):
    half_ref, me_ref = place
    return (half_ref[0] == 0) & (me_ref[0] == 0)


def store_spectra(s_ref, total, spectra, edge, first):
    block = spectra.shape[2]
    height = spectra.shape[3]
    row = lax.broadcasted_iota(jnp.int32, (block, height), 0)
    packed = (row == 0) & holds_packed(s_ref)
    for t in range(total.shape[0] // (2 * block)):
        real = total[2 * t * block : (2 * t + 1) * block]
        imag = total[(2 * t + 1) * block : (2 * t + 2) * block]
        cr, sr = real[:, :height], real[:, height:]
        ci, si = imag[:, :height], imag[:, height:]
        spectra[first + t, 0] = jnp.where(packed, cr, cr + si).astype(jnp.bfloat16)
        spectra[first + t, 1] = jnp.where(packed, -sr, ci - sr).astype(jnp.bfloat16)
        edge[first + t, 0] = ci[:16].astype(jnp.bfloat16)
        edge[first + t, 1] = (-si[:16]).astype(jnp.bfloat16)


def normalised(left_real, left_imag, right_real, right_imag):
    lr = left_real.astype(jnp.float32)
    li = left_imag.astype(jnp.float32)
    rr = right_real.astype(jnp.float32)
    ri = right_imag.astype(jnp.float32)
    cross_real = lr * rr + li * ri
    cross_imag = li * rr - lr * ri
    factor = 1.0 / (jnp.sqrt(cross_real * cross_real + cross_imag * cross_imag) + FLOOR)
    return (
        (cross_real * factor).astype(jnp.bfloat16),
        (cross_imag * factor).astype(jnp.bfloat16),
    )


def correlate(s_ref, picks, phases):
    height = phases.shape[2]
    lead = lax.broadcasted_iota(jnp.int32, (16, height), 0)
    packed = (lead == 0) & holds_packed(s_ref)
    for p, ((left, left_edge, a), (right, right_edge, c)) in enumerate(picks):
        q_real, q_imag = normalised(left[a, 0], left[a, 1], right[c, 0], right[c, 1])
        e_real, e_imag = normalised(
            left_edge[a, 0], left_edge[a, 1], right_edge[c, 0], right_edge[c, 1]
        )
        phases[2 * p] = q_real
        phases[2 * p + 1] = q_imag
        top_real = q_real[:16].astype(jnp.float32)
        top_imag = q_imag[:16].astype(jnp.float32)
        mixed_real = jnp.where(packed, top_real - e_imag.astype(jnp.float32), top_real)
        mixed_imag = jnp.where(packed, top_imag + e_real.astype(jnp.float32), top_imag)
        phases[2 * p, :16] = mixed_real.astype(jnp.bfloat16)
        phases[2 * p + 1, :16] = mixed_imag.astype(jnp.bfloat16)

def invert_columns(s_ref, me, phases, table_ref, outs):
    _, block, height = phases.shape
    slots = phases.shape[0] // 2
    rows = next(iter(outs.values())).shape[2]
    row = lax.broadcasted_iota(jnp.int32, (block, rows), 0)
    twice = jnp.where((row == 0) & holds_packed(s_ref), 1.0, 2.0)
    flat = phases[...].reshape(2 * slots * block, height)
    for k, out in outs.items():
        start = pl.multiple_of((me ^ k) * rows, rows)
        c_part = jnp.dot(
            flat, table_ref[:, pl.ds(start, rows)], preferred_element_type=jnp.float32
        )
        start = pl.multiple_of(height + (me ^ k) * rows, rows)
        s_part = jnp.dot(
            flat, table_ref[:, pl.ds(start, rows)], preferred_element_type=jnp.float32
        )
        for p in range(slots):
            re = slice(2 * p * block, (2 * p + 1) * block)
            im = slice((2 * p + 1) * block, (2 * p + 2) * block)
            out[p, :block] = ((c_part[re] - s_part[im]) * twice).astype(jnp.bfloat16)
            out[p, block:] = ((s_part[re] + c_part[im]) * twice).astype(jnp.bfloat16)


def own_spectra(place, pieces, short):
    peers, count, double, rows = pieces.shape
    height = peers * rows

    def body(half_ref, me_ref, pieces_ref, short_ref, *refs):
        spectra, edge, table_ref = refs[-3:]
        total = None
        for k in range(peers):
            make_table(short_ref, table_ref, k * rows, rows)
            term = jnp.dot(
                pieces_ref[k].reshape(count * double, rows),
                table_ref[k * rows : (k + 1) * rows],
                preferred_element_type=jnp.float32,
            )
            total = term if total is None else total + term
        store_spectra((half_ref, me_ref), total, spectra, edge, 0)

    return pl.pallas_call(
        body,
        in_specs=[pl.BlockSpec(memory_space=pltpu.SMEM)] * 2
        + [pl.BlockSpec(memory_space=pltpu.VMEM)] * 2,
        out_specs=[pl.BlockSpec(memory_space=pltpu.VMEM)] * 3,
        out_shape=[
            jax.ShapeDtypeStruct((count, 2, double // 2, height), jnp.bfloat16),
            jax.ShapeDtypeStruct((count, 2, 16, height), jnp.bfloat16),
            jax.ShapeDtypeStruct((height, 2 * height), jnp.bfloat16),
        ],
        compiler_params=params(),
        cost_estimate=cost(4 * count * double * height * height, 8 * height * height),
        name="own_spectra",
    )(*place, pieces, short)


def first_slot(place, theirs, near, far, table, spectra, edge):
    peers = len(near) + len(far)
    count, double, rows = near[0].shape
    height = table.shape[0]
    block = double // 2

    def body(half_ref, me_ref, theirs_ref, *refs):
        s_ref = (half_ref, me_ref)
        me = me_ref[0]
        left = theirs_ref[0, 0, 0]
        pieces = [ref[left] for ref in refs[:2]] + [ref[...] for ref in refs[2:peers]]
        table_ref, own, own_edge, out, lead, lead_edge, phases = refs[peers:]
        store_spectra(s_ref, gather_rows(pieces, table_ref, me), lead, lead_edge, 0)
        right = theirs_ref[0, 0, 1] - count
        correlate(s_ref, [((lead, lead_edge, 0), (own, own_edge, right))], phases)
        invert_columns(s_ref, me, phases, table_ref, {k: out.at[k] for k in range(2)})

    return pl.pallas_call(
        body,
        in_specs=[pl.BlockSpec(memory_space=pltpu.SMEM)] * 3
        + [pl.BlockSpec(memory_space=pltpu.VMEM)] * (peers + 3),
        out_specs=[pl.BlockSpec(memory_space=pltpu.VMEM)] * 4,
        out_shape=[
            jax.ShapeDtypeStruct((2, 1, double, rows), jnp.bfloat16),
            jax.ShapeDtypeStruct((1, 2, block, height), jnp.bfloat16),
            jax.ShapeDtypeStruct((1, 2, 16, height), jnp.bfloat16),
            jax.ShapeDtypeStruct((2, block, height), jnp.bfloat16),
        ],
        compiler_params=params(),
        cost_estimate=cost(8 * double * height * height, 8 * height * height),
        name="first_slot",
    )(*place, theirs, *near, *far, table, spectra, edge)


def other_slots(place, theirs, near, far, table, spectra, edge, lead, lead_edge, phases):
    peers = 2 + len(far[0])
    count, double, rows = near[0].shape
    height = table.shape[0]
    block = double // 2
    slots = theirs.shape[1]
    rest = count - 1

    def body(half_ref, me_ref, theirs_ref, *refs):
        s_ref = (half_ref, me_ref)
        me = me_ref[0]
        first = theirs_ref[0, 0, 0]
        near_refs = refs[:2]
        far_refs = refs[2 : 2 + rest * (peers - 2)]
        tail = refs[2 + rest * (peers - 2) :]
        table_ref, own, own_edge, lead_ref, lead_edge_ref, done_ref = tail[:6]
        out, every, edges = tail[6:9]
        distant, phases_ref = tail[9:-1], tail[-1]
        every[:count] = own[...]
        edges[:count] = own_edge[...]
        every[count : count + 1] = lead_ref[...]
        edges[count : count + 1] = lead_edge_ref[...]
        for i in range(1, count):
            pieces = [ref[(first + i) % count] for ref in near_refs]
            pieces += [ref[...] for ref in far_refs[(i - 1) * (peers - 2) : i * (peers - 2)]]
            store_spectra(s_ref, gather_rows(pieces, table_ref, me), every, edges, count + i)
        picks = []
        for p in range(1, slots):
            a, c = theirs_ref[0, p, 0], theirs_ref[0, p, 1]
            left = count + (a + count - first) % count
            right = jnp.where(c < count, count + (c + count - first) % count, c - count)
            picks.append(((every, edges, left), (every, edges, right)))
        phases_ref[:2] = done_ref[...]
        fresh = phases_ref.at[pl.ds(2, 2 * slots - 2)]
        correlate(s_ref, picks, fresh)
        invert_columns(s_ref, me, fresh, table_ref, {k: out.at[k] for k in range(2)})
        if distant:
            outs = {k: distant[k - 2] for k in range(2, peers)}
            invert_columns(s_ref, me, phases_ref, table_ref, outs)

    flat = [piece for pieces in far for piece in pieces]
    return pl.pallas_call(
        body,
        in_specs=[pl.BlockSpec(memory_space=pltpu.SMEM)] * 3
        + [pl.BlockSpec(memory_space=pltpu.VMEM)] * (8 + len(flat)),
        out_specs=[pl.BlockSpec(memory_space=pltpu.VMEM)] * (1 + peers),
        out_shape=[
            jax.ShapeDtypeStruct((2, slots - 1, double, rows), jnp.bfloat16),
            jax.ShapeDtypeStruct((2 * count, 2, block, height), jnp.bfloat16),
            jax.ShapeDtypeStruct((2 * count, 2, 16, height), jnp.bfloat16),
            *[jax.ShapeDtypeStruct((slots, double, rows), jnp.bfloat16)] * (peers - 2),
        ],
        scratch_shapes=[pltpu.VMEM((2 * slots, block, height), jnp.bfloat16)],
        compiler_params=params(),
        cost_estimate=cost(8 * double * height * height, 8 * height * height),
        name="other_slots",
    )(*place, theirs, *near, *flat, table, spectra, edge, lead, lead_edge, phases)


def own_slots(place, pairs, theirs, table, spectra, edge, peers):
    block, height = spectra.shape[2:]
    count = spectra.shape[0] // 2
    rows = height // peers
    slots = pairs.shape[1]

    def body(half_ref, me_ref, pairs_ref, theirs_ref, table_ref, every, edges, out_ref, work):
        s_ref = (half_ref, me_ref)
        first = theirs_ref[0, 0, 0]
        picks = []
        for p in range(slots):
            a, c = pairs_ref[0, p, 0], pairs_ref[0, p, 1]
            right = jnp.where(c < count, c, count + (c - first) % count)
            picks.append(((every, edges, a), (every, edges, right)))
        correlate(s_ref, picks, work)
        invert_columns(s_ref, 0, work, table_ref, {k: out_ref.at[k] for k in range(peers)})

    return pl.pallas_call(
        body,
        in_specs=[pl.BlockSpec(memory_space=pltpu.SMEM)] * 4
        + [pl.BlockSpec(memory_space=pltpu.VMEM)] * 3,
        out_specs=pl.BlockSpec(memory_space=pltpu.VMEM),
        out_shape=jax.ShapeDtypeStruct((peers, slots, 2 * block, rows), jnp.bfloat16),
        scratch_shapes=[pltpu.VMEM((2 * slots, block, height), jnp.bfloat16)],
        compiler_params=params(),
        cost_estimate=cost(8 * slots * block * height * height, 8 * height * height),
        name="own_slots",
    )(*place, pairs, theirs, table, spectra, edge)


def own_surfaces(half, own, table):
    peers, slots, double, rows = own.shape
    width = table.shape[0]
    span = peers * double

    def body(half_ref, own_ref, table_ref, out_ref):
        out_ref[0] = lax.dot_general(
            own_ref[:, 0].reshape(span, rows),
            table_ref[...],
            (((0,), (0,)), ((), ())),
            preferred_element_type=jnp.float32,
        )

    return pl.pallas_call(
        body,
        grid_spec=pltpu.PrefetchScalarGridSpec(
            num_scalar_prefetch=1,
            grid=(slots,),
            in_specs=[
                pl.BlockSpec((peers, 1, double, rows), lambda p, half: (0, p, 0, 0)),
                pl.BlockSpec((span, width), lambda p, half: (half[0], 0)),
            ],
            out_specs=pl.BlockSpec((1, rows, width), lambda p, half: (p, 0, 0)),
        ),
        out_shape=jax.ShapeDtypeStruct((slots, rows, width), jnp.float32),
        compiler_params=params(),
        cost_estimate=cost(2 * slots * rows * width * span, 4 * slots * rows * width),
        name="own_surfaces",
    )(scalar(half), own, table)


def surfaces_of(half, me, counts, part, lead, rest, far, table):
    peers = 2 + len(far)
    slots, rows, width = part.shape
    double = lead[1].shape[1]
    span = peers * double

    def body(half_ref, me_ref, counts_ref, part_ref, *refs):
        leads, rests, fars = refs[:2], refs[2:4], refs[4:-3]
        table_ref, out_ref, work = refs[-3:]
        slot = pl.program_id(0)

        def put(k, piece):
            place = pl.multiple_of((me_ref[0] ^ k) * double, double)
            work[pl.ds(place, double), :] = piece

        @pl.when(slot == 0)
        def _():
            put(0, leads[0][0, 0])
            put(1, leads[1][0])

        @pl.when(slot > 0)
        def _():
            put(0, rests[0][0, 0])
            put(1, rests[1][0])

        for k, ref in enumerate(fars):
            put(k + 2, ref[0])
        total = lax.dot_general(
            work[...], table_ref[...], (((0,), (0,)), ((), ())), preferred_element_type=jnp.float32
        )
        live = slot < counts_ref[0]
        out_ref[0] = jnp.where(live, part_ref[0] + total, 0.0)

    plane = pl.BlockSpec((1, rows, width), lambda p, half, me, counts: (p, 0, 0))
    piece = pl.BlockSpec((1, double, rows), lambda p, half, me, counts: (p, 0, 0))

    def late(p):
        return jnp.maximum(p - 1, 0)

    return pl.pallas_call(
        body,
        grid_spec=pltpu.PrefetchScalarGridSpec(
            num_scalar_prefetch=3,
            grid=(slots,),
            in_specs=[
                plane,
                pl.BlockSpec((1, 1, double, rows), lambda p, half, me, counts: (0, 0, 0, 0)),
                pl.BlockSpec((1, double, rows), lambda p, half, me, counts: (0, 0, 0)),
                pl.BlockSpec((1, 1, double, rows), lambda p, half, me, counts: (0, late(p), 0, 0)),
                pl.BlockSpec((1, double, rows), lambda p, half, me, counts: (late(p), 0, 0)),
                *[piece] * (peers - 2),
                pl.BlockSpec((span, width), lambda p, half, me, counts: (1 - half[0], 0)),
            ],
            out_specs=plane,
            scratch_shapes=[pltpu.VMEM((span, rows), jnp.bfloat16)],
        ),
        out_shape=jax.ShapeDtypeStruct((slots, rows, width), jnp.float32),
        compiler_params=params(),
        cost_estimate=cost(2 * slots * rows * width * span, 8 * slots * rows * width),
        name="surfaces",
    )(scalar(half), scalar(me), counts, part, *lead, *rest, *far, table)


def local(tiles, pairs, counts):
    groups = lax.axis_size("blk")
    peers = lax.axis_size("rows")
    group = lax.axis_index("blk")
    me = lax.axis_index("rows")
    count, rows, width = tiles.shape
    height = rows * peers
    turn = groups // 2
    half = group // turn
    axes = ("blk", "rows")

    def across(value, k):
        moves = [
            (b * peers + r, (b + turn) % groups * peers + (r ^ k))
            for b in range(groups)
            for r in range(peers)
        ]
        return lax.ppermute(value, axes, moves)

    def along(blocks):
        return lax.all_to_all(blocks, "rows", split_axis=0, concat_axis=0)

    def swap(value):
        return lax.ppermute(value, "rows", [(r, r ^ 1) for r in range(peers)])

    table_w = jnp.asarray(width_table(width, 2 * peers))
    down = jnp.asarray(np.tile(hann(height), (8, 1)))
    sideways = jnp.asarray(hann(width)[None, :])

    sent = near_columns(tiles, down, sideways, table_w, half, me, peers)
    near = [across(sent[k], k) for k in range(2)]
    *sent, held = lax.optimization_barrier((*sent, half))
    kept, *sent = rest_columns(
        tiles, down, sideways, table_w, held, me, pairs, peers
    )
    *sent, kept, told = lax.optimization_barrier((*sent, kept, pairs))
    distant = peers - 2
    far = [[across(sent[k - 2], k) for k in range(2, peers)]]
    theirs = across(told, 0)
    for i in range(1, count):
        far.append([across(sent[i * distant + k - 2], k) for k in range(2, peers)])
    mine = along(kept)

    place = (scalar(half), scalar(me))
    spectra, edge, table_h = own_spectra(place, mine, scaled_tables(height, near))
    lead, lead_spectra, lead_edge, phases = first_slot(
        place, theirs, near, far[0], table_h, spectra, edge
    )
    lead = across(lead, 0)
    rest, spectra, edge, *back = other_slots(
        place, theirs, near, far[1:], table_h, spectra, edge, lead_spectra, lead_edge, phases
    )
    rest = across(rest, 0)
    lead, *back = lax.optimization_barrier((lead, *back))
    back = [across(back[k - 2], k) for k in range(2, peers)]
    own = own_slots(place, pairs, theirs, table_h, spectra, edge, peers)
    part = own_surfaces(half, along(own), table_w)
    *back, part = lax.optimization_barrier((*back, part))
    return surfaces_of(
        half, me, counts, part, (lead, swap(lead[1])), (rest, swap(rest[1])), back, table_w
    )


def solution(mesh):
    from jax.sharding import PartitionSpec as P

    return jax.shard_map(
        local,
        mesh=mesh,
        in_specs=(
            P(("parts", "blk"), "rows", None),
            P(("parts", "blk"), None, None),
            P(("parts", "blk")),
        ),
        out_specs=P(("parts", "blk"), "rows", None),
        check_vma=False,
    )
```

```python
import math

import jax
import jax.numpy as jnp
import numpy as np
from jax import lax
from jax.experimental import pallas as pl
from jax.experimental.pallas import tpu as pltpu

FLOOR = 0.05
VMEM_LIMIT = 24 * 1024 * 1024
FIRST_LIMIT = 60 * 1024 * 1024


def hann(length):
    return np.asarray(0.5 - 0.5 * np.cos(2.0 * math.pi / length * np.arange(length)), np.float32)


def scalar(value):
    return jnp.reshape(value, (1,)).astype(jnp.int32)


def width_table(width, owners):
    half = width // 2
    phase = np.arange(half)[:, None] * np.arange(width)[None, :] % width
    angle = 2.0 * math.pi / width * phase
    factor = 1.0 / math.sqrt(width)
    cosine = np.cos(angle) * factor
    sine = -np.sin(angle) * factor
    sine[0] = np.where(np.arange(width) % 2 == 0, factor, -factor)
    shape = (owners, half // owners, width)
    table = np.stack([cosine.reshape(shape), sine.reshape(shape)], axis=1)
    return table.reshape(width, width).astype(jnp.bfloat16)


def height_table(height):
    fine = 32
    coarse = height // fine
    column = np.arange(height)[None, :]
    rough = 2.0 * math.pi / height * (np.arange(coarse)[:, None] * fine * column % height)
    small = 2.0 * math.pi / height * (np.arange(fine)[:, None] * column % height)
    factor = 1.0 / math.sqrt(height)
    short = [np.cos(small), np.sin(small), np.cos(rough) * factor, np.sin(rough) * factor]

    def body(short_ref, out_ref):
        sc, ss = short_ref[:fine], short_ref[fine : 2 * fine]
        for a in range(2 * fine, 2 * fine + coarse):
            rc, rs = short_ref[a : a + 1, :], short_ref[a + coarse : a + coarse + 1, :]
            here = slice((a - 2 * fine) * fine, (a - 2 * fine + 1) * fine)
            out_ref[here, :height] = (rc * sc - rs * ss).astype(jnp.bfloat16)
            out_ref[here, height:] = (rs * sc + rc * ss).astype(jnp.bfloat16)

    return pl.pallas_call(
        body,
        in_specs=[pl.BlockSpec(memory_space=pltpu.VMEM)],
        out_specs=pl.BlockSpec(memory_space=pltpu.VMEM),
        out_shape=jax.ShapeDtypeStruct((height, 2 * height), jnp.bfloat16),
        compiler_params=params(),
        cost_estimate=cost(1 << 33, 4 * height * height),
        name="height_table",
    )(jnp.asarray(np.concatenate(short), jnp.float32))


def cost(flops, moved):
    return pl.CostEstimate(flops=flops, transcendentals=0, bytes_accessed=moved)


def params(limit=VMEM_LIMIT):
    return pltpu.CompilerParams(vmem_limit_bytes=limit)


def shade(tile, down_ref, across_ref):
    return (tile * (down_ref[...].T[:, :1] * across_ref[...])).astype(jnp.bfloat16)


def times_table(table, shaded):
    y = lax.dot_general(
        table, shaded, (((1,), (1,)), ((), ())), preferred_element_type=jnp.float32
    )
    return y.astype(jnp.bfloat16)


def near_columns(tiles, down, across, table, half, me, peers):
    count, rows, width = tiles.shape
    span = table.shape[0] // 2
    block = span // peers

    def body(half_ref, me_ref, tile_hbm, down_hbm, across_hbm, table_hbm, *refs):
        outs = refs[:2]
        tile_ref, table_ref, work, down_ref, across_ref, done = refs[2:]
        t = pl.program_id(0)
        me = me_ref[0]
        start = pl.multiple_of((1 - half_ref[0]) * span + me // 2 * 2 * block, 2 * block)
        fetch = pltpu.make_async_copy(
            table_hbm.at[pl.ds(start, 2 * block)], table_ref, done.at[count]
        )
        loads = [
            pltpu.make_async_copy(tile_hbm.at[i], tile_ref.at[i], done.at[i]) for i in range(count)
        ]

        lane = pl.multiple_of(me * rows, rows)
        extra = [
            pltpu.make_async_copy(down_hbm.at[:, pl.ds(lane, rows)], down_ref, done.at[count + 1]),
            pltpu.make_async_copy(across_hbm, across_ref, done.at[count + 2]),
        ]

        @pl.when(t == 0)
        def _():
            for copy in extra:
                copy.start()
            fetch.start()
            for load in loads:
                load.start()
            for copy in extra:
                copy.wait()
            fetch.wait()

        for i in range(count):

            @pl.when(t == i)
            def _():
                loads[i].wait()
                work[...] = times_table(table_ref[...], shade(tile_ref[i], down_ref, across_ref))

        for k in range(2):
            place = pl.multiple_of((me % 2 ^ k) * block, block)
            outs[k][0] = work[pl.ds(place, block), :]

    return pl.pallas_call(
        body,
        grid_spec=pltpu.PrefetchScalarGridSpec(
            num_scalar_prefetch=2,
            grid=(count,),
            in_specs=[
                pl.BlockSpec(memory_space=pltpu.HBM),
                pl.BlockSpec(memory_space=pltpu.HBM),
                pl.BlockSpec(memory_space=pltpu.HBM),
                pl.BlockSpec(memory_space=pltpu.HBM),
            ],
            out_specs=[pl.BlockSpec((1, block, rows), lambda t, half, me: (t, 0, 0))] * 2,
            scratch_shapes=[
                pltpu.VMEM((count, rows, width), tiles.dtype),
                pltpu.VMEM((2 * block, width), table.dtype),
                pltpu.VMEM((2 * block, rows), jnp.bfloat16),
                pltpu.VMEM((8, rows), jnp.float32),
                pltpu.VMEM((1, width), jnp.float32),
                pltpu.SemaphoreType.DMA((count + 3,)),
            ],
        ),
        out_shape=[jax.ShapeDtypeStruct((count, block, rows), jnp.bfloat16)] * 2,
        compiler_params=params(FIRST_LIMIT),
        cost_estimate=cost(4 * count * rows * width * block, 4 * tiles.size + 4 * block * width),
        name="near_columns",
    )(scalar(half), scalar(me), tiles, down, across, table)


def rest_columns(tiles, down, across, table, half, me, peers):
    count, rows, width = tiles.shape
    span = table.shape[0] // 2
    block = span // peers

    def body(half_ref, me_ref, tile_ref, down_ref, across_ref, table_ref, *refs):
        out_ref, far, work = refs[0], refs[1:-1], refs[-1]
        half, me = half_ref[0], me_ref[0]
        shaded = shade(tile_ref[0], down_ref, across_ref)
        for j in range(1, peers // 2):
            start = pl.multiple_of((1 - half) * span + (me // 2 ^ j) * 2 * block, 2 * block)
            work[...] = times_table(table_ref[pl.ds(start, 2 * block), :], shaded)
            for k in range(2):
                place = pl.multiple_of((me % 2 ^ k) * block, block)
                far[2 * j - 2 + k][0] = work[pl.ds(place, block), :]
        start = pl.multiple_of(half * span, span)
        y = times_table(table_ref[pl.ds(start, span), :], shaded)
        out_ref[:, 0] = y.reshape(peers, block, rows)

    piece = pl.BlockSpec((1, block, rows), lambda t, half, me: (t, 0, 0))
    return pl.pallas_call(
        body,
        grid_spec=pltpu.PrefetchScalarGridSpec(
            num_scalar_prefetch=2,
            grid=(count,),
            in_specs=[
                pl.BlockSpec((1, rows, width), lambda t, half, me: (t, 0, 0)),
                pl.BlockSpec((8, rows), lambda t, half, me: (0, me[0])),
                pl.BlockSpec((1, width), lambda t, half, me: (0, 0)),
                pl.BlockSpec((width, width), lambda t, half, me: (0, 0)),
            ],
            out_specs=[
                pl.BlockSpec((peers, 1, block, rows), lambda t, half, me: (0, t, 0, 0)),
                *[piece] * (peers - 2),
            ],
            scratch_shapes=[pltpu.VMEM((2 * block, rows), jnp.bfloat16)],
        ),
        out_shape=[
            jax.ShapeDtypeStruct((peers, count, block, rows), jnp.bfloat16),
            *[jax.ShapeDtypeStruct((count, block, rows), jnp.bfloat16)] * (peers - 2),
        ],
        compiler_params=params(),
        cost_estimate=cost(3 * count * rows * width * span, 4 * tiles.size + 2 * width * width),
        name="rest_columns",
    )(scalar(half), scalar(me), tiles, down, across, table)


def gather_rows(pieces, table_ref, me, first=0, total=None):
    for k, piece in enumerate(pieces, first):
        count, block, rows = piece.shape
        start = pl.multiple_of((me ^ k) * rows, rows)
        term = jnp.dot(
            piece[...].reshape(count * block, rows),
            table_ref[pl.ds(start, rows), :],
            preferred_element_type=jnp.float32,
        )
        total = term if total is None else total + term
    return total


def holds_packed(place):
    half_ref, me_ref = place
    return (half_ref[0] == 0) & (me_ref[0] == 0)


def store_spectra(s_ref, total, spectra, edge, first):
    block = spectra.shape[2]
    height = spectra.shape[3]
    row = lax.broadcasted_iota(jnp.int32, (block, height), 0)
    packed = (row == 0) & holds_packed(s_ref)
    for t in range(total.shape[0] // (2 * block)):
        real = total[2 * t * block : (2 * t + 1) * block]
        imag = total[(2 * t + 1) * block : (2 * t + 2) * block]
        cr, sr = real[:, :height], real[:, height:]
        ci, si = imag[:, :height], imag[:, height:]
        spectra[first + t, 0] = jnp.where(packed, cr, cr + si).astype(jnp.bfloat16)
        spectra[first + t, 1] = jnp.where(packed, -sr, ci - sr).astype(jnp.bfloat16)
        edge[first + t, 0] = ci[:16].astype(jnp.bfloat16)
        edge[first + t, 1] = (-si[:16]).astype(jnp.bfloat16)


def normalised(left_real, left_imag, right_real, right_imag):
    lr = left_real.astype(jnp.float32)
    li = left_imag.astype(jnp.float32)
    rr = right_real.astype(jnp.float32)
    ri = right_imag.astype(jnp.float32)
    cross_real = lr * rr + li * ri
    cross_imag = li * rr - lr * ri
    factor = 1.0 / (jnp.sqrt(cross_real * cross_real + cross_imag * cross_imag) + FLOOR)
    return (
        (cross_real * factor).astype(jnp.bfloat16),
        (cross_imag * factor).astype(jnp.bfloat16),
    )


def correlate(s_ref, picks, spectra, edge, phases):
    slots = len(picks)
    height = spectra.shape[3]
    lead = lax.broadcasted_iota(jnp.int32, (16, height), 0)
    packed = (lead == 0) & holds_packed(s_ref)
    for p in range(slots):
        a, c = picks[p]
        q_real, q_imag = normalised(spectra[a, 0], spectra[a, 1], spectra[c, 0], spectra[c, 1])
        e_real, e_imag = normalised(edge[a, 0], edge[a, 1], edge[c, 0], edge[c, 1])
        phases[2 * p] = q_real
        phases[2 * p + 1] = q_imag
        top_real = q_real[:16].astype(jnp.float32)
        top_imag = q_imag[:16].astype(jnp.float32)
        mixed_real = jnp.where(packed, top_real - e_imag.astype(jnp.float32), top_real)
        mixed_imag = jnp.where(packed, top_imag + e_real.astype(jnp.float32), top_imag)
        phases[2 * p, :16] = mixed_real.astype(jnp.bfloat16)
        phases[2 * p + 1, :16] = mixed_imag.astype(jnp.bfloat16)

def invert_columns(s_ref, me, phases, table_ref, outs):
    _, block, height = phases.shape
    slots = phases.shape[0] // 2
    rows = next(iter(outs.values())).shape[2]
    row = lax.broadcasted_iota(jnp.int32, (block, rows), 0)
    twice = jnp.where((row == 0) & holds_packed(s_ref), 1.0, 2.0)
    flat = phases[...].reshape(2 * slots * block, height)
    for k, out in outs.items():
        start = pl.multiple_of((me ^ k) * rows, rows)
        c_part = jnp.dot(
            flat, table_ref[:, pl.ds(start, rows)], preferred_element_type=jnp.float32
        )
        start = pl.multiple_of(height + (me ^ k) * rows, rows)
        s_part = jnp.dot(
            flat, table_ref[:, pl.ds(start, rows)], preferred_element_type=jnp.float32
        )
        for p in range(slots):
            re = slice(2 * p * block, (2 * p + 1) * block)
            im = slice((2 * p + 1) * block, (2 * p + 2) * block)
            out[p, :block] = ((c_part[re] - s_part[im]) * twice).astype(jnp.bfloat16)
            out[p, block:] = ((s_part[re] + c_part[im]) * twice).astype(jnp.bfloat16)


def own_spectra(place, pieces, near, table):
    peers, count, double, rows = pieces.shape
    height = table.shape[0]

    def body(half_ref, me_ref, pieces_ref, near_a, near_b, table_ref, spectra, edge, share):
        inputs = [pieces_ref.at[k] for k in range(peers)]
        store_spectra((half_ref, me_ref), gather_rows(inputs, table_ref, 0), spectra, edge, 0)
        share[...] = gather_rows([near_a, near_b], table_ref, me_ref[0])

    return pl.pallas_call(
        body,
        in_specs=[pl.BlockSpec(memory_space=pltpu.SMEM)] * 2
        + [pl.BlockSpec(memory_space=pltpu.VMEM)] * 4,
        out_specs=[pl.BlockSpec(memory_space=pltpu.VMEM)] * 3,
        out_shape=[
            jax.ShapeDtypeStruct((count, 2, double // 2, height), jnp.bfloat16),
            jax.ShapeDtypeStruct((count, 2, 16, height), jnp.bfloat16),
            jax.ShapeDtypeStruct((count * double, 2 * height), jnp.float32),
        ],
        compiler_params=params(),
        cost_estimate=cost(6 * count * double * height * height, 8 * height * height),
        name="own_spectra",
    )(*place, pieces, *near, table)


def partner_slots(place, theirs, pieces, share, table, spectra, edge):
    distant = len(pieces)
    count, double, rows = pieces[0].shape
    height = table.shape[0]
    block = double // 2
    slots = theirs.shape[1]

    def body(half_ref, me_ref, theirs_ref, *refs):
        s_ref = (half_ref, me_ref)
        me = me_ref[0]
        picks = [
            [(theirs_ref[0, p, i] + count) % (2 * count) for i in range(2)] for p in range(slots)
        ]
        inputs = refs[:distant]
        share_ref, table_ref, own_ref, own_edge, near, every, edges, phases = refs[distant:]
        every[:count] = own_ref[...]
        edges[:count] = own_edge[...]
        total = gather_rows(inputs, table_ref, me, 2, share_ref[...])
        store_spectra(s_ref, total, every, edges, count)
        correlate(s_ref, picks, every, edges, phases)
        invert_columns(s_ref, me, phases, table_ref, {k: near.at[k] for k in range(2)})

    return pl.pallas_call(
        body,
        in_specs=[pl.BlockSpec(memory_space=pltpu.SMEM)] * 3
        + [pl.BlockSpec(memory_space=pltpu.VMEM)] * (distant + 4),
        out_specs=[pl.BlockSpec(memory_space=pltpu.VMEM)] * 4,
        out_shape=[
            jax.ShapeDtypeStruct((2, slots, double, rows), jnp.bfloat16),
            jax.ShapeDtypeStruct((2 * count, 2, block, height), jnp.bfloat16),
            jax.ShapeDtypeStruct((2 * count, 2, 16, height), jnp.bfloat16),
            jax.ShapeDtypeStruct((2 * slots, block, height), jnp.bfloat16),
        ],
        compiler_params=params(),
        cost_estimate=cost(4 * (count + slots) * double * height * height, 8 * height * height),
        name="partner_slots",
    )(*place, theirs, *pieces, share, table, spectra, edge)


def own_slots(place, pairs, table, spectra, edge, phases, peers):
    block, height = spectra.shape[2:]
    rows = height // peers
    slots = pairs.shape[1]

    def body(half_ref, me_ref, pairs_ref, table_ref, every, edges, theirs, out_ref, *refs):
        s_ref = (half_ref, me_ref)
        far, work = refs[:-1], refs[-1]
        picks = [[pairs_ref[0, p, i] for i in range(2)] for p in range(slots)]
        if far:
            outs = {k: far[k - 2] for k in range(2, peers)}
            invert_columns(s_ref, me_ref[0], theirs, table_ref, outs)
        correlate(s_ref, picks, every, edges, work)
        invert_columns(s_ref, 0, work, table_ref, {k: out_ref.at[k] for k in range(peers)})

    return pl.pallas_call(
        body,
        in_specs=[pl.BlockSpec(memory_space=pltpu.SMEM)] * 3
        + [pl.BlockSpec(memory_space=pltpu.VMEM)] * 4,
        out_specs=[pl.BlockSpec(memory_space=pltpu.VMEM)] * (peers - 1),
        out_shape=[
            jax.ShapeDtypeStruct((peers, slots, 2 * block, rows), jnp.bfloat16),
            *[jax.ShapeDtypeStruct((slots, 2 * block, rows), jnp.bfloat16)] * (peers - 2),
        ],
        scratch_shapes=[pltpu.VMEM((2 * slots, block, height), jnp.bfloat16)],
        compiler_params=params(),
        cost_estimate=cost(8 * slots * block * height * height, 8 * height * height),
        name="own_slots",
    )(*place, pairs, table, spectra, edge, phases)


def own_surfaces(half, own, table):
    peers, slots, double, rows = own.shape
    width = table.shape[0]
    span = peers * double

    def body(half_ref, own_ref, table_ref, out_ref):
        out_ref[0] = lax.dot_general(
            own_ref[:, 0].reshape(span, rows),
            table_ref[...],
            (((0,), (0,)), ((), ())),
            preferred_element_type=jnp.float32,
        )

    return pl.pallas_call(
        body,
        grid_spec=pltpu.PrefetchScalarGridSpec(
            num_scalar_prefetch=1,
            grid=(slots,),
            in_specs=[
                pl.BlockSpec((peers, 1, double, rows), lambda p, half: (0, p, 0, 0)),
                pl.BlockSpec((span, width), lambda p, half: (half[0], 0)),
            ],
            out_specs=pl.BlockSpec((1, rows, width), lambda p, half: (p, 0, 0)),
        ),
        out_shape=jax.ShapeDtypeStruct((slots, rows, width), jnp.float32),
        compiler_params=params(),
        cost_estimate=cost(2 * slots * rows * width * span, 4 * slots * rows * width),
        name="own_surfaces",
    )(scalar(half), own, table)


def surfaces_of(half, me, counts, part, near, other, table):
    peers = 1 + len(other)
    slots, double, rows = other[0].shape
    width = table.shape[0]
    span = peers * double

    def body(half_ref, me_ref, counts_ref, part_ref, *refs):
        other_refs = refs[:peers]
        table_ref, out_ref, work = refs[peers:]
        for k in range(peers):
            place = pl.multiple_of((me_ref[0] ^ k) * double, double)
            piece = other_refs[k][0] if k else other_refs[k][0, 0]
            work[pl.ds(place, double), :] = piece
        rest = lax.dot_general(
            work[...], table_ref[...], (((0,), (0,)), ((), ())), preferred_element_type=jnp.float32
        )
        live = pl.program_id(0) < counts_ref[0]
        out_ref[0] = jnp.where(live, part_ref[0] + rest, 0.0)

    pair = pl.BlockSpec((1, 1, double, rows), lambda p, half, me, counts: (0, p, 0, 0))
    piece = pl.BlockSpec((1, double, rows), lambda p, half, me, counts: (p, 0, 0))
    plane = pl.BlockSpec((1, rows, width), lambda p, half, me, counts: (p, 0, 0))
    return pl.pallas_call(
        body,
        grid_spec=pltpu.PrefetchScalarGridSpec(
            num_scalar_prefetch=3,
            grid=(slots,),
            in_specs=[
                plane,
                pair,
                *[piece] * (peers - 1),
                pl.BlockSpec((span, width), lambda p, half, me, counts: (1 - half[0], 0)),
            ],
            out_specs=plane,
            scratch_shapes=[pltpu.VMEM((span, rows), jnp.bfloat16)],
        ),
        out_shape=jax.ShapeDtypeStruct((slots, rows, width), jnp.float32),
        compiler_params=params(),
        cost_estimate=cost(2 * slots * rows * width * span, 8 * slots * rows * width),
        name="surfaces",
    )(scalar(half), scalar(me), counts, part, near, *other, table)


def local(tiles, pairs, counts):
    groups = lax.axis_size("blk")
    peers = lax.axis_size("rows")
    group = lax.axis_index("blk")
    me = lax.axis_index("rows")
    count, rows, width = tiles.shape
    height = rows * peers
    turn = groups // 2
    half = group // turn
    axes = ("blk", "rows")

    def across(value, k):
        moves = [
            (b * peers + r, (b + turn) % groups * peers + (r ^ k))
            for b in range(groups)
            for r in range(peers)
        ]
        return lax.ppermute(value, axes, moves)

    def along(blocks):
        return lax.all_to_all(blocks, "rows", split_axis=0, concat_axis=0)

    def swap(value):
        return lax.ppermute(value, "rows", [(r, r ^ 1) for r in range(peers)])

    table_w = jnp.asarray(width_table(width, 2 * peers))
    down = jnp.asarray(np.tile(hann(height), (8, 1)))
    sideways = jnp.asarray(hann(width)[None, :])

    sent = near_columns(tiles, down, sideways, table_w, half, me, peers)
    arrived = [across(sent[k], k) for k in range(2)]
    *sent, held = lax.optimization_barrier((*sent, half))
    kept, *sent = rest_columns(tiles, down, sideways, table_w, held, me, peers)
    *sent, kept, pairs = lax.optimization_barrier((*sent, kept, pairs))
    arrived += [across(sent[k - 2], k) for k in range(2, peers)]
    mine = along(kept)

    table_h = height_table(height)
    theirs = across(pairs, 0)
    place = (scalar(half), scalar(me))
    spectra, edge, share = own_spectra(place, mine, arrived[:2], table_h)
    near, spectra, edge, phases = partner_slots(
        place, theirs, arrived[2:], share, table_h, spectra, edge
    )
    near = across(near, 0)
    own, *far = own_slots(place, pairs, table_h, spectra, edge, phases, peers)
    far = [across(far[k - 2], k) for k in range(2, peers)]
    part = own_surfaces(half, along(own), table_w)
    *far, part = lax.optimization_barrier((*far, part))
    return surfaces_of(half, me, counts, part, near, [swap(near[1]), *far], table_w)


def solution(mesh):
    from jax.sharding import PartitionSpec as P

    return jax.shard_map(
        local,
        mesh=mesh,
        in_specs=(
            P(("parts", "blk"), "rows", None),
            P(("parts", "blk"), None, None),
            P(("parts", "blk")),
        ),
        out_specs=P(("parts", "blk"), "rows", None),
        check_vma=False,
    )
```

```python
import math

import jax
import jax.numpy as jnp
import numpy as np
from jax import lax
from jax.experimental import pallas as pl
from jax.experimental.pallas import tpu as pltpu

FLOOR = 0.05
VMEM_LIMIT = 24 * 1024 * 1024
FIRST_LIMIT = 60 * 1024 * 1024


def hann(length):
    return np.asarray(0.5 - 0.5 * np.cos(2.0 * math.pi / length * np.arange(length)), np.float32)


def scalar(value):
    return jnp.reshape(value, (1,)).astype(jnp.int32)


def width_table(width, owners):
    half = width // 2
    phase = np.arange(half)[:, None] * np.arange(width)[None, :] % width
    angle = 2.0 * math.pi / width * phase
    factor = 1.0 / math.sqrt(width)
    cosine = np.cos(angle) * factor
    sine = -np.sin(angle) * factor
    sine[0] = np.where(np.arange(width) % 2 == 0, factor, -factor)
    shape = (owners, half // owners, width)
    table = np.stack([cosine.reshape(shape), sine.reshape(shape)], axis=1)
    return table.reshape(width, width).astype(jnp.bfloat16)


FINE = 32


def short_tables(height):
    column = np.arange(height)[None, :]
    rough = 2.0 * math.pi / height * (np.arange(height // FINE)[:, None] * FINE * column % height)
    small = 2.0 * math.pi / height * (np.arange(FINE)[:, None] * column % height)
    short = [np.cos(small), np.sin(small), np.cos(rough), np.sin(rough)]
    return jnp.asarray(np.concatenate(short), jnp.float32)


def scaled_tables(height, after):
    factor = 1.0 / math.sqrt(height)

    def body(short_ref, *refs):
        refs[-1][: 2 * FINE] = short_ref[: 2 * FINE]
        refs[-1][2 * FINE :] = short_ref[2 * FINE :] * factor

    short = short_tables(height)
    return pl.pallas_call(
        body,
        in_specs=[pl.BlockSpec(memory_space=pltpu.VMEM)]
        + [pl.BlockSpec(memory_space=pl.ANY)] * len(after),
        out_specs=pl.BlockSpec(memory_space=pltpu.VMEM),
        out_shape=jax.ShapeDtypeStruct(short.shape, short.dtype),
        compiler_params=params(),
        cost_estimate=cost(1 << 33, 8 * short.size),
        name="scaled_tables",
    )(short, *after)


def make_table(short_ref, out_ref, first, rows):
    height = short_ref.shape[1]
    coarse = height // FINE
    sc, ss = short_ref[:FINE], short_ref[FINE : 2 * FINE]
    for j in range(first // FINE, (first + rows) // FINE):
        a = 2 * FINE + j
        rc, rs = short_ref[a : a + 1, :], short_ref[a + coarse : a + coarse + 1, :]
        here = slice(j * FINE, (j + 1) * FINE)
        out_ref[here, :height] = (rc * sc - rs * ss).astype(jnp.bfloat16)
        out_ref[here, height:] = (rs * sc + rc * ss).astype(jnp.bfloat16)


def cost(flops, moved):
    return pl.CostEstimate(flops=flops, transcendentals=0, bytes_accessed=moved)


def params(limit=VMEM_LIMIT):
    return pltpu.CompilerParams(vmem_limit_bytes=limit)


def shade(tile, down_ref, across_ref):
    return (tile * (down_ref[...].T[:, :1] * across_ref[...])).astype(jnp.bfloat16)


def times_table(table, shaded):
    y = lax.dot_general(
        table, shaded, (((1,), (1,)), ((), ())), preferred_element_type=jnp.float32
    )
    return y.astype(jnp.bfloat16)


def near_columns(tiles, down, across, table, half, me, peers):
    count, rows, width = tiles.shape
    span = table.shape[0] // 2
    block = span // peers

    def body(half_ref, me_ref, tile_hbm, down_hbm, across_hbm, table_hbm, *refs):
        outs = refs[:2]
        tile_ref, table_ref, work, down_ref, across_ref, done = refs[2:]
        t = pl.program_id(0)
        me = me_ref[0]
        start = pl.multiple_of((1 - half_ref[0]) * span + me // 2 * 2 * block, 2 * block)
        fetch = pltpu.make_async_copy(
            table_hbm.at[pl.ds(start, 2 * block)], table_ref, done.at[count]
        )
        loads = [
            pltpu.make_async_copy(tile_hbm.at[i], tile_ref.at[i], done.at[i]) for i in range(count)
        ]

        lane = pl.multiple_of(me * rows, rows)
        extra = [
            pltpu.make_async_copy(down_hbm.at[:, pl.ds(lane, rows)], down_ref, done.at[count + 1]),
            pltpu.make_async_copy(across_hbm, across_ref, done.at[count + 2]),
        ]

        @pl.when(t == 0)
        def _():
            for copy in extra:
                copy.start()
            fetch.start()
            for load in loads:
                load.start()
            for copy in extra:
                copy.wait()
            fetch.wait()

        for i in range(count):

            @pl.when(t == i)
            def _():
                loads[i].wait()
                work[...] = times_table(table_ref[...], shade(tile_ref[i], down_ref, across_ref))

        for k in range(2):
            place = pl.multiple_of((me % 2 ^ k) * block, block)
            outs[k][0] = work[pl.ds(place, block), :]

    return pl.pallas_call(
        body,
        grid_spec=pltpu.PrefetchScalarGridSpec(
            num_scalar_prefetch=2,
            grid=(count,),
            in_specs=[
                pl.BlockSpec(memory_space=pltpu.HBM),
                pl.BlockSpec(memory_space=pltpu.HBM),
                pl.BlockSpec(memory_space=pltpu.HBM),
                pl.BlockSpec(memory_space=pltpu.HBM),
            ],
            out_specs=[pl.BlockSpec((1, block, rows), lambda t, half, me: (t, 0, 0))] * 2,
            scratch_shapes=[
                pltpu.VMEM((count, rows, width), tiles.dtype),
                pltpu.VMEM((2 * block, width), table.dtype),
                pltpu.VMEM((2 * block, rows), jnp.bfloat16),
                pltpu.VMEM((8, rows), jnp.float32),
                pltpu.VMEM((1, width), jnp.float32),
                pltpu.SemaphoreType.DMA((count + 3,)),
            ],
        ),
        out_shape=[jax.ShapeDtypeStruct((count, block, rows), jnp.bfloat16)] * 2,
        compiler_params=params(FIRST_LIMIT),
        cost_estimate=cost(4 * count * rows * width * block, 4 * tiles.size + 4 * block * width),
        name="near_columns",
    )(scalar(half), scalar(me), tiles, down, across, table)


def rest_columns(tiles, down, across, table, half, me, peers):
    count, rows, width = tiles.shape
    span = table.shape[0] // 2
    block = span // peers

    def body(half_ref, me_ref, tile_ref, down_ref, across_ref, table_ref, *refs):
        out_ref, far, work = refs[0], refs[1:-1], refs[-1]
        half, me = half_ref[0], me_ref[0]
        shaded = shade(tile_ref[0], down_ref, across_ref)
        for j in range(1, peers // 2):
            start = pl.multiple_of((1 - half) * span + (me // 2 ^ j) * 2 * block, 2 * block)
            work[...] = times_table(table_ref[pl.ds(start, 2 * block), :], shaded)
            for k in range(2):
                place = pl.multiple_of((me % 2 ^ k) * block, block)
                far[2 * j - 2 + k][0] = work[pl.ds(place, block), :]
        start = pl.multiple_of(half * span, span)
        y = times_table(table_ref[pl.ds(start, span), :], shaded)
        out_ref[:, 0] = y.reshape(peers, block, rows)

    piece = pl.BlockSpec((1, block, rows), lambda t, half, me: (t, 0, 0))
    return pl.pallas_call(
        body,
        grid_spec=pltpu.PrefetchScalarGridSpec(
            num_scalar_prefetch=2,
            grid=(count,),
            in_specs=[
                pl.BlockSpec((1, rows, width), lambda t, half, me: (t, 0, 0)),
                pl.BlockSpec((8, rows), lambda t, half, me: (0, me[0])),
                pl.BlockSpec((1, width), lambda t, half, me: (0, 0)),
                pl.BlockSpec((width, width), lambda t, half, me: (0, 0)),
            ],
            out_specs=[
                pl.BlockSpec((peers, 1, block, rows), lambda t, half, me: (0, t, 0, 0)),
                *[piece] * (peers - 2),
            ],
            scratch_shapes=[pltpu.VMEM((2 * block, rows), jnp.bfloat16)],
        ),
        out_shape=[
            jax.ShapeDtypeStruct((peers, count, block, rows), jnp.bfloat16),
            *[jax.ShapeDtypeStruct((count, block, rows), jnp.bfloat16)] * (peers - 2),
        ],
        compiler_params=params(),
        cost_estimate=cost(3 * count * rows * width * span, 4 * tiles.size + 2 * width * width),
        name="rest_columns",
    )(scalar(half), scalar(me), tiles, down, across, table)


def gather_rows(pieces, table_ref, me, first=0, total=None):
    for k, piece in enumerate(pieces, first):
        count, block, rows = piece.shape
        start = pl.multiple_of((me ^ k) * rows, rows)
        term = jnp.dot(
            piece[...].reshape(count * block, rows),
            table_ref[pl.ds(start, rows), :],
            preferred_element_type=jnp.float32,
        )
        total = term if total is None else total + term
    return total


def holds_packed(place):
    half_ref, me_ref = place
    return (half_ref[0] == 0) & (me_ref[0] == 0)


def store_spectra(s_ref, total, spectra, edge, first):
    block = spectra.shape[2]
    height = spectra.shape[3]
    row = lax.broadcasted_iota(jnp.int32, (block, height), 0)
    packed = (row == 0) & holds_packed(s_ref)
    for t in range(total.shape[0] // (2 * block)):
        real = total[2 * t * block : (2 * t + 1) * block]
        imag = total[(2 * t + 1) * block : (2 * t + 2) * block]
        cr, sr = real[:, :height], real[:, height:]
        ci, si = imag[:, :height], imag[:, height:]
        spectra[first + t, 0] = jnp.where(packed, cr, cr + si).astype(jnp.bfloat16)
        spectra[first + t, 1] = jnp.where(packed, -sr, ci - sr).astype(jnp.bfloat16)
        edge[first + t, 0] = ci[:16].astype(jnp.bfloat16)
        edge[first + t, 1] = (-si[:16]).astype(jnp.bfloat16)


def normalised(left_real, left_imag, right_real, right_imag):
    lr = left_real.astype(jnp.float32)
    li = left_imag.astype(jnp.float32)
    rr = right_real.astype(jnp.float32)
    ri = right_imag.astype(jnp.float32)
    cross_real = lr * rr + li * ri
    cross_imag = li * rr - lr * ri
    factor = 1.0 / (jnp.sqrt(cross_real * cross_real + cross_imag * cross_imag) + FLOOR)
    return (
        (cross_real * factor).astype(jnp.bfloat16),
        (cross_imag * factor).astype(jnp.bfloat16),
    )


def correlate(s_ref, picks, spectra, edge, phases):
    slots = len(picks)
    height = spectra.shape[3]
    lead = lax.broadcasted_iota(jnp.int32, (16, height), 0)
    packed = (lead == 0) & holds_packed(s_ref)
    for p in range(slots):
        a, c = picks[p]
        q_real, q_imag = normalised(spectra[a, 0], spectra[a, 1], spectra[c, 0], spectra[c, 1])
        e_real, e_imag = normalised(edge[a, 0], edge[a, 1], edge[c, 0], edge[c, 1])
        phases[2 * p] = q_real
        phases[2 * p + 1] = q_imag
        top_real = q_real[:16].astype(jnp.float32)
        top_imag = q_imag[:16].astype(jnp.float32)
        mixed_real = jnp.where(packed, top_real - e_imag.astype(jnp.float32), top_real)
        mixed_imag = jnp.where(packed, top_imag + e_real.astype(jnp.float32), top_imag)
        phases[2 * p, :16] = mixed_real.astype(jnp.bfloat16)
        phases[2 * p + 1, :16] = mixed_imag.astype(jnp.bfloat16)

def invert_columns(s_ref, me, phases, table_ref, outs):
    _, block, height = phases.shape
    slots = phases.shape[0] // 2
    rows = next(iter(outs.values())).shape[2]
    row = lax.broadcasted_iota(jnp.int32, (block, rows), 0)
    twice = jnp.where((row == 0) & holds_packed(s_ref), 1.0, 2.0)
    flat = phases[...].reshape(2 * slots * block, height)
    for k, out in outs.items():
        start = pl.multiple_of((me ^ k) * rows, rows)
        c_part = jnp.dot(
            flat, table_ref[:, pl.ds(start, rows)], preferred_element_type=jnp.float32
        )
        start = pl.multiple_of(height + (me ^ k) * rows, rows)
        s_part = jnp.dot(
            flat, table_ref[:, pl.ds(start, rows)], preferred_element_type=jnp.float32
        )
        for p in range(slots):
            re = slice(2 * p * block, (2 * p + 1) * block)
            im = slice((2 * p + 1) * block, (2 * p + 2) * block)
            out[p, :block] = ((c_part[re] - s_part[im]) * twice).astype(jnp.bfloat16)
            out[p, block:] = ((s_part[re] + c_part[im]) * twice).astype(jnp.bfloat16)


def own_spectra(place, pieces, near, short):
    peers, count, double, rows = pieces.shape
    height = peers * rows

    def body(half_ref, me_ref, pieces_ref, near_a, near_b, short_ref, spectra, edge, share, table_ref):
        total = None
        for k in range(peers):
            make_table(short_ref, table_ref, k * rows, rows)
            term = jnp.dot(
                pieces_ref[k].reshape(count * double, rows),
                table_ref[k * rows : (k + 1) * rows],
                preferred_element_type=jnp.float32,
            )
            total = term if total is None else total + term
        store_spectra((half_ref, me_ref), total, spectra, edge, 0)
        share[...] = gather_rows([near_a, near_b], table_ref, me_ref[0])

    return pl.pallas_call(
        body,
        in_specs=[pl.BlockSpec(memory_space=pltpu.SMEM)] * 2
        + [pl.BlockSpec(memory_space=pltpu.VMEM)] * 4,
        out_specs=[pl.BlockSpec(memory_space=pltpu.VMEM)] * 4,
        out_shape=[
            jax.ShapeDtypeStruct((count, 2, double // 2, height), jnp.bfloat16),
            jax.ShapeDtypeStruct((count, 2, 16, height), jnp.bfloat16),
            jax.ShapeDtypeStruct((count * double, 2 * height), jnp.float32),
            jax.ShapeDtypeStruct((height, 2 * height), jnp.bfloat16),
        ],
        compiler_params=params(),
        cost_estimate=cost(6 * count * double * height * height, 8 * height * height),
        name="own_spectra",
    )(*place, pieces, *near, short)


def partner_slots(place, theirs, pieces, share, table, spectra, edge):
    distant = len(pieces)
    count, double, rows = pieces[0].shape
    height = table.shape[0]
    block = double // 2
    slots = theirs.shape[1]

    def body(half_ref, me_ref, theirs_ref, *refs):
        s_ref = (half_ref, me_ref)
        me = me_ref[0]
        picks = [
            [(theirs_ref[0, p, i] + count) % (2 * count) for i in range(2)] for p in range(slots)
        ]
        inputs = refs[:distant]
        share_ref, table_ref, own_ref, own_edge, near, every, edges, phases = refs[distant:]
        every[:count] = own_ref[...]
        edges[:count] = own_edge[...]
        total = gather_rows(inputs, table_ref, me, 2, share_ref[...])
        store_spectra(s_ref, total, every, edges, count)
        correlate(s_ref, picks, every, edges, phases)
        invert_columns(s_ref, me, phases, table_ref, {k: near.at[k] for k in range(2)})

    return pl.pallas_call(
        body,
        in_specs=[pl.BlockSpec(memory_space=pltpu.SMEM)] * 3
        + [pl.BlockSpec(memory_space=pltpu.VMEM)] * (distant + 4),
        out_specs=[pl.BlockSpec(memory_space=pltpu.VMEM)] * 4,
        out_shape=[
            jax.ShapeDtypeStruct((2, slots, double, rows), jnp.bfloat16),
            jax.ShapeDtypeStruct((2 * count, 2, block, height), jnp.bfloat16),
            jax.ShapeDtypeStruct((2 * count, 2, 16, height), jnp.bfloat16),
            jax.ShapeDtypeStruct((2 * slots, block, height), jnp.bfloat16),
        ],
        compiler_params=params(),
        cost_estimate=cost(4 * (count + slots) * double * height * height, 8 * height * height),
        name="partner_slots",
    )(*place, theirs, *pieces, share, table, spectra, edge)


def own_slots(place, pairs, table, spectra, edge, phases, peers):
    block, height = spectra.shape[2:]
    rows = height // peers
    slots = pairs.shape[1]

    def body(half_ref, me_ref, pairs_ref, table_ref, every, edges, theirs, out_ref, *refs):
        s_ref = (half_ref, me_ref)
        far, work = refs[:-1], refs[-1]
        picks = [[pairs_ref[0, p, i] for i in range(2)] for p in range(slots)]
        if far:
            outs = {k: far[k - 2] for k in range(2, peers)}
            invert_columns(s_ref, me_ref[0], theirs, table_ref, outs)
        correlate(s_ref, picks, every, edges, work)
        invert_columns(s_ref, 0, work, table_ref, {k: out_ref.at[k] for k in range(peers)})

    return pl.pallas_call(
        body,
        in_specs=[pl.BlockSpec(memory_space=pltpu.SMEM)] * 3
        + [pl.BlockSpec(memory_space=pltpu.VMEM)] * 4,
        out_specs=[pl.BlockSpec(memory_space=pltpu.VMEM)] * (peers - 1),
        out_shape=[
            jax.ShapeDtypeStruct((peers, slots, 2 * block, rows), jnp.bfloat16),
            *[jax.ShapeDtypeStruct((slots, 2 * block, rows), jnp.bfloat16)] * (peers - 2),
        ],
        scratch_shapes=[pltpu.VMEM((2 * slots, block, height), jnp.bfloat16)],
        compiler_params=params(),
        cost_estimate=cost(8 * slots * block * height * height, 8 * height * height),
        name="own_slots",
    )(*place, pairs, table, spectra, edge, phases)


def own_surfaces(half, own, table):
    peers, slots, double, rows = own.shape
    width = table.shape[0]
    span = peers * double

    def body(half_ref, own_ref, table_ref, out_ref):
        out_ref[0] = lax.dot_general(
            own_ref[:, 0].reshape(span, rows),
            table_ref[...],
            (((0,), (0,)), ((), ())),
            preferred_element_type=jnp.float32,
        )

    return pl.pallas_call(
        body,
        grid_spec=pltpu.PrefetchScalarGridSpec(
            num_scalar_prefetch=1,
            grid=(slots,),
            in_specs=[
                pl.BlockSpec((peers, 1, double, rows), lambda p, half: (0, p, 0, 0)),
                pl.BlockSpec((span, width), lambda p, half: (half[0], 0)),
            ],
            out_specs=pl.BlockSpec((1, rows, width), lambda p, half: (p, 0, 0)),
        ),
        out_shape=jax.ShapeDtypeStruct((slots, rows, width), jnp.float32),
        compiler_params=params(),
        cost_estimate=cost(2 * slots * rows * width * span, 4 * slots * rows * width),
        name="own_surfaces",
    )(scalar(half), own, table)


def surfaces_of(half, me, counts, part, near, other, table):
    peers = 1 + len(other)
    slots, double, rows = other[0].shape
    width = table.shape[0]
    span = peers * double

    def body(half_ref, me_ref, counts_ref, part_ref, *refs):
        other_refs = refs[:peers]
        table_ref, out_ref, work = refs[peers:]
        for k in range(peers):
            place = pl.multiple_of((me_ref[0] ^ k) * double, double)
            piece = other_refs[k][0] if k else other_refs[k][0, 0]
            work[pl.ds(place, double), :] = piece
        rest = lax.dot_general(
            work[...], table_ref[...], (((0,), (0,)), ((), ())), preferred_element_type=jnp.float32
        )
        live = pl.program_id(0) < counts_ref[0]
        out_ref[0] = jnp.where(live, part_ref[0] + rest, 0.0)

    pair = pl.BlockSpec((1, 1, double, rows), lambda p, half, me, counts: (0, p, 0, 0))
    piece = pl.BlockSpec((1, double, rows), lambda p, half, me, counts: (p, 0, 0))
    plane = pl.BlockSpec((1, rows, width), lambda p, half, me, counts: (p, 0, 0))
    return pl.pallas_call(
        body,
        grid_spec=pltpu.PrefetchScalarGridSpec(
            num_scalar_prefetch=3,
            grid=(slots,),
            in_specs=[
                plane,
                pair,
                *[piece] * (peers - 1),
                pl.BlockSpec((span, width), lambda p, half, me, counts: (1 - half[0], 0)),
            ],
            out_specs=plane,
            scratch_shapes=[pltpu.VMEM((span, rows), jnp.bfloat16)],
        ),
        out_shape=jax.ShapeDtypeStruct((slots, rows, width), jnp.float32),
        compiler_params=params(),
        cost_estimate=cost(2 * slots * rows * width * span, 8 * slots * rows * width),
        name="surfaces",
    )(scalar(half), scalar(me), counts, part, near, *other, table)


def local(tiles, pairs, counts):
    groups = lax.axis_size("blk")
    peers = lax.axis_size("rows")
    group = lax.axis_index("blk")
    me = lax.axis_index("rows")
    count, rows, width = tiles.shape
    height = rows * peers
    turn = groups // 2
    half = group // turn
    axes = ("blk", "rows")

    def across(value, k):
        moves = [
            (b * peers + r, (b + turn) % groups * peers + (r ^ k))
            for b in range(groups)
            for r in range(peers)
        ]
        return lax.ppermute(value, axes, moves)

    def along(blocks):
        return lax.all_to_all(blocks, "rows", split_axis=0, concat_axis=0)

    def swap(value):
        return lax.ppermute(value, "rows", [(r, r ^ 1) for r in range(peers)])

    table_w = jnp.asarray(width_table(width, 2 * peers))
    down = jnp.asarray(np.tile(hann(height), (8, 1)))
    sideways = jnp.asarray(hann(width)[None, :])

    sent = near_columns(tiles, down, sideways, table_w, half, me, peers)
    arrived = [across(sent[k], k) for k in range(2)]
    *sent, held = lax.optimization_barrier((*sent, half))
    kept, *sent = rest_columns(tiles, down, sideways, table_w, held, me, peers)
    *sent, kept, pairs = lax.optimization_barrier((*sent, kept, pairs))
    arrived += [across(sent[k - 2], k) for k in range(2, peers)]
    mine = along(kept)

    theirs = across(pairs, 0)
    place = (scalar(half), scalar(me))
    spectra, edge, share, table_h = own_spectra(
        place, mine, arrived[:2], scaled_tables(height, [])
    )
    near, spectra, edge, phases = partner_slots(
        place, theirs, arrived[2:], share, table_h, spectra, edge
    )
    near = across(near, 0)
    own, *far = own_slots(place, pairs, table_h, spectra, edge, phases, peers)
    far = [across(far[k - 2], k) for k in range(2, peers)]
    part = own_surfaces(half, along(own), table_w)
    *far, part = lax.optimization_barrier((*far, part))
    return surfaces_of(half, me, counts, part, near, [swap(near[1]), *far], table_w)


def solution(mesh):
    from jax.sharding import PartitionSpec as P

    return jax.shard_map(
        local,
        mesh=mesh,
        in_specs=(
            P(("parts", "blk"), "rows", None),
            P(("parts", "blk"), None, None),
            P(("parts", "blk")),
        ),
        out_specs=P(("parts", "blk"), "rows", None),
        check_vma=False,
    )
```

```python
import math

import jax
import jax.numpy as jnp
import numpy as np
from jax import lax
from jax.experimental import pallas as pl
from jax.experimental.pallas import tpu as pltpu

FLOOR = 0.05
VMEM_LIMIT = 24 * 1024 * 1024
FIRST_LIMIT = 58 * 1024 * 1024


def hann(length):
    return np.asarray(0.5 - 0.5 * np.cos(2.0 * math.pi / length * np.arange(length)), np.float32)


def scalar(value):
    return jnp.reshape(value, (1,)).astype(jnp.int32)


def width_table(width, owners):
    half = width // 2
    phase = np.arange(half)[:, None] * np.arange(width)[None, :] % width
    angle = 2.0 * math.pi / width * phase
    factor = 1.0 / math.sqrt(width)
    cosine = np.cos(angle) * factor
    sine = -np.sin(angle) * factor
    sine[0] = np.where(np.arange(width) % 2 == 0, factor, -factor)
    shape = (owners, half // owners, width)
    table = np.stack([cosine.reshape(shape), sine.reshape(shape)], axis=1)
    return table.reshape(width, width).astype(jnp.bfloat16)


FINE = 32


def short_tables(height):
    column = np.arange(height)[None, :]
    rough = 2.0 * math.pi / height * (np.arange(height // FINE)[:, None] * FINE * column % height)
    small = 2.0 * math.pi / height * (np.arange(FINE)[:, None] * column % height)
    short = [np.cos(small), np.sin(small), np.cos(rough), np.sin(rough)]
    return jnp.asarray(np.concatenate(short), jnp.float32)


def scaled_tables(height, after):
    factor = 1.0 / math.sqrt(height)

    def body(short_ref, *refs):
        refs[-1][: 2 * FINE] = short_ref[: 2 * FINE]
        refs[-1][2 * FINE :] = short_ref[2 * FINE :] * factor

    short = short_tables(height)
    return pl.pallas_call(
        body,
        in_specs=[pl.BlockSpec(memory_space=pltpu.VMEM)]
        + [pl.BlockSpec(memory_space=pl.ANY)] * len(after),
        out_specs=pl.BlockSpec(memory_space=pltpu.VMEM),
        out_shape=jax.ShapeDtypeStruct(short.shape, short.dtype),
        compiler_params=params(),
        cost_estimate=cost(1 << 33, 8 * short.size),
        name="scaled_tables",
    )(short, *after)


def make_table(short_ref, out_ref, first, rows):
    height = short_ref.shape[1]
    coarse = height // FINE
    sc, ss = short_ref[:FINE], short_ref[FINE : 2 * FINE]
    for j in range(first // FINE, (first + rows) // FINE):
        a = 2 * FINE + j
        rc, rs = short_ref[a : a + 1, :], short_ref[a + coarse : a + coarse + 1, :]
        here = slice(j * FINE, (j + 1) * FINE)
        out_ref[here, :height] = (rc * sc - rs * ss).astype(jnp.bfloat16)
        out_ref[here, height:] = (rs * sc + rc * ss).astype(jnp.bfloat16)


def cost(flops, moved):
    return pl.CostEstimate(flops=flops, transcendentals=0, bytes_accessed=moved)


def params(limit=VMEM_LIMIT):
    return pltpu.CompilerParams(vmem_limit_bytes=limit)


def shade(tile, down_ref, across_ref):
    return (tile * (down_ref[...].T[:, :1] * across_ref[...])).astype(jnp.bfloat16)


def times_table(table, shaded):
    y = lax.dot_general(
        table, shaded, (((1,), (1,)), ((), ())), preferred_element_type=jnp.float32
    )
    return y.astype(jnp.bfloat16)


def near_columns(tiles, down, across, table, half, me, peers):
    count, rows, width = tiles.shape
    span = table.shape[0] // 2
    block = span // peers

    def body(half_ref, me_ref, tile_hbm, down_hbm, across_hbm, table_hbm, *refs):
        outs = refs[:2]
        tile_ref, table_ref, work, down_ref, across_ref, done = refs[2:]
        t = pl.program_id(0)
        me = me_ref[0]
        start = pl.multiple_of((1 - half_ref[0]) * span + me // 2 * 2 * block, 2 * block)
        fetch = pltpu.make_async_copy(
            table_hbm.at[pl.ds(start, 2 * block)], table_ref, done.at[count]
        )
        loads = [
            pltpu.make_async_copy(tile_hbm.at[i], tile_ref.at[i], done.at[i]) for i in range(count)
        ]

        lane = pl.multiple_of(me * rows, rows)
        extra = [
            pltpu.make_async_copy(down_hbm.at[:, pl.ds(lane, rows)], down_ref, done.at[count + 1]),
            pltpu.make_async_copy(across_hbm, across_ref, done.at[count + 2]),
        ]

        @pl.when(t == 0)
        def _():
            for copy in extra:
                copy.start()
            fetch.start()
            for load in loads:
                load.start()
            for copy in extra:
                copy.wait()
            fetch.wait()

        for i in range(count):

            @pl.when(t == i)
            def _():
                loads[i].wait()
                work[...] = times_table(table_ref[...], shade(tile_ref[i], down_ref, across_ref))

        for k in range(2):
            place = pl.multiple_of((me % 2 ^ k) * block, block)
            outs[k][0] = work[pl.ds(place, block), :]

    return pl.pallas_call(
        body,
        grid_spec=pltpu.PrefetchScalarGridSpec(
            num_scalar_prefetch=2,
            grid=(count,),
            in_specs=[
                pl.BlockSpec(memory_space=pltpu.HBM),
                pl.BlockSpec(memory_space=pltpu.HBM),
                pl.BlockSpec(memory_space=pltpu.HBM),
                pl.BlockSpec(memory_space=pltpu.HBM),
            ],
            out_specs=[pl.BlockSpec((1, block, rows), lambda t, half, me: (t, 0, 0))] * 2,
            scratch_shapes=[
                pltpu.VMEM((count, rows, width), tiles.dtype),
                pltpu.VMEM((2 * block, width), table.dtype),
                pltpu.VMEM((2 * block, rows), jnp.bfloat16),
                pltpu.VMEM((8, rows), jnp.float32),
                pltpu.VMEM((1, width), jnp.float32),
                pltpu.SemaphoreType.DMA((count + 3,)),
            ],
        ),
        out_shape=[jax.ShapeDtypeStruct((count, block, rows), jnp.bfloat16)] * 2,
        compiler_params=params(FIRST_LIMIT),
        cost_estimate=cost(4 * count * rows * width * block, 4 * tiles.size + 4 * block * width),
        name="near_columns",
    )(scalar(half), scalar(me), tiles, down, across, table)


def rest_columns(tiles, down, across, table, half, me, peers):
    count, rows, width = tiles.shape
    span = table.shape[0] // 2
    block = span // peers

    def body(half_ref, me_ref, tile_ref, down_ref, across_ref, table_ref, *refs):
        out_ref, far, work = refs[0], refs[1:-1], refs[-1]
        half, me = half_ref[0], me_ref[0]
        shaded = shade(tile_ref[0], down_ref, across_ref)
        for j in range(1, peers // 2):
            start = pl.multiple_of((1 - half) * span + (me // 2 ^ j) * 2 * block, 2 * block)
            work[...] = times_table(table_ref[pl.ds(start, 2 * block), :], shaded)
            for k in range(2):
                place = pl.multiple_of((me % 2 ^ k) * block, block)
                far[2 * j - 2 + k][0] = work[pl.ds(place, block), :]
        start = pl.multiple_of(half * span, span)
        y = times_table(table_ref[pl.ds(start, span), :], shaded)
        out_ref[:, 0] = y.reshape(peers, block, rows)

    piece = pl.BlockSpec((1, block, rows), lambda t, half, me: (t, 0, 0))
    return pl.pallas_call(
        body,
        grid_spec=pltpu.PrefetchScalarGridSpec(
            num_scalar_prefetch=2,
            grid=(count,),
            in_specs=[
                pl.BlockSpec((1, rows, width), lambda t, half, me: (t, 0, 0)),
                pl.BlockSpec((8, rows), lambda t, half, me: (0, me[0])),
                pl.BlockSpec((1, width), lambda t, half, me: (0, 0)),
                pl.BlockSpec((width, width), lambda t, half, me: (0, 0)),
            ],
            out_specs=[
                pl.BlockSpec((peers, 1, block, rows), lambda t, half, me: (0, t, 0, 0)),
                *[piece] * (peers - 2),
            ],
            scratch_shapes=[pltpu.VMEM((2 * block, rows), jnp.bfloat16)],
        ),
        out_shape=[
            jax.ShapeDtypeStruct((peers, count, block, rows), jnp.bfloat16),
            *[jax.ShapeDtypeStruct((count, block, rows), jnp.bfloat16)] * (peers - 2),
        ],
        compiler_params=params(),
        cost_estimate=cost(3 * count * rows * width * span, 4 * tiles.size + 2 * width * width),
        name="rest_columns",
    )(scalar(half), scalar(me), tiles, down, across, table)


def gather_rows(pieces, table_ref, me, first=0, total=None):
    for k, piece in enumerate(pieces, first):
        count, block, rows = piece.shape
        start = pl.multiple_of((me ^ k) * rows, rows)
        term = jnp.dot(
            piece[...].reshape(count * block, rows),
            table_ref[pl.ds(start, rows), :],
            preferred_element_type=jnp.float32,
        )
        total = term if total is None else total + term
    return total


def holds_packed(place):
    half_ref, me_ref = place
    return (half_ref[0] == 0) & (me_ref[0] == 0)


def store_spectra(s_ref, total, spectra, edge, first):
    block = spectra.shape[2]
    height = spectra.shape[3]
    row = lax.broadcasted_iota(jnp.int32, (block, height), 0)
    packed = (row == 0) & holds_packed(s_ref)
    for t in range(total.shape[0] // (2 * block)):
        real = total[2 * t * block : (2 * t + 1) * block]
        imag = total[(2 * t + 1) * block : (2 * t + 2) * block]
        cr, sr = real[:, :height], real[:, height:]
        ci, si = imag[:, :height], imag[:, height:]
        spectra[first + t, 0] = jnp.where(packed, cr, cr + si).astype(jnp.bfloat16)
        spectra[first + t, 1] = jnp.where(packed, -sr, ci - sr).astype(jnp.bfloat16)
        edge[first + t, 0] = ci[:16].astype(jnp.bfloat16)
        edge[first + t, 1] = (-si[:16]).astype(jnp.bfloat16)


def normalised(left_real, left_imag, right_real, right_imag):
    lr = left_real.astype(jnp.float32)
    li = left_imag.astype(jnp.float32)
    rr = right_real.astype(jnp.float32)
    ri = right_imag.astype(jnp.float32)
    cross_real = lr * rr + li * ri
    cross_imag = li * rr - lr * ri
    factor = 1.0 / (jnp.sqrt(cross_real * cross_real + cross_imag * cross_imag) + FLOOR)
    return (
        (cross_real * factor).astype(jnp.bfloat16),
        (cross_imag * factor).astype(jnp.bfloat16),
    )


def correlate(s_ref, picks, spectra, edge, phases):
    slots = len(picks)
    height = spectra.shape[3]
    lead = lax.broadcasted_iota(jnp.int32, (16, height), 0)
    packed = (lead == 0) & holds_packed(s_ref)
    for p in range(slots):
        a, c = picks[p]
        q_real, q_imag = normalised(spectra[a, 0], spectra[a, 1], spectra[c, 0], spectra[c, 1])
        e_real, e_imag = normalised(edge[a, 0], edge[a, 1], edge[c, 0], edge[c, 1])
        phases[2 * p] = q_real
        phases[2 * p + 1] = q_imag
        top_real = q_real[:16].astype(jnp.float32)
        top_imag = q_imag[:16].astype(jnp.float32)
        mixed_real = jnp.where(packed, top_real - e_imag.astype(jnp.float32), top_real)
        mixed_imag = jnp.where(packed, top_imag + e_real.astype(jnp.float32), top_imag)
        phases[2 * p, :16] = mixed_real.astype(jnp.bfloat16)
        phases[2 * p + 1, :16] = mixed_imag.astype(jnp.bfloat16)

def invert_columns(s_ref, me, phases, table_ref, outs):
    _, block, height = phases.shape
    slots = phases.shape[0] // 2
    rows = next(iter(outs.values())).shape[2]
    row = lax.broadcasted_iota(jnp.int32, (block, rows), 0)
    twice = jnp.where((row == 0) & holds_packed(s_ref), 1.0, 2.0)
    flat = phases[...].reshape(2 * slots * block, height)
    for k, out in outs.items():
        start = pl.multiple_of((me ^ k) * rows, rows)
        c_part = jnp.dot(
            flat, table_ref[:, pl.ds(start, rows)], preferred_element_type=jnp.float32
        )
        start = pl.multiple_of(height + (me ^ k) * rows, rows)
        s_part = jnp.dot(
            flat, table_ref[:, pl.ds(start, rows)], preferred_element_type=jnp.float32
        )
        for p in range(slots):
            re = slice(2 * p * block, (2 * p + 1) * block)
            im = slice((2 * p + 1) * block, (2 * p + 2) * block)
            out[p, :block] = ((c_part[re] - s_part[im]) * twice).astype(jnp.bfloat16)
            out[p, block:] = ((s_part[re] + c_part[im]) * twice).astype(jnp.bfloat16)


def own_spectra(place, pieces, near, short):
    peers, count, double, rows = pieces.shape
    height = peers * rows

    def body(half_ref, me_ref, pieces_ref, near_a, near_b, short_ref, spectra, edge, share, table_ref):
        total = None
        for k in range(peers):
            make_table(short_ref, table_ref, k * rows, rows)
            term = jnp.dot(
                pieces_ref[k].reshape(count * double, rows),
                table_ref[k * rows : (k + 1) * rows],
                preferred_element_type=jnp.float32,
            )
            total = term if total is None else total + term
        store_spectra((half_ref, me_ref), total, spectra, edge, 0)
        share[...] = gather_rows([near_a, near_b], table_ref, me_ref[0])

    return pl.pallas_call(
        body,
        in_specs=[pl.BlockSpec(memory_space=pltpu.SMEM)] * 2
        + [pl.BlockSpec(memory_space=pltpu.VMEM)] * 4,
        out_specs=[pl.BlockSpec(memory_space=pltpu.VMEM)] * 4,
        out_shape=[
            jax.ShapeDtypeStruct((count, 2, double // 2, height), jnp.bfloat16),
            jax.ShapeDtypeStruct((count, 2, 16, height), jnp.bfloat16),
            jax.ShapeDtypeStruct((count * double, 2 * height), jnp.float32),
            jax.ShapeDtypeStruct((height, 2 * height), jnp.bfloat16),
        ],
        compiler_params=params(),
        cost_estimate=cost(6 * count * double * height * height, 8 * height * height),
        name="own_spectra",
    )(*place, pieces, *near, short)


def partner_slots(place, theirs, pieces, share, table, spectra, edge):
    distant = len(pieces)
    count, double, rows = pieces[0].shape
    height = table.shape[0]
    block = double // 2
    slots = theirs.shape[1]

    def body(half_ref, me_ref, theirs_ref, *refs):
        s_ref = (half_ref, me_ref)
        me = me_ref[0]
        picks = [
            [(theirs_ref[0, p, i] + count) % (2 * count) for i in range(2)] for p in range(slots)
        ]
        inputs = refs[:distant]
        share_ref, table_ref, own_ref, own_edge, near, every, edges, phases = refs[distant:]
        every[:count] = own_ref[...]
        edges[:count] = own_edge[...]
        total = gather_rows(inputs, table_ref, me, 2, share_ref[...])
        store_spectra(s_ref, total, every, edges, count)
        correlate(s_ref, picks, every, edges, phases)
        invert_columns(s_ref, me, phases, table_ref, {k: near.at[k] for k in range(2)})

    return pl.pallas_call(
        body,
        in_specs=[pl.BlockSpec(memory_space=pltpu.SMEM)] * 3
        + [pl.BlockSpec(memory_space=pltpu.VMEM)] * (distant + 4),
        out_specs=[pl.BlockSpec(memory_space=pltpu.VMEM)] * 4,
        out_shape=[
            jax.ShapeDtypeStruct((2, slots, double, rows), jnp.bfloat16),
            jax.ShapeDtypeStruct((2 * count, 2, block, height), jnp.bfloat16),
            jax.ShapeDtypeStruct((2 * count, 2, 16, height), jnp.bfloat16),
            jax.ShapeDtypeStruct((2 * slots, block, height), jnp.bfloat16),
        ],
        compiler_params=params(),
        cost_estimate=cost(4 * (count + slots) * double * height * height, 8 * height * height),
        name="partner_slots",
    )(*place, theirs, *pieces, share, table, spectra, edge)


def own_slots(place, pairs, table, spectra, edge, phases, peers):
    block, height = spectra.shape[2:]
    rows = height // peers
    slots = pairs.shape[1]

    def body(half_ref, me_ref, pairs_ref, table_ref, every, edges, theirs, out_ref, *refs):
        s_ref = (half_ref, me_ref)
        far, work = refs[:-1], refs[-1]
        picks = [[pairs_ref[0, p, i] for i in range(2)] for p in range(slots)]
        if far:
            outs = {k: far[k - 2] for k in range(2, peers)}
            invert_columns(s_ref, me_ref[0], theirs, table_ref, outs)
        correlate(s_ref, picks, every, edges, work)
        invert_columns(s_ref, 0, work, table_ref, {k: out_ref.at[k] for k in range(peers)})

    return pl.pallas_call(
        body,
        in_specs=[pl.BlockSpec(memory_space=pltpu.SMEM)] * 3
        + [pl.BlockSpec(memory_space=pltpu.VMEM)] * 4,
        out_specs=[pl.BlockSpec(memory_space=pltpu.VMEM)] * (peers - 1),
        out_shape=[
            jax.ShapeDtypeStruct((peers, slots, 2 * block, rows), jnp.bfloat16),
            *[jax.ShapeDtypeStruct((slots, 2 * block, rows), jnp.bfloat16)] * (peers - 2),
        ],
        scratch_shapes=[pltpu.VMEM((2 * slots, block, height), jnp.bfloat16)],
        compiler_params=params(),
        cost_estimate=cost(8 * slots * block * height * height, 8 * height * height),
        name="own_slots",
    )(*place, pairs, table, spectra, edge, phases)


def own_surfaces(half, own, table):
    peers, slots, double, rows = own.shape
    width = table.shape[0]
    span = peers * double

    def body(half_ref, own_ref, table_ref, out_ref):
        out_ref[0] = lax.dot_general(
            own_ref[:, 0].reshape(span, rows),
            table_ref[...],
            (((0,), (0,)), ((), ())),
            preferred_element_type=jnp.float32,
        )

    return pl.pallas_call(
        body,
        grid_spec=pltpu.PrefetchScalarGridSpec(
            num_scalar_prefetch=1,
            grid=(slots,),
            in_specs=[
                pl.BlockSpec((peers, 1, double, rows), lambda p, half: (0, p, 0, 0)),
                pl.BlockSpec((span, width), lambda p, half: (half[0], 0)),
            ],
            out_specs=pl.BlockSpec((1, rows, width), lambda p, half: (p, 0, 0)),
        ),
        out_shape=jax.ShapeDtypeStruct((slots, rows, width), jnp.float32),
        compiler_params=params(),
        cost_estimate=cost(2 * slots * rows * width * span, 4 * slots * rows * width),
        name="own_surfaces",
    )(scalar(half), own, table)


def surfaces_of(half, me, counts, part, near, other, table):
    peers = 1 + len(other)
    slots, double, rows = other[0].shape
    width = table.shape[0]
    span = peers * double

    def body(half_ref, me_ref, counts_ref, part_ref, *refs):
        other_refs = refs[:peers]
        table_ref, out_ref, work = refs[peers:]
        for k in range(peers):
            place = pl.multiple_of((me_ref[0] ^ k) * double, double)
            piece = other_refs[k][0] if k else other_refs[k][0, 0]
            work[pl.ds(place, double), :] = piece
        rest = lax.dot_general(
            work[...], table_ref[...], (((0,), (0,)), ((), ())), preferred_element_type=jnp.float32
        )
        live = pl.program_id(0) < counts_ref[0]
        out_ref[0] = jnp.where(live, part_ref[0] + rest, 0.0)

    pair = pl.BlockSpec((1, 1, double, rows), lambda p, half, me, counts: (0, p, 0, 0))
    piece = pl.BlockSpec((1, double, rows), lambda p, half, me, counts: (p, 0, 0))
    plane = pl.BlockSpec((1, rows, width), lambda p, half, me, counts: (p, 0, 0))
    return pl.pallas_call(
        body,
        grid_spec=pltpu.PrefetchScalarGridSpec(
            num_scalar_prefetch=3,
            grid=(slots,),
            in_specs=[
                plane,
                pair,
                *[piece] * (peers - 1),
                pl.BlockSpec((span, width), lambda p, half, me, counts: (1 - half[0], 0)),
            ],
            out_specs=plane,
            scratch_shapes=[pltpu.VMEM((span, rows), jnp.bfloat16)],
        ),
        out_shape=jax.ShapeDtypeStruct((slots, rows, width), jnp.float32),
        compiler_params=params(),
        cost_estimate=cost(2 * slots * rows * width * span, 8 * slots * rows * width),
        name="surfaces",
    )(scalar(half), scalar(me), counts, part, near, *other, table)


def local(tiles, pairs, counts):
    groups = lax.axis_size("blk")
    peers = lax.axis_size("rows")
    group = lax.axis_index("blk")
    me = lax.axis_index("rows")
    count, rows, width = tiles.shape
    height = rows * peers
    turn = groups // 2
    half = group // turn
    axes = ("blk", "rows")

    def across(value, k):
        moves = [
            (b * peers + r, (b + turn) % groups * peers + (r ^ k))
            for b in range(groups)
            for r in range(peers)
        ]
        return lax.ppermute(value, axes, moves)

    def along(blocks):
        return lax.all_to_all(blocks, "rows", split_axis=0, concat_axis=0)

    def swap(value):
        return lax.ppermute(value, "rows", [(r, r ^ 1) for r in range(peers)])

    table_w = jnp.asarray(width_table(width, 2 * peers))
    down = jnp.asarray(np.tile(hann(height), (8, 1)))
    sideways = jnp.asarray(hann(width)[None, :])

    sent = near_columns(tiles, down, sideways, table_w, half, me, peers)
    arrived = [across(sent[k], k) for k in range(2)]
    *sent, held = lax.optimization_barrier((*sent, half))
    kept, *sent = rest_columns(tiles, down, sideways, table_w, held, me, peers)
    *sent, kept, pairs = lax.optimization_barrier((*sent, kept, pairs))
    arrived += [across(sent[k - 2], k) for k in range(2, peers)]
    mine = along(kept)

    theirs = across(pairs, 0)
    place = (scalar(half), scalar(me))
    spectra, edge, share, table_h = own_spectra(
        place, mine, arrived[:2], scaled_tables(height, [])
    )
    near, spectra, edge, phases = partner_slots(
        place, theirs, arrived[2:], share, table_h, spectra, edge
    )
    near = across(near, 0)
    own, *far = own_slots(place, pairs, table_h, spectra, edge, phases, peers)
    far = [across(far[k - 2], k) for k in range(2, peers)]
    part = own_surfaces(half, along(own), table_w)
    *far, part = lax.optimization_barrier((*far, part))
    return surfaces_of(half, me, counts, part, near, [swap(near[1]), *far], table_w)


def solution(mesh):
    from jax.sharding import PartitionSpec as P

    return jax.shard_map(
        local,
        mesh=mesh,
        in_specs=(
            P(("parts", "blk"), "rows", None),
            P(("parts", "blk"), None, None),
            P(("parts", "blk")),
        ),
        out_specs=P(("parts", "blk"), "rows", None),
        check_vma=False,
    )
```

```python
import math

import jax
import jax.numpy as jnp
import numpy as np
from jax import lax
from jax.experimental import pallas as pl
from jax.experimental.pallas import tpu as pltpu

FLOOR = 0.05
VMEM_LIMIT = 24 * 1024 * 1024
FIRST_LIMIT = 58 * 1024 * 1024


def hann(length):
    return np.asarray(0.5 - 0.5 * np.cos(2.0 * math.pi / length * np.arange(length)), np.float32)


def scalar(value):
    return jnp.reshape(value, (1,)).astype(jnp.int32)


def width_table(width, owners):
    half = width // 2
    phase = np.arange(half)[:, None] * np.arange(width)[None, :] % width
    angle = 2.0 * math.pi / width * phase
    factor = 1.0 / math.sqrt(width)
    cosine = np.cos(angle) * factor
    sine = -np.sin(angle) * factor
    sine[0] = np.where(np.arange(width) % 2 == 0, factor, -factor)
    shape = (owners, half // owners, width)
    table = np.stack([cosine.reshape(shape), sine.reshape(shape)], axis=1)
    return table.reshape(width, width).astype(jnp.bfloat16)


FINE = 32


def short_tables(height):
    column = np.arange(height)[None, :]
    rough = 2.0 * math.pi / height * (np.arange(height // FINE)[:, None] * FINE * column % height)
    small = 2.0 * math.pi / height * (np.arange(FINE)[:, None] * column % height)
    short = [np.cos(small), np.sin(small), np.cos(rough), np.sin(rough)]
    return jnp.asarray(np.concatenate(short), jnp.float32)


def scaled_tables(height, after):
    factor = 1.0 / math.sqrt(height)

    def body(short_ref, *refs):
        refs[-1][: 2 * FINE] = short_ref[: 2 * FINE]
        refs[-1][2 * FINE :] = short_ref[2 * FINE :] * factor

    short = short_tables(height)
    return pl.pallas_call(
        body,
        in_specs=[pl.BlockSpec(memory_space=pltpu.VMEM)]
        + [pl.BlockSpec(memory_space=pl.ANY)] * len(after),
        out_specs=pl.BlockSpec(memory_space=pltpu.VMEM),
        out_shape=jax.ShapeDtypeStruct(short.shape, short.dtype),
        compiler_params=params(),
        cost_estimate=cost(1 << 33, 8 * short.size),
        name="scaled_tables",
    )(short, *after)


def make_table(short_ref, out_ref, first, rows):
    height = short_ref.shape[1]
    coarse = height // FINE
    sc, ss = short_ref[:FINE], short_ref[FINE : 2 * FINE]
    for j in range(first // FINE, (first + rows) // FINE):
        a = 2 * FINE + j
        rc, rs = short_ref[a : a + 1, :], short_ref[a + coarse : a + coarse + 1, :]
        here = slice(j * FINE, (j + 1) * FINE)
        out_ref[here, :height] = (rc * sc - rs * ss).astype(jnp.bfloat16)
        out_ref[here, height:] = (rs * sc + rc * ss).astype(jnp.bfloat16)


def cost(flops, moved):
    return pl.CostEstimate(flops=flops, transcendentals=0, bytes_accessed=moved)


def params(limit=VMEM_LIMIT):
    return pltpu.CompilerParams(vmem_limit_bytes=limit)


def shade(tile, down_ref, across_ref):
    return (tile * (down_ref[...].T[:, :1] * across_ref[...])).astype(jnp.bfloat16)


def times_table(table, shaded):
    y = lax.dot_general(
        table, shaded, (((1,), (1,)), ((), ())), preferred_element_type=jnp.float32
    )
    return y.astype(jnp.bfloat16)


def near_columns(tiles, down, across, table, half, me, peers):
    count, rows, width = tiles.shape
    span = table.shape[0] // 2
    block = span // peers

    def body(half_ref, me_ref, tile_hbm, down_hbm, across_hbm, table_hbm, *refs):
        outs = refs[:2]
        tile_ref, table_ref, work, down_ref, across_ref, done = refs[2:]
        t = pl.program_id(0)
        me = me_ref[0]
        start = pl.multiple_of((1 - half_ref[0]) * span + me // 2 * 2 * block, 2 * block)
        fetch = pltpu.make_async_copy(
            table_hbm.at[pl.ds(start, 2 * block)], table_ref, done.at[count]
        )
        loads = [
            pltpu.make_async_copy(tile_hbm.at[i], tile_ref.at[i], done.at[i]) for i in range(count)
        ]

        lane = pl.multiple_of(me * rows, rows)
        extra = [
            pltpu.make_async_copy(down_hbm.at[:, pl.ds(lane, rows)], down_ref, done.at[count + 1]),
            pltpu.make_async_copy(across_hbm, across_ref, done.at[count + 2]),
        ]

        @pl.when(t == 0)
        def _():
            for copy in extra:
                copy.start()
            fetch.start()
            for load in loads:
                load.start()
            for copy in extra:
                copy.wait()
            fetch.wait()

        for i in range(count):

            @pl.when(t == i)
            def _():
                loads[i].wait()
                work[...] = times_table(table_ref[...], shade(tile_ref[i], down_ref, across_ref))

        for k in range(2):
            place = pl.multiple_of((me % 2 ^ k) * block, block)
            outs[k][0] = work[pl.ds(place, block), :]

    return pl.pallas_call(
        body,
        grid_spec=pltpu.PrefetchScalarGridSpec(
            num_scalar_prefetch=2,
            grid=(count,),
            in_specs=[
                pl.BlockSpec(memory_space=pltpu.HBM),
                pl.BlockSpec(memory_space=pltpu.HBM),
                pl.BlockSpec(memory_space=pltpu.HBM),
                pl.BlockSpec(memory_space=pltpu.HBM),
            ],
            out_specs=[pl.BlockSpec((1, block, rows), lambda t, half, me: (t, 0, 0))] * 2,
            scratch_shapes=[
                pltpu.VMEM((count, rows, width), tiles.dtype),
                pltpu.VMEM((2 * block, width), table.dtype),
                pltpu.VMEM((2 * block, rows), jnp.bfloat16),
                pltpu.VMEM((8, rows), jnp.float32),
                pltpu.VMEM((1, width), jnp.float32),
                pltpu.SemaphoreType.DMA((count + 3,)),
            ],
        ),
        out_shape=[jax.ShapeDtypeStruct((count, block, rows), jnp.bfloat16)] * 2,
        compiler_params=params(FIRST_LIMIT),
        cost_estimate=cost(4 * count * rows * width * block, 4 * tiles.size + 4 * block * width),
        name="near_columns",
    )(scalar(half), scalar(me), tiles, down, across, table)


def rest_columns(tiles, down, across, table, half, me, peers):
    count, rows, width = tiles.shape
    span = table.shape[0] // 2
    block = span // peers

    def body(half_ref, me_ref, tile_ref, down_ref, across_ref, table_ref, *refs):
        out_ref, far, work = refs[0], refs[1:-1], refs[-1]
        half, me = half_ref[0], me_ref[0]
        shaded = shade(tile_ref[pl.program_id(0)], down_ref, across_ref)
        for j in range(1, peers // 2):
            start = pl.multiple_of((1 - half) * span + (me // 2 ^ j) * 2 * block, 2 * block)
            work[...] = times_table(table_ref[pl.ds(start, 2 * block), :], shaded)
            for k in range(2):
                place = pl.multiple_of((me % 2 ^ k) * block, block)
                far[2 * j - 2 + k][0] = work[pl.ds(place, block), :]
        start = pl.multiple_of(half * span, span)
        y = times_table(table_ref[pl.ds(start, span), :], shaded)
        out_ref[:, 0] = y.reshape(peers, block, rows)

    piece = pl.BlockSpec((1, block, rows), lambda t, half, me: (t, 0, 0))
    return pl.pallas_call(
        body,
        grid_spec=pltpu.PrefetchScalarGridSpec(
            num_scalar_prefetch=2,
            grid=(count,),
            in_specs=[
                pl.BlockSpec(memory_space=pltpu.VMEM),
                pl.BlockSpec((8, rows), lambda t, half, me: (0, me[0])),
                pl.BlockSpec((1, width), lambda t, half, me: (0, 0)),
                pl.BlockSpec(memory_space=pltpu.VMEM),
            ],
            out_specs=[
                pl.BlockSpec((peers, 1, block, rows), lambda t, half, me: (0, t, 0, 0)),
                *[piece] * (peers - 2),
            ],
            scratch_shapes=[pltpu.VMEM((2 * block, rows), jnp.bfloat16)],
        ),
        out_shape=[
            jax.ShapeDtypeStruct((peers, count, block, rows), jnp.bfloat16),
            *[jax.ShapeDtypeStruct((count, block, rows), jnp.bfloat16)] * (peers - 2),
        ],
        compiler_params=params(),
        cost_estimate=cost(3 * count * rows * width * span, 4 * tiles.size + 2 * width * width),
        name="rest_columns",
    )(scalar(half), scalar(me), tiles, down, across, table)


def gather_rows(pieces, table_ref, me, first=0, total=None):
    for k, piece in enumerate(pieces, first):
        count, block, rows = piece.shape
        start = pl.multiple_of((me ^ k) * rows, rows)
        term = jnp.dot(
            piece[...].reshape(count * block, rows),
            table_ref[pl.ds(start, rows), :],
            preferred_element_type=jnp.float32,
        )
        total = term if total is None else total + term
    return total


def holds_packed(place):
    half_ref, me_ref = place
    return (half_ref[0] == 0) & (me_ref[0] == 0)


def store_spectra(s_ref, total, spectra, edge, first):
    block = spectra.shape[2]
    height = spectra.shape[3]
    row = lax.broadcasted_iota(jnp.int32, (block, height), 0)
    packed = (row == 0) & holds_packed(s_ref)
    for t in range(total.shape[0] // (2 * block)):
        real = total[2 * t * block : (2 * t + 1) * block]
        imag = total[(2 * t + 1) * block : (2 * t + 2) * block]
        cr, sr = real[:, :height], real[:, height:]
        ci, si = imag[:, :height], imag[:, height:]
        spectra[first + t, 0] = jnp.where(packed, cr, cr + si).astype(jnp.bfloat16)
        spectra[first + t, 1] = jnp.where(packed, -sr, ci - sr).astype(jnp.bfloat16)
        edge[first + t, 0] = ci[:16].astype(jnp.bfloat16)
        edge[first + t, 1] = (-si[:16]).astype(jnp.bfloat16)


def normalised(left_real, left_imag, right_real, right_imag):
    lr = left_real.astype(jnp.float32)
    li = left_imag.astype(jnp.float32)
    rr = right_real.astype(jnp.float32)
    ri = right_imag.astype(jnp.float32)
    cross_real = lr * rr + li * ri
    cross_imag = li * rr - lr * ri
    factor = 1.0 / (jnp.sqrt(cross_real * cross_real + cross_imag * cross_imag) + FLOOR)
    return (
        (cross_real * factor).astype(jnp.bfloat16),
        (cross_imag * factor).astype(jnp.bfloat16),
    )


def correlate(s_ref, picks, spectra, edge, phases):
    slots = len(picks)
    height = spectra.shape[3]
    lead = lax.broadcasted_iota(jnp.int32, (16, height), 0)
    packed = (lead == 0) & holds_packed(s_ref)
    for p in range(slots):
        a, c = picks[p]
        q_real, q_imag = normalised(spectra[a, 0], spectra[a, 1], spectra[c, 0], spectra[c, 1])
        e_real, e_imag = normalised(edge[a, 0], edge[a, 1], edge[c, 0], edge[c, 1])
        phases[2 * p] = q_real
        phases[2 * p + 1] = q_imag
        top_real = q_real[:16].astype(jnp.float32)
        top_imag = q_imag[:16].astype(jnp.float32)
        mixed_real = jnp.where(packed, top_real - e_imag.astype(jnp.float32), top_real)
        mixed_imag = jnp.where(packed, top_imag + e_real.astype(jnp.float32), top_imag)
        phases[2 * p, :16] = mixed_real.astype(jnp.bfloat16)
        phases[2 * p + 1, :16] = mixed_imag.astype(jnp.bfloat16)

def invert_columns(s_ref, me, phases, table_ref, outs):
    _, block, height = phases.shape
    slots = phases.shape[0] // 2
    rows = next(iter(outs.values())).shape[2]
    row = lax.broadcasted_iota(jnp.int32, (block, rows), 0)
    twice = jnp.where((row == 0) & holds_packed(s_ref), 1.0, 2.0)
    flat = phases[...].reshape(2 * slots * block, height)
    for k, out in outs.items():
        start = pl.multiple_of((me ^ k) * rows, rows)
        c_part = jnp.dot(
            flat, table_ref[:, pl.ds(start, rows)], preferred_element_type=jnp.float32
        )
        start = pl.multiple_of(height + (me ^ k) * rows, rows)
        s_part = jnp.dot(
            flat, table_ref[:, pl.ds(start, rows)], preferred_element_type=jnp.float32
        )
        for p in range(slots):
            re = slice(2 * p * block, (2 * p + 1) * block)
            im = slice((2 * p + 1) * block, (2 * p + 2) * block)
            out[p, :block] = ((c_part[re] - s_part[im]) * twice).astype(jnp.bfloat16)
            out[p, block:] = ((s_part[re] + c_part[im]) * twice).astype(jnp.bfloat16)


def own_spectra(place, pieces, near, short):
    peers, count, double, rows = pieces.shape
    height = peers * rows

    def body(half_ref, me_ref, pieces_ref, near_a, near_b, short_ref, spectra, edge, share, table_ref):
        total = None
        for k in range(peers):
            make_table(short_ref, table_ref, k * rows, rows)
            term = jnp.dot(
                pieces_ref[k].reshape(count * double, rows),
                table_ref[k * rows : (k + 1) * rows],
                preferred_element_type=jnp.float32,
            )
            total = term if total is None else total + term
        store_spectra((half_ref, me_ref), total, spectra, edge, 0)
        share[...] = gather_rows([near_a, near_b], table_ref, me_ref[0])

    return pl.pallas_call(
        body,
        in_specs=[pl.BlockSpec(memory_space=pltpu.SMEM)] * 2
        + [pl.BlockSpec(memory_space=pltpu.VMEM)] * 4,
        out_specs=[pl.BlockSpec(memory_space=pltpu.VMEM)] * 4,
        out_shape=[
            jax.ShapeDtypeStruct((count, 2, double // 2, height), jnp.bfloat16),
            jax.ShapeDtypeStruct((count, 2, 16, height), jnp.bfloat16),
            jax.ShapeDtypeStruct((count * double, 2 * height), jnp.float32),
            jax.ShapeDtypeStruct((height, 2 * height), jnp.bfloat16),
        ],
        compiler_params=params(),
        cost_estimate=cost(6 * count * double * height * height, 8 * height * height),
        name="own_spectra",
    )(*place, pieces, *near, short)


def partner_slots(place, theirs, pieces, share, table, spectra, edge):
    distant = len(pieces)
    count, double, rows = pieces[0].shape
    height = table.shape[0]
    block = double // 2
    slots = theirs.shape[1]

    def body(half_ref, me_ref, theirs_ref, *refs):
        s_ref = (half_ref, me_ref)
        me = me_ref[0]
        picks = [
            [(theirs_ref[0, p, i] + count) % (2 * count) for i in range(2)] for p in range(slots)
        ]
        inputs = refs[:distant]
        share_ref, table_ref, own_ref, own_edge, near, every, edges, phases = refs[distant:]
        every[:count] = own_ref[...]
        edges[:count] = own_edge[...]
        total = gather_rows(inputs, table_ref, me, 2, share_ref[...])
        store_spectra(s_ref, total, every, edges, count)
        correlate(s_ref, picks, every, edges, phases)
        invert_columns(s_ref, me, phases, table_ref, {k: near.at[k] for k in range(2)})

    return pl.pallas_call(
        body,
        in_specs=[pl.BlockSpec(memory_space=pltpu.SMEM)] * 3
        + [pl.BlockSpec(memory_space=pltpu.VMEM)] * (distant + 4),
        out_specs=[pl.BlockSpec(memory_space=pltpu.VMEM)] * 4,
        out_shape=[
            jax.ShapeDtypeStruct((2, slots, double, rows), jnp.bfloat16),
            jax.ShapeDtypeStruct((2 * count, 2, block, height), jnp.bfloat16),
            jax.ShapeDtypeStruct((2 * count, 2, 16, height), jnp.bfloat16),
            jax.ShapeDtypeStruct((2 * slots, block, height), jnp.bfloat16),
        ],
        compiler_params=params(),
        cost_estimate=cost(4 * (count + slots) * double * height * height, 8 * height * height),
        name="partner_slots",
    )(*place, theirs, *pieces, share, table, spectra, edge)


def own_slots(place, pairs, table, spectra, edge, phases, peers):
    block, height = spectra.shape[2:]
    rows = height // peers
    slots = pairs.shape[1]

    def body(half_ref, me_ref, pairs_ref, table_ref, every, edges, theirs, out_ref, *refs):
        s_ref = (half_ref, me_ref)
        far, work = refs[:-1], refs[-1]
        picks = [[pairs_ref[0, p, i] for i in range(2)] for p in range(slots)]
        if far:
            outs = {k: far[k - 2] for k in range(2, peers)}
            invert_columns(s_ref, me_ref[0], theirs, table_ref, outs)
        correlate(s_ref, picks, every, edges, work)
        invert_columns(s_ref, 0, work, table_ref, {k: out_ref.at[k] for k in range(peers)})

    return pl.pallas_call(
        body,
        in_specs=[pl.BlockSpec(memory_space=pltpu.SMEM)] * 3
        + [pl.BlockSpec(memory_space=pltpu.VMEM)] * 4,
        out_specs=[pl.BlockSpec(memory_space=pltpu.VMEM)] * (peers - 1),
        out_shape=[
            jax.ShapeDtypeStruct((peers, slots, 2 * block, rows), jnp.bfloat16),
            *[jax.ShapeDtypeStruct((slots, 2 * block, rows), jnp.bfloat16)] * (peers - 2),
        ],
        scratch_shapes=[pltpu.VMEM((2 * slots, block, height), jnp.bfloat16)],
        compiler_params=params(),
        cost_estimate=cost(8 * slots * block * height * height, 8 * height * height),
        name="own_slots",
    )(*place, pairs, table, spectra, edge, phases)


def own_surfaces(half, own, table):
    peers, slots, double, rows = own.shape
    width = table.shape[0]
    span = peers * double

    def body(half_ref, own_ref, table_ref, out_ref):
        out_ref[0] = lax.dot_general(
            own_ref[:, 0].reshape(span, rows),
            table_ref[...],
            (((0,), (0,)), ((), ())),
            preferred_element_type=jnp.float32,
        )

    return pl.pallas_call(
        body,
        grid_spec=pltpu.PrefetchScalarGridSpec(
            num_scalar_prefetch=1,
            grid=(slots,),
            in_specs=[
                pl.BlockSpec((peers, 1, double, rows), lambda p, half: (0, p, 0, 0)),
                pl.BlockSpec((span, width), lambda p, half: (half[0], 0)),
            ],
            out_specs=pl.BlockSpec((1, rows, width), lambda p, half: (p, 0, 0)),
        ),
        out_shape=jax.ShapeDtypeStruct((slots, rows, width), jnp.float32),
        compiler_params=params(),
        cost_estimate=cost(2 * slots * rows * width * span, 4 * slots * rows * width),
        name="own_surfaces",
    )(scalar(half), own, table)


def surfaces_of(half, me, counts, part, near, other, table):
    peers = 1 + len(other)
    slots, double, rows = other[0].shape
    width = table.shape[0]
    span = peers * double

    def body(half_ref, me_ref, counts_ref, part_ref, *refs):
        other_refs = refs[:peers]
        table_ref, out_ref, work = refs[peers:]
        for k in range(peers):
            place = pl.multiple_of((me_ref[0] ^ k) * double, double)
            piece = other_refs[k][0] if k else other_refs[k][0, 0]
            work[pl.ds(place, double), :] = piece
        start = pl.multiple_of((1 - half_ref[0]) * span, span)
        rest = lax.dot_general(
            work[...],
            table_ref[pl.ds(start, span), :],
            (((0,), (0,)), ((), ())),
            preferred_element_type=jnp.float32,
        )
        live = pl.program_id(0) < counts_ref[0]
        out_ref[0] = jnp.where(live, part_ref[pl.program_id(0)] + rest, 0.0)

    pair = pl.BlockSpec((1, 1, double, rows), lambda p, half, me, counts: (0, p, 0, 0))
    piece = pl.BlockSpec((1, double, rows), lambda p, half, me, counts: (p, 0, 0))
    plane = pl.BlockSpec((1, rows, width), lambda p, half, me, counts: (p, 0, 0))
    return pl.pallas_call(
        body,
        grid_spec=pltpu.PrefetchScalarGridSpec(
            num_scalar_prefetch=3,
            grid=(slots,),
            in_specs=[
                pl.BlockSpec(memory_space=pltpu.VMEM),
                pair,
                *[piece] * (peers - 1),
                pl.BlockSpec(memory_space=pltpu.VMEM),
            ],
            out_specs=plane,
            scratch_shapes=[pltpu.VMEM((span, rows), jnp.bfloat16)],
        ),
        out_shape=jax.ShapeDtypeStruct((slots, rows, width), jnp.float32),
        compiler_params=params(),
        cost_estimate=cost(2 * slots * rows * width * span, 8 * slots * rows * width),
        name="surfaces",
    )(scalar(half), scalar(me), counts, part, near, *other, table)


def local(tiles, pairs, counts):
    groups = lax.axis_size("blk")
    peers = lax.axis_size("rows")
    group = lax.axis_index("blk")
    me = lax.axis_index("rows")
    count, rows, width = tiles.shape
    height = rows * peers
    turn = groups // 2
    half = group // turn
    axes = ("blk", "rows")

    def across(value, k):
        moves = [
            (b * peers + r, (b + turn) % groups * peers + (r ^ k))
            for b in range(groups)
            for r in range(peers)
        ]
        return lax.ppermute(value, axes, moves)

    def along(blocks):
        return lax.all_to_all(blocks, "rows", split_axis=0, concat_axis=0)

    def swap(value):
        return lax.ppermute(value, "rows", [(r, r ^ 1) for r in range(peers)])

    table_w = jnp.asarray(width_table(width, 2 * peers))
    down = jnp.asarray(np.tile(hann(height), (8, 1)))
    sideways = jnp.asarray(hann(width)[None, :])

    sent = near_columns(tiles, down, sideways, table_w, half, me, peers)
    arrived = [across(sent[k], k) for k in range(2)]
    *sent, held = lax.optimization_barrier((*sent, half))
    kept, *sent = rest_columns(tiles, down, sideways, table_w, held, me, peers)
    *sent, kept, pairs = lax.optimization_barrier((*sent, kept, pairs))
    arrived += [across(sent[k - 2], k) for k in range(2, peers)]
    mine = along(kept)

    theirs = across(pairs, 0)
    place = (scalar(half), scalar(me))
    spectra, edge, share, table_h = own_spectra(
        place, mine, arrived[:2], scaled_tables(height, [])
    )
    near, spectra, edge, phases = partner_slots(
        place, theirs, arrived[2:], share, table_h, spectra, edge
    )
    near = across(near, 0)
    own, *far = own_slots(place, pairs, table_h, spectra, edge, phases, peers)
    far = [across(far[k - 2], k) for k in range(2, peers)]
    part = own_surfaces(half, along(own), table_w)
    *far, part = lax.optimization_barrier((*far, part))
    return surfaces_of(half, me, counts, part, near, [swap(near[1]), *far], table_w)


def solution(mesh):
    from jax.sharding import PartitionSpec as P

    return jax.shard_map(
        local,
        mesh=mesh,
        in_specs=(
            P(("parts", "blk"), "rows", None),
            P(("parts", "blk"), None, None),
            P(("parts", "blk")),
        ),
        out_specs=P(("parts", "blk"), "rows", None),
        check_vma=False,
    )
```

```python
import math

import jax
import jax.numpy as jnp
import numpy as np
from jax import lax
from jax.experimental import pallas as pl
from jax.experimental.pallas import tpu as pltpu

FLOOR = 0.05
VMEM_LIMIT = 24 * 1024 * 1024
FIRST_LIMIT = 58 * 1024 * 1024


def hann(length):
    return np.asarray(0.5 - 0.5 * np.cos(2.0 * math.pi / length * np.arange(length)), np.float32)


def scalar(value):
    return jnp.reshape(value, (1,)).astype(jnp.int32)


def width_table(width, owners):
    half = width // 2
    phase = np.arange(half)[:, None] * np.arange(width)[None, :] % width
    angle = 2.0 * math.pi / width * phase
    factor = 1.0 / math.sqrt(width)
    cosine = np.cos(angle) * factor
    sine = -np.sin(angle) * factor
    sine[0] = np.where(np.arange(width) % 2 == 0, factor, -factor)
    shape = (owners, half // owners, width)
    table = np.stack([cosine.reshape(shape), sine.reshape(shape)], axis=1)
    return table.reshape(width, width).astype(jnp.bfloat16)


FINE = 32


def short_tables(height):
    column = np.arange(height)[None, :]
    rough = 2.0 * math.pi / height * (np.arange(height // FINE)[:, None] * FINE * column % height)
    small = 2.0 * math.pi / height * (np.arange(FINE)[:, None] * column % height)
    short = [np.cos(small), np.sin(small), np.cos(rough), np.sin(rough)]
    return jnp.asarray(np.concatenate(short), jnp.float32)


def scaled_tables(height, after):
    factor = 1.0 / math.sqrt(height)

    def body(short_ref, *refs):
        refs[-1][: 2 * FINE] = short_ref[: 2 * FINE]
        refs[-1][2 * FINE :] = short_ref[2 * FINE :] * factor

    short = short_tables(height)
    return pl.pallas_call(
        body,
        in_specs=[pl.BlockSpec(memory_space=pltpu.VMEM)]
        + [pl.BlockSpec(memory_space=pl.ANY)] * len(after),
        out_specs=pl.BlockSpec(memory_space=pltpu.VMEM),
        out_shape=jax.ShapeDtypeStruct(short.shape, short.dtype),
        compiler_params=params(),
        cost_estimate=cost(1 << 33, 8 * short.size),
        name="scaled_tables",
    )(short, *after)


def make_table(short_ref, out_ref, first, rows):
    height = short_ref.shape[1]
    coarse = height // FINE
    sc, ss = short_ref[:FINE], short_ref[FINE : 2 * FINE]
    for j in range(first // FINE, (first + rows) // FINE):
        a = 2 * FINE + j
        rc, rs = short_ref[a : a + 1, :], short_ref[a + coarse : a + coarse + 1, :]
        here = slice(j * FINE, (j + 1) * FINE)
        out_ref[here, :height] = (rc * sc - rs * ss).astype(jnp.bfloat16)
        out_ref[here, height:] = (rs * sc + rc * ss).astype(jnp.bfloat16)


def cost(flops, moved):
    return pl.CostEstimate(flops=flops, transcendentals=0, bytes_accessed=moved)


def params(limit=VMEM_LIMIT):
    return pltpu.CompilerParams(vmem_limit_bytes=limit)


def shade(tile, down_ref, across_ref):
    return (tile * (down_ref[...].T[:, :1] * across_ref[...])).astype(jnp.bfloat16)


def times_table(table, shaded):
    y = lax.dot_general(
        table, shaded, (((1,), (1,)), ((), ())), preferred_element_type=jnp.float32
    )
    return y.astype(jnp.bfloat16)


def near_columns(tiles, down, across, table, half, me, peers):
    count, rows, width = tiles.shape
    span = table.shape[0] // 2
    block = span // peers

    def body(half_ref, me_ref, tile_hbm, down_hbm, across_hbm, table_hbm, *refs):
        outs = refs[:2]
        tile_ref, table_ref, work, down_ref, across_ref, done = refs[2:]
        t = pl.program_id(0)
        me = me_ref[0]
        start = pl.multiple_of((1 - half_ref[0]) * span + me // 2 * 2 * block, 2 * block)
        fetch = pltpu.make_async_copy(
            table_hbm.at[pl.ds(start, 2 * block)], table_ref, done.at[count]
        )
        loads = [
            pltpu.make_async_copy(tile_hbm.at[i], tile_ref.at[i], done.at[i]) for i in range(count)
        ]

        lane = pl.multiple_of(me * rows, rows)
        extra = [
            pltpu.make_async_copy(down_hbm.at[:, pl.ds(lane, rows)], down_ref, done.at[count + 1]),
            pltpu.make_async_copy(across_hbm, across_ref, done.at[count + 2]),
        ]

        @pl.when(t == 0)
        def _():
            for copy in extra:
                copy.start()
            fetch.start()
            for load in loads:
                load.start()
            for copy in extra:
                copy.wait()
            fetch.wait()

        for i in range(count):

            @pl.when(t == i)
            def _():
                loads[i].wait()
                work[...] = times_table(table_ref[...], shade(tile_ref[i], down_ref, across_ref))

        for k in range(2):
            place = pl.multiple_of((me % 2 ^ k) * block, block)
            outs[k][0] = work[pl.ds(place, block), :]

    return pl.pallas_call(
        body,
        grid_spec=pltpu.PrefetchScalarGridSpec(
            num_scalar_prefetch=2,
            grid=(count,),
            in_specs=[
                pl.BlockSpec(memory_space=pltpu.HBM),
                pl.BlockSpec(memory_space=pltpu.HBM),
                pl.BlockSpec(memory_space=pltpu.HBM),
                pl.BlockSpec(memory_space=pltpu.HBM),
            ],
            out_specs=[pl.BlockSpec((1, block, rows), lambda t, half, me: (t, 0, 0))] * 2,
            scratch_shapes=[
                pltpu.VMEM((count, rows, width), tiles.dtype),
                pltpu.VMEM((2 * block, width), table.dtype),
                pltpu.VMEM((2 * block, rows), jnp.bfloat16),
                pltpu.VMEM((8, rows), jnp.float32),
                pltpu.VMEM((1, width), jnp.float32),
                pltpu.SemaphoreType.DMA((count + 3,)),
            ],
        ),
        out_shape=[jax.ShapeDtypeStruct((count, block, rows), jnp.bfloat16)] * 2,
        compiler_params=params(FIRST_LIMIT),
        cost_estimate=cost(4 * count * rows * width * block, 4 * tiles.size + 4 * block * width),
        name="near_columns",
    )(scalar(half), scalar(me), tiles, down, across, table)


def rest_columns(tiles, down, across, table, half, me, peers):
    count, rows, width = tiles.shape
    span = table.shape[0] // 2
    block = span // peers

    def body(half_ref, me_ref, tile_ref, down_ref, across_ref, table_ref, *refs):
        out_ref, far, work = refs[0], refs[1:-1], refs[-1]
        half, me = half_ref[0], me_ref[0]
        shaded = shade(tile_ref[pl.program_id(0)], down_ref, across_ref)
        for j in range(1, peers // 2):
            start = pl.multiple_of((1 - half) * span + (me // 2 ^ j) * 2 * block, 2 * block)
            work[...] = times_table(table_ref[pl.ds(start, 2 * block), :], shaded)
            for k in range(2):
                place = pl.multiple_of((me % 2 ^ k) * block, block)
                far[2 * j - 2 + k][0] = work[pl.ds(place, block), :]
        start = pl.multiple_of(half * span, span)
        y = times_table(table_ref[pl.ds(start, span), :], shaded)
        out_ref[:, 0] = y.reshape(peers, block, rows)

    piece = pl.BlockSpec((1, block, rows), lambda t, half, me: (t, 0, 0))
    return pl.pallas_call(
        body,
        grid_spec=pltpu.PrefetchScalarGridSpec(
            num_scalar_prefetch=2,
            grid=(count,),
            in_specs=[
                pl.BlockSpec(memory_space=pltpu.VMEM),
                pl.BlockSpec((8, rows), lambda t, half, me: (0, me[0])),
                pl.BlockSpec((1, width), lambda t, half, me: (0, 0)),
                pl.BlockSpec(memory_space=pltpu.VMEM),
            ],
            out_specs=[
                pl.BlockSpec((peers, 1, block, rows), lambda t, half, me: (0, t, 0, 0)),
                *[piece] * (peers - 2),
            ],
            scratch_shapes=[pltpu.VMEM((2 * block, rows), jnp.bfloat16)],
        ),
        out_shape=[
            jax.ShapeDtypeStruct((peers, count, block, rows), jnp.bfloat16),
            *[jax.ShapeDtypeStruct((count, block, rows), jnp.bfloat16)] * (peers - 2),
        ],
        compiler_params=params(),
        cost_estimate=cost(3 * count * rows * width * span, 4 * tiles.size + 2 * width * width),
        name="rest_columns",
    )(scalar(half), scalar(me), tiles, down, across, table)


def gather_rows(pieces, table_ref, me, first=0, total=None):
    for k, piece in enumerate(pieces, first):
        count, block, rows = piece.shape
        start = pl.multiple_of((me ^ k) * rows, rows)
        term = jnp.dot(
            piece[...].reshape(count * block, rows),
            table_ref[pl.ds(start, rows), :],
            preferred_element_type=jnp.float32,
        )
        total = term if total is None else total + term
    return total


def holds_packed(place):
    half_ref, me_ref = place
    return (half_ref[0] == 0) & (me_ref[0] == 0)


def store_spectra(s_ref, total, spectra, edge, first):
    block = spectra.shape[2]
    height = spectra.shape[3]
    row = lax.broadcasted_iota(jnp.int32, (block, height), 0)
    packed = (row == 0) & holds_packed(s_ref)
    for t in range(total.shape[0] // (2 * block)):
        real = total[2 * t * block : (2 * t + 1) * block]
        imag = total[(2 * t + 1) * block : (2 * t + 2) * block]
        cr, sr = real[:, :height], real[:, height:]
        ci, si = imag[:, :height], imag[:, height:]
        spectra[first + t, 0] = jnp.where(packed, cr, cr + si).astype(jnp.bfloat16)
        spectra[first + t, 1] = jnp.where(packed, -sr, ci - sr).astype(jnp.bfloat16)
        edge[first + t, 0] = ci[:16].astype(jnp.bfloat16)
        edge[first + t, 1] = (-si[:16]).astype(jnp.bfloat16)


def normalised(left_real, left_imag, right_real, right_imag):
    lr = left_real.astype(jnp.float32)
    li = left_imag.astype(jnp.float32)
    rr = right_real.astype(jnp.float32)
    ri = right_imag.astype(jnp.float32)
    cross_real = lr * rr + li * ri
    cross_imag = li * rr - lr * ri
    factor = 1.0 / (jnp.sqrt(cross_real * cross_real + cross_imag * cross_imag) + FLOOR)
    return (
        (cross_real * factor).astype(jnp.bfloat16),
        (cross_imag * factor).astype(jnp.bfloat16),
    )


def correlate(s_ref, picks, spectra, edge, phases):
    slots = len(picks)
    height = spectra.shape[3]
    lead = lax.broadcasted_iota(jnp.int32, (16, height), 0)
    packed = (lead == 0) & holds_packed(s_ref)
    for p in range(slots):
        a, c = picks[p]
        q_real, q_imag = normalised(spectra[a, 0], spectra[a, 1], spectra[c, 0], spectra[c, 1])
        e_real, e_imag = normalised(edge[a, 0], edge[a, 1], edge[c, 0], edge[c, 1])
        phases[2 * p] = q_real
        phases[2 * p + 1] = q_imag
        top_real = q_real[:16].astype(jnp.float32)
        top_imag = q_imag[:16].astype(jnp.float32)
        mixed_real = jnp.where(packed, top_real - e_imag.astype(jnp.float32), top_real)
        mixed_imag = jnp.where(packed, top_imag + e_real.astype(jnp.float32), top_imag)
        phases[2 * p, :16] = mixed_real.astype(jnp.bfloat16)
        phases[2 * p + 1, :16] = mixed_imag.astype(jnp.bfloat16)

def invert_columns(s_ref, me, phases, table_ref, outs):
    _, block, height = phases.shape
    slots = phases.shape[0] // 2
    rows = next(iter(outs.values())).shape[2]
    row = lax.broadcasted_iota(jnp.int32, (block, rows), 0)
    twice = jnp.where((row == 0) & holds_packed(s_ref), 1.0, 2.0)
    flat = phases[...].reshape(2 * slots * block, height)
    for k, out in outs.items():
        start = pl.multiple_of((me ^ k) * rows, rows)
        c_part = jnp.dot(
            flat, table_ref[:, pl.ds(start, rows)], preferred_element_type=jnp.float32
        )
        start = pl.multiple_of(height + (me ^ k) * rows, rows)
        s_part = jnp.dot(
            flat, table_ref[:, pl.ds(start, rows)], preferred_element_type=jnp.float32
        )
        for p in range(slots):
            re = slice(2 * p * block, (2 * p + 1) * block)
            im = slice((2 * p + 1) * block, (2 * p + 2) * block)
            out[p, :block] = ((c_part[re] - s_part[im]) * twice).astype(jnp.bfloat16)
            out[p, block:] = ((s_part[re] + c_part[im]) * twice).astype(jnp.bfloat16)


def own_spectra(place, pieces, near, short):
    peers, count, double, rows = pieces.shape
    height = peers * rows

    def body(half_ref, me_ref, pieces_ref, near_a, near_b, short_ref, spectra, edge, share, table_ref):
        total = None
        for k in range(peers):
            make_table(short_ref, table_ref, k * rows, rows)
            term = jnp.dot(
                pieces_ref[k].reshape(count * double, rows),
                table_ref[k * rows : (k + 1) * rows],
                preferred_element_type=jnp.float32,
            )
            total = term if total is None else total + term
        store_spectra((half_ref, me_ref), total, spectra, edge, 0)
        share[...] = gather_rows([near_a, near_b], table_ref, me_ref[0])

    return pl.pallas_call(
        body,
        in_specs=[pl.BlockSpec(memory_space=pltpu.SMEM)] * 2
        + [pl.BlockSpec(memory_space=pltpu.VMEM)] * 4,
        out_specs=[pl.BlockSpec(memory_space=pltpu.VMEM)] * 4,
        out_shape=[
            jax.ShapeDtypeStruct((count, 2, double // 2, height), jnp.bfloat16),
            jax.ShapeDtypeStruct((count, 2, 16, height), jnp.bfloat16),
            jax.ShapeDtypeStruct((count * double, 2 * height), jnp.float32),
            jax.ShapeDtypeStruct((height, 2 * height), jnp.bfloat16),
        ],
        compiler_params=params(),
        cost_estimate=cost(6 * count * double * height * height, 8 * height * height),
        name="own_spectra",
    )(*place, pieces, *near, short)


def partner_slots(place, theirs, pieces, share, table, spectra, edge):
    distant = len(pieces)
    count, double, rows = pieces[0].shape
    height = table.shape[0]
    block = double // 2
    slots = theirs.shape[1]

    def body(half_ref, me_ref, theirs_ref, *refs):
        s_ref = (half_ref, me_ref)
        me = me_ref[0]
        picks = [
            [(theirs_ref[0, p, i] + count) % (2 * count) for i in range(2)] for p in range(slots)
        ]
        inputs = refs[:distant]
        share_ref, table_ref, own_ref, own_edge, near, every, edges, phases = refs[distant:]
        every[:count] = own_ref[...]
        edges[:count] = own_edge[...]
        total = gather_rows(inputs, table_ref, me, 2, share_ref[...])
        store_spectra(s_ref, total, every, edges, count)
        correlate(s_ref, picks, every, edges, phases)
        invert_columns(s_ref, me, phases, table_ref, {k: near.at[k] for k in range(2)})

    return pl.pallas_call(
        body,
        in_specs=[pl.BlockSpec(memory_space=pltpu.SMEM)] * 3
        + [pl.BlockSpec(memory_space=pltpu.VMEM)] * (distant + 4),
        out_specs=[pl.BlockSpec(memory_space=pltpu.VMEM)] * 4,
        out_shape=[
            jax.ShapeDtypeStruct((2, slots, double, rows), jnp.bfloat16),
            jax.ShapeDtypeStruct((2 * count, 2, block, height), jnp.bfloat16),
            jax.ShapeDtypeStruct((2 * count, 2, 16, height), jnp.bfloat16),
            jax.ShapeDtypeStruct((2 * slots, block, height), jnp.bfloat16),
        ],
        compiler_params=params(),
        cost_estimate=cost(4 * (count + slots) * double * height * height, 8 * height * height),
        name="partner_slots",
    )(*place, theirs, *pieces, share, table, spectra, edge)


def own_slots(place, pairs, table, spectra, edge, phases, peers):
    block, height = spectra.shape[2:]
    rows = height // peers
    slots = pairs.shape[1]

    def body(half_ref, me_ref, pairs_ref, table_ref, every, edges, theirs, out_ref, *refs):
        s_ref = (half_ref, me_ref)
        far, work = refs[:-1], refs[-1]
        picks = [[pairs_ref[0, p, i] for i in range(2)] for p in range(slots)]
        if far:
            outs = {k: far[k - 2] for k in range(2, peers)}
            invert_columns(s_ref, me_ref[0], theirs, table_ref, outs)
        correlate(s_ref, picks, every, edges, work)
        invert_columns(s_ref, 0, work, table_ref, {k: out_ref.at[k] for k in range(peers)})

    return pl.pallas_call(
        body,
        in_specs=[pl.BlockSpec(memory_space=pltpu.SMEM)] * 3
        + [pl.BlockSpec(memory_space=pltpu.VMEM)] * 4,
        out_specs=[pl.BlockSpec(memory_space=pltpu.VMEM)] * (peers - 1),
        out_shape=[
            jax.ShapeDtypeStruct((peers, slots, 2 * block, rows), jnp.bfloat16),
            *[jax.ShapeDtypeStruct((slots, 2 * block, rows), jnp.bfloat16)] * (peers - 2),
        ],
        scratch_shapes=[pltpu.VMEM((2 * slots, block, height), jnp.bfloat16)],
        compiler_params=params(),
        cost_estimate=cost(8 * slots * block * height * height, 8 * height * height),
        name="own_slots",
    )(*place, pairs, table, spectra, edge, phases)


def own_surfaces(half, own, table):
    peers, slots, double, rows = own.shape
    width = table.shape[0]
    span = peers * double

    def body(half_ref, own_ref, table_ref, out_ref):
        out_ref[0] = lax.dot_general(
            own_ref[:, 0].reshape(span, rows),
            table_ref[...],
            (((0,), (0,)), ((), ())),
            preferred_element_type=jnp.float32,
        )

    return pl.pallas_call(
        body,
        grid_spec=pltpu.PrefetchScalarGridSpec(
            num_scalar_prefetch=1,
            grid=(slots,),
            in_specs=[
                pl.BlockSpec((peers, 1, double, rows), lambda p, half: (0, p, 0, 0)),
                pl.BlockSpec((span, width), lambda p, half: (half[0], 0)),
            ],
            out_specs=pl.BlockSpec((1, rows, width), lambda p, half: (p, 0, 0)),
        ),
        out_shape=jax.ShapeDtypeStruct((slots, rows, width), jnp.float32),
        compiler_params=params(),
        cost_estimate=cost(2 * slots * rows * width * span, 4 * slots * rows * width),
        name="own_surfaces",
    )(scalar(half), own, table)


def surfaces_of(half, me, counts, part, near, other, table):
    peers = 1 + len(other)
    slots, double, rows = other[0].shape
    width = table.shape[0]
    span = peers * double

    def body(half_ref, me_ref, counts_ref, part_ref, *refs):
        other_refs = refs[:peers]
        table_ref, out_ref, work = refs[peers:]
        for k in range(peers):
            place = pl.multiple_of((me_ref[0] ^ k) * double, double)
            piece = other_refs[k][0] if k else other_refs[k][0, 0]
            work[pl.ds(place, double), :] = piece
        start = pl.multiple_of((1 - half_ref[0]) * span, span)
        rest = lax.dot_general(
            work[...],
            table_ref[pl.ds(start, span), :],
            (((0,), (0,)), ((), ())),
            preferred_element_type=jnp.float32,
        )
        live = pl.program_id(0) < counts_ref[0]
        out_ref[0] = jnp.where(live, part_ref[pl.program_id(0)] + rest, 0.0)

    pair = pl.BlockSpec((1, 1, double, rows), lambda p, half, me, counts: (0, p, 0, 0))
    piece = pl.BlockSpec((1, double, rows), lambda p, half, me, counts: (p, 0, 0))
    plane = pl.BlockSpec((1, rows, width), lambda p, half, me, counts: (p, 0, 0))
    return pl.pallas_call(
        body,
        grid_spec=pltpu.PrefetchScalarGridSpec(
            num_scalar_prefetch=3,
            grid=(slots,),
            in_specs=[
                pl.BlockSpec(memory_space=pltpu.VMEM),
                pair,
                *[piece] * (peers - 1),
                pl.BlockSpec(memory_space=pltpu.VMEM),
            ],
            out_specs=plane,
            scratch_shapes=[pltpu.VMEM((span, rows), jnp.bfloat16)],
        ),
        out_shape=jax.ShapeDtypeStruct((slots, rows, width), jnp.float32),
        compiler_params=params(),
        cost_estimate=cost(2 * slots * rows * width * span, 8 * slots * rows * width),
        name="surfaces",
    )(scalar(half), scalar(me), counts, part, near, *other, table)


def local(tiles, pairs, counts):
    groups = lax.axis_size("blk")
    peers = lax.axis_size("rows")
    group = lax.axis_index("blk")
    me = lax.axis_index("rows")
    count, rows, width = tiles.shape
    height = rows * peers
    turn = groups // 2
    half = group // turn
    axes = ("blk", "rows")

    def across(value, k):
        moves = [
            (b * peers + r, (b + turn) % groups * peers + (r ^ k))
            for b in range(groups)
            for r in range(peers)
        ]
        return lax.ppermute(value, axes, moves)

    def along(blocks):
        return lax.all_to_all(blocks, "rows", split_axis=0, concat_axis=0)

    def swap(value):
        return lax.ppermute(value, "rows", [(r, r ^ 1) for r in range(peers)])

    table_w = jnp.asarray(width_table(width, 2 * peers))
    down = jnp.asarray(np.tile(hann(height), (8, 1)))
    sideways = jnp.asarray(hann(width)[None, :])

    sent = near_columns(tiles, down, sideways, table_w, half, me, peers)
    arrived = [across(sent[k], k) for k in range(2)]
    *sent, held = lax.optimization_barrier((*sent, half))
    kept, *sent = rest_columns(tiles, down, sideways, table_w, held, me, peers)
    *sent, kept, pairs = lax.optimization_barrier((*sent, kept, pairs))
    mine = along(kept)
    *sent, short = lax.optimization_barrier((*sent, scaled_tables(height, [])))
    arrived += [across(sent[k - 2], k) for k in range(2, peers)]

    theirs = across(pairs, 0)
    place = (scalar(half), scalar(me))
    spectra, edge, share, table_h = own_spectra(place, mine, arrived[:2], short)
    near, spectra, edge, phases = partner_slots(
        place, theirs, arrived[2:], share, table_h, spectra, edge
    )
    near = across(near, 0)
    own, *far = own_slots(place, pairs, table_h, spectra, edge, phases, peers)
    far = [across(far[k - 2], k) for k in range(2, peers)]
    part = own_surfaces(half, along(own), table_w)
    *far, part = lax.optimization_barrier((*far, part))
    return surfaces_of(half, me, counts, part, near, [swap(near[1]), *far], table_w)


def solution(mesh):
    from jax.sharding import PartitionSpec as P

    return jax.shard_map(
        local,
        mesh=mesh,
        in_specs=(
            P(("parts", "blk"), "rows", None),
            P(("parts", "blk"), None, None),
            P(("parts", "blk")),
        ),
        out_specs=P(("parts", "blk"), "rows", None),
        check_vma=False,
    )
```

```python
import math

import jax
import jax.numpy as jnp
import numpy as np
from jax import lax
from jax.experimental import pallas as pl
from jax.experimental.pallas import tpu as pltpu

FLOOR = 0.05
VMEM_LIMIT = 24 * 1024 * 1024
FIRST_LIMIT = 58 * 1024 * 1024


def hann(length):
    return np.asarray(0.5 - 0.5 * np.cos(2.0 * math.pi / length * np.arange(length)), np.float32)


def scalar(value):
    return jnp.reshape(value, (1,)).astype(jnp.int32)


def width_table(width, owners):
    half = width // 2
    phase = np.arange(half)[:, None] * np.arange(width)[None, :] % width
    angle = 2.0 * math.pi / width * phase
    factor = 1.0 / math.sqrt(width)
    cosine = np.cos(angle) * factor
    sine = -np.sin(angle) * factor
    sine[0] = np.where(np.arange(width) % 2 == 0, factor, -factor)
    shape = (owners, half // owners, width)
    table = np.stack([cosine.reshape(shape), sine.reshape(shape)], axis=1)
    return table.reshape(width, width).astype(jnp.bfloat16)


FINE = 32


def short_tables(height):
    column = np.arange(height)[None, :]
    rough = 2.0 * math.pi / height * (np.arange(height // FINE)[:, None] * FINE * column % height)
    small = 2.0 * math.pi / height * (np.arange(FINE)[:, None] * column % height)
    short = [np.cos(small), np.sin(small), np.cos(rough), np.sin(rough)]
    return jnp.asarray(np.concatenate(short), jnp.float32)


def scaled_tables(height, after):
    factor = 1.0 / math.sqrt(height)

    def body(short_ref, *refs):
        refs[-1][: 2 * FINE] = short_ref[: 2 * FINE]
        refs[-1][2 * FINE :] = short_ref[2 * FINE :] * factor

    short = short_tables(height)
    return pl.pallas_call(
        body,
        in_specs=[pl.BlockSpec(memory_space=pltpu.VMEM)]
        + [pl.BlockSpec(memory_space=pl.ANY)] * len(after),
        out_specs=pl.BlockSpec(memory_space=pltpu.VMEM),
        out_shape=jax.ShapeDtypeStruct(short.shape, short.dtype),
        compiler_params=params(),
        cost_estimate=cost(1 << 33, 8 * short.size),
        name="scaled_tables",
    )(short, *after)


def make_table(short_ref, out_ref, first, rows):
    height = short_ref.shape[1]
    coarse = height // FINE
    sc, ss = short_ref[:FINE], short_ref[FINE : 2 * FINE]
    for j in range(first // FINE, (first + rows) // FINE):
        a = 2 * FINE + j
        rc, rs = short_ref[a : a + 1, :], short_ref[a + coarse : a + coarse + 1, :]
        here = slice(j * FINE, (j + 1) * FINE)
        out_ref[here, :height] = (rc * sc - rs * ss).astype(jnp.bfloat16)
        out_ref[here, height:] = (rs * sc + rc * ss).astype(jnp.bfloat16)


def cost(flops, moved):
    return pl.CostEstimate(flops=flops, transcendentals=0, bytes_accessed=moved)


def params(limit=VMEM_LIMIT):
    return pltpu.CompilerParams(vmem_limit_bytes=limit)


def shade(tile, down_ref, across_ref):
    return (tile * (down_ref[...].T[:, :1] * across_ref[...])).astype(jnp.bfloat16)


def times_table(table, shaded):
    y = lax.dot_general(
        table, shaded, (((1,), (1,)), ((), ())), preferred_element_type=jnp.float32
    )
    return y.astype(jnp.bfloat16)


def near_columns(tiles, down, across, table, half, me, peers):
    count, rows, width = tiles.shape
    span = table.shape[0] // 2
    block = span // peers

    def body(half_ref, me_ref, tile_hbm, down_hbm, across_hbm, table_hbm, *refs):
        outs = refs[:2]
        tile_ref, table_ref, work, down_ref, across_ref, done = refs[2:]
        t = pl.program_id(0)
        me = me_ref[0]
        start = pl.multiple_of((1 - half_ref[0]) * span + me // 2 * 2 * block, 2 * block)
        fetch = pltpu.make_async_copy(
            table_hbm.at[pl.ds(start, 2 * block)], table_ref, done.at[count]
        )
        loads = [
            pltpu.make_async_copy(tile_hbm.at[i], tile_ref.at[i], done.at[i]) for i in range(count)
        ]

        lane = pl.multiple_of(me * rows, rows)
        extra = [
            pltpu.make_async_copy(down_hbm.at[:, pl.ds(lane, rows)], down_ref, done.at[count + 1]),
            pltpu.make_async_copy(across_hbm, across_ref, done.at[count + 2]),
        ]

        @pl.when(t == 0)
        def _():
            for copy in extra:
                copy.start()
            fetch.start()
            for load in loads:
                load.start()
            for copy in extra:
                copy.wait()
            fetch.wait()

        for i in range(count):

            @pl.when(t == i)
            def _():
                loads[i].wait()
                work[...] = times_table(table_ref[...], shade(tile_ref[i], down_ref, across_ref))

        for k in range(2):
            place = pl.multiple_of((me % 2 ^ k) * block, block)
            outs[k][0] = work[pl.ds(place, block), :]

    return pl.pallas_call(
        body,
        grid_spec=pltpu.PrefetchScalarGridSpec(
            num_scalar_prefetch=2,
            grid=(count,),
            in_specs=[
                pl.BlockSpec(memory_space=pltpu.HBM),
                pl.BlockSpec(memory_space=pltpu.HBM),
                pl.BlockSpec(memory_space=pltpu.HBM),
                pl.BlockSpec(memory_space=pltpu.HBM),
            ],
            out_specs=[pl.BlockSpec((1, block, rows), lambda t, half, me: (t, 0, 0))] * 2,
            scratch_shapes=[
                pltpu.VMEM((count, rows, width), tiles.dtype),
                pltpu.VMEM((2 * block, width), table.dtype),
                pltpu.VMEM((2 * block, rows), jnp.bfloat16),
                pltpu.VMEM((8, rows), jnp.float32),
                pltpu.VMEM((1, width), jnp.float32),
                pltpu.SemaphoreType.DMA((count + 3,)),
            ],
        ),
        out_shape=[jax.ShapeDtypeStruct((count, block, rows), jnp.bfloat16)] * 2,
        compiler_params=params(FIRST_LIMIT),
        cost_estimate=cost(4 * count * rows * width * block, 4 * tiles.size + 4 * block * width),
        name="near_columns",
    )(scalar(half), scalar(me), tiles, down, across, table)


def rest_columns(tiles, down, across, table, half, me, peers):
    count, rows, width = tiles.shape
    span = table.shape[0] // 2
    block = span // peers

    def body(half_ref, me_ref, tile_ref, down_ref, across_ref, table_ref, *refs):
        out_ref, far, work = refs[0], refs[1:-1], refs[-1]
        half, me = half_ref[0], me_ref[0]
        shaded = shade(tile_ref[pl.program_id(0)], down_ref, across_ref)
        for j in range(1, peers // 2):
            start = pl.multiple_of((1 - half) * span + (me // 2 ^ j) * 2 * block, 2 * block)
            work[...] = times_table(table_ref[pl.ds(start, 2 * block), :], shaded)
            for k in range(2):
                place = pl.multiple_of((me % 2 ^ k) * block, block)
                far[2 * j - 2 + k][0] = work[pl.ds(place, block), :]
        start = pl.multiple_of(half * span, span)
        y = times_table(table_ref[pl.ds(start, span), :], shaded)
        out_ref[:, 0] = y.reshape(peers, block, rows)

    piece = pl.BlockSpec((1, block, rows), lambda t, half, me: (t, 0, 0))
    return pl.pallas_call(
        body,
        grid_spec=pltpu.PrefetchScalarGridSpec(
            num_scalar_prefetch=2,
            grid=(count,),
            in_specs=[
                pl.BlockSpec(memory_space=pltpu.VMEM),
                pl.BlockSpec((8, rows), lambda t, half, me: (0, me[0])),
                pl.BlockSpec((1, width), lambda t, half, me: (0, 0)),
                pl.BlockSpec(memory_space=pltpu.VMEM),
            ],
            out_specs=[
                pl.BlockSpec((peers, 1, block, rows), lambda t, half, me: (0, t, 0, 0)),
                *[piece] * (peers - 2),
            ],
            scratch_shapes=[pltpu.VMEM((2 * block, rows), jnp.bfloat16)],
        ),
        out_shape=[
            jax.ShapeDtypeStruct((peers, count, block, rows), jnp.bfloat16),
            *[jax.ShapeDtypeStruct((count, block, rows), jnp.bfloat16)] * (peers - 2),
        ],
        compiler_params=params(),
        cost_estimate=cost(3 * count * rows * width * span, 4 * tiles.size + 2 * width * width),
        name="rest_columns",
    )(scalar(half), scalar(me), tiles, down, across, table)


def gather_rows(pieces, table_ref, me, first=0, total=None):
    for k, piece in enumerate(pieces, first):
        count, block, rows = piece.shape
        start = pl.multiple_of((me ^ k) * rows, rows)
        term = jnp.dot(
            piece[...].reshape(count * block, rows),
            table_ref[pl.ds(start, rows), :],
            preferred_element_type=jnp.float32,
        )
        total = term if total is None else total + term
    return total


def holds_packed(place):
    half_ref, me_ref = place
    return (half_ref[0] == 0) & (me_ref[0] == 0)


def store_spectra(s_ref, total, spectra, edge, first):
    block = spectra.shape[2]
    height = spectra.shape[3]
    row = lax.broadcasted_iota(jnp.int32, (block, height), 0)
    packed = (row == 0) & holds_packed(s_ref)
    for t in range(total.shape[0] // (2 * block)):
        real = total[2 * t * block : (2 * t + 1) * block]
        imag = total[(2 * t + 1) * block : (2 * t + 2) * block]
        cr, sr = real[:, :height], real[:, height:]
        ci, si = imag[:, :height], imag[:, height:]
        spectra[first + t, 0] = jnp.where(packed, cr, cr + si).astype(jnp.bfloat16)
        spectra[first + t, 1] = jnp.where(packed, -sr, ci - sr).astype(jnp.bfloat16)
        edge[first + t, 0] = ci[:16].astype(jnp.bfloat16)
        edge[first + t, 1] = (-si[:16]).astype(jnp.bfloat16)


def normalised(left_real, left_imag, right_real, right_imag):
    lr = left_real.astype(jnp.float32)
    li = left_imag.astype(jnp.float32)
    rr = right_real.astype(jnp.float32)
    ri = right_imag.astype(jnp.float32)
    cross_real = lr * rr + li * ri
    cross_imag = li * rr - lr * ri
    factor = 1.0 / (jnp.sqrt(cross_real * cross_real + cross_imag * cross_imag) + FLOOR)
    return (
        (cross_real * factor).astype(jnp.bfloat16),
        (cross_imag * factor).astype(jnp.bfloat16),
    )


def correlate(s_ref, picks, spectra, edge, phases):
    slots = len(picks)
    height = spectra.shape[3]
    lead = lax.broadcasted_iota(jnp.int32, (16, height), 0)
    packed = (lead == 0) & holds_packed(s_ref)
    for p in range(slots):
        a, c = picks[p]
        q_real, q_imag = normalised(spectra[a, 0], spectra[a, 1], spectra[c, 0], spectra[c, 1])
        e_real, e_imag = normalised(edge[a, 0], edge[a, 1], edge[c, 0], edge[c, 1])
        phases[2 * p] = q_real
        phases[2 * p + 1] = q_imag
        top_real = q_real[:16].astype(jnp.float32)
        top_imag = q_imag[:16].astype(jnp.float32)
        mixed_real = jnp.where(packed, top_real - e_imag.astype(jnp.float32), top_real)
        mixed_imag = jnp.where(packed, top_imag + e_real.astype(jnp.float32), top_imag)
        phases[2 * p, :16] = mixed_real.astype(jnp.bfloat16)
        phases[2 * p + 1, :16] = mixed_imag.astype(jnp.bfloat16)

def invert_columns(s_ref, me, phases, table_ref, outs):
    _, block, height = phases.shape
    slots = phases.shape[0] // 2
    rows = next(iter(outs.values()))[0].shape[1]
    row = lax.broadcasted_iota(jnp.int32, (block, rows), 0)
    twice = jnp.where((row == 0) & holds_packed(s_ref), 1.0, 2.0)
    flat = phases[...].reshape(2 * slots * block, height)
    for k, out in outs.items():
        start = pl.multiple_of((me ^ k) * rows, rows)
        c_part = jnp.dot(
            flat, table_ref[:, pl.ds(start, rows)], preferred_element_type=jnp.float32
        )
        start = pl.multiple_of(height + (me ^ k) * rows, rows)
        s_part = jnp.dot(
            flat, table_ref[:, pl.ds(start, rows)], preferred_element_type=jnp.float32
        )
        for p in range(slots):
            re = slice(2 * p * block, (2 * p + 1) * block)
            im = slice((2 * p + 1) * block, (2 * p + 2) * block)
            out[p][:block] = ((c_part[re] - s_part[im]) * twice).astype(jnp.bfloat16)
            out[p][block:] = ((s_part[re] + c_part[im]) * twice).astype(jnp.bfloat16)


def own_spectra(place, pieces, near, short):
    peers, count, double, rows = pieces.shape
    height = peers * rows

    def body(half_ref, me_ref, pieces_ref, near_a, near_b, short_ref, spectra, edge, share, table_ref):
        total = None
        for k in range(peers):
            make_table(short_ref, table_ref, k * rows, rows)
            term = jnp.dot(
                pieces_ref[k].reshape(count * double, rows),
                table_ref[k * rows : (k + 1) * rows],
                preferred_element_type=jnp.float32,
            )
            total = term if total is None else total + term
        store_spectra((half_ref, me_ref), total, spectra, edge, 0)
        share[...] = gather_rows([near_a, near_b], table_ref, me_ref[0])

    return pl.pallas_call(
        body,
        in_specs=[pl.BlockSpec(memory_space=pltpu.SMEM)] * 2
        + [pl.BlockSpec(memory_space=pltpu.VMEM)] * 4,
        out_specs=[pl.BlockSpec(memory_space=pltpu.VMEM)] * 4,
        out_shape=[
            jax.ShapeDtypeStruct((count, 2, double // 2, height), jnp.bfloat16),
            jax.ShapeDtypeStruct((count, 2, 16, height), jnp.bfloat16),
            jax.ShapeDtypeStruct((count * double, 2 * height), jnp.float32),
            jax.ShapeDtypeStruct((height, 2 * height), jnp.bfloat16),
        ],
        compiler_params=params(),
        cost_estimate=cost(6 * count * double * height * height, 8 * height * height),
        name="own_spectra",
    )(*place, pieces, *near, short)


def partner_slots(place, theirs, pieces, share, table, spectra, edge):
    distant = len(pieces)
    count, double, rows = pieces[0].shape
    height = table.shape[0]
    block = double // 2
    slots = theirs.shape[1]

    def body(half_ref, me_ref, theirs_ref, *refs):
        s_ref = (half_ref, me_ref)
        me = me_ref[0]
        picks = [
            [(theirs_ref[0, p, i] + count) % (2 * count) for i in range(2)] for p in range(slots)
        ]
        inputs = refs[:distant]
        share_ref, table_ref, own_ref, own_edge, near, every, edges, phases = refs[distant:]
        every[:count] = own_ref[...]
        edges[:count] = own_edge[...]
        total = gather_rows(inputs, table_ref, me, 2, share_ref[...])
        store_spectra(s_ref, total, every, edges, count)
        correlate(s_ref, picks, every, edges, phases)
        invert_columns(s_ref, me, phases, table_ref, {k: [near.at[k, p] for p in range(slots)] for k in range(2)})

    return pl.pallas_call(
        body,
        in_specs=[pl.BlockSpec(memory_space=pltpu.SMEM)] * 3
        + [pl.BlockSpec(memory_space=pltpu.VMEM)] * (distant + 4),
        out_specs=[pl.BlockSpec(memory_space=pltpu.VMEM)] * 4,
        out_shape=[
            jax.ShapeDtypeStruct((2, slots, double, rows), jnp.bfloat16),
            jax.ShapeDtypeStruct((2 * count, 2, block, height), jnp.bfloat16),
            jax.ShapeDtypeStruct((2 * count, 2, 16, height), jnp.bfloat16),
            jax.ShapeDtypeStruct((2 * slots, block, height), jnp.bfloat16),
        ],
        compiler_params=params(),
        cost_estimate=cost(4 * (count + slots) * double * height * height, 8 * height * height),
        name="partner_slots",
    )(*place, theirs, *pieces, share, table, spectra, edge)


def own_slots(place, pairs, table, spectra, edge, phases, peers):
    block, height = spectra.shape[2:]
    rows = height // peers
    slots = pairs.shape[1]

    def body(half_ref, me_ref, pairs_ref, table_ref, every, edges, theirs, out_ref, *refs):
        s_ref = (half_ref, me_ref)
        far, work = refs[:-1], refs[-1]
        picks = [[pairs_ref[0, p, i] for i in range(2)] for p in range(slots)]
        if far:
            outs = {
                k: [far[(k - 2) * slots + p].at[0] for p in range(slots)] for k in range(2, peers)
            }
            invert_columns(s_ref, me_ref[0], theirs, table_ref, outs)
        correlate(s_ref, picks, every, edges, work)
        outs = {k: [out_ref.at[k, p] for p in range(slots)] for k in range(peers)}
        invert_columns(s_ref, 0, work, table_ref, outs)

    return pl.pallas_call(
        body,
        in_specs=[pl.BlockSpec(memory_space=pltpu.SMEM)] * 3
        + [pl.BlockSpec(memory_space=pltpu.VMEM)] * 4,
        out_specs=[pl.BlockSpec(memory_space=pltpu.VMEM)] * (1 + (peers - 2) * slots),
        out_shape=[
            jax.ShapeDtypeStruct((peers, slots, 2 * block, rows), jnp.bfloat16),
            *[jax.ShapeDtypeStruct((1, 2 * block, rows), jnp.bfloat16)] * ((peers - 2) * slots),
        ],
        scratch_shapes=[pltpu.VMEM((2 * slots, block, height), jnp.bfloat16)],
        compiler_params=params(),
        cost_estimate=cost(8 * slots * block * height * height, 8 * height * height),
        name="own_slots",
    )(*place, pairs, table, spectra, edge, phases)


def own_surfaces(half, own, table):
    peers, slots, double, rows = own.shape
    width = table.shape[0]
    span = peers * double

    def body(half_ref, own_ref, table_ref, out_ref):
        out_ref[0] = lax.dot_general(
            own_ref[:, 0].reshape(span, rows),
            table_ref[...],
            (((0,), (0,)), ((), ())),
            preferred_element_type=jnp.float32,
        )

    return pl.pallas_call(
        body,
        grid_spec=pltpu.PrefetchScalarGridSpec(
            num_scalar_prefetch=1,
            grid=(slots,),
            in_specs=[
                pl.BlockSpec((peers, 1, double, rows), lambda p, half: (0, p, 0, 0)),
                pl.BlockSpec((span, width), lambda p, half: (half[0], 0)),
            ],
            out_specs=pl.BlockSpec((1, rows, width), lambda p, half: (p, 0, 0)),
        ),
        out_shape=jax.ShapeDtypeStruct((slots, rows, width), jnp.float32),
        compiler_params=params(),
        cost_estimate=cost(2 * slots * rows * width * span, 4 * slots * rows * width),
        name="own_surfaces",
    )(scalar(half), own, table)


def surface_of(slot, half, me, counts, part, near, swapped, far, table, before):
    peers = 2 + len(far)
    slots, double, rows = swapped.shape
    width = table.shape[0]
    span = peers * double

    def body(half_ref, me_ref, counts_ref, part_ref, near_ref, swapped_ref, *refs):
        far_refs, table_ref, out_ref, work = refs[: peers - 2], refs[peers - 2], refs[-2], refs[-1]
        pieces = [near_ref[0, 0], swapped_ref[0]] + [ref[0] for ref in far_refs]
        for k, piece in enumerate(pieces):
            place = pl.multiple_of((me_ref[0] ^ k) * double, double)
            work[pl.ds(place, double), :] = piece
        start = pl.multiple_of((1 - half_ref[0]) * span, span)
        rest = lax.dot_general(
            work[...],
            table_ref[pl.ds(start, span), :],
            (((0,), (0,)), ((), ())),
            preferred_element_type=jnp.float32,
        )
        out_ref[0] = jnp.where(slot < counts_ref[0], part_ref[slot] + rest, 0.0)

    return pl.pallas_call(
        body,
        grid_spec=pltpu.PrefetchScalarGridSpec(
            num_scalar_prefetch=3,
            grid=(1,),
            in_specs=[
                pl.BlockSpec(memory_space=pltpu.VMEM),
                pl.BlockSpec((1, 1, double, rows), lambda i, half, me, counts: (0, slot, 0, 0)),
                pl.BlockSpec((1, double, rows), lambda i, half, me, counts: (slot, 0, 0)),
                *[pl.BlockSpec((1, double, rows), lambda i, half, me, counts: (0, 0, 0))]
                * (peers - 2),
                pl.BlockSpec(memory_space=pltpu.VMEM),
                *[pl.BlockSpec(memory_space=pl.ANY)] * len(before),
            ],
            out_specs=pl.BlockSpec((1, rows, width), lambda i, half, me, counts: (slot, 0, 0)),
            scratch_shapes=[pltpu.VMEM((span, rows), jnp.bfloat16)],
        ),
        out_shape=jax.ShapeDtypeStruct((slots, rows, width), jnp.float32),
        input_output_aliases={7 + peers - 2: 0} if before else {},
        compiler_params=params(),
        cost_estimate=cost(2 * rows * width * span, 8 * rows * width),
        name="surface",
    )(scalar(half), scalar(me), counts, part, near, swapped, *far, table, *before)


def local(tiles, pairs, counts):
    groups = lax.axis_size("blk")
    peers = lax.axis_size("rows")
    group = lax.axis_index("blk")
    me = lax.axis_index("rows")
    count, rows, width = tiles.shape
    height = rows * peers
    turn = groups // 2
    half = group // turn
    axes = ("blk", "rows")

    def across(value, k):
        moves = [
            (b * peers + r, (b + turn) % groups * peers + (r ^ k))
            for b in range(groups)
            for r in range(peers)
        ]
        return lax.ppermute(value, axes, moves)

    def along(blocks):
        return lax.all_to_all(blocks, "rows", split_axis=0, concat_axis=0)

    def swap(value):
        return lax.ppermute(value, "rows", [(r, r ^ 1) for r in range(peers)])

    table_w = jnp.asarray(width_table(width, 2 * peers))
    down = jnp.asarray(np.tile(hann(height), (8, 1)))
    sideways = jnp.asarray(hann(width)[None, :])

    sent = near_columns(tiles, down, sideways, table_w, half, me, peers)
    arrived = [across(sent[k], k) for k in range(2)]
    *sent, held = lax.optimization_barrier((*sent, half))
    kept, *sent = rest_columns(tiles, down, sideways, table_w, held, me, peers)
    *sent, kept, pairs = lax.optimization_barrier((*sent, kept, pairs))
    arrived += [across(sent[k - 2], k) for k in range(2, peers)]
    mine = along(kept)

    theirs = across(pairs, 0)
    place = (scalar(half), scalar(me))
    spectra, edge, share, table_h = own_spectra(
        place, mine, arrived[:2], scaled_tables(height, [])
    )
    near, spectra, edge, phases = partner_slots(
        place, theirs, arrived[2:], share, table_h, spectra, edge
    )
    near = across(near, 0)
    own, *far = own_slots(place, pairs, table_h, spectra, edge, phases, peers)
    slots = pairs.shape[1]
    far = [
        [across(far[(k - 2) * slots + p], k) for k in range(2, peers)] for p in range(slots)
    ]
    part = own_surfaces(half, along(own), table_w)
    *far[0], part = lax.optimization_barrier((*far[0], part))
    swapped = swap(near[1])
    before = []
    for p in range(slots):
        before = [
            surface_of(p, half, me, counts, part, near, swapped, far[p], table_w, before)
        ]
    return before[0]


def solution(mesh):
    from jax.sharding import PartitionSpec as P

    return jax.shard_map(
        local,
        mesh=mesh,
        in_specs=(
            P(("parts", "blk"), "rows", None),
            P(("parts", "blk"), None, None),
            P(("parts", "blk")),
        ),
        out_specs=P(("parts", "blk"), "rows", None),
        check_vma=False,
    )
```

```python
import math

import jax
import jax.numpy as jnp
import numpy as np
from jax import lax
from jax.experimental import pallas as pl
from jax.experimental.pallas import tpu as pltpu

FLOOR = 0.05
VMEM_LIMIT = 24 * 1024 * 1024
FIRST_LIMIT = 58 * 1024 * 1024


def hann(length):
    return np.asarray(0.5 - 0.5 * np.cos(2.0 * math.pi / length * np.arange(length)), np.float32)


def scalar(value):
    return jnp.reshape(value, (1,)).astype(jnp.int32)


def width_table(width, owners):
    half = width // 2
    phase = np.arange(half)[:, None] * np.arange(width)[None, :] % width
    angle = 2.0 * math.pi / width * phase
    factor = 1.0 / math.sqrt(width)
    cosine = np.cos(angle) * factor
    sine = -np.sin(angle) * factor
    sine[0] = np.where(np.arange(width) % 2 == 0, factor, -factor)
    shape = (owners, half // owners, width)
    table = np.stack([cosine.reshape(shape), sine.reshape(shape)], axis=1)
    return table.reshape(width, width).astype(jnp.bfloat16)


FINE = 32


LANES = 128


def short_tables(height):
    coarse = height // FINE
    column = np.arange(height)[None, :]
    rough = 2.0 * math.pi / height * (np.arange(coarse)[:, None] * FINE * column % height)
    small = 2.0 * math.pi / height * (np.arange(FINE)[:, None] * column % height)
    rough = rough[:, :LANES]
    return (
        jnp.asarray(np.concatenate([np.cos(small), np.sin(small)]), jnp.float32),
        jnp.asarray(np.concatenate([np.cos(rough), np.sin(rough)]), jnp.float32),
    )


def scaled_tables(height):
    factor = 1.0 / math.sqrt(height)

    def body(fine_ref, rough_ref, fine_out, rough_out):
        fine_out[...] = fine_ref[...]
        rough_out[...] = rough_ref[...] * factor

    short = short_tables(height)
    return pl.pallas_call(
        body,
        in_specs=[pl.BlockSpec(memory_space=pltpu.VMEM)] * 2,
        out_specs=[pl.BlockSpec(memory_space=pltpu.VMEM)] * 2,
        out_shape=[jax.ShapeDtypeStruct(table.shape, table.dtype) for table in short],
        compiler_params=params(),
        cost_estimate=cost(1 << 33, 8 * short[0].size),
        name="scaled_tables",
    )(*short)


def make_table(fine_ref, rough_ref, out_ref, first, rows):
    height = fine_ref.shape[1]
    coarse = height // FINE
    copies = height // LANES
    sc, ss = fine_ref[:FINE], fine_ref[FINE:]
    for j in range(first // FINE, (first + rows) // FINE):
        rc = jnp.concatenate([rough_ref[j : j + 1, :]] * copies, axis=1)
        rs = jnp.concatenate([rough_ref[coarse + j : coarse + j + 1, :]] * copies, axis=1)
        here = slice(j * FINE, (j + 1) * FINE)
        out_ref[here, :height] = (rc * sc - rs * ss).astype(jnp.bfloat16)
        out_ref[here, height:] = (rs * sc + rc * ss).astype(jnp.bfloat16)


def cost(flops, moved):
    return pl.CostEstimate(flops=flops, transcendentals=0, bytes_accessed=moved)


def params(limit=VMEM_LIMIT):
    return pltpu.CompilerParams(vmem_limit_bytes=limit)


def shade(tile, down_ref, across_ref):
    return (tile * (down_ref[...].T[:, :1] * across_ref[...])).astype(jnp.bfloat16)


def times_table(table, shaded):
    y = lax.dot_general(
        table, shaded, (((1,), (1,)), ((), ())), preferred_element_type=jnp.float32
    )
    return y.astype(jnp.bfloat16)


def near_columns(tiles, down, across, table, half, me, peers):
    count, rows, width = tiles.shape
    span = table.shape[0] // 2
    block = span // peers

    def body(half_ref, me_ref, tile_hbm, down_hbm, across_hbm, table_hbm, *refs):
        outs = refs[:2]
        tile_ref, table_ref, work, down_ref, across_ref, done = refs[2:]
        t = pl.program_id(0)
        me = me_ref[0]
        start = pl.multiple_of((1 - half_ref[0]) * span + me // 2 * 2 * block, 2 * block)
        fetch = pltpu.make_async_copy(
            table_hbm.at[pl.ds(start, 2 * block)], table_ref, done.at[count]
        )
        loads = [
            pltpu.make_async_copy(tile_hbm.at[i], tile_ref.at[i], done.at[i]) for i in range(count)
        ]

        lane = pl.multiple_of(me * rows, rows)
        extra = [
            pltpu.make_async_copy(down_hbm.at[:, pl.ds(lane, rows)], down_ref, done.at[count + 1]),
            pltpu.make_async_copy(across_hbm, across_ref, done.at[count + 2]),
        ]

        @pl.when(t == 0)
        def _():
            for copy in extra:
                copy.start()
            fetch.start()
            for load in loads:
                load.start()
            for copy in extra:
                copy.wait()
            fetch.wait()

        for i in range(count):

            @pl.when(t == i)
            def _():
                loads[i].wait()
                work[...] = times_table(table_ref[...], shade(tile_ref[i], down_ref, across_ref))

        for k in range(2):
            place = pl.multiple_of((me % 2 ^ k) * block, block)
            outs[k][0] = work[pl.ds(place, block), :]

    return pl.pallas_call(
        body,
        grid_spec=pltpu.PrefetchScalarGridSpec(
            num_scalar_prefetch=2,
            grid=(count,),
            in_specs=[
                pl.BlockSpec(memory_space=pltpu.HBM),
                pl.BlockSpec(memory_space=pltpu.HBM),
                pl.BlockSpec(memory_space=pltpu.HBM),
                pl.BlockSpec(memory_space=pltpu.HBM),
            ],
            out_specs=[pl.BlockSpec((1, block, rows), lambda t, half, me: (t, 0, 0))] * 2,
            scratch_shapes=[
                pltpu.VMEM((count, rows, width), tiles.dtype),
                pltpu.VMEM((2 * block, width), table.dtype),
                pltpu.VMEM((2 * block, rows), jnp.bfloat16),
                pltpu.VMEM((8, rows), jnp.float32),
                pltpu.VMEM((1, width), jnp.float32),
                pltpu.SemaphoreType.DMA((count + 3,)),
            ],
        ),
        out_shape=[jax.ShapeDtypeStruct((count, block, rows), jnp.bfloat16)] * 2,
        compiler_params=params(FIRST_LIMIT),
        cost_estimate=cost(4 * count * rows * width * block, 4 * tiles.size + 4 * block * width),
        name="near_columns",
    )(scalar(half), scalar(me), tiles, down, across, table)


def rest_columns(tiles, down, across, table, half, me, peers):
    count, rows, width = tiles.shape
    span = table.shape[0] // 2
    block = span // peers

    def body(half_ref, me_ref, tile_ref, down_ref, across_ref, table_ref, *refs):
        out_ref, far, work = refs[0], refs[1:-1], refs[-1]
        half, me = half_ref[0], me_ref[0]
        shaded = shade(tile_ref[pl.program_id(0)], down_ref, across_ref)
        for j in range(1, peers // 2):
            start = pl.multiple_of((1 - half) * span + (me // 2 ^ j) * 2 * block, 2 * block)
            work[...] = times_table(table_ref[pl.ds(start, 2 * block), :], shaded)
            for k in range(2):
                place = pl.multiple_of((me % 2 ^ k) * block, block)
                far[2 * j - 2 + k][0] = work[pl.ds(place, block), :]
        start = pl.multiple_of(half * span, span)
        y = times_table(table_ref[pl.ds(start, span), :], shaded)
        out_ref[:, 0] = y.reshape(peers, block, rows)

    piece = pl.BlockSpec((1, block, rows), lambda t, half, me: (t, 0, 0))
    return pl.pallas_call(
        body,
        grid_spec=pltpu.PrefetchScalarGridSpec(
            num_scalar_prefetch=2,
            grid=(count,),
            in_specs=[
                pl.BlockSpec(memory_space=pltpu.VMEM),
                pl.BlockSpec((8, rows), lambda t, half, me: (0, me[0])),
                pl.BlockSpec((1, width), lambda t, half, me: (0, 0)),
                pl.BlockSpec(memory_space=pltpu.VMEM),
            ],
            out_specs=[
                pl.BlockSpec((peers, 1, block, rows), lambda t, half, me: (0, t, 0, 0)),
                *[piece] * (peers - 2),
            ],
            scratch_shapes=[pltpu.VMEM((2 * block, rows), jnp.bfloat16)],
        ),
        out_shape=[
            jax.ShapeDtypeStruct((peers, count, block, rows), jnp.bfloat16),
            *[jax.ShapeDtypeStruct((count, block, rows), jnp.bfloat16)] * (peers - 2),
        ],
        compiler_params=params(),
        cost_estimate=cost(3 * count * rows * width * span, 4 * tiles.size + 2 * width * width),
        name="rest_columns",
    )(scalar(half), scalar(me), tiles, down, across, table)


def gather_rows(pieces, table_ref, me, first=0, total=None):
    for k, piece in enumerate(pieces, first):
        count, block, rows = piece.shape
        start = pl.multiple_of((me ^ k) * rows, rows)
        term = jnp.dot(
            piece[...].reshape(count * block, rows),
            table_ref[pl.ds(start, rows), :],
            preferred_element_type=jnp.float32,
        )
        total = term if total is None else total + term
    return total


def holds_packed(place):
    half_ref, me_ref = place
    return (half_ref[0] == 0) & (me_ref[0] == 0)


def store_spectra(s_ref, total, spectra, edge, first):
    block = spectra.shape[2]
    height = spectra.shape[3]
    row = lax.broadcasted_iota(jnp.int32, (block, height), 0)
    packed = (row == 0) & holds_packed(s_ref)
    for t in range(total.shape[0] // (2 * block)):
        real = total[2 * t * block : (2 * t + 1) * block]
        imag = total[(2 * t + 1) * block : (2 * t + 2) * block]
        cr, sr = real[:, :height], real[:, height:]
        ci, si = imag[:, :height], imag[:, height:]
        spectra[first + t, 0] = jnp.where(packed, cr, cr + si).astype(jnp.bfloat16)
        spectra[first + t, 1] = jnp.where(packed, -sr, ci - sr).astype(jnp.bfloat16)
        edge[first + t, 0] = ci[:16].astype(jnp.bfloat16)
        edge[first + t, 1] = (-si[:16]).astype(jnp.bfloat16)


def normalised(left_real, left_imag, right_real, right_imag):
    lr = left_real.astype(jnp.float32)
    li = left_imag.astype(jnp.float32)
    rr = right_real.astype(jnp.float32)
    ri = right_imag.astype(jnp.float32)
    cross_real = lr * rr + li * ri
    cross_imag = li * rr - lr * ri
    factor = 1.0 / (jnp.sqrt(cross_real * cross_real + cross_imag * cross_imag) + FLOOR)
    return (
        (cross_real * factor).astype(jnp.bfloat16),
        (cross_imag * factor).astype(jnp.bfloat16),
    )


def correlate(s_ref, picks, spectra, edge, phases):
    slots = len(picks)
    height = spectra.shape[3]
    lead = lax.broadcasted_iota(jnp.int32, (16, height), 0)
    packed = (lead == 0) & holds_packed(s_ref)
    for p in range(slots):
        a, c = picks[p]
        q_real, q_imag = normalised(spectra[a, 0], spectra[a, 1], spectra[c, 0], spectra[c, 1])
        e_real, e_imag = normalised(edge[a, 0], edge[a, 1], edge[c, 0], edge[c, 1])
        phases[2 * p] = q_real
        phases[2 * p + 1] = q_imag
        top_real = q_real[:16].astype(jnp.float32)
        top_imag = q_imag[:16].astype(jnp.float32)
        mixed_real = jnp.where(packed, top_real - e_imag.astype(jnp.float32), top_real)
        mixed_imag = jnp.where(packed, top_imag + e_real.astype(jnp.float32), top_imag)
        phases[2 * p, :16] = mixed_real.astype(jnp.bfloat16)
        phases[2 * p + 1, :16] = mixed_imag.astype(jnp.bfloat16)

def invert_columns(s_ref, me, phases, table_ref, outs):
    _, block, height = phases.shape
    slots = phases.shape[0] // 2
    rows = next(iter(outs.values())).shape[2]
    row = lax.broadcasted_iota(jnp.int32, (block, rows), 0)
    twice = jnp.where((row == 0) & holds_packed(s_ref), 1.0, 2.0)
    flat = phases[...].reshape(2 * slots * block, height)
    for k, out in outs.items():
        start = pl.multiple_of((me ^ k) * rows, rows)
        c_part = jnp.dot(
            flat, table_ref[:, pl.ds(start, rows)], preferred_element_type=jnp.float32
        )
        start = pl.multiple_of(height + (me ^ k) * rows, rows)
        s_part = jnp.dot(
            flat, table_ref[:, pl.ds(start, rows)], preferred_element_type=jnp.float32
        )
        for p in range(slots):
            re = slice(2 * p * block, (2 * p + 1) * block)
            im = slice((2 * p + 1) * block, (2 * p + 2) * block)
            out[p, :block] = ((c_part[re] - s_part[im]) * twice).astype(jnp.bfloat16)
            out[p, block:] = ((s_part[re] + c_part[im]) * twice).astype(jnp.bfloat16)


def own_spectra(place, pieces, near, short):
    peers, count, double, rows = pieces.shape
    height = peers * rows

    def body(half_ref, me_ref, pieces_ref, near_a, near_b, *refs):
        fine_ref, rough_ref, spectra, edge, share, table_ref = refs
        total = None
        for k in range(peers):
            make_table(fine_ref, rough_ref, table_ref, k * rows, rows)
            term = jnp.dot(
                pieces_ref[k].reshape(count * double, rows),
                table_ref[k * rows : (k + 1) * rows],
                preferred_element_type=jnp.float32,
            )
            total = term if total is None else total + term
        store_spectra((half_ref, me_ref), total, spectra, edge, 0)
        share[...] = gather_rows([near_a, near_b], table_ref, me_ref[0])

    return pl.pallas_call(
        body,
        in_specs=[pl.BlockSpec(memory_space=pltpu.SMEM)] * 2
        + [pl.BlockSpec(memory_space=pltpu.VMEM)] * 5,
        out_specs=[pl.BlockSpec(memory_space=pltpu.VMEM)] * 4,
        out_shape=[
            jax.ShapeDtypeStruct((count, 2, double // 2, height), jnp.bfloat16),
            jax.ShapeDtypeStruct((count, 2, 16, height), jnp.bfloat16),
            jax.ShapeDtypeStruct((count * double, 2 * height), jnp.float32),
            jax.ShapeDtypeStruct((height, 2 * height), jnp.bfloat16),
        ],
        compiler_params=params(),
        cost_estimate=cost(6 * count * double * height * height, 8 * height * height),
        name="own_spectra",
    )(*place, pieces, *near, *short)


def partner_slots(place, theirs, pieces, share, table, spectra, edge):
    distant = len(pieces)
    count, double, rows = pieces[0].shape
    height = table.shape[0]
    block = double // 2
    slots = theirs.shape[1]

    def body(half_ref, me_ref, theirs_ref, *refs):
        s_ref = (half_ref, me_ref)
        me = me_ref[0]
        picks = [
            [(theirs_ref[0, p, i] + count) % (2 * count) for i in range(2)] for p in range(slots)
        ]
        inputs = refs[:distant]
        share_ref, table_ref, own_ref, own_edge, near, every, edges, phases = refs[distant:]
        every[:count] = own_ref[...]
        edges[:count] = own_edge[...]
        total = gather_rows(inputs, table_ref, me, 2, share_ref[...])
        store_spectra(s_ref, total, every, edges, count)
        correlate(s_ref, picks, every, edges, phases)
        invert_columns(s_ref, me, phases, table_ref, {k: near.at[k] for k in range(2)})

    return pl.pallas_call(
        body,
        in_specs=[pl.BlockSpec(memory_space=pltpu.SMEM)] * 3
        + [pl.BlockSpec(memory_space=pltpu.VMEM)] * (distant + 4),
        out_specs=[pl.BlockSpec(memory_space=pltpu.VMEM)] * 4,
        out_shape=[
            jax.ShapeDtypeStruct((2, slots, double, rows), jnp.bfloat16),
            jax.ShapeDtypeStruct((2 * count, 2, block, height), jnp.bfloat16),
            jax.ShapeDtypeStruct((2 * count, 2, 16, height), jnp.bfloat16),
            jax.ShapeDtypeStruct((2 * slots, block, height), jnp.bfloat16),
        ],
        compiler_params=params(),
        cost_estimate=cost(4 * (count + slots) * double * height * height, 8 * height * height),
        name="partner_slots",
    )(*place, theirs, *pieces, share, table, spectra, edge)


def own_slots(place, pairs, table, spectra, edge, phases, peers):
    block, height = spectra.shape[2:]
    rows = height // peers
    slots = pairs.shape[1]

    def body(half_ref, me_ref, pairs_ref, table_ref, every, edges, theirs, out_ref, *refs):
        s_ref = (half_ref, me_ref)
        far, work = refs[:-1], refs[-1]
        picks = [[pairs_ref[0, p, i] for i in range(2)] for p in range(slots)]
        if far:
            outs = {k: far[k - 2] for k in range(2, peers)}
            invert_columns(s_ref, me_ref[0], theirs, table_ref, outs)
        correlate(s_ref, picks, every, edges, work)
        invert_columns(s_ref, 0, work, table_ref, {k: out_ref.at[k] for k in range(peers)})

    return pl.pallas_call(
        body,
        in_specs=[pl.BlockSpec(memory_space=pltpu.SMEM)] * 3
        + [pl.BlockSpec(memory_space=pltpu.VMEM)] * 4,
        out_specs=[pl.BlockSpec(memory_space=pltpu.VMEM)] * (peers - 1),
        out_shape=[
            jax.ShapeDtypeStruct((peers, slots, 2 * block, rows), jnp.bfloat16),
            *[jax.ShapeDtypeStruct((slots, 2 * block, rows), jnp.bfloat16)] * (peers - 2),
        ],
        scratch_shapes=[pltpu.VMEM((2 * slots, block, height), jnp.bfloat16)],
        compiler_params=params(),
        cost_estimate=cost(8 * slots * block * height * height, 8 * height * height),
        name="own_slots",
    )(*place, pairs, table, spectra, edge, phases)


def own_surfaces(half, own, table):
    peers, slots, double, rows = own.shape
    width = table.shape[0]
    span = peers * double

    def body(half_ref, own_ref, table_ref, out_ref):
        out_ref[0] = lax.dot_general(
            own_ref[:, 0].reshape(span, rows),
            table_ref[...],
            (((0,), (0,)), ((), ())),
            preferred_element_type=jnp.float32,
        )

    return pl.pallas_call(
        body,
        grid_spec=pltpu.PrefetchScalarGridSpec(
            num_scalar_prefetch=1,
            grid=(slots,),
            in_specs=[
                pl.BlockSpec((peers, 1, double, rows), lambda p, half: (0, p, 0, 0)),
                pl.BlockSpec((span, width), lambda p, half: (half[0], 0)),
            ],
            out_specs=pl.BlockSpec((1, rows, width), lambda p, half: (p, 0, 0)),
        ),
        out_shape=jax.ShapeDtypeStruct((slots, rows, width), jnp.float32),
        compiler_params=params(),
        cost_estimate=cost(2 * slots * rows * width * span, 4 * slots * rows * width),
        name="own_surfaces",
    )(scalar(half), own, table)


def surfaces_of(half, me, counts, part, near, other, table):
    peers = 1 + len(other)
    slots, double, rows = other[0].shape
    width = table.shape[0]
    span = peers * double

    def body(half_ref, me_ref, counts_ref, part_ref, *refs):
        other_refs = refs[:peers]
        table_ref, out_ref, work = refs[peers:]
        for k in range(peers):
            place = pl.multiple_of((me_ref[0] ^ k) * double, double)
            piece = other_refs[k][0] if k else other_refs[k][0, 0]
            work[pl.ds(place, double), :] = piece
        start = pl.multiple_of((1 - half_ref[0]) * span, span)
        rest = lax.dot_general(
            work[...],
            table_ref[pl.ds(start, span), :],
            (((0,), (0,)), ((), ())),
            preferred_element_type=jnp.float32,
        )
        live = pl.program_id(0) < counts_ref[0]
        out_ref[0] = jnp.where(live, part_ref[pl.program_id(0)] + rest, 0.0)

    pair = pl.BlockSpec((1, 1, double, rows), lambda p, half, me, counts: (0, p, 0, 0))
    piece = pl.BlockSpec((1, double, rows), lambda p, half, me, counts: (p, 0, 0))
    plane = pl.BlockSpec((1, rows, width), lambda p, half, me, counts: (p, 0, 0))
    return pl.pallas_call(
        body,
        grid_spec=pltpu.PrefetchScalarGridSpec(
            num_scalar_prefetch=3,
            grid=(slots,),
            in_specs=[
                pl.BlockSpec(memory_space=pltpu.VMEM),
                pair,
                *[piece] * (peers - 1),
                pl.BlockSpec(memory_space=pltpu.VMEM),
            ],
            out_specs=plane,
            scratch_shapes=[pltpu.VMEM((span, rows), jnp.bfloat16)],
        ),
        out_shape=jax.ShapeDtypeStruct((slots, rows, width), jnp.float32),
        compiler_params=params(),
        cost_estimate=cost(2 * slots * rows * width * span, 8 * slots * rows * width),
        name="surfaces",
    )(scalar(half), scalar(me), counts, part, near, *other, table)


def local(tiles, pairs, counts):
    groups = lax.axis_size("blk")
    peers = lax.axis_size("rows")
    group = lax.axis_index("blk")
    me = lax.axis_index("rows")
    count, rows, width = tiles.shape
    height = rows * peers
    turn = groups // 2
    half = group // turn
    axes = ("blk", "rows")

    def across(value, k):
        moves = [
            (b * peers + r, (b + turn) % groups * peers + (r ^ k))
            for b in range(groups)
            for r in range(peers)
        ]
        return lax.ppermute(value, axes, moves)

    def along(blocks):
        return lax.all_to_all(blocks, "rows", split_axis=0, concat_axis=0)

    def swap(value):
        return lax.ppermute(value, "rows", [(r, r ^ 1) for r in range(peers)])

    table_w = jnp.asarray(width_table(width, 2 * peers))
    down = jnp.asarray(np.tile(hann(height), (8, 1)))
    sideways = jnp.asarray(hann(width)[None, :])

    sent = near_columns(tiles, down, sideways, table_w, half, me, peers)
    arrived = [across(sent[k], k) for k in range(2)]
    *sent, held = lax.optimization_barrier((*sent, half))
    kept, *sent = rest_columns(tiles, down, sideways, table_w, held, me, peers)
    *sent, kept, pairs = lax.optimization_barrier((*sent, kept, pairs))
    arrived += [across(sent[k - 2], k) for k in range(2, peers)]
    mine = along(kept)

    theirs = across(pairs, 0)
    place = (scalar(half), scalar(me))
    spectra, edge, share, table_h = own_spectra(
        place, mine, arrived[:2], scaled_tables(height)
    )
    near, spectra, edge, phases = partner_slots(
        place, theirs, arrived[2:], share, table_h, spectra, edge
    )
    near = across(near, 0)
    own, *far = own_slots(place, pairs, table_h, spectra, edge, phases, peers)
    far = [across(far[k - 2], k) for k in range(2, peers)]
    part = own_surfaces(half, along(own), table_w)
    *far, part = lax.optimization_barrier((*far, part))
    return surfaces_of(half, me, counts, part, near, [swap(near[1]), *far], table_w)


def solution(mesh):
    from jax.sharding import PartitionSpec as P

    return jax.shard_map(
        local,
        mesh=mesh,
        in_specs=(
            P(("parts", "blk"), "rows", None),
            P(("parts", "blk"), None, None),
            P(("parts", "blk")),
        ),
        out_specs=P(("parts", "blk"), "rows", None),
        check_vma=False,
    )
```

```python
import math

import jax
import jax.numpy as jnp
import numpy as np
from jax import lax
from jax.experimental import pallas as pl
from jax.experimental.pallas import tpu as pltpu

FLOOR = 0.05
VMEM_LIMIT = 24 * 1024 * 1024
FIRST_LIMIT = 58 * 1024 * 1024


def hann(length):
    return np.asarray(0.5 - 0.5 * np.cos(2.0 * math.pi / length * np.arange(length)), np.float32)


def scalar(value):
    return jnp.reshape(value, (1,)).astype(jnp.int32)


def width_table(width, owners):
    half = width // 2
    phase = np.arange(half)[:, None] * np.arange(width)[None, :] % width
    angle = 2.0 * math.pi / width * phase
    factor = 1.0 / math.sqrt(width)
    cosine = np.cos(angle) * factor
    sine = -np.sin(angle) * factor
    sine[0] = np.where(np.arange(width) % 2 == 0, factor, -factor)
    shape = (owners, half // owners, width)
    table = np.stack([cosine.reshape(shape), sine.reshape(shape)], axis=1)
    return table.reshape(width, width).astype(jnp.bfloat16)


FINE = 32


LANES = 128


def short_tables(height):
    coarse = height // FINE
    column = np.arange(height)[None, :]
    rough = 2.0 * math.pi / height * (np.arange(coarse)[:, None] * FINE * column % height)
    small = 2.0 * math.pi / height * (np.arange(FINE)[:, None] * column % height)
    rough = rough[:, :LANES]
    return (
        jnp.asarray(np.concatenate([np.cos(small), np.sin(small)]), jnp.float32),
        jnp.asarray(np.concatenate([np.cos(rough), np.sin(rough)]), jnp.float32),
    )


def scaled_tables(height):
    factor = 1.0 / math.sqrt(height)

    def body(fine_ref, rough_ref, fine_out, rough_out):
        fine_out[...] = fine_ref[...]
        rough_out[...] = rough_ref[...] * factor

    short = short_tables(height)
    return pl.pallas_call(
        body,
        in_specs=[pl.BlockSpec(memory_space=pltpu.VMEM)] * 2,
        out_specs=[pl.BlockSpec(memory_space=pltpu.VMEM)] * 2,
        out_shape=[jax.ShapeDtypeStruct(table.shape, table.dtype) for table in short],
        compiler_params=params(),
        cost_estimate=cost(1 << 33, 8 * short[0].size),
        name="scaled_tables",
    )(*short)


def make_table(fine_ref, rough_ref, out_ref, first, rows):
    height = fine_ref.shape[1]
    coarse = height // FINE
    copies = height // LANES
    sc, ss = fine_ref[:FINE], fine_ref[FINE:]
    for j in range(first // FINE, (first + rows) // FINE):
        rc = jnp.concatenate([rough_ref[j : j + 1, :]] * copies, axis=1)
        rs = jnp.concatenate([rough_ref[coarse + j : coarse + j + 1, :]] * copies, axis=1)
        here = slice(j * FINE, (j + 1) * FINE)
        out_ref[here, :height] = (rc * sc - rs * ss).astype(jnp.bfloat16)
        out_ref[here, height:] = (rs * sc + rc * ss).astype(jnp.bfloat16)


def cost(flops, moved):
    return pl.CostEstimate(flops=flops, transcendentals=0, bytes_accessed=moved)


def params(limit=VMEM_LIMIT):
    return pltpu.CompilerParams(vmem_limit_bytes=limit)


def shade(tile, down_ref, across_ref):
    return (tile * (down_ref[...].T[:, :1] * across_ref[...])).astype(jnp.bfloat16)


def times_table(table, shaded):
    y = lax.dot_general(
        table, shaded, (((1,), (1,)), ((), ())), preferred_element_type=jnp.float32
    )
    return y.astype(jnp.bfloat16)


def near_columns(tiles, down, across, table, half, me, peers):
    count, rows, width = tiles.shape
    span = table.shape[0] // 2
    block = span // peers

    def body(half_ref, me_ref, tile_hbm, down_hbm, across_hbm, table_hbm, *refs):
        outs = refs[:2]
        tile_ref, table_ref, work, down_ref, across_ref, done = refs[2:]
        t = pl.program_id(0)
        me = me_ref[0]
        start = pl.multiple_of((1 - half_ref[0]) * span + me // 2 * 2 * block, 2 * block)
        fetch = pltpu.make_async_copy(
            table_hbm.at[pl.ds(start, 2 * block)], table_ref, done.at[count]
        )
        loads = [
            pltpu.make_async_copy(tile_hbm.at[i], tile_ref.at[i], done.at[i]) for i in range(count)
        ]

        lane = pl.multiple_of(me * rows, rows)
        extra = [
            pltpu.make_async_copy(down_hbm.at[:, pl.ds(lane, rows)], down_ref, done.at[count + 1]),
            pltpu.make_async_copy(across_hbm, across_ref, done.at[count + 2]),
        ]

        @pl.when(t == 0)
        def _():
            for copy in extra:
                copy.start()
            fetch.start()
            for load in loads:
                load.start()
            for copy in extra:
                copy.wait()
            fetch.wait()

        for i in range(count):

            @pl.when(t == i)
            def _():
                loads[i].wait()
                work[...] = times_table(table_ref[...], shade(tile_ref[i], down_ref, across_ref))

        for k in range(2):
            place = pl.multiple_of((me % 2 ^ k) * block, block)
            outs[k][0] = work[pl.ds(place, block), :]

    return pl.pallas_call(
        body,
        grid_spec=pltpu.PrefetchScalarGridSpec(
            num_scalar_prefetch=2,
            grid=(count,),
            in_specs=[
                pl.BlockSpec(memory_space=pltpu.HBM),
                pl.BlockSpec(memory_space=pltpu.HBM),
                pl.BlockSpec(memory_space=pltpu.HBM),
                pl.BlockSpec(memory_space=pltpu.HBM),
            ],
            out_specs=[pl.BlockSpec((1, block, rows), lambda t, half, me: (t, 0, 0))] * 2,
            scratch_shapes=[
                pltpu.VMEM((count, rows, width), tiles.dtype),
                pltpu.VMEM((2 * block, width), table.dtype),
                pltpu.VMEM((2 * block, rows), jnp.bfloat16),
                pltpu.VMEM((8, rows), jnp.float32),
                pltpu.VMEM((1, width), jnp.float32),
                pltpu.SemaphoreType.DMA((count + 3,)),
            ],
        ),
        out_shape=[jax.ShapeDtypeStruct((count, block, rows), jnp.bfloat16)] * 2,
        compiler_params=params(FIRST_LIMIT),
        cost_estimate=cost(4 * count * rows * width * block, 4 * tiles.size + 4 * block * width),
        name="near_columns",
    )(scalar(half), scalar(me), tiles, down, across, table)


def rest_columns(tiles, down, across, table, half, me, peers):
    count, rows, width = tiles.shape
    span = table.shape[0] // 2
    block = span // peers

    def body(half_ref, me_ref, tile_ref, down_ref, across_ref, table_ref, *refs):
        out_ref, far, work = refs[0], refs[1:-1], refs[-1]
        half, me = half_ref[0], me_ref[0]
        shaded = shade(tile_ref[pl.program_id(0)], down_ref, across_ref)
        for j in range(1, peers // 2):
            start = pl.multiple_of((1 - half) * span + (me // 2 ^ j) * 2 * block, 2 * block)
            work[...] = times_table(table_ref[pl.ds(start, 2 * block), :], shaded)
            for k in range(2):
                place = pl.multiple_of((me % 2 ^ k) * block, block)
                far[2 * j - 2 + k][0] = work[pl.ds(place, block), :]
        start = pl.multiple_of(half * span, span)
        y = times_table(table_ref[pl.ds(start, span), :], shaded)
        out_ref[:, 0] = y.reshape(peers, block, rows)

    piece = pl.BlockSpec((1, block, rows), lambda t, half, me: (t, 0, 0))
    return pl.pallas_call(
        body,
        grid_spec=pltpu.PrefetchScalarGridSpec(
            num_scalar_prefetch=2,
            grid=(count,),
            in_specs=[
                pl.BlockSpec(memory_space=pltpu.VMEM),
                pl.BlockSpec((8, rows), lambda t, half, me: (0, me[0])),
                pl.BlockSpec((1, width), lambda t, half, me: (0, 0)),
                pl.BlockSpec(memory_space=pltpu.VMEM),
            ],
            out_specs=[
                pl.BlockSpec((peers, 1, block, rows), lambda t, half, me: (0, t, 0, 0)),
                *[piece] * (peers - 2),
            ],
            scratch_shapes=[pltpu.VMEM((2 * block, rows), jnp.bfloat16)],
        ),
        out_shape=[
            jax.ShapeDtypeStruct((peers, count, block, rows), jnp.bfloat16),
            *[jax.ShapeDtypeStruct((count, block, rows), jnp.bfloat16)] * (peers - 2),
        ],
        compiler_params=params(),
        cost_estimate=cost(3 * count * rows * width * span, 4 * tiles.size + 2 * width * width),
        name="rest_columns",
    )(scalar(half), scalar(me), tiles, down, across, table)


def gather_rows(pieces, table_ref, me, first=0, total=None):
    for k, piece in enumerate(pieces, first):
        count, block, rows = piece.shape
        start = pl.multiple_of((me ^ k) * rows, rows)
        term = jnp.dot(
            piece[...].reshape(count * block, rows),
            table_ref[pl.ds(start, rows), :],
            preferred_element_type=jnp.float32,
        )
        total = term if total is None else total + term
    return total


def holds_packed(place):
    half_ref, me_ref = place
    return (half_ref[0] == 0) & (me_ref[0] == 0)


def store_spectra(s_ref, total, spectra, edge, first):
    block = spectra.shape[2]
    height = spectra.shape[3]
    row = lax.broadcasted_iota(jnp.int32, (block, height), 0)
    packed = (row == 0) & holds_packed(s_ref)
    for t in range(total.shape[0] // (2 * block)):
        real = total[2 * t * block : (2 * t + 1) * block]
        imag = total[(2 * t + 1) * block : (2 * t + 2) * block]
        cr, sr = real[:, :height], real[:, height:]
        ci, si = imag[:, :height], imag[:, height:]
        spectra[first + t, 0] = jnp.where(packed, cr, cr + si).astype(jnp.bfloat16)
        spectra[first + t, 1] = jnp.where(packed, -sr, ci - sr).astype(jnp.bfloat16)
        edge[first + t, 0] = ci[:16].astype(jnp.bfloat16)
        edge[first + t, 1] = (-si[:16]).astype(jnp.bfloat16)


def normalised(left_real, left_imag, right_real, right_imag):
    lr = left_real.astype(jnp.float32)
    li = left_imag.astype(jnp.float32)
    rr = right_real.astype(jnp.float32)
    ri = right_imag.astype(jnp.float32)
    cross_real = lr * rr + li * ri
    cross_imag = li * rr - lr * ri
    factor = 1.0 / (jnp.sqrt(cross_real * cross_real + cross_imag * cross_imag) + FLOOR)
    return (
        (cross_real * factor).astype(jnp.bfloat16),
        (cross_imag * factor).astype(jnp.bfloat16),
    )


def correlate(s_ref, picks, spectra, edge, phases):
    slots = len(picks)
    height = spectra.shape[3]
    lead = lax.broadcasted_iota(jnp.int32, (16, height), 0)
    packed = (lead == 0) & holds_packed(s_ref)
    for p in range(slots):
        a, c = picks[p]
        q_real, q_imag = normalised(spectra[a, 0], spectra[a, 1], spectra[c, 0], spectra[c, 1])
        e_real, e_imag = normalised(edge[a, 0], edge[a, 1], edge[c, 0], edge[c, 1])
        phases[2 * p] = q_real
        phases[2 * p + 1] = q_imag
        top_real = q_real[:16].astype(jnp.float32)
        top_imag = q_imag[:16].astype(jnp.float32)
        mixed_real = jnp.where(packed, top_real - e_imag.astype(jnp.float32), top_real)
        mixed_imag = jnp.where(packed, top_imag + e_real.astype(jnp.float32), top_imag)
        phases[2 * p, :16] = mixed_real.astype(jnp.bfloat16)
        phases[2 * p + 1, :16] = mixed_imag.astype(jnp.bfloat16)

def invert_columns(s_ref, me, phases, table_ref, outs):
    _, block, height = phases.shape
    slots = phases.shape[0] // 2
    rows = next(iter(outs.values())).shape[2]
    row = lax.broadcasted_iota(jnp.int32, (block, rows), 0)
    twice = jnp.where((row == 0) & holds_packed(s_ref), 1.0, 2.0)
    flat = phases[...].reshape(2 * slots * block, height)
    for k, out in outs.items():
        start = pl.multiple_of((me ^ k) * rows, rows)
        c_part = jnp.dot(
            flat, table_ref[:, pl.ds(start, rows)], preferred_element_type=jnp.float32
        )
        start = pl.multiple_of(height + (me ^ k) * rows, rows)
        s_part = jnp.dot(
            flat, table_ref[:, pl.ds(start, rows)], preferred_element_type=jnp.float32
        )
        for p in range(slots):
            re = slice(2 * p * block, (2 * p + 1) * block)
            im = slice((2 * p + 1) * block, (2 * p + 2) * block)
            out[p, :block] = ((c_part[re] - s_part[im]) * twice).astype(jnp.bfloat16)
            out[p, block:] = ((s_part[re] + c_part[im]) * twice).astype(jnp.bfloat16)


def own_spectra(place, pieces, near, short):
    peers, count, double, rows = pieces.shape
    height = peers * rows

    def body(half_ref, me_ref, pieces_ref, near_a, near_b, *refs):
        fine_ref, rough_ref, spectra, edge, share, table_ref = refs
        total = None
        for k in range(peers):
            make_table(fine_ref, rough_ref, table_ref, k * rows, rows)
            term = jnp.dot(
                pieces_ref[k].reshape(count * double, rows),
                table_ref[k * rows : (k + 1) * rows],
                preferred_element_type=jnp.float32,
            )
            total = term if total is None else total + term
        store_spectra((half_ref, me_ref), total, spectra, edge, 0)
        share[...] = gather_rows([near_a, near_b], table_ref, me_ref[0])

    return pl.pallas_call(
        body,
        in_specs=[pl.BlockSpec(memory_space=pltpu.SMEM)] * 2
        + [pl.BlockSpec(memory_space=pltpu.VMEM)] * 5,
        out_specs=[pl.BlockSpec(memory_space=pltpu.VMEM)] * 4,
        out_shape=[
            jax.ShapeDtypeStruct((2 * count, 2, double // 2, height), jnp.bfloat16),
            jax.ShapeDtypeStruct((2 * count, 2, 16, height), jnp.bfloat16),
            jax.ShapeDtypeStruct((count * double, 2 * height), jnp.float32),
            jax.ShapeDtypeStruct((height, 2 * height), jnp.bfloat16),
        ],
        compiler_params=params(),
        cost_estimate=cost(6 * count * double * height * height, 8 * height * height),
        name="own_spectra",
    )(*place, pieces, *near, *short)


def partner_slots(place, theirs, pieces, share, table, spectra, edge):
    distant = len(pieces)
    count, double, rows = pieces[0].shape
    height = table.shape[0]
    block = double // 2
    slots = theirs.shape[1]

    def body(half_ref, me_ref, theirs_ref, *refs):
        s_ref = (half_ref, me_ref)
        me = me_ref[0]
        picks = [
            [(theirs_ref[0, p, i] + count) % (2 * count) for i in range(2)] for p in range(slots)
        ]
        inputs = refs[:distant]
        share_ref, table_ref, _, _, near, every, edges, phases = refs[distant:]
        total = gather_rows(inputs, table_ref, me, 2, share_ref[...])
        store_spectra(s_ref, total, every, edges, count)
        correlate(s_ref, picks, every, edges, phases)
        invert_columns(s_ref, me, phases, table_ref, {k: near.at[k] for k in range(2)})

    return pl.pallas_call(
        body,
        in_specs=[pl.BlockSpec(memory_space=pltpu.SMEM)] * 3
        + [pl.BlockSpec(memory_space=pltpu.VMEM)] * (distant + 4),
        out_specs=[pl.BlockSpec(memory_space=pltpu.VMEM)] * 4,
        out_shape=[
            jax.ShapeDtypeStruct((2, slots, double, rows), jnp.bfloat16),
            jax.ShapeDtypeStruct((2 * count, 2, block, height), jnp.bfloat16),
            jax.ShapeDtypeStruct((2 * count, 2, 16, height), jnp.bfloat16),
            jax.ShapeDtypeStruct((2 * slots, block, height), jnp.bfloat16),
        ],
        input_output_aliases={5 + distant: 1, 6 + distant: 2},
        compiler_params=params(),
        cost_estimate=cost(4 * (count + slots) * double * height * height, 8 * height * height),
        name="partner_slots",
    )(*place, theirs, *pieces, share, table, spectra, edge)


def own_slots(place, pairs, table, spectra, edge, phases, peers):
    block, height = spectra.shape[2:]
    rows = height // peers
    slots = pairs.shape[1]

    def body(half_ref, me_ref, pairs_ref, table_ref, every, edges, theirs, out_ref, *refs):
        s_ref = (half_ref, me_ref)
        far, work = refs[:-1], refs[-1]
        picks = [[pairs_ref[0, p, i] for i in range(2)] for p in range(slots)]
        if far:
            outs = {k: far[k - 2] for k in range(2, peers)}
            invert_columns(s_ref, me_ref[0], theirs, table_ref, outs)
        correlate(s_ref, picks, every, edges, work)
        invert_columns(s_ref, 0, work, table_ref, {k: out_ref.at[k] for k in range(peers)})

    return pl.pallas_call(
        body,
        in_specs=[pl.BlockSpec(memory_space=pltpu.SMEM)] * 3
        + [pl.BlockSpec(memory_space=pltpu.VMEM)] * 4,
        out_specs=[pl.BlockSpec(memory_space=pltpu.VMEM)] * (peers - 1),
        out_shape=[
            jax.ShapeDtypeStruct((peers, slots, 2 * block, rows), jnp.bfloat16),
            *[jax.ShapeDtypeStruct((slots, 2 * block, rows), jnp.bfloat16)] * (peers - 2),
        ],
        scratch_shapes=[pltpu.VMEM((2 * slots, block, height), jnp.bfloat16)],
        compiler_params=params(),
        cost_estimate=cost(8 * slots * block * height * height, 8 * height * height),
        name="own_slots",
    )(*place, pairs, table, spectra, edge, phases)


def own_surfaces(half, own, table):
    peers, slots, double, rows = own.shape
    width = table.shape[0]
    span = peers * double

    def body(half_ref, own_ref, table_ref, out_ref):
        out_ref[0] = lax.dot_general(
            own_ref[:, 0].reshape(span, rows),
            table_ref[...],
            (((0,), (0,)), ((), ())),
            preferred_element_type=jnp.float32,
        )

    return pl.pallas_call(
        body,
        grid_spec=pltpu.PrefetchScalarGridSpec(
            num_scalar_prefetch=1,
            grid=(slots,),
            in_specs=[
                pl.BlockSpec((peers, 1, double, rows), lambda p, half: (0, p, 0, 0)),
                pl.BlockSpec((span, width), lambda p, half: (half[0], 0)),
            ],
            out_specs=pl.BlockSpec((1, rows, width), lambda p, half: (p, 0, 0)),
        ),
        out_shape=jax.ShapeDtypeStruct((slots, rows, width), jnp.float32),
        compiler_params=params(),
        cost_estimate=cost(2 * slots * rows * width * span, 4 * slots * rows * width),
        name="own_surfaces",
    )(scalar(half), own, table)


def surfaces_of(half, me, counts, part, near, other, table):
    peers = 1 + len(other)
    slots, double, rows = other[0].shape
    width = table.shape[0]
    span = peers * double

    def body(half_ref, me_ref, counts_ref, part_ref, *refs):
        other_refs = refs[:peers]
        table_ref, out_ref, work = refs[peers:]
        for k in range(peers):
            place = pl.multiple_of((me_ref[0] ^ k) * double, double)
            piece = other_refs[k][0] if k else other_refs[k][0, 0]
            work[pl.ds(place, double), :] = piece
        start = pl.multiple_of((1 - half_ref[0]) * span, span)
        rest = lax.dot_general(
            work[...],
            table_ref[pl.ds(start, span), :],
            (((0,), (0,)), ((), ())),
            preferred_element_type=jnp.float32,
        )
        live = pl.program_id(0) < counts_ref[0]
        out_ref[0] = jnp.where(live, part_ref[pl.program_id(0)] + rest, 0.0)

    pair = pl.BlockSpec((1, 1, double, rows), lambda p, half, me, counts: (0, p, 0, 0))
    piece = pl.BlockSpec((1, double, rows), lambda p, half, me, counts: (p, 0, 0))
    plane = pl.BlockSpec((1, rows, width), lambda p, half, me, counts: (p, 0, 0))
    return pl.pallas_call(
        body,
        grid_spec=pltpu.PrefetchScalarGridSpec(
            num_scalar_prefetch=3,
            grid=(slots,),
            in_specs=[
                pl.BlockSpec(memory_space=pltpu.VMEM),
                pair,
                *[piece] * (peers - 1),
                pl.BlockSpec(memory_space=pltpu.VMEM),
            ],
            out_specs=plane,
            scratch_shapes=[pltpu.VMEM((span, rows), jnp.bfloat16)],
        ),
        out_shape=jax.ShapeDtypeStruct((slots, rows, width), jnp.float32),
        compiler_params=params(),
        cost_estimate=cost(2 * slots * rows * width * span, 8 * slots * rows * width),
        name="surfaces",
    )(scalar(half), scalar(me), counts, part, near, *other, table)


def local(tiles, pairs, counts):
    groups = lax.axis_size("blk")
    peers = lax.axis_size("rows")
    group = lax.axis_index("blk")
    me = lax.axis_index("rows")
    count, rows, width = tiles.shape
    height = rows * peers
    turn = groups // 2
    half = group // turn
    axes = ("blk", "rows")

    def across(value, k):
        moves = [
            (b * peers + r, (b + turn) % groups * peers + (r ^ k))
            for b in range(groups)
            for r in range(peers)
        ]
        return lax.ppermute(value, axes, moves)

    def along(blocks):
        return lax.all_to_all(blocks, "rows", split_axis=0, concat_axis=0)

    def swap(value):
        return lax.ppermute(value, "rows", [(r, r ^ 1) for r in range(peers)])

    table_w = jnp.asarray(width_table(width, 2 * peers))
    down = jnp.asarray(np.tile(hann(height), (8, 1)))
    sideways = jnp.asarray(hann(width)[None, :])

    sent = near_columns(tiles, down, sideways, table_w, half, me, peers)
    arrived = [across(sent[k], k) for k in range(2)]
    *sent, held = lax.optimization_barrier((*sent, half))
    kept, *sent = rest_columns(tiles, down, sideways, table_w, held, me, peers)
    *sent, kept, pairs = lax.optimization_barrier((*sent, kept, pairs))
    arrived += [across(sent[k - 2], k) for k in range(2, peers)]
    mine = along(kept)

    theirs = across(pairs, 0)
    place = (scalar(half), scalar(me))
    spectra, edge, share, table_h = own_spectra(
        place, mine, arrived[:2], scaled_tables(height)
    )
    near, spectra, edge, phases = partner_slots(
        place, theirs, arrived[2:], share, table_h, spectra, edge
    )
    near = across(near, 0)
    own, *far = own_slots(place, pairs, table_h, spectra, edge, phases, peers)
    far = [across(far[k - 2], k) for k in range(2, peers)]
    part = own_surfaces(half, along(own), table_w)
    *far, part = lax.optimization_barrier((*far, part))
    return surfaces_of(half, me, counts, part, near, [swap(near[1]), *far], table_w)


def solution(mesh):
    from jax.sharding import PartitionSpec as P

    return jax.shard_map(
        local,
        mesh=mesh,
        in_specs=(
            P(("parts", "blk"), "rows", None),
            P(("parts", "blk"), None, None),
            P(("parts", "blk")),
        ),
        out_specs=P(("parts", "blk"), "rows", None),
        check_vma=False,
    )
```
